128 devices in a mesh: gx: 2 (over core), gy: 4 (over x), gz: 16 (over z, y).
Axes of the slice: x: 4, y: 4, z: 4, core: 2. Of those that a mesh axis runs over, the one named last changes fastest.
Arguments:
- right_side: float32 [96, 192, 768], P('gx', 'gy', 'gz'), may hold values from -6 to 6
- start_guess: float32 [96, 192, 768], P('gx', 'gy', 'gz'), may hold values from -3 to 3
- reaction: float32 [96, 192, 768], P('gx', 'gy', 'gz'), may hold values from 0.0005 to 0.005
Outputs:
- solution_field: float32 [96, 192, 768], P('gx', 'gy', 'gz')
- residual: float32 [96, 192, 768], P('gx', 'gy', 'gz')
The draws below stay inside these ranges and needn't reach their ends.
All inputs are finite; a program needn't handle non-finite values.
Results may differ from the reference program's by a relative error of at most 0.0003.
Values sent between devices are 32-bit elements.
A program may use at most 128 MiB of HBM per device.

```python
import math
import jax
import jax.numpy as jnp

LEVELS = 5
BOTTOM_ITERS = 6
NX = 96
NY = 192
NZ = 768


def block_scale(rng, shape, cuts, low, largest):
    def one(axis_at, parts):
        heights = jax.random.uniform(jax.random.fold_in(jax.random.fold_in(rng, 6), axis_at), (parts,), jnp.float32, low / len(cuts), largest / len(cuts))
        return jnp.repeat(jnp.exp(heights), shape[axis_at] // parts).reshape((-1,) + (1,) * (len(shape) - axis_at - 1))

    gain = one(*cuts[0])
    for cut in cuts[1:]:
        gain = gain * one(*cut)
    return gain


def scatter_about(own_key, extent, scale, bound, shards=(), dtype=jnp.bfloat16):
    values = jax.random.normal(own_key, extent, jnp.float32) * scale
    if len(shards) > 0:
        values = block_scale(own_key, extent, shards, -0.22, 0.18) * values
    return jnp.clip(values, min=-bound, max=bound).astype(dtype)


def setup_inputs(seed: int = 0) -> dict:
    key_list = jax.random.split(jax.random.key(seed), 4)
    right_side = scatter_about(key_list[0], (NX, NY, NZ), 1.0, 6.0, ((0, 2), (1, 4), (2, 16)), jnp.float32)
    start_guess = scatter_about(key_list[1], (NX, NY, NZ), 0.2, 3.0, ((0, 2), (1, 4), (2, 16)), jnp.float32)
    reaction = jnp.clip(jnp.exp(math.log(0.005) - 2.30258502 * jax.random.uniform(key_list[2], (NX, NY, NZ), jnp.float32) ** block_scale(key_list[2], (NX, NY, NZ), ((0, 2), (1, 4), (2, 16)), -0.2, 0.2)), 0.0005, 0.005)
    return {"right_side": right_side, "start_guess": start_guess, "reaction": reaction}


damping = 6.0 / 7.0


def operate(values, shifted, factor):
    padded = jnp.pad(values, 1)
    beside = padded[2:, 1:-1, 1:-1] + padded[:-2, 1:-1, 1:-1]
    beside = beside + padded[1:-1, 2:, 1:-1] + padded[1:-1, :-2, 1:-1]
    beside = beside + padded[1:-1, 1:-1, 2:] + padded[1:-1, 1:-1, :-2]
    return factor * (6.0 * values - beside) + shifted * values


def coarsen(values):
    size_x, size_y, size_z = values.shape
    blocks = values.reshape(size_x // 2, 2, size_y // 2, 2, size_z // 2, 2)
    return jnp.mean(blocks, axis=(1, 3, 5))


def refine(values):
    size_x, size_y, size_z = values.shape
    spread = jnp.broadcast_to(values[:, None, :, None, :, None], (size_x, 2, size_y, 2, size_z, 2))
    return spread.reshape(2 * size_x, 2 * size_y, 2 * size_z)


def smooth_once(estimate, source, shifted, factor):
    return estimate + damping * (source - operate(estimate, shifted, factor)) / (6.0 * factor + shifted)


def bottom(source, shifted, factor):
    estimate = jnp.zeros_like(source)
    leftover = source
    direction = source
    norm_now = jnp.sum(leftover * leftover)
    for repeat_index in range(BOTTOM_ITERS):
        applied = operate(direction, shifted, factor)
        step_length = norm_now / jnp.sum(direction * applied)
        estimate = estimate + step_length * direction
        leftover = leftover - step_length * applied
        norm_next = jnp.sum(leftover * leftover)
        direction = leftover + (norm_next / norm_now) * direction
        norm_now = norm_next
    return estimate


def vcycle_level(source, shifts, depth_index):
    factor = 0.25 ** depth_index
    shifted = shifts[depth_index]
    if depth_index == LEVELS - 1:
        return bottom(source, shifted, factor)
    estimate = damping * source / (6.0 * factor + shifted)
    estimate = smooth_once(estimate, source, shifted, factor)
    leftover = source - operate(estimate, shifted, factor)
    estimate = estimate + refine(vcycle_level(coarsen(leftover), shifts, depth_index + 1))
    estimate = smooth_once(estimate, source, shifted, factor)
    estimate = smooth_once(estimate, source, shifted, factor)
    return estimate


def reference(right_side, start_guess, reaction):
    shifts = [reaction]
    for depth_index in range(LEVELS - 1):
        shifts.append(coarsen(shifts[-1]))
    start_residual = right_side - operate(start_guess, reaction, 1.0)
    precond = vcycle_level(start_residual, shifts, 0)
    upper = jnp.sum(start_residual * precond)
    applied = operate(precond, reaction, 1.0)
    step_length = upper / jnp.sum(precond * applied)
    solution_field = start_guess + step_length * precond
    residual = start_residual - step_length * applied
    return solution_field, residual
```

```python
import functools

import jax
import jax.numpy as jnp
from jax import lax
from jax.experimental import pallas as pl
from jax.experimental.pallas import tpu as pltpu
from jax.sharding import PartitionSpec as P

MESH = pl.DeviceIdType.MESH
F32 = jnp.float32
BF16 = jnp.bfloat16
DAMP = 6.0 / 7.0
GUARD = 8
BOTTOM_ITERS = 6


class Geo:
    def __init__(self, nx, ny, nz, halo, rows, y0, depth):
        self.nx, self.ny, self.nz, self.halo, self.R, self.y0 = nx, ny, nz, halo, rows, y0
        self.factor = 0.25**depth
        self.total = 2 * GUARD + (nx + 2 * halo) * rows

    def row(self, x, y):
        return GUARD + (self.halo + x) * self.R + self.y0 + y


L0 = Geo(24, 48, 48, 4, 56, 4, 0)
L1 = Geo(12, 24, 24, 6, 40, 8, 1)
L2 = Geo(6, 12, 12, 5, 24, 6, 2)
FACTOR3 = 0.25**3
FACTOR4 = 0.25**4


def lanes(rows):
    return lax.broadcasted_iota(jnp.int32, (rows, 128), 1)


def iota2(shape, dim):
    return lax.broadcasted_iota(jnp.int32, shape, dim)


def roll(v, shift):
    shift = shift % 128
    return v if shift == 0 else pltpu.roll(v, shift, 1)


def split3(a):
    hi = a.astype(BF16)
    rest = a - hi.astype(F32)
    mid = rest.astype(BF16)
    low = (rest - mid.astype(F32)).astype(BF16)
    return hi, mid, low


def mm(a, b):
    parts = split3(a)
    out = [jnp.dot(p, b, preferred_element_type=F32) for p in parts]
    return out[0] + (out[1] + out[2])


def beside_of(ref, r, R):
    c = ref[pl.ds(r, R), :]
    b = ref[pl.ds(r + R, R), :] + ref[pl.ds(r - R, R), :]
    b = b + (ref[pl.ds(r + 1, R), :] + ref[pl.ds(r - 1, R), :])
    b = b + (roll(c, 1) + roll(c, -1))
    return c, b


def image_of(ref, s_ref, g, r):
    c, b = beside_of(ref, r, g.R)
    return c, g.factor * (6.0 * c - b) + s_ref[pl.ds(r, g.R), :] * c


def planes(g, a, b, body):
    def step(i, carry):
        body(pl.multiple_of(GUARD + i * g.R, 8), i)
        return carry

    lax.fori_loop(g.halo + a, g.halo + b, step, 0)


def inverse(s, factor):
    return jnp.where(s > 0.0, DAMP / (6.0 * factor + s), 0.0)


def relax(g, src, dst, f, s, inv, a, b):
    def body(r, i):
        c, image = image_of(src, s, g, r)
        at = pl.ds(r, g.R)
        dst[at, :] = c + inv[at, :] * (f[at, :] - image)

    planes(g, a, b, body)


def first(g, dst, f, inv, a, b):
    def body(r, i):
        at = pl.ds(r, g.R)
        dst[at, :] = inv[at, :] * f[at, :]

    planes(g, a, b, body)


def leftover(g, src, dst, f, s, a, b):
    def body(r, i):
        c, image = image_of(src, s, g, r)
        at = pl.ds(r, g.R)
        dst[at, :] = f[at, :] - image

    planes(g, a, b, body)


def restrict(src, gs, dst, gd, x0, x1, y0, count, matrix, tmp):
    step = -(-count // 8) * 8
    for x in range(x0, x1):
        r = gs.row(2 * x, 2 * y0)
        t = src[pl.ds(r, count, stride=2), :] + src[pl.ds(r + 1, count, stride=2), :]
        r = r + gs.R
        t = t + (src[pl.ds(r, count, stride=2), :] + src[pl.ds(r + 1, count, stride=2), :])
        tmp[pl.ds((x - x0) * step, count), :] = t
    for x in range(x0, x1):
        out = mm(tmp[pl.ds((x - x0) * step, step), :], matrix[...])
        dst[pl.ds(gd.row(x, y0), count), :] = out[0:count]


def prolong(src, gc, dst, gf, x0, x1, y0, count, matrix, tmp):
    for x in range(x0, x1):
        o = (x - x0) * 56
        u = mm(src[pl.ds(gc.row(x, y0), count), :], matrix[...])
        tmp[pl.ds(o, count, stride=2), :] = u
        tmp[pl.ds(o + 1, count, stride=2), :] = u
    for x in range(x0, x1):
        o = (x - x0) * 56
        v = tmp[pl.ds(o, 2 * count), :]
        for k in range(2):
            at = pl.ds(gf.row(2 * x + k, 2 * y0), 2 * count)
            dst[at, :] = dst[at, :] + v


class Item:
    def __init__(self, geo, w, diamond):
        self.g, self.w, self.diamond = geo, w, diamond
        self.slots = 64 // w
        self.wz = w - 1 if diamond else w
        self.wd = w - 2 if diamond else w
        self.ztiles = -(-(geo.nx + 2 * self.wz) // self.slots)

    def wy(self, d):
        return self.w - d if self.diamond else self.w


class Plan:
    def __init__(self, items):
        self.items = items
        self.yrows = sum(it.g.nx + 2 * it.wy(d) for it in items for d in range(1, it.w + 1))
        self.yrows = -(-self.yrows // 8) * 8
        self.zrows = sum(it.ztiles * it.g.ny for it in items)
        self.zrows = -(-self.zrows // 8) * 8
        self.drows = max(it.g.nx + 2 * it.wd for it in items)
        self.drows = -(-self.drows // 8) * 8
        assert sum(it.w * it.w for it in items) <= 64

    def scratch(self):
        x = [pltpu.VMEM((it.w * it.g.R, 128), F32) for it in self.items]
        return x + [
            pltpu.VMEM((2, self.yrows, 128), F32),
            pltpu.VMEM((2, self.yrows, 128), F32),
            pltpu.VMEM((2, self.zrows, 128), F32),
            pltpu.VMEM((2, self.zrows, 128), F32),
            pltpu.VMEM((4, self.drows, 128), F32),
            pltpu.VMEM((4, self.drows, 128), F32),
            pltpu.SemaphoreType.DMA((11,)),
            pltpu.SemaphoreType.DMA((11,)),
        ]


class Exchange:
    def __init__(self, plan, refs, scratch, place):
        n = len(plan.items)
        self.plan, self.refs, self.place = plan, refs, place
        self.xr = scratch[:n]
        self.ys, self.yr, self.zs, self.zr, self.ds, self.dr, self.ss, self.rs = scratch[n:]
        gx, gy, gz = place.me
        self.x_copies = []
        for k, it in enumerate(plan.items):
            g = it.g
            start = jnp.where(gx == 0, g.nx - it.w, 0)
            r = pl.multiple_of(GUARD + (g.halo + start) * g.R, 8)
            self.x_copies.append(
                self.copy(refs[k].at[pl.ds(r, it.w * g.R), :], self.xr[k], k, (1 - gx, gy, gz))
            )
        self.copies = []
        for d in range(2):
            self.copies.append(self.copy(self.ys.at[d], self.yr.at[d], 3 + d, place.beside(0, 1 - 2 * d, 0)))
            self.copies.append(self.copy(self.zs.at[d], self.zr.at[d], 5 + d, place.beside(0, 0, 1 - 2 * d)))
            for e in range(2):
                self.copies.append(
                    self.copy(
                        self.ds.at[2 * d + e], self.dr.at[2 * d + e], 7 + 2 * d + e,
                        place.beside(0, 1 - 2 * d, 1 - 2 * e),
                    )
                )

    def copy(self, src, dst, k, peer):
        return pltpu.make_async_remote_copy(
            src_ref=src, dst_ref=dst, send_sem=self.ss.at[k], recv_sem=self.rs.at[k],
            device_id=peer, device_id_type=MESH,
        )

    def x_send(self):
        for c in self.x_copies:
            c.start()

    def x_fill(self):
        for c in self.x_copies:
            c.wait()
        m0, m1 = self.place.x_masks
        for k, it in enumerate(self.plan.items):
            g, w, ref = it.g, it.w, self.refs[k]
            upper = lanes(g.R) >= 64
            for j in range(w):
                got = self.xr[k][pl.ds(j * g.R, g.R), :]
                top = ref[pl.ds(GUARD + (g.halo + g.nx - w + j) * g.R, g.R), :]
                low = ref[pl.ds(GUARD + (g.halo + j) * g.R, g.R), :]
                ref[pl.ds(GUARD + (g.halo - w + j) * g.R, g.R), :] = roll(jnp.where(upper, got * m1, top), 64)
                ref[pl.ds(GUARD + (g.halo + g.nx + j) * g.R, g.R), :] = roll(jnp.where(upper, low, got * m0), 64)

    def pack_send(self):
        yo, zo, co = 0, 0, 0
        corner = [None] * 4
        for k, it in enumerate(self.plan.items):
            g, w, ref = it.g, it.w, self.refs[k]
            for d in range(1, w + 1):
                n = g.nx + 2 * it.wy(d)
                for e, y in enumerate((g.ny - d, d - 1)):
                    self.ys[e, pl.ds(yo, n), :] = ref[pl.ds(g.row(-it.wy(d), y), n, stride=g.R), :]
                yo += n
            lane = lanes(self.plan.drows) & 63
            for d in range(1, w + 1):
                at = co + (d - 1) * w
                pick = (lane >= at) & (lane < at + w)
                for e, y in enumerate((g.ny - d, d - 1)):
                    n = g.nx + 2 * it.wd
                    v = ref[pl.ds(g.row(-it.wd, y), n, stride=g.R), :]
                    if n < self.plan.drows:
                        v = jnp.concatenate([v, jnp.zeros((self.plan.drows - n, 128), F32)], axis=0)
                    for q, z in enumerate((g.nz - w, 0)):
                        moved = roll(v, at - z)
                        old = corner[2 * e + q]
                        corner[2 * e + q] = moved if old is None else jnp.where(pick, moved, old)
            co += w * w
            lane = lanes(g.ny) & 63
            count = g.nx + 2 * it.wz
            for t in range(it.ztiles):
                acc = [None, None]
                for j in range(min(it.slots, count - t * it.slots)):
                    x = t * it.slots + j - it.wz
                    v = ref[pl.ds(g.row(x, 0), g.ny), :]
                    pick = (lane >= j * w) & (lane < j * w + w)
                    for q, z in enumerate((g.nz - w, 0)):
                        moved = roll(v, j * w - z)
                        acc[q] = moved if j == 0 else jnp.where(pick, moved, acc[q])
                for q in range(2):
                    self.zs[q, pl.ds(zo, g.ny), :] = acc[q]
                zo += g.ny
        for q in range(4):
            self.ds[q] = corner[q]
        for c in self.copies:
            c.start()

    def unpack(self):
        for c in self.copies:
            c.wait()
        my, mz = self.place.y_masks, self.place.z_masks
        yo, zo, co = 0, 0, 0
        for k, it in enumerate(self.plan.items):
            g, w, ref = it.g, it.w, self.refs[k]
            for d in range(1, w + 1):
                n = g.nx + 2 * it.wy(d)
                for e, y in enumerate((-d, g.ny + d - 1)):
                    ref[pl.ds(g.row(-it.wy(d), y), n, stride=g.R), :] = self.yr[e, pl.ds(yo, n), :] * my[e]
                yo += n
            n = g.nx + 2 * it.wd
            lane = lanes(n) & 63
            into = (lane >= 64 - w, (lane >= g.nz) & (lane < g.nz + w))
            for d in range(1, w + 1):
                at = co + (d - 1) * w
                for e, y in enumerate((-d, g.ny + d - 1)):
                    rows = pl.ds(g.row(-it.wd, y), n, stride=g.R)
                    v = ref[rows, :]
                    for q, z in enumerate((-w, g.nz)):
                        got = self.dr[2 * e + q, pl.ds(0, n), :] * (my[e] * mz[q])
                        v = jnp.where(into[q], roll(got, z - at), v)
                    ref[rows, :] = v
            co += w * w
            lane = lanes(g.ny) & 63
            into = (lane >= 64 - w, (lane >= g.nz) & (lane < g.nz + w))
            count = g.nx + 2 * it.wz
            for t in range(it.ztiles):
                got = [self.zr[q, pl.ds(zo, g.ny), :] * mz[q] for q in range(2)]
                for j in range(min(it.slots, count - t * it.slots)):
                    x = t * it.slots + j - it.wz
                    rows = pl.ds(g.row(x, 0), g.ny)
                    v = ref[rows, :]
                    for q, z in enumerate((-w, g.nz)):
                        v = jnp.where(into[q], roll(got[q], z - j * w), v)
                    ref[rows, :] = v
                zo += g.ny


class Place:
    def __init__(self, sizes):
        self.sizes = sizes
        self.me = tuple(lax.axis_index(a) for a in ("gx", "gy", "gz"))
        gx, gy, gz = self.me
        one = lambda c: jnp.where(c, 1.0, 0.0).astype(F32)
        self.x_masks = (one(gx == 0), one(gx == 1))
        self.y_masks = (one(gy > 0), one(gy < sizes[1] - 1))
        self.z_masks = (one(gz > 0), one(gz < sizes[2] - 1))

    def beside(self, dx, dy, dz):
        return tuple(
            lax.rem(m + d % n, n) if d % n else m for m, d, n in zip(self.me, (dx, dy, dz), self.sizes)
        )


class Gather:
    def __init__(self, place, scratch):
        self.place = place
        self.mine, self.got, self.sum, self.s1, self.r1, self.s2, self.r2 = scratch
        n = place.sizes
        self.near = [(a, b) for a in range(n[0]) for b in range(n[1])][1:]

    def first_copies(self):
        n = self.place.sizes
        out = []
        for a, b in self.near:
            k = a * n[1] + b
            out.append(
                pltpu.make_async_remote_copy(
                    src_ref=self.mine, dst_ref=self.got.at[k], send_sem=self.s1.at[k], recv_sem=self.r1.at[k],
                    device_id=self.place.beside(a, b, 0), device_id_type=MESH,
                )
            )
        return out

    def second_copies(self, target):
        out = []
        for c in range(1, self.place.sizes[2]):
            out.append(
                pltpu.make_async_remote_copy(
                    src_ref=self.sum, dst_ref=target(c), send_sem=self.s2.at[c], recv_sem=self.r2.at[c],
                    device_id=self.place.beside(0, 0, c), device_id_type=MESH,
                )
            )
        return out

    def send(self):
        for c in self.first_copies():
            c.start()

    def relay(self, target):
        for c in self.first_copies():
            c.wait()
        total = self.mine[...]
        n = self.place.sizes
        for a, b in self.near:
            total = total + self.got[a * n[1] + b]
        self.sum[...] = total
        for c in self.second_copies(target):
            c.start()
        return total

    def finish(self, target):
        for c in self.second_copies(target):
            c.wait()


def gather_scratch(sizes, rows):
    near = sizes[0] * sizes[1]
    return [
        pltpu.VMEM((rows, 128), F32),
        pltpu.VMEM((near, rows, 128), F32),
        pltpu.VMEM((rows, 128), F32),
        pltpu.SemaphoreType.DMA((near,)),
        pltpu.SemaphoreType.DMA((near,)),
        pltpu.SemaphoreType.DMA((sizes[2],)),
        pltpu.SemaphoreType.DMA((sizes[2],)),
    ]


def to_level3(src, mine, square, turned, place):
    g = L2
    gx, gy, gz = place.me
    for i in range(3):
        r = g.row(2 * i, 0)
        t = src[pl.ds(r, 6, stride=2), :] + src[pl.ds(r + 1, 6, stride=2), :]
        r = r + g.R
        t = t + (src[pl.ds(r, 6, stride=2), :] + src[pl.ds(r + 1, 6, stride=2), :])
        square[pl.ds(8 * i, 6), :] = t
    turned[...] = jnp.transpose(square[...])
    a = turned[pl.ds(0, 8, stride=2), :] + turned[pl.ds(1, 8, stride=2), :]
    b = turned[pl.ds(64, 8, stride=2), :] + turned[pl.ds(65, 8, stride=2), :]
    a = (a + roll(b, 64)) * 0.125
    r = iota2((128, 384), 0)
    l = iota2((128, 384), 1)
    x = 6 * gx + 3 * (r >> 6) + ((r & 63) >> 3)
    y = 6 * gy + (r & 7)
    hit = (x == (l >> 5)) & (y == (l & 31)) & ((r & 7) < 6) & ((r & 63) < 24)
    out = mm(a, jnp.where(hit, 1.0, 0.0).astype(BF16))
    for k in range(3):
        mine[pl.ds(k, 6, stride=4), :] = out[0:6, 128 * k : 128 * k + 128]


def image3(ref, s_ref, r, n):
    lane = lanes(n)
    c = ref[pl.ds(r, n), :]
    b = ref[pl.ds(r + 4, n), :] + ref[pl.ds(r - 4, n), :]
    b = b + (roll(c, 1) + roll(c, -1))
    b = b + roll(jnp.where(lane < 32, ref[pl.ds(r + 1, n), :], c), -32)
    b = b + roll(jnp.where(lane >= 96, ref[pl.ds(r - 1, n), :], c), 32)
    return c, FACTOR3 * (6.0 * c - b) + s_ref[pl.ds(r, n), :] * c


def chunks3(rows, body):
    n = 48

    def step(i, carry):
        body(pl.multiple_of(GUARD + i * n, 8), n)
        return carry

    lax.fori_loop(0, rows // n, step, 0)


def match4(k, shape, coarse_dim, ny):
    c = iota2(shape, coarse_dim)
    l = iota2(shape, 1 - coarse_dim)
    return ((c >> 4) == 2 * k + (l >> 6)) & ((c & 15) == ((l & 31) >> 1)) & ((l & 31) < ny)


def restrict4(src, n, ny):
    total = None
    for k in range(3):
        t = src[pl.ds(GUARD + k, n, stride=8), :] + src[pl.ds(GUARD + k + 4, n, stride=8), :]
        part = mm(t, jnp.where(match4(k, (128, 128), 1, ny), 0.125, 0.0).astype(BF16))
        total = part if total is None else total + part
    return total


def dot_all(a, b):
    return jnp.sum(jnp.sum(a * b, axis=0, keepdims=True), axis=1, keepdims=True)


def bottom(source, s4, p4, n, ny):
    estimate = jnp.zeros_like(source)
    left = source
    direction = source
    now = dot_all(left, left)
    shifted = s4[...]
    for it in range(BOTTOM_ITERS):
        p4[pl.ds(GUARD, n), :] = direction
        b = p4[pl.ds(GUARD + 1, n), :] + p4[pl.ds(GUARD - 1, n), :]
        b = b + (roll(direction, 1) + roll(direction, -1))
        b = b + (roll(direction, 16) + roll(direction, -16))
        inside = (lanes(n) < 96) & ((lanes(n) & 15) < ny)
        image = FACTOR4 * (6.0 * direction - jnp.where(inside, b, 0.0)) + shifted * direction
        step = now / dot_all(direction, image)
        estimate = estimate + step * direction
        if it < BOTTOM_ITERS - 1:
            left = left - step * image
            after = dot_all(left, left)
            direction = left + (after / now) * direction
            now = after
    return estimate


PLAN_A = Plan([Item(L0, 3, True), Item(L0, 2, True), Item(L0, 2, True)])
PLAN_S = Plan([Item(L1, 6, False), Item(L2, 5, False)])
PLAN_B = Plan([Item(L1, 6, False)])
PLAN_C = Plan([Item(L0, 3, True)])
PLAN_D = Plan([Item(L2, 5, False)])
PLANS = (PLAN_A, PLAN_S, PLAN_B, PLAN_C, PLAN_D)


def kernel(sizes, counts, right_ref, guess_ref, react_ref, field_ref, resid_ref, *scratch):
    scratch = list(scratch)

    def take(n):
        out = scratch[:n]
        del scratch[:n]
        return out

    guess, right, react, r0, inv0, ea0, eb0, left0 = take(8)
    f1, s1, inv1, ea1, eb1, left1 = take(6)
    f2, s2, inv2, ea2, eb2, left2 = take(6)
    f3, s3, inv3, ea3, eb3, left3 = take(6)
    s4, p4, down_m, up_m, tmp, square, turned, spread, slab = take(9)
    scr = [take(n) for n in counts]
    place = Place(sizes)
    gx, gy, gz = place.me
    n3, n4, ny3 = 24 * sizes[2], 3 * sizes[2], 6 * sizes[1]

    peers = {(a, b, 0) for a in range(sizes[0]) for b in range(sizes[1])}
    peers |= {(0, 0, c) for c in range(sizes[2])}
    peers |= {(0, b % sizes[1], c % sizes[2]) for b in (1, -1) for c in (1, -1)}
    peers = sorted(peers - {(0, 0, 0)})
    barrier = pltpu.get_barrier_semaphore()

    def clear(ref):
        n = ref.shape[0]

        def step(i, carry):
            ref[pl.ds(pl.multiple_of(i * 8, 8), 8), :] = jnp.zeros((8, 128), F32)
            return carry

        lax.fori_loop(0, n // 8, step, 0)

    clear(f3)
    clear(s3)
    for p in peers:
        pl.semaphore_signal(barrier, inc=1, device_id=place.beside(*p), device_id_type=MESH)
    for ref in (guess, right, react, r0, inv0, ea0, eb0, left0, f1, s1, inv1, ea1, eb1, left1):
        clear(ref)
    for ref in (f2, s2, inv2, ea2, eb2, left2, inv3, ea3, eb3, left3, p4, square, tmp):
        clear(ref)
    spread[...] = jnp.zeros_like(spread)

    def load(i, carry):
        r = L0.row(i, 0)
        for src, dst in ((guess_ref, guess), (right_ref, right), (react_ref, react)):
            dst[pl.ds(r, 48), 0:48] = src[i]
            dst[pl.ds(r, 48), 64:112] = src[i + 24]
        return carry

    lax.fori_loop(0, 24, load, 0)

    a = iota2((128, 128), 0)
    b = iota2((128, 128), 1)
    signed = lambda v: ((v + 8) & 63) - 8
    base = lambda v: ((v + 8) & 127) & 64
    zb = signed(b)
    hit = ((a == ((base(b) + 2 * zb) & 127)) | (a == ((base(b) + 2 * zb + 1) & 127))) & (zb >= -8) & (zb < 24)
    down_m[...] = jnp.where(hit, 0.125, 0.0).astype(BF16)
    hit = a == ((base(b) + (zb >> 1)) & 127)
    up_m[...] = jnp.where(hit, 1.0, 0.0).astype(BF16)

    ex_a = Exchange(PLAN_A, (guess, right, react), scr[0], place)
    ex_s = Exchange(PLAN_S, (s1, s2), scr[1], place)
    ex_b = Exchange(PLAN_B, (f1,), scr[2], place)
    ex_c = Exchange(PLAN_C, (eb0,), scr[3], place)
    ex_d = Exchange(PLAN_D, (f2,), scr[4], place)
    ga_s = Gather(place, scr[5])
    ga_f = Gather(place, scr[6])
    ga_r = Gather(place, scr[7])
    reduced = scr[8][0]

    def slot(ref):
        return lambda c: ref.at[pl.ds(pl.multiple_of(GUARD + 24 * gz, 8), 24), :]

    pl.semaphore_wait(barrier, len(peers))
    ex_a.x_send()

    restrict(react, L0, s1, L1, 0, 12, 0, 24, down_m, tmp)
    restrict(s1, L1, s2, L2, 0, 6, 0, 12, down_m, tmp)
    ex_s.x_send()
    ga_s.mine[...] = jnp.zeros((24, 128), F32)
    ga_f.mine[...] = jnp.zeros((24, 128), F32)
    to_level3(s2, ga_s.mine, square, turned, place)

    ex_a.x_fill()
    ex_a.pack_send()
    ga_s.send()
    ex_s.x_fill()
    ex_s.pack_send()
    s3[pl.ds(pl.multiple_of(GUARD + 24 * gz, 8), 24), :] = ga_s.relay(slot(s3))
    ex_a.unpack()

    def start(r, i):
        at = pl.ds(r, L0.R)
        c, image = image_of(guess, react, L0, r)
        res = right[at, :] - image
        inv = inverse(react[at, :], 1.0)
        r0[at, :] = res
        inv0[at, :] = inv
        ea0[at, :] = inv * res

    planes(L0, -2, 26, start)
    relax(L0, ea0, eb0, r0, react, inv0, -1, 25)
    leftover(L0, eb0, left0, r0, react, 0, 24)
    restrict(left0, L0, f1, L1, 0, 12, 0, 24, down_m, tmp)
    ex_b.x_send()
    ex_c.x_send()
    ex_b.x_fill()
    ex_b.pack_send()

    ex_s.unpack()

    def inverse_of(g, s, inv):
        def body(r, i):
            at = pl.ds(r, g.R)
            inv[at, :] = inverse(s[at, :], g.factor)

        planes(g, -g.halo, g.nx + g.halo, body)

    inverse_of(L1, s1, inv1)
    inverse_of(L2, s2, inv2)
    ex_c.x_fill()
    ex_c.pack_send()

    ex_b.unpack()
    first(L1, ea1, f1, inv1, -6, 18)
    relax(L1, ea1, eb1, f1, s1, inv1, -5, 17)
    leftover(L1, eb1, left1, f1, s1, -4, 16)
    restrict(left1, L1, f2, L2, -2, 8, -2, 16, down_m, tmp)
    first(L2, ea2, f2, inv2, -2, 8)
    relax(L2, ea2, eb2, f2, s2, inv2, -1, 7)
    leftover(L2, eb2, left2, f2, s2, 0, 6)
    to_level3(left2, ga_f.mine, square, turned, place)
    ga_f.send()
    ex_d.x_send()

    ga_s.finish(slot(s3))

    def inverse3(r, n):
        inv3[pl.ds(r, n), :] = inverse(s3[pl.ds(r, n), :], FACTOR3)

    chunks3(n3, inverse3)
    s4[...] = restrict4(s3, n4, ny3)
    ex_d.x_fill()
    ex_d.pack_send()

    f3[pl.ds(pl.multiple_of(GUARD + 24 * gz, 8), 24), :] = ga_f.relay(slot(f3))
    ex_d.unpack()
    first(L2, ea2, f2, inv2, -5, 11)
    relax(L2, ea2, eb2, f2, s2, inv2, -4, 10)
    ex_c.unpack()
    ga_f.finish(slot(f3))

    def relax3(src, dst):
        def body(r, n):
            c, image = image3(src, s3, r, n)
            at = pl.ds(r, n)
            dst[at, :] = c + inv3[at, :] * (f3[at, :] - image)

        chunks3(n3, body)

    def first3(r, n):
        ea3[pl.ds(r, n), :] = inv3[pl.ds(r, n), :] * f3[pl.ds(r, n), :]

    def left_3(r, n):
        c, image = image3(eb3, s3, r, n)
        left3[pl.ds(r, n), :] = f3[pl.ds(r, n), :] - image

    chunks3(n3, first3)
    relax3(ea3, eb3)
    chunks3(n3, left_3)
    e4 = bottom(restrict4(left3, n4, ny3), s4, p4, n4, ny3 // 2)
    for k in range(3):
        u = mm(e4, jnp.where(match4(k, (128, 128), 0, ny3), 1.0, 0.0).astype(BF16))
        for q in (k, k + 4):
            at = pl.ds(GUARD + q, n4, stride=8)
            eb3[at, :] = eb3[at, :] + u
    relax3(eb3, ea3)
    relax3(ea3, eb3)

    slab[...] = eb3[pl.ds(pl.multiple_of(24 * gz, 8), 40), :]
    for k in range(3):
        v = slab[pl.ds(k, 10, stride=4), :]
        for h in range(2):
            for q in range(2):
                spread[k, pl.ds(64 * h + q, 10, stride=2), :] = v
    wide = [jnp.concatenate(p, axis=1) for p in zip(*[split3(spread[k]) for k in range(3)])]
    coarse = []
    for h in range(2):
        r = iota2((112, 384), 0)
        l = iota2((112, 384), 1)
        hit = (6 * gx + 3 * h + (r >> 4) - 2 == (l >> 5)) & (6 * gy + (r & 15) - 2 == (l & 31)) & ((r & 15) < 10)
        pick = jnp.where(hit, 1.0, 0.0).astype(BF16)
        parts = [
            lax.dot_general(pick, p, (((1,), (1,)), ((), ())), preferred_element_type=F32) for p in wide
        ]
        coarse.append(parts[0] + (parts[1] + parts[2]))
    fine = roll(jnp.where(lanes(112) < 64, coarse[0], coarse[1]), -4)
    for i in range(7):
        u = fine[16 * i : 16 * i + 10]
        tmp[pl.ds(24 * i, 10, stride=2), :] = u
        tmp[pl.ds(24 * i + 1, 10, stride=2), :] = u
    for i in range(7):
        v = tmp[pl.ds(24 * i, 20), :]
        for q in range(2):
            at = pl.ds(L2.row(2 * (i - 2) + q, -4), 20)
            eb2[at, :] = eb2[at, :] + v
    relax(L2, eb2, ea2, f2, s2, inv2, -3, 9)
    relax(L2, ea2, eb2, f2, s2, inv2, -2, 8)
    prolong(eb2, L2, eb1, L1, -2, 8, -2, 16, up_m, tmp)
    relax(L1, eb1, ea1, f1, s1, inv1, -3, 15)
    relax(L1, ea1, eb1, f1, s1, inv1, -2, 14)
    prolong(eb1, L1, eb0, L0, -2, 14, -2, 28, up_m, tmp)
    relax(L0, eb0, ea0, r0, react, inv0, -2, 26)
    relax(L0, ea0, eb0, r0, react, inv0, -1, 25)

    row = iota2((L0.R, 128), 0)
    inside = ((lanes(L0.R) & 63) < 48) & (row >= L0.y0) & (row < L0.y0 + 48)

    def last(i, sums):
        r = pl.multiple_of(GUARD + (L0.halo + i) * L0.R, 8)
        at = pl.ds(r, L0.R)
        c, image = image_of(eb0, react, L0, r)
        left0[at, :] = image
        upper = jnp.where(inside, c * r0[at, :], 0.0)
        lower = jnp.where(inside, c * image, 0.0)
        return sums[0] + upper, sums[1] + lower

    zero = jnp.zeros((L0.R, 128), F32)
    upper, lower = lax.fori_loop(0, 24, last, (zero, zero))
    upper = jnp.sum(upper, axis=0, keepdims=True)
    lower = jnp.sum(lower, axis=0, keepdims=True)
    half = lanes(1) < 64
    ga_r.mine[...] = jnp.where(half, upper + roll(upper, 64), lower + roll(lower, 64))
    ga_r.send()
    own = ga_r.relay(lambda c: reduced.at[c])
    ga_r.finish(lambda c: reduced.at[c])
    total = own
    for c in range(1, sizes[2]):
        total = total + reduced[c]
    upper = jnp.sum(jnp.where(half, total, 0.0), axis=1, keepdims=True)
    lower = jnp.sum(jnp.where(half, 0.0, total), axis=1, keepdims=True)
    step = upper / lower

    def store(i, carry):
        at = pl.ds(L0.row(i, 0), 48)
        e = eb0[at, :]
        v = guess[at, :] + step * e
        field_ref[i] = v[:, 0:48]
        field_ref[i + 24] = roll(v, 64)[:, 0:48]
        v = r0[at, :] - step * left0[at, :]
        resid_ref[i] = v[:, 0:48]
        resid_ref[i + 24] = roll(v, 64)[:, 0:48]
        return carry

    lax.fori_loop(0, 24, store, 0)


def solution(mesh):
    sizes = tuple(mesh.shape[a] for a in ("gx", "gy", "gz"))
    n3, n4 = 24 * sizes[2] + 2 * GUARD, 3 * sizes[2]
    scratch = [pltpu.VMEM((L0.total, 128), F32)] * 8
    scratch += [pltpu.VMEM((L1.total, 128), F32)] * 6
    scratch += [pltpu.VMEM((L2.total, 128), F32)] * 6
    scratch += [pltpu.VMEM((n3, 128), F32)] * 6
    scratch += [pltpu.VMEM((n4, 128), F32), pltpu.VMEM((n4 + 2 * GUARD, 128), F32)]
    scratch += [pltpu.VMEM((128, 128), BF16)] * 2 + [pltpu.VMEM((16 * 56, 128), F32)]
    scratch += [pltpu.VMEM((128, 128), F32)] * 2
    scratch += [pltpu.VMEM((3, 128, 128), F32), pltpu.VMEM((40, 128), F32)]
    groups = [p.scratch() for p in PLANS] + [gather_scratch(sizes, 24)] * 2 + [gather_scratch(sizes, 1)]
    groups += [[pltpu.VMEM((sizes[2], 1, 128), F32)]]
    for g in groups:
        scratch += g
    counts = tuple(len(g) for g in groups)
    vmem = pl.BlockSpec(memory_space=pltpu.VMEM)

    def body(right_side, start_guess, reaction):
        shape = jax.ShapeDtypeStruct(right_side.shape, F32)
        return tuple(
            pl.pallas_call(
                functools.partial(kernel, sizes, counts),
                out_shape=[shape, shape],
                in_specs=[vmem] * 3,
                out_specs=[vmem] * 2,
                scratch_shapes=scratch,
                compiler_params=pltpu.CompilerParams(collective_id=0, has_side_effects=True),
            )(right_side, start_guess, reaction)
        )

    placed = P("gx", "gy", "gz")
    return jax.shard_map(
        body, mesh=mesh, in_specs=(placed,) * 3, out_specs=(placed,) * 2, check_vma=False
    )
```

```python
import functools

import jax
import jax.numpy as jnp
from jax import lax
from jax.experimental import pallas as pl
from jax.experimental.pallas import tpu as pltpu
from jax.sharding import PartitionSpec as P

MESH = pl.DeviceIdType.MESH
F32 = jnp.float32
BF16 = jnp.bfloat16
DAMP = 6.0 / 7.0
GUARD = 8
BOTTOM_ITERS = 6


class Geo:
    def __init__(self, nx, ny, nz, halo, rows, y0, depth, unroll):
        self.nx, self.ny, self.nz, self.halo, self.R, self.y0 = nx, ny, nz, halo, rows, y0
        self.factor = 0.25**depth
        self.unroll = unroll
        self.total = 2 * GUARD + (nx + 2 * halo) * rows

    def row(self, x, y):
        return GUARD + (self.halo + x) * self.R + self.y0 + y


L0 = Geo(24, 48, 48, 4, 56, 4, 0, 4)
L1 = Geo(12, 24, 24, 6, 40, 8, 1, 6)
L2 = Geo(6, 12, 12, 5, 24, 6, 2, 8)
FACTOR3 = 0.25**3
FACTOR4 = 0.25**4


def lanes(rows):
    return lax.broadcasted_iota(jnp.int32, (rows, 128), 1)


def iota2(shape, dim):
    return lax.broadcasted_iota(jnp.int32, shape, dim)


def roll(v, shift):
    shift = shift % 128
    return v if shift == 0 else pltpu.roll(v, shift, 1)


def split3(a):
    hi = a.astype(BF16)
    rest = a - hi.astype(F32)
    mid = rest.astype(BF16)
    low = (rest - mid.astype(F32)).astype(BF16)
    return hi, mid, low


def mm(a, b):
    parts = split3(a)
    out = [jnp.dot(p, b, preferred_element_type=F32) for p in parts]
    return out[0] + (out[1] + out[2])


def beside_of(ref, r, R):
    c = ref[pl.ds(r, R), :]
    b = ref[pl.ds(r + R, R), :] + ref[pl.ds(r - R, R), :]
    b = b + (ref[pl.ds(r + 1, R), :] + ref[pl.ds(r - 1, R), :])
    b = b + (roll(c, 1) + roll(c, -1))
    return c, b


def image_of(ref, s_ref, g, r):
    c, b = beside_of(ref, r, g.R)
    return c, g.factor * (6.0 * c - b) + s_ref[pl.ds(r, g.R), :] * c


def planes(g, a, b, body):
    unroll = g.unroll

    def group(start, count):
        todo = []
        for k in range(count):
            r = start + k * g.R
            r = r if isinstance(r, int) else pl.multiple_of(r, 8)
            todo.append((r, body(r)))
        for r, pairs in todo:
            for ref, value in pairs:
                ref[pl.ds(r, g.R), :] = value

    trips = (b - a) // unroll
    origin = GUARD + (g.halo + a) * g.R
    if trips == 1:
        group(origin, unroll)
    elif trips:

        def step(i, carry):
            group(pl.multiple_of(origin + i * (unroll * g.R), 8), unroll)
            return carry

        lax.fori_loop(0, trips, step, 0)
    if (b - a) % unroll:
        group(origin + trips * unroll * g.R, (b - a) % unroll)


def inverse(s, factor):
    return jnp.where(s > 0.0, DAMP / (6.0 * factor + s), 0.0)


def relax(g, src, dst, f, s, inv, a, b):
    def body(r):
        c, image = image_of(src, s, g, r)
        at = pl.ds(r, g.R)
        return [(dst, c + inv[at, :] * (f[at, :] - image))]

    planes(g, a, b, body)


def first(g, dst, f, inv, a, b):
    def body(r):
        at = pl.ds(r, g.R)
        return [(dst, inv[at, :] * f[at, :])]

    planes(g, a, b, body)


def leftover(g, src, dst, f, s, a, b):
    def body(r):
        c, image = image_of(src, s, g, r)
        return [(dst, f[pl.ds(r, g.R), :] - image)]

    planes(g, a, b, body)


def restrict(src, gs, dst, gd, x0, x1, y0, count, matrix, tmp):
    step = -(-count // 8) * 8
    for x in range(x0, x1):
        r = gs.row(2 * x, 2 * y0)
        t = src[pl.ds(r, count, stride=2), :] + src[pl.ds(r + 1, count, stride=2), :]
        r = r + gs.R
        t = t + (src[pl.ds(r, count, stride=2), :] + src[pl.ds(r + 1, count, stride=2), :])
        tmp[pl.ds((x - x0) * step, count), :] = t
    for x in range(x0, x1):
        out = mm(tmp[pl.ds((x - x0) * step, step), :], matrix[...])
        dst[pl.ds(gd.row(x, y0), count), :] = out[0:count]


def prolong(src, gc, dst, gf, x0, x1, y0, count, matrix, tmp):
    for x in range(x0, x1):
        o = (x - x0) * 56
        u = mm(src[pl.ds(gc.row(x, y0), count), :], matrix[...])
        tmp[pl.ds(o, count, stride=2), :] = u
        tmp[pl.ds(o + 1, count, stride=2), :] = u
    for x in range(x0, x1):
        o = (x - x0) * 56
        v = tmp[pl.ds(o, 2 * count), :]
        for k in range(2):
            at = pl.ds(gf.row(2 * x + k, 2 * y0), 2 * count)
            dst[at, :] = dst[at, :] + v


class Item:
    def __init__(self, geo, w):
        self.g, self.w = geo, w


class Plan:
    def __init__(self, items):
        self.items = items
        self.yrows = sum(it.g.nx * it.w for it in items)
        self.yrows = -(-self.yrows // 8) * 8
        self.tiles = []
        for k, it in enumerate(items):
            for x in range(it.g.nx):
                for t in self.tiles:
                    if t[0] is it.g and t[1] + it.w <= 64:
                        break
                else:
                    t = [it.g, 0, []]
                    self.tiles.append(t)
                t[2].append((k, x, t[1]))
                t[1] += it.w
        self.zrows = sum(t[0].ny for t in self.tiles)
        self.zrows = -(-self.zrows // 8) * 8
        self.drows = max(it.g.nx for it in items)
        self.drows = -(-self.drows // 8) * 8
        assert sum(it.w * it.w for it in items) <= 64

    def scratch(self):
        x = [pltpu.VMEM((it.w * it.g.R, 128), F32) for it in self.items]
        return x + [
            pltpu.VMEM((2, self.yrows, 128), F32),
            pltpu.VMEM((2, self.yrows, 128), F32),
            pltpu.VMEM((2, self.zrows, 128), F32),
            pltpu.VMEM((2, self.zrows, 128), F32),
            pltpu.VMEM((4, self.drows, 128), F32),
            pltpu.VMEM((4, self.drows, 128), F32),
            pltpu.SemaphoreType.DMA((11,)),
            pltpu.SemaphoreType.DMA((11,)),
        ]


class Exchange:
    def __init__(self, plan, refs, scratch, place):
        n = len(plan.items)
        self.plan, self.refs, self.place = plan, refs, place
        self.xr = scratch[:n]
        self.ys, self.yr, self.zs, self.zr, self.ds, self.dr, self.ss, self.rs = scratch[n:]
        gx, gy, gz = place.me
        self.x_copies = []
        for k, it in enumerate(plan.items):
            g = it.g
            start = jnp.where(gx == 0, g.nx - it.w, 0)
            r = pl.multiple_of(GUARD + (g.halo + start) * g.R, 8)
            self.x_copies.append(
                self.copy(refs[k].at[pl.ds(r, it.w * g.R), :], self.xr[k], k, (1 - gx, gy, gz))
            )
        self.y_copies, self.z_copies, self.d_copies = [], [], []
        for d in range(2):
            self.y_copies.append(self.copy(self.ys.at[d], self.yr.at[d], 3 + d, place.beside(0, 1 - 2 * d, 0)))
            self.z_copies.append(self.copy(self.zs.at[d], self.zr.at[d], 5 + d, place.beside(0, 0, 1 - 2 * d)))
            for e in range(2):
                self.d_copies.append(
                    self.copy(
                        self.ds.at[2 * d + e], self.dr.at[2 * d + e], 7 + 2 * d + e,
                        place.beside(0, 1 - 2 * d, 1 - 2 * e),
                    )
                )
        self.copies = self.y_copies + self.z_copies + self.d_copies

    def copy(self, src, dst, k, peer):
        return pltpu.make_async_remote_copy(
            src_ref=src, dst_ref=dst, send_sem=self.ss.at[k], recv_sem=self.rs.at[k],
            device_id=peer, device_id_type=MESH,
        )

    def x_send(self):
        for c in self.x_copies:
            c.start()

    def x_fill(self):
        for c in self.x_copies:
            c.wait()
        m0, m1 = self.place.x_masks
        for k, it in enumerate(self.plan.items):
            g, w, ref = it.g, it.w, self.refs[k]
            upper = ((lanes(g.R) + 8) & 127) >= 64
            for j in range(w):
                got = self.xr[k][pl.ds(j * g.R, g.R), :]
                top = ref[pl.ds(GUARD + (g.halo + g.nx - w + j) * g.R, g.R), :]
                low = ref[pl.ds(GUARD + (g.halo + j) * g.R, g.R), :]
                ref[pl.ds(GUARD + (g.halo - w + j) * g.R, g.R), :] = roll(jnp.where(upper, got * m1, top), 64)
                ref[pl.ds(GUARD + (g.halo + g.nx + j) * g.R, g.R), :] = roll(jnp.where(upper, low, got * m0), 64)

    def pack_send(self):
        zo = 0
        for g, _, slots in self.plan.tiles:
            lane = lanes(g.ny) & 63
            acc = [None, None]
            for k, x, at in slots:
                w = self.plan.items[k].w
                v = self.refs[k][pl.ds(g.row(x, 0), g.ny), :]
                for q, z in enumerate((g.nz - w, 0)):
                    moved = roll(v, at - z)
                    acc[q] = moved if acc[q] is None else jnp.where(lane >= at, moved, acc[q])
            for q in range(2):
                self.zs[q, pl.ds(zo, g.ny), :] = acc[q]
            zo += g.ny
        for c in self.z_copies:
            c.start()
        yo, co = 0, 0
        corner = [None] * 4
        for k, it in enumerate(self.plan.items):
            g, w, ref = it.g, it.w, self.refs[k]
            n = g.nx
            lane = lanes(self.plan.drows) & 63
            for d in range(1, w + 1):
                at = co + (d - 1) * w
                for e, y in enumerate((g.ny - d, d - 1)):
                    v = ref[pl.ds(g.row(0, y), n, stride=g.R), :]
                    self.ys[e, pl.ds(yo, n), :] = v
                    if n < self.plan.drows:
                        v = jnp.concatenate([v, jnp.zeros((self.plan.drows - n, 128), F32)], axis=0)
                    for q, z in enumerate((g.nz - w, 0)):
                        moved = roll(v, at - z)
                        old = corner[2 * e + q]
                        corner[2 * e + q] = moved if old is None else jnp.where(lane >= at, moved, old)
                yo += n
            co += w * w
        for q in range(4):
            self.ds[q] = corner[q]
        for c in self.d_copies + self.y_copies:
            c.start()

    def unpack(self):
        my, mz = self.place.y_masks, self.place.z_masks
        for c in self.copies:
            c.wait()
        zo = 0
        for g, _, slots in self.plan.tiles:
            lane = lanes(g.ny) & 63
            got = [self.zr[q, pl.ds(zo, g.ny), :] * mz[q] for q in range(2)]
            for k, x, at in slots:
                w = self.plan.items[k].w
                rows = pl.ds(g.row(x, 0), g.ny)
                v = self.refs[k][rows, :]
                v = jnp.where(lane >= 64 - w, roll(got[0], -w - at), v)
                v = jnp.where((lane >= g.nz) & (lane < g.nz + w), roll(got[1], g.nz - at), v)
                self.refs[k][rows, :] = v
            zo += g.ny
        yo, co = 0, 0
        for k, it in enumerate(self.plan.items):
            g, w, ref = it.g, it.w, self.refs[k]
            n = g.nx
            lane = lanes(n) & 63
            into = (lane >= 64 - w, (lane >= g.nz) & (lane < g.nz + w))
            for d in range(1, w + 1):
                at = co + (d - 1) * w
                for e, y in enumerate((-d, g.ny + d - 1)):
                    v = self.yr[e, pl.ds(yo, n), :]
                    for q, z in enumerate((-w, g.nz)):
                        got = self.dr[2 * e + q, pl.ds(0, n), :] * mz[q]
                        v = jnp.where(into[q], roll(got, z - at), v)
                    ref[pl.ds(g.row(0, y), n, stride=g.R), :] = v * my[e]
                yo += n
            co += w * w


class Place:
    def __init__(self, sizes):
        self.sizes = sizes
        self.me = tuple(lax.axis_index(a) for a in ("gx", "gy", "gz"))
        gx, gy, gz = self.me
        one = lambda c: jnp.where(c, 1.0, 0.0).astype(F32)
        self.x_masks = (one(gx == 0), one(gx == 1))
        self.y_masks = (one(gy > 0), one(gy < sizes[1] - 1))
        self.z_masks = (one(gz > 0), one(gz < sizes[2] - 1))

    def beside(self, dx, dy, dz):
        return tuple(
            lax.rem(m + d % n, n) if d % n else m for m, d, n in zip(self.me, (dx, dy, dz), self.sizes)
        )


class Gather:
    def __init__(self, place, scratch):
        self.place = place
        self.mine, self.got, self.sum, self.s1, self.r1, self.s2, self.r2 = scratch
        n = place.sizes
        self.near = [(a, b) for a in range(n[0]) for b in range(n[1])][1:]

    def first_copies(self):
        n = self.place.sizes
        out = []
        for a, b in self.near:
            k = a * n[1] + b
            out.append(
                pltpu.make_async_remote_copy(
                    src_ref=self.mine, dst_ref=self.got.at[k], send_sem=self.s1.at[k], recv_sem=self.r1.at[k],
                    device_id=self.place.beside(a, b, 0), device_id_type=MESH,
                )
            )
        return out

    def second_copies(self, target):
        out = []
        for c in range(1, self.place.sizes[2]):
            out.append(
                pltpu.make_async_remote_copy(
                    src_ref=self.sum, dst_ref=target(c), send_sem=self.s2.at[c], recv_sem=self.r2.at[c],
                    device_id=self.place.beside(0, 0, c), device_id_type=MESH,
                )
            )
        return out

    def send(self):
        for c in self.first_copies():
            c.start()

    def relay(self, target):
        for c in self.first_copies():
            c.wait()
        total = self.mine[...]
        n = self.place.sizes
        for a, b in self.near:
            total = total + self.got[a * n[1] + b]
        self.sum[...] = total
        for c in self.second_copies(target):
            c.start()
        return total

    def finish(self, target):
        for c in self.second_copies(target):
            c.wait()


def gather_scratch(sizes, rows):
    near = sizes[0] * sizes[1]
    return [
        pltpu.VMEM((rows, 128), F32),
        pltpu.VMEM((near, rows, 128), F32),
        pltpu.VMEM((rows, 128), F32),
        pltpu.SemaphoreType.DMA((near,)),
        pltpu.SemaphoreType.DMA((near,)),
        pltpu.SemaphoreType.DMA((sizes[2],)),
        pltpu.SemaphoreType.DMA((sizes[2],)),
    ]


def to_level3(src, mine, square, turned, place):
    g = L2
    gx, gy, gz = place.me
    for i in range(3):
        r = g.row(2 * i, 0)
        t = src[pl.ds(r, 6, stride=2), :] + src[pl.ds(r + 1, 6, stride=2), :]
        r = r + g.R
        t = t + (src[pl.ds(r, 6, stride=2), :] + src[pl.ds(r + 1, 6, stride=2), :])
        square[pl.ds(8 * i, 6), :] = t
    turned[...] = jnp.transpose(square[...])
    a = turned[pl.ds(0, 8, stride=2), :] + turned[pl.ds(1, 8, stride=2), :]
    b = turned[pl.ds(64, 8, stride=2), :] + turned[pl.ds(65, 8, stride=2), :]
    a = (a + roll(b, 64)) * 0.125
    r = iota2((128, 384), 0)
    l = iota2((128, 384), 1)
    x = 6 * gx + 3 * (r >> 6) + ((r & 63) >> 3)
    y = 6 * gy + (r & 7)
    hit = (x == (l >> 5)) & (y == (l & 31)) & ((r & 7) < 6) & ((r & 63) < 24)
    out = mm(a, jnp.where(hit, 1.0, 0.0).astype(BF16))
    for k in range(3):
        mine[pl.ds(k, 6, stride=4), :] = out[0:6, 128 * k : 128 * k + 128]


def image3(ref, s_ref, r, n):
    lane = lanes(n)
    c = ref[pl.ds(r, n), :]
    b = ref[pl.ds(r + 4, n), :] + ref[pl.ds(r - 4, n), :]
    b = b + (roll(c, 1) + roll(c, -1))
    b = b + roll(jnp.where(lane < 32, ref[pl.ds(r + 1, n), :], c), -32)
    b = b + roll(jnp.where(lane >= 96, ref[pl.ds(r - 1, n), :], c), 32)
    return c, FACTOR3 * (6.0 * c - b) + s_ref[pl.ds(r, n), :] * c


def chunks3(rows, ref, body):
    n = min(rows, 192)

    def step(i, carry):
        r = pl.multiple_of(GUARD + i * n, 8)
        ref[pl.ds(r, n), :] = body(r, n)
        return carry

    lax.fori_loop(0, rows // n, step, 0)


def match4(k, shape, coarse_dim, ny):
    c = iota2(shape, coarse_dim)
    l = iota2(shape, 1 - coarse_dim)
    return ((c >> 4) == 2 * k + (l >> 6)) & ((c & 15) == ((l & 31) >> 1)) & ((l & 31) < ny)


def restrict4(src, n, ny):
    total = None
    for k in range(3):
        t = src[pl.ds(GUARD + k, n, stride=8), :] + src[pl.ds(GUARD + k + 4, n, stride=8), :]
        part = mm(t, jnp.where(match4(k, (128, 128), 1, ny), 0.125, 0.0).astype(BF16))
        total = part if total is None else total + part
    return total


def dot_all(a, b):
    return jnp.sum(jnp.sum(a * b, axis=0, keepdims=True), axis=1, keepdims=True)


def bottom(source, s4, p4, n, ny):
    estimate = jnp.zeros_like(source)
    left = source
    direction = source
    now = dot_all(left, left)
    shifted = s4[...]
    for it in range(BOTTOM_ITERS):
        p4[pl.ds(GUARD, n), :] = direction
        b = p4[pl.ds(GUARD + 1, n), :] + p4[pl.ds(GUARD - 1, n), :]
        b = b + (roll(direction, 1) + roll(direction, -1))
        b = b + (roll(direction, 16) + roll(direction, -16))
        inside = (lanes(n) < 96) & ((lanes(n) & 15) < ny)
        image = FACTOR4 * (6.0 * direction - jnp.where(inside, b, 0.0)) + shifted * direction
        step = now / dot_all(direction, image)
        estimate = estimate + step * direction
        if it < BOTTOM_ITERS - 1:
            left = left - step * image
            after = dot_all(left, left)
            direction = left + (after / now) * direction
            now = after
    return estimate


PLAN_A = Plan([Item(L0, 3), Item(L0, 2), Item(L0, 2)])
PLAN_S = Plan([Item(L1, 6), Item(L2, 5)])
PLAN_B = Plan([Item(L1, 6)])
PLAN_C = Plan([Item(L0, 3)])
PLAN_D = Plan([Item(L2, 5)])
PLANS = (PLAN_A, PLAN_S, PLAN_B, PLAN_C, PLAN_D)


def kernel(sizes, counts, right_in, guess_in, react_in, guess, r0, eb0, left0, step_out, *scratch):
    scratch = list(scratch)

    def take(n):
        out = scratch[:n]
        del scratch[:n]
        return out

    raw = take(3)
    (in_sems,) = take(1)
    right, react, inv0, ea0 = take(4)
    f1, s1, inv1, ea1, eb1, left1 = take(6)
    f2, s2, inv2, ea2, eb2, left2 = take(6)
    f3, s3, inv3, ea3, eb3, left3 = take(6)
    s4, p4, down_m, up_m, tmp, square, turned, spread, slab = take(9)
    scr = [take(n) for n in counts]
    place = Place(sizes)
    gx, gy, gz = place.me
    n3, n4, ny3 = 24 * sizes[2], 3 * sizes[2], 6 * sizes[1]

    loads = [
        pltpu.make_async_copy(src, dst, in_sems.at[k])
        for k, (src, dst) in enumerate(zip((guess_in, right_in, react_in), raw))
    ]
    for c in loads:
        c.start()

    def clear(ref):
        n = ref.shape[0]
        size = next(k for k in (128, 122 * 8, 80, 8) if n % k == 0) if n > 128 else n
        size = {1808: 904, 976: 488}.get(n, size)

        def step(i, carry):
            ref[pl.ds(pl.multiple_of(i * size, 8), size), :] = jnp.zeros((size, 128), F32)
            return carry

        lax.fori_loop(0, n // size, step, 0)

    clear(f3)
    clear(s3)
    peers = {(a, b, 0) for a in range(sizes[0]) for b in range(sizes[1])}
    peers |= {(0, 0, c) for c in range(sizes[2])}
    peers |= {(0, b % sizes[1], c % sizes[2]) for b in (1, -1) for c in (1, -1)}
    peers = sorted(peers - {(0, 0, 0)})
    barrier = pltpu.get_barrier_semaphore()
    for p in peers:
        pl.semaphore_signal(barrier, inc=1, device_id=place.beside(*p), device_id_type=MESH)
    for ref in (guess, right, react, f1, s1, ea1, eb1, f2, s2, ea2, eb2, ea3, eb3, p4, square):
        clear(ref)
    spread[...] = jnp.zeros_like(spread)

    for c in loads:
        c.wait()

    def load(i, carry):
        for src, dst in zip(raw, (guess, right, react)):
            for k in range(2):
                r = GUARD + (L0.halo + 2 * i + k) * L0.R + L0.y0
                dst[pl.ds(r, 48), 0:48] = src[2 * i + k]
                dst[pl.ds(r, 48), 64:112] = src[2 * i + k + 24]
        return carry

    lax.fori_loop(0, 12, load, 0)

    a = iota2((128, 128), 0)
    b = iota2((128, 128), 1)
    signed = lambda v: ((v + 8) & 63) - 8
    base = lambda v: ((v + 8) & 127) & 64
    zb = signed(b)
    hit = ((a == ((base(b) + 2 * zb) & 127)) | (a == ((base(b) + 2 * zb + 1) & 127))) & (zb >= -8) & (zb < 24)
    down_m[...] = jnp.where(hit, 0.125, 0.0).astype(BF16)
    hit = a == ((base(b) + (zb >> 1)) & 127)
    up_m[...] = jnp.where(hit, 1.0, 0.0).astype(BF16)

    ex_a = Exchange(PLAN_A, (guess, right, react), scr[0], place)
    ex_s = Exchange(PLAN_S, (s1, s2), scr[1], place)
    ex_b = Exchange(PLAN_B, (f1,), scr[2], place)
    ex_c = Exchange(PLAN_C, (eb0,), scr[3], place)
    ex_d = Exchange(PLAN_D, (f2,), scr[4], place)
    ga_s = Gather(place, scr[5])
    ga_f = Gather(place, scr[6])
    ga_r = Gather(place, scr[7])
    reduced = scr[8][0]

    def slot(ref):
        return lambda c: ref.at[pl.ds(pl.multiple_of(GUARD + 24 * gz, 8), 24), :]

    pl.semaphore_wait(barrier, len(peers))
    ex_a.pack_send()

    restrict(react, L0, s1, L1, 0, 12, 0, 24, down_m, tmp)
    restrict(s1, L1, s2, L2, 0, 6, 0, 12, down_m, tmp)
    ex_s.pack_send()
    ga_s.mine[...] = jnp.zeros((24, 128), F32)
    ga_f.mine[...] = jnp.zeros((24, 128), F32)
    to_level3(s2, ga_s.mine, square, turned, place)
    ga_s.send()

    def start(r):
        at = pl.ds(r, L0.R)
        c, image = image_of(guess, react, L0, r)
        res = right[at, :] - image
        inv = inverse(react[at, :], 1.0)
        return [(r0, res), (inv0, inv), (ea0, inv * res)]

    ex_a.unpack()
    ex_a.x_send()
    planes(L0, 1, 23, start)
    ex_a.x_fill()
    planes(L0, -2, 1, start)
    planes(L0, 23, 26, start)
    relax(L0, ea0, eb0, r0, react, inv0, -1, 25)
    leftover(L0, eb0, left0, r0, react, 0, 24)
    restrict(left0, L0, f1, L1, 0, 12, 0, 24, down_m, tmp)
    ex_b.pack_send()

    ex_s.unpack()
    ex_s.x_send()
    ex_c.pack_send()
    ex_s.x_fill()
    for g, sh, inv in ((L1, s1, inv1), (L2, s2, inv2)):
        planes(g, -g.halo, g.nx + g.halo, lambda r: [(inv, inverse(sh[pl.ds(r, g.R), :], g.factor))])
    s3[pl.ds(pl.multiple_of(GUARD + 24 * gz, 8), 24), :] = ga_s.relay(slot(s3))

    ex_b.unpack()
    ex_b.x_send()
    first(L1, ea1, f1, inv1, 0, 12)
    relax(L1, ea1, eb1, f1, s1, inv1, 1, 11)
    ex_b.x_fill()
    first(L1, ea1, f1, inv1, -6, 0)
    first(L1, ea1, f1, inv1, 12, 18)
    relax(L1, ea1, eb1, f1, s1, inv1, -5, 1)
    relax(L1, ea1, eb1, f1, s1, inv1, 11, 17)
    leftover(L1, eb1, left1, f1, s1, -4, 16)
    restrict(left1, L1, f2, L2, -2, 8, -2, 16, down_m, tmp)
    first(L2, ea2, f2, inv2, -2, 8)
    relax(L2, ea2, eb2, f2, s2, inv2, -1, 7)
    leftover(L2, eb2, left2, f2, s2, 0, 6)
    to_level3(left2, ga_f.mine, square, turned, place)
    ga_f.send()
    ex_d.pack_send()

    ex_c.unpack()
    ex_c.x_send()
    ga_s.finish(slot(s3))
    chunks3(n3, inv3, lambda r, n: inverse(s3[pl.ds(r, n), :], FACTOR3))
    s4[...] = restrict4(s3, n4, ny3)

    f3[pl.ds(pl.multiple_of(GUARD + 24 * gz, 8), 24), :] = ga_f.relay(slot(f3))
    ex_d.unpack()
    ex_d.x_send()
    ex_c.x_fill()
    ex_d.x_fill()
    first(L2, ea2, f2, inv2, -5, 11)
    relax(L2, ea2, eb2, f2, s2, inv2, -4, 10)
    ga_f.finish(slot(f3))

    def relax3(src, dst):
        def body(r, n):
            c, image = image3(src, s3, r, n)
            at = pl.ds(r, n)
            return c + inv3[at, :] * (f3[at, :] - image)

        chunks3(n3, dst, body)

    chunks3(n3, ea3, lambda r, n: inv3[pl.ds(r, n), :] * f3[pl.ds(r, n), :])
    relax3(ea3, eb3)
    chunks3(n3, left3, lambda r, n: f3[pl.ds(r, n), :] - image3(eb3, s3, r, n)[1])
    e4 = bottom(restrict4(left3, n4, ny3), s4, p4, n4, ny3 // 2)
    for k in range(3):
        u = mm(e4, jnp.where(match4(k, (128, 128), 0, ny3), 1.0, 0.0).astype(BF16))
        for q in (k, k + 4):
            at = pl.ds(GUARD + q, n4, stride=8)
            eb3[at, :] = eb3[at, :] + u
    relax3(eb3, ea3)
    relax3(ea3, eb3)

    slab[...] = eb3[pl.ds(pl.multiple_of(24 * gz, 8), 40), :]
    for k in range(3):
        v = slab[pl.ds(k, 10, stride=4), :]
        for h in range(2):
            for q in range(2):
                spread[k, pl.ds(64 * h + q, 10, stride=2), :] = v
    wide = [jnp.concatenate(p, axis=1) for p in zip(*[split3(spread[k]) for k in range(3)])]
    coarse = []
    for h in range(2):
        r = iota2((112, 384), 0)
        l = iota2((112, 384), 1)
        hit = (6 * gx + 3 * h + (r >> 4) - 2 == (l >> 5)) & (6 * gy + (r & 15) - 2 == (l & 31)) & ((r & 15) < 10)
        pick = jnp.where(hit, 1.0, 0.0).astype(BF16)
        parts = [
            lax.dot_general(pick, p, (((1,), (1,)), ((), ())), preferred_element_type=F32) for p in wide
        ]
        coarse.append(parts[0] + (parts[1] + parts[2]))
    fine = roll(jnp.where(lanes(112) < 64, coarse[0], coarse[1]), -4)
    for i in range(7):
        u = fine[16 * i : 16 * i + 10]
        tmp[pl.ds(24 * i, 10, stride=2), :] = u
        tmp[pl.ds(24 * i + 1, 10, stride=2), :] = u
    for i in range(7):
        v = tmp[pl.ds(24 * i, 20), :]
        for q in range(2):
            at = pl.ds(L2.row(2 * (i - 2) + q, -4), 20)
            eb2[at, :] = eb2[at, :] + v
    relax(L2, eb2, ea2, f2, s2, inv2, -3, 9)
    relax(L2, ea2, eb2, f2, s2, inv2, -2, 8)
    prolong(eb2, L2, eb1, L1, -2, 8, -2, 16, up_m, tmp)
    relax(L1, eb1, ea1, f1, s1, inv1, -3, 15)
    relax(L1, ea1, eb1, f1, s1, inv1, -2, 14)
    prolong(eb1, L1, eb0, L0, -2, 14, -2, 28, up_m, tmp)
    relax(L0, eb0, ea0, r0, react, inv0, -2, 26)
    relax(L0, ea0, eb0, r0, react, inv0, -1, 25)

    row = iota2((L0.R, 128), 0)
    inside = ((lanes(L0.R) & 63) < 48) & (row >= L0.y0) & (row < L0.y0 + 48)

    def last(i, sums):
        upper, lower = sums
        images = []
        for k in range(4):
            r = pl.multiple_of(GUARD + (L0.halo + 4 * i + k) * L0.R, 8)
            c, image = image_of(eb0, react, L0, r)
            images.append((r, image))
            upper = upper + jnp.where(inside, c * r0[pl.ds(r, L0.R), :], 0.0)
            lower = lower + jnp.where(inside, c * image, 0.0)
        for r, image in images:
            left0[pl.ds(r, L0.R), :] = image
        return upper, lower

    zero = jnp.zeros((L0.R, 128), F32)
    upper, lower = lax.fori_loop(0, 6, last, (zero, zero))
    upper = jnp.sum(upper, axis=0, keepdims=True)
    lower = jnp.sum(lower, axis=0, keepdims=True)
    half = lanes(1) < 64
    ga_r.mine[...] = jnp.where(half, upper + roll(upper, 64), lower + roll(lower, 64))
    ga_r.send()
    own = ga_r.relay(lambda c: reduced.at[c])
    ga_r.finish(lambda c: reduced.at[c])
    total = own
    for c in range(1, sizes[2]):
        total = total + reduced[c]
    upper = jnp.sum(jnp.where(half, total, 0.0), axis=1, keepdims=True)
    lower = jnp.sum(jnp.where(half, 0.0, total), axis=1, keepdims=True)
    step_out[...] = jnp.broadcast_to(upper / lower, (8, 128))


def finish(guess, r0, eb0, left0, step_ref, field_out, resid_out, field, resid, sems):
    step = step_ref[0:1, :]
    copies = []
    parts, size = 4, 6
    for p in range(parts):
        def body(i, carry):
            for k in range(2):
                x = p * size + 2 * i + k
                at = pl.ds(GUARD + (L0.halo + x) * L0.R + L0.y0, 48)
                e = eb0[at, :]
                v = guess[at, :] + step * e
                field[x] = v[:, 0:48]
                field[x + 24] = roll(v, 64)[:, 0:48]
                v = r0[at, :] - step * left0[at, :]
                resid[x] = v[:, 0:48]
                resid[x + 24] = roll(v, 64)[:, 0:48]
            return carry

        lax.fori_loop(0, size // 2, body, 0)
        for q, (src, dst) in enumerate(((field, field_out), (resid, resid_out))):
            for h in range(2):
                at = pl.ds(p * size + 24 * h, size)
                c = pltpu.make_async_copy(src.at[at], dst.at[at], sems.at[4 * p + 2 * q + h])
                c.start()
                copies.append(c)
    for c in copies:
        c.wait()


def solution(mesh):
    sizes = tuple(mesh.shape[a] for a in ("gx", "gy", "gz"))
    n3, n4 = 24 * sizes[2] + 2 * GUARD, 3 * sizes[2]
    scratch = [pltpu.VMEM((48, 48, 48), F32)] * 3 + [pltpu.SemaphoreType.DMA((3,))]
    scratch += [pltpu.VMEM((L0.total, 128), F32)] * 4
    scratch += [pltpu.VMEM((L1.total, 128), F32)] * 6
    scratch += [pltpu.VMEM((L2.total, 128), F32)] * 6
    scratch += [pltpu.VMEM((n3, 128), F32)] * 6
    scratch += [pltpu.VMEM((n4, 128), F32), pltpu.VMEM((n4 + 2 * GUARD, 128), F32)]
    scratch += [pltpu.VMEM((128, 128), BF16)] * 2 + [pltpu.VMEM((16 * 56, 128), F32)]
    scratch += [pltpu.VMEM((128, 128), F32)] * 2
    scratch += [pltpu.VMEM((3, 128, 128), F32), pltpu.VMEM((40, 128), F32)]
    groups = [p.scratch() for p in PLANS] + [gather_scratch(sizes, 24)] * 2 + [gather_scratch(sizes, 1)]
    groups += [[pltpu.VMEM((sizes[2], 1, 128), F32)]]
    for g in groups:
        scratch += g
    counts = tuple(len(g) for g in groups)
    vmem = pl.BlockSpec(memory_space=pltpu.VMEM)

    anywhere = pl.BlockSpec(memory_space=pl.ANY)

    def body(right_side, start_guess, reaction):
        whole = pltpu.VMEM((L0.total, 128), F32)
        parts = pl.pallas_call(
            functools.partial(kernel, sizes, counts),
            out_shape=[whole] * 4 + [pltpu.VMEM((8, 128), F32)],
            in_specs=[anywhere] * 3,
            out_specs=[vmem] * 5,
            scratch_shapes=scratch,
            compiler_params=pltpu.CompilerParams(
                collective_id=0, has_side_effects=True, vmem_limit_bytes=60 * 2**20
            ),
        )(right_side, start_guess, reaction)
        shape = jax.ShapeDtypeStruct(right_side.shape, F32)
        return tuple(
            pl.pallas_call(
                finish,
                out_shape=[shape, shape],
                in_specs=[vmem] * 5,
                out_specs=[anywhere] * 2,
                scratch_shapes=[pltpu.VMEM(right_side.shape, F32)] * 2 + [pltpu.SemaphoreType.DMA((16,))],
                compiler_params=pltpu.CompilerParams(vmem_limit_bytes=16 * 2**20),
            )(*parts)
        )

    placed = P("gx", "gy", "gz")
    return jax.shard_map(
        body, mesh=mesh, in_specs=(placed,) * 3, out_specs=(placed,) * 2, check_vma=False
    )
```

```python
import functools

import jax
import jax.numpy as jnp
from jax import lax
from jax.experimental import pallas as pl
from jax.experimental.pallas import tpu as pltpu
from jax.sharding import PartitionSpec as P

MESH = pl.DeviceIdType.MESH
F32 = jnp.float32
BF16 = jnp.bfloat16
DAMP = 6.0 / 7.0
GUARD = 8
BOTTOM_ITERS = 6


class Geo:
    def __init__(self, nx, ny, nz, halo, rows, y0, depth, unroll):
        self.nx, self.ny, self.nz, self.halo, self.R, self.y0 = nx, ny, nz, halo, rows, y0
        self.factor = 0.25**depth
        self.unroll = unroll
        self.total = 2 * GUARD + (nx + 2 * halo) * rows

    def row(self, x, y):
        return GUARD + (self.halo + x) * self.R + self.y0 + y


L0 = Geo(24, 48, 48, 4, 56, 4, 0, 4)
L1 = Geo(12, 24, 24, 6, 40, 8, 1, 6)
L2 = Geo(6, 12, 12, 5, 24, 6, 2, 8)
FACTOR3 = 0.25**3
FACTOR4 = 0.25**4


def lanes(rows):
    return lax.broadcasted_iota(jnp.int32, (rows, 128), 1)


def iota2(shape, dim):
    return lax.broadcasted_iota(jnp.int32, shape, dim)


def roll(v, shift):
    shift = shift % 128
    return v if shift == 0 else pltpu.roll(v, shift, 1)


def split3(a):
    hi = a.astype(BF16)
    rest = a - hi.astype(F32)
    mid = rest.astype(BF16)
    low = (rest - mid.astype(F32)).astype(BF16)
    return hi, mid, low


def mm(a, b):
    parts = split3(a)
    out = [jnp.dot(p, b, preferred_element_type=F32) for p in parts]
    return out[0] + (out[1] + out[2])


def beside_of(ref, r, R):
    c = ref[pl.ds(r, R), :]
    b = ref[pl.ds(r + R, R), :] + ref[pl.ds(r - R, R), :]
    b = b + (ref[pl.ds(r + 1, R), :] + ref[pl.ds(r - 1, R), :])
    b = b + (roll(c, 1) + roll(c, -1))
    return c, b


def image_of(ref, s_ref, g, r):
    c, b = beside_of(ref, r, g.R)
    return c, g.factor * (6.0 * c - b) + s_ref[pl.ds(r, g.R), :] * c


def planes(g, a, b, body):
    unroll = g.unroll

    def group(start, count):
        todo = []
        for k in range(count):
            r = start + k * g.R
            r = r if isinstance(r, int) else pl.multiple_of(r, 8)
            todo.append((r, body(r)))
        for r, pairs in todo:
            for ref, value in pairs:
                ref[pl.ds(r, g.R), :] = value

    trips = (b - a) // unroll
    origin = GUARD + (g.halo + a) * g.R
    if trips == 1:
        group(origin, unroll)
    elif trips:

        def step(i, carry):
            group(pl.multiple_of(origin + i * (unroll * g.R), 8), unroll)
            return carry

        lax.fori_loop(0, trips, step, 0)
    if (b - a) % unroll:
        group(origin + trips * unroll * g.R, (b - a) % unroll)


def inverse(s, factor):
    return jnp.where(s > 0.0, DAMP / (6.0 * factor + s), 0.0)


def relax(g, src, dst, f, s, inv, a, b):
    def body(r):
        c, image = image_of(src, s, g, r)
        at = pl.ds(r, g.R)
        return [(dst, c + inv[at, :] * (f[at, :] - image))]

    planes(g, a, b, body)


def first(g, dst, f, inv, a, b):
    def body(r):
        at = pl.ds(r, g.R)
        return [(dst, inv[at, :] * f[at, :])]

    planes(g, a, b, body)


def leftover(g, src, dst, f, s, a, b):
    def body(r):
        c, image = image_of(src, s, g, r)
        return [(dst, f[pl.ds(r, g.R), :] - image)]

    planes(g, a, b, body)


def restrict(src, gs, dst, gd, x0, x1, y0, count, matrix, tmp):
    step = -(-count // 8) * 8
    for x in range(x0, x1):
        r = gs.row(2 * x, 2 * y0)
        t = src[pl.ds(r, count, stride=2), :] + src[pl.ds(r + 1, count, stride=2), :]
        r = r + gs.R
        t = t + (src[pl.ds(r, count, stride=2), :] + src[pl.ds(r + 1, count, stride=2), :])
        tmp[pl.ds((x - x0) * step, count), :] = t
    for x in range(x0, x1):
        out = mm(tmp[pl.ds((x - x0) * step, step), :], matrix[...])
        dst[pl.ds(gd.row(x, y0), count), :] = out[0:count]


def prolong(src, gc, dst, gf, x0, x1, y0, count, matrix, tmp):
    for x in range(x0, x1):
        o = (x - x0) * 56
        u = mm(src[pl.ds(gc.row(x, y0), count), :], matrix[...])
        tmp[pl.ds(o, count, stride=2), :] = u
        tmp[pl.ds(o + 1, count, stride=2), :] = u
    for x in range(x0, x1):
        o = (x - x0) * 56
        v = tmp[pl.ds(o, 2 * count), :]
        for k in range(2):
            at = pl.ds(gf.row(2 * x + k, 2 * y0), 2 * count)
            dst[at, :] = dst[at, :] + v


class Item:
    def __init__(self, geo, w):
        self.g, self.w = geo, w


class Plan:
    def __init__(self, items):
        self.items = items
        self.yrows = sum(it.g.nx * it.w for it in items)
        self.yrows = -(-self.yrows // 8) * 8
        self.tiles = []
        for k, it in enumerate(items):
            for x in range(it.g.nx):
                for t in self.tiles:
                    if t[0] is it.g and t[1] + it.w <= 64:
                        break
                else:
                    t = [it.g, 0, []]
                    self.tiles.append(t)
                t[2].append((k, x, t[1]))
                t[1] += it.w
        self.zrows = sum(t[0].ny for t in self.tiles)
        self.zrows = -(-self.zrows // 8) * 8
        self.drows = max(it.g.nx for it in items)
        self.drows = -(-self.drows // 8) * 8
        assert sum(it.w * it.w for it in items) <= 64

        self.z0 = [0, self.zrows]
        self.d0 = [2 * self.zrows + q * self.drows for q in range(4)]
        self.y0 = [2 * self.zrows + 4 * self.drows + q * self.yrows for q in range(2)]
        self.total = 2 * (self.zrows + self.yrows) + 4 * self.drows
        self.xtotal = sum(it.w * it.g.R for it in items)

    def scratch(self):
        return [
            pltpu.VMEM((self.xtotal, 128), F32),
            pltpu.VMEM((self.total, 128), F32),
            pltpu.VMEM((self.total, 128), F32),
            pltpu.SemaphoreType.DMA((2,)),
            pltpu.SemaphoreType.DMA((2,)),
        ]


class Exchange:
    def __init__(self, plan, refs, scratch, place):
        self.plan, self.refs, self.place = plan, refs, place
        self.xr, self.sent, self.got, self.ss, self.rs = scratch
        gx, gy, gz = place.me
        self.partner = (1 - gx, gy, gz)
        self.x_copies = []
        o = 0
        for k, it in enumerate(plan.items):
            g = it.g
            start = jnp.where(gx == 0, g.nx - it.w, 0)
            r = pl.multiple_of(GUARD + (g.halo + start) * g.R, 8)
            n = it.w * g.R
            self.x_copies.append(self.copy(refs[k].at[pl.ds(r, n), :], self.xr.at[pl.ds(o, n), :], 0, self.partner))
            o += n
        self.y_copies, self.z_copies, self.d_copies = [], [], []
        for d in range(2):
            self.y_copies.append(self.segment(plan.y0[d], plan.yrows, place.beside(0, 1 - 2 * d, 0)))
            self.z_copies.append(self.segment(plan.z0[d], plan.zrows, place.beside(0, 0, 1 - 2 * d)))
            for e in range(2):
                self.d_copies.append(
                    self.segment(plan.d0[2 * d + e], plan.drows, place.beside(0, 1 - 2 * d, 1 - 2 * e))
                )

    def segment(self, start, n, peer):
        return self.copy(self.sent.at[pl.ds(start, n), :], self.got.at[pl.ds(start, n), :], 1, peer)

    def copy(self, src, dst, k, peer):
        return pltpu.make_async_remote_copy(
            src_ref=src, dst_ref=dst, send_sem=self.ss.at[k], recv_sem=self.rs.at[k],
            device_id=peer, device_id_type=MESH,
        )

    def x_send(self):
        for c in self.x_copies:
            c.start()

    def x_fill(self):
        self.copy(self.xr, self.xr, 0, self.partner).wait()
        m0, m1 = self.place.x_masks
        o = 0
        for k, it in enumerate(self.plan.items):
            g, w, ref = it.g, it.w, self.refs[k]
            upper = ((lanes(g.R) + 8) & 127) >= 64
            for j in range(w):
                got = self.xr[pl.ds(o + j * g.R, g.R), :]
                top = ref[pl.ds(GUARD + (g.halo + g.nx - w + j) * g.R, g.R), :]
                low = ref[pl.ds(GUARD + (g.halo + j) * g.R, g.R), :]
                ref[pl.ds(GUARD + (g.halo - w + j) * g.R, g.R), :] = roll(jnp.where(upper, got * m1, top), 64)
                ref[pl.ds(GUARD + (g.halo + g.nx + j) * g.R, g.R), :] = roll(jnp.where(upper, low, got * m0), 64)
            o += w * g.R

    def pack_send(self):
        self.pack(True)
        for c in self.d_copies + self.y_copies:
            c.start()

    def send(self):
        for c in self.z_copies + self.d_copies + self.y_copies:
            c.start()

    def pack(self, early=False):
        zo = 0
        for g, _, slots in self.plan.tiles:
            lane = lanes(g.ny) & 63
            acc = [None, None]
            for k, x, at in slots:
                w = self.plan.items[k].w
                v = self.refs[k][pl.ds(g.row(x, 0), g.ny), :]
                for q, z in enumerate((g.nz - w, 0)):
                    moved = roll(v, at - z)
                    acc[q] = moved if acc[q] is None else jnp.where(lane >= at, moved, acc[q])
            for q in range(2):
                self.sent[pl.ds(self.plan.z0[q] + zo, g.ny), :] = acc[q]
            zo += g.ny
        if early:
            for c in self.z_copies:
                c.start()
        yo, co = 0, 0
        corner = [None] * 4
        for k, it in enumerate(self.plan.items):
            g, w, ref = it.g, it.w, self.refs[k]
            n = g.nx
            lane = lanes(self.plan.drows) & 63
            for d in range(1, w + 1):
                at = co + (d - 1) * w
                for e, y in enumerate((g.ny - d, d - 1)):
                    v = ref[pl.ds(g.row(0, y), n, stride=g.R), :]
                    self.sent[pl.ds(self.plan.y0[e] + yo, n), :] = v
                    if n < self.plan.drows:
                        v = jnp.concatenate([v, jnp.zeros((self.plan.drows - n, 128), F32)], axis=0)
                    for q, z in enumerate((g.nz - w, 0)):
                        moved = roll(v, at - z)
                        old = corner[2 * e + q]
                        corner[2 * e + q] = moved if old is None else jnp.where(lane >= at, moved, old)
                yo += n
            co += w * w
        for q in range(4):
            self.sent[pl.ds(self.plan.d0[q], self.plan.drows), :] = corner[q]

    def unpack(self):
        my, mz = self.place.y_masks, self.place.z_masks
        self.copy(self.sent, self.got, 1, self.partner).wait()
        zo = 0
        for g, _, slots in self.plan.tiles:
            lane = lanes(g.ny) & 63
            got = [self.got[pl.ds(self.plan.z0[q] + zo, g.ny), :] * mz[q] for q in range(2)]
            for k, x, at in slots:
                w = self.plan.items[k].w
                rows = pl.ds(g.row(x, 0), g.ny)
                v = self.refs[k][rows, :]
                v = jnp.where(lane >= 64 - w, roll(got[0], -w - at), v)
                v = jnp.where((lane >= g.nz) & (lane < g.nz + w), roll(got[1], g.nz - at), v)
                self.refs[k][rows, :] = v
            zo += g.ny
        yo, co = 0, 0
        for k, it in enumerate(self.plan.items):
            g, w, ref = it.g, it.w, self.refs[k]
            n = g.nx
            lane = lanes(n) & 63
            into = (lane >= 64 - w, (lane >= g.nz) & (lane < g.nz + w))
            for d in range(1, w + 1):
                at = co + (d - 1) * w
                for e, y in enumerate((-d, g.ny + d - 1)):
                    v = self.got[pl.ds(self.plan.y0[e] + yo, n), :]
                    for q, z in enumerate((-w, g.nz)):
                        got = self.got[pl.ds(self.plan.d0[2 * e + q], n), :] * mz[q]
                        v = jnp.where(into[q], roll(got, z - at), v)
                    ref[pl.ds(g.row(0, y), n, stride=g.R), :] = v * my[e]
                yo += n
            co += w * w


class Place:
    def __init__(self, sizes):
        self.sizes = sizes
        self.me = tuple(lax.axis_index(a) for a in ("gx", "gy", "gz"))
        gx, gy, gz = self.me
        one = lambda c: jnp.where(c, 1.0, 0.0).astype(F32)
        self.x_masks = (one(gx == 0), one(gx == 1))
        self.y_masks = (one(gy > 0), one(gy < sizes[1] - 1))
        self.z_masks = (one(gz > 0), one(gz < sizes[2] - 1))

    def beside(self, dx, dy, dz):
        return tuple(
            lax.rem(m + d % n, n) if d % n else m for m, d, n in zip(self.me, (dx, dy, dz), self.sizes)
        )


class Gather:
    rows = 24

    def __init__(self, place, scratch, whole):
        self.place, self.whole = place, whole
        self.mine, self.got, self.sum, self.ss, self.rs = scratch
        n = place.sizes
        self.near = [(a, b) for a in range(n[0]) for b in range(n[1])][1:]
        self.at = pl.ds(pl.multiple_of(GUARD + self.rows * place.me[2], 8), self.rows)

    def copy(self, src, dst, k, peer):
        return pltpu.make_async_remote_copy(
            src_ref=src, dst_ref=dst, send_sem=self.ss.at[k], recv_sem=self.rs.at[k],
            device_id=peer, device_id_type=MESH,
        )

    def send(self):
        for k, (a, b) in enumerate(self.near):
            self.copy(self.mine, self.got.at[k], 0, self.place.beside(a, b, 0)).start()

    def relay(self):
        self.copy(self.got, self.got, 0, self.place.beside(1, 0, 0)).wait()
        total = self.mine[...]
        for k in range(len(self.near)):
            total = total + self.got[k]
        self.sum[...] = total
        for c in range(1, self.place.sizes[2]):
            self.copy(self.sum, self.whole.at[self.at, :], 1, self.place.beside(0, 0, c)).start()
        self.whole[self.at, :] = total

    def finish(self):
        most = self.whole.at[pl.ds(GUARD, self.rows * (self.place.sizes[2] - 1)), :]
        self.copy(most, most, 1, self.place.beside(1, 0, 0)).wait()


def gather_scratch(sizes):
    return [
        pltpu.VMEM((24, 128), F32),
        pltpu.VMEM((sizes[0] * sizes[1] - 1, 24, 128), F32),
        pltpu.VMEM((24, 128), F32),
        pltpu.SemaphoreType.DMA((2,)),
        pltpu.SemaphoreType.DMA((2,)),
    ]


def to_level3(src, mine, square, turned, place):
    g = L2
    gx, gy, gz = place.me
    for i in range(3):
        r = g.row(2 * i, 0)
        t = src[pl.ds(r, 6, stride=2), :] + src[pl.ds(r + 1, 6, stride=2), :]
        r = r + g.R
        t = t + (src[pl.ds(r, 6, stride=2), :] + src[pl.ds(r + 1, 6, stride=2), :])
        square[pl.ds(8 * i, 6), :] = t
    turned[...] = jnp.transpose(square[...])
    a = turned[pl.ds(0, 8, stride=2), :] + turned[pl.ds(1, 8, stride=2), :]
    b = turned[pl.ds(64, 8, stride=2), :] + turned[pl.ds(65, 8, stride=2), :]
    a = (a + roll(b, 64)) * 0.125
    r = iota2((128, 384), 0)
    l = iota2((128, 384), 1)
    x = 6 * gx + 3 * (r >> 6) + ((r & 63) >> 3)
    y = 6 * gy + (r & 7)
    hit = (x == (l >> 5)) & (y == (l & 31)) & ((r & 7) < 6) & ((r & 63) < 24)
    out = mm(a, jnp.where(hit, 1.0, 0.0).astype(BF16))
    for k in range(3):
        mine[pl.ds(k, 6, stride=4), :] = out[0:6, 128 * k : 128 * k + 128]


def image3(ref, s_ref, r, n):
    lane = lanes(n)
    c = ref[pl.ds(r, n), :]
    b = ref[pl.ds(r + 4, n), :] + ref[pl.ds(r - 4, n), :]
    b = b + (roll(c, 1) + roll(c, -1))
    b = b + roll(jnp.where(lane < 32, ref[pl.ds(r + 1, n), :], c), -32)
    b = b + roll(jnp.where(lane >= 96, ref[pl.ds(r - 1, n), :], c), 32)
    return c, FACTOR3 * (6.0 * c - b) + s_ref[pl.ds(r, n), :] * c


def chunks3(rows, ref, body):
    n = min(rows, 192)

    def step(i, carry):
        r = pl.multiple_of(GUARD + i * n, 8)
        ref[pl.ds(r, n), :] = body(r, n)
        return carry

    lax.fori_loop(0, rows // n, step, 0)


def match4(k, shape, coarse_dim, ny):
    c = iota2(shape, coarse_dim)
    l = iota2(shape, 1 - coarse_dim)
    return ((c >> 4) == 2 * k + (l >> 6)) & ((c & 15) == ((l & 31) >> 1)) & ((l & 31) < ny)


def restrict4(src, n, ny):
    total = None
    for k in range(3):
        t = src[pl.ds(GUARD + k, n, stride=8), :] + src[pl.ds(GUARD + k + 4, n, stride=8), :]
        part = mm(t, jnp.where(match4(k, (128, 128), 1, ny), 0.125, 0.0).astype(BF16))
        total = part if total is None else total + part
    return total


def dot_all(a, b):
    return jnp.sum(jnp.sum(a * b, axis=0, keepdims=True), axis=1, keepdims=True)


def bottom(source, s4, p4, n, ny):
    estimate = jnp.zeros_like(source)
    left = source
    inside = (lanes(n) < 96) & ((lanes(n) & 15) < ny)
    shifted = 6.0 * FACTOR4 + s4[...]
    for it in range(BOTTOM_ITERS):
        p4[pl.ds(GUARD, n), :] = left
        b = p4[pl.ds(GUARD + 1, n), :] + p4[pl.ds(GUARD - 1, n), :]
        b = b + (roll(left, 1) + roll(left, -1))
        b = b + (roll(left, 16) + roll(left, -16))
        image = shifted * left - FACTOR4 * jnp.where(inside, b, 0.0)
        now = dot_all(left, left)
        bent = dot_all(left, image)
        if it == 0:
            step = now / bent
            direction, turned = left, image
        else:
            ratio = now / before
            step = now / (bent - ratio * now / step)
            direction = left + ratio * direction
            turned = image + ratio * turned
        before = now
        estimate = estimate + step * direction
        if it < BOTTOM_ITERS - 1:
            left = left - step * turned
    return estimate


PLAN_A = Plan([Item(L0, 3), Item(L0, 2), Item(L0, 2)])
PLAN_S = Plan([Item(L1, 6), Item(L2, 5)])
PLAN_B = Plan([Item(L1, 6)])
PLAN_C = Plan([Item(L0, 3)])
PLAN_D = Plan([Item(L2, 5)])
PLANS = (PLAN_A, PLAN_S, PLAN_B, PLAN_C, PLAN_D)


def far(p, sizes):
    ring = lambda d, n: min(d % n, -d % n)
    return p[0] + ring(p[1], sizes[1]) + ring(p[2], 4) + ring(p[2] // 4, 4)


def kernel(sizes, counts, right_in, guess_in, react_in, guess, r0, eb0, left0, step_out, *scratch):
    scratch = list(scratch)

    def take(n):
        out = scratch[:n]
        del scratch[:n]
        return out

    raw = take(3)
    (in_sems,) = take(1)
    right, react, inv0, ea0 = take(4)
    f1, s1, inv1, ea1, eb1, left1 = take(6)
    f2, s2, inv2, ea2, eb2, left2 = take(6)
    f3, s3, inv3, ea3, eb3, left3 = take(6)
    s4, p4, down_m, up_m, tmp, square, turned, spread, slab = take(9)
    scr = [take(n) for n in counts]
    place = Place(sizes)
    gx, gy, gz = place.me
    n3, n4, ny3 = 24 * sizes[2], 3 * sizes[2], 6 * sizes[1]

    inputs = (guess_in, right_in, react_in)
    for k in range(3):
        for q in range(4):
            at = pl.ds(12 * q, 12)
            pltpu.make_async_copy(inputs[k].at[at], raw[k].at[at], in_sems.at[k]).start()

    def clear(ref):
        n = ref.shape[0]
        size = next(k for k in (128, 122 * 8, 80, 8) if n % k == 0) if n > 128 else n
        size = {1808: 904, 976: 488}.get(n, size)

        def step(i, carry):
            ref[pl.ds(pl.multiple_of(i * size, 8), size), :] = jnp.zeros((size, 128), F32)
            return carry

        lax.fori_loop(0, n // size, step, 0)

    peers = [(a, b, c) for a in range(sizes[0]) for b in range(sizes[1]) for c in range(sizes[2])][1:]
    peers.sort(key=lambda p: -far(p, sizes))
    barrier = pltpu.get_barrier_semaphore()
    for p in peers:
        pl.semaphore_signal(barrier, inc=1, device_id=place.beside(*p), device_id_type=MESH)
    for ref in (guess, right, react, f1, s1, ea1, eb1, f2, s2, ea2, eb2, ea3, eb3, p4, square):
        clear(ref)
    spread[...] = jnp.zeros_like(spread)
    for ref in (f3, s3):
        for r in (0, GUARD + n3):
            ref[pl.ds(r, GUARD), :] = jnp.zeros((GUARD, 128), F32)

    a = iota2((128, 128), 0)
    b = iota2((128, 128), 1)
    signed = lambda v: ((v + 8) & 63) - 8
    base = lambda v: ((v + 8) & 127) & 64
    zb = signed(b)
    hit = ((a == ((base(b) + 2 * zb) & 127)) | (a == ((base(b) + 2 * zb + 1) & 127))) & (zb >= -8) & (zb < 24)
    down_m[...] = jnp.where(hit, 0.125, 0.0).astype(BF16)
    hit = a == ((base(b) + (zb >> 1)) & 127)
    up_m[...] = jnp.where(hit, 1.0, 0.0).astype(BF16)

    for k, dst in enumerate((guess, right, react)):
        pltpu.make_async_copy(inputs[k], raw[k], in_sems.at[k]).wait()

        def load(i, carry):
            for q in range(4):
                r = GUARD + (L0.halo + 4 * i + q) * L0.R + L0.y0
                dst[pl.ds(r, 48), 0:48] = raw[k][4 * i + q]
                dst[pl.ds(r, 48), 64:112] = raw[k][4 * i + q + 24]
            return carry

        lax.fori_loop(0, 6, load, 0)

    ex_a = Exchange(PLAN_A, (guess, right, react), scr[0], place)
    ex_s = Exchange(PLAN_S, (s1, s2), scr[1], place)
    ex_b = Exchange(PLAN_B, (f1,), scr[2], place)
    ex_c = Exchange(PLAN_C, (eb0,), scr[3], place)
    ex_d = Exchange(PLAN_D, (f2,), scr[4], place)
    ga_s = Gather(place, scr[5], s3)
    ga_f = Gather(place, scr[6], f3)
    reduced, red_send, red_recv = scr[7]

    ex_a.pack()
    pl.semaphore_wait(barrier, len(peers))
    ex_a.send()

    restrict(react, L0, s1, L1, 0, 12, 0, 24, down_m, tmp)
    restrict(s1, L1, s2, L2, 0, 6, 0, 12, down_m, tmp)
    ex_s.pack_send()
    ga_s.mine[...] = jnp.zeros((24, 128), F32)
    ga_f.mine[...] = jnp.zeros((24, 128), F32)
    to_level3(s2, ga_s.mine, square, turned, place)
    ga_s.send()

    def start(r):
        at = pl.ds(r, L0.R)
        c, image = image_of(guess, react, L0, r)
        res = right[at, :] - image
        inv = inverse(react[at, :], 1.0)
        return [(r0, res), (inv0, inv), (ea0, inv * res)]

    ex_a.unpack()
    ex_a.x_send()
    planes(L0, 1, 23, start)
    ex_a.x_fill()
    planes(L0, -2, 1, start)
    planes(L0, 23, 26, start)
    relax(L0, ea0, eb0, r0, react, inv0, -1, 25)
    leftover(L0, eb0, left0, r0, react, 0, 24)
    restrict(left0, L0, f1, L1, 0, 12, 0, 24, down_m, tmp)
    ex_b.pack_send()

    ex_s.unpack()
    ex_s.x_send()
    ex_c.pack_send()
    ex_s.x_fill()
    for g, sh, inv in ((L1, s1, inv1), (L2, s2, inv2)):
        planes(g, -g.halo, g.nx + g.halo, lambda r: [(inv, inverse(sh[pl.ds(r, g.R), :], g.factor))])
    ga_s.relay()

    ex_b.unpack()
    ex_b.x_send()
    first(L1, ea1, f1, inv1, 0, 12)
    relax(L1, ea1, eb1, f1, s1, inv1, 1, 11)
    ex_b.x_fill()
    first(L1, ea1, f1, inv1, -6, 0)
    first(L1, ea1, f1, inv1, 12, 18)
    relax(L1, ea1, eb1, f1, s1, inv1, -5, 1)
    relax(L1, ea1, eb1, f1, s1, inv1, 11, 17)
    leftover(L1, eb1, left1, f1, s1, -4, 16)
    restrict(left1, L1, f2, L2, -2, 8, -2, 16, down_m, tmp)
    first(L2, ea2, f2, inv2, -2, 8)
    relax(L2, ea2, eb2, f2, s2, inv2, -1, 7)
    leftover(L2, eb2, left2, f2, s2, 0, 6)
    to_level3(left2, ga_f.mine, square, turned, place)
    ga_f.send()
    ex_d.pack_send()

    ex_c.unpack()
    ex_c.x_send()
    ga_s.finish()
    chunks3(n3, inv3, lambda r, n: inverse(s3[pl.ds(r, n), :], FACTOR3))
    s4[...] = restrict4(s3, n4, ny3)

    ga_f.relay()
    ex_d.unpack()
    ex_d.x_send()
    ex_c.x_fill()
    ex_d.x_fill()
    first(L2, ea2, f2, inv2, -5, 11)
    relax(L2, ea2, eb2, f2, s2, inv2, -4, 10)
    ga_f.finish()

    def relax3(src, dst):
        def body(r, n):
            c, image = image3(src, s3, r, n)
            at = pl.ds(r, n)
            return c + inv3[at, :] * (f3[at, :] - image)

        chunks3(n3, dst, body)

    chunks3(n3, ea3, lambda r, n: inv3[pl.ds(r, n), :] * f3[pl.ds(r, n), :])
    relax3(ea3, eb3)
    chunks3(n3, left3, lambda r, n: f3[pl.ds(r, n), :] - image3(eb3, s3, r, n)[1])
    e4 = bottom(restrict4(left3, n4, ny3), s4, p4, n4, ny3 // 2)
    for k in range(3):
        u = mm(e4, jnp.where(match4(k, (128, 128), 0, ny3), 1.0, 0.0).astype(BF16))
        for q in (k, k + 4):
            at = pl.ds(GUARD + q, n4, stride=8)
            eb3[at, :] = eb3[at, :] + u
    relax3(eb3, ea3)
    relax3(ea3, eb3)

    slab[...] = eb3[pl.ds(pl.multiple_of(24 * gz, 8), 40), :]
    for k in range(3):
        v = slab[pl.ds(k, 10, stride=4), :]
        for h in range(2):
            for q in range(2):
                spread[k, pl.ds(64 * h + q, 10, stride=2), :] = v
    wide = [jnp.concatenate(p, axis=1) for p in zip(*[split3(spread[k]) for k in range(3)])]
    coarse = []
    for h in range(2):
        r = iota2((112, 384), 0)
        l = iota2((112, 384), 1)
        hit = (6 * gx + 3 * h + (r >> 4) - 2 == (l >> 5)) & (6 * gy + (r & 15) - 2 == (l & 31)) & ((r & 15) < 10)
        pick = jnp.where(hit, 1.0, 0.0).astype(BF16)
        parts = [
            lax.dot_general(pick, p, (((1,), (1,)), ((), ())), preferred_element_type=F32) for p in wide
        ]
        coarse.append(parts[0] + (parts[1] + parts[2]))
    fine = roll(jnp.where(lanes(112) < 64, coarse[0], coarse[1]), -4)
    for i in range(7):
        u = fine[16 * i : 16 * i + 10]
        tmp[pl.ds(24 * i, 10, stride=2), :] = u
        tmp[pl.ds(24 * i + 1, 10, stride=2), :] = u
    for i in range(7):
        v = tmp[pl.ds(24 * i, 20), :]
        for q in range(2):
            at = pl.ds(L2.row(2 * (i - 2) + q, -4), 20)
            eb2[at, :] = eb2[at, :] + v
    relax(L2, eb2, ea2, f2, s2, inv2, -3, 9)
    relax(L2, ea2, eb2, f2, s2, inv2, -2, 8)
    prolong(eb2, L2, eb1, L1, -2, 8, -2, 16, up_m, tmp)
    relax(L1, eb1, ea1, f1, s1, inv1, -3, 15)
    relax(L1, ea1, eb1, f1, s1, inv1, -2, 14)
    prolong(eb1, L1, eb0, L0, -2, 14, -2, 28, up_m, tmp)
    relax(L0, eb0, ea0, r0, react, inv0, -2, 26)
    relax(L0, ea0, eb0, r0, react, inv0, -1, 25)

    row = iota2((L0.R, 128), 0)
    inside = ((lanes(L0.R) & 63) < 48) & (row >= L0.y0) & (row < L0.y0 + 48)

    def last(i, sums):
        upper, lower = sums
        images = []
        for k in range(4):
            r = pl.multiple_of(GUARD + (L0.halo + 4 * i + k) * L0.R, 8)
            c, image = image_of(eb0, react, L0, r)
            images.append((r, image))
            upper = upper + jnp.where(inside, c * r0[pl.ds(r, L0.R), :], 0.0)
            lower = lower + jnp.where(inside, c * image, 0.0)
        for r, image in images:
            left0[pl.ds(r, L0.R), :] = image
        return upper, lower

    zero = jnp.zeros((L0.R, 128), F32)
    upper, lower = lax.fori_loop(0, 6, last, (zero, zero))
    upper = jnp.sum(upper, axis=0, keepdims=True)
    lower = jnp.sum(lower, axis=0, keepdims=True)
    half = lanes(1) < 64
    number = (gx * sizes[1] + gy) * sizes[2] + gz
    reduced[number] = jnp.where(half, upper + roll(upper, 64), lower + roll(lower, 64))
    own = reduced.at[number]

    def summed(src, dst, p):
        return pltpu.make_async_remote_copy(
            src_ref=src, dst_ref=dst, send_sem=red_send.at[0], recv_sem=red_recv.at[0],
            device_id=place.beside(*p), device_id_type=MESH,
        )

    for p in peers:
        summed(own, own, p).start()
    most = reduced.at[pl.ds(0, len(peers))]
    summed(most, most, peers[0]).wait()
    sums = [reduced[k] for k in range(8)]
    for k in range(8, len(peers) + 1):
        sums[k % 8] = sums[k % 8] + reduced[k]
    while len(sums) > 1:
        sums = [x + y for x, y in zip(sums[::2], sums[1::2])]
    total = sums[0]
    upper = jnp.sum(jnp.where(half, total, 0.0), axis=1, keepdims=True)
    lower = jnp.sum(jnp.where(half, 0.0, total), axis=1, keepdims=True)
    step_out[...] = jnp.broadcast_to(upper / lower, (8, 128))


def finish(guess, r0, eb0, left0, step_ref, field_out, resid_out, field, resid, sems):
    step = step_ref[0:1, :]
    copies = []
    parts, size = 4, 6
    for p in range(parts):
        def body(i, carry):
            for k in range(2):
                x = p * size + 2 * i + k
                at = pl.ds(GUARD + (L0.halo + x) * L0.R + L0.y0, 48)
                e = eb0[at, :]
                v = guess[at, :] + step * e
                field[x] = v[:, 0:48]
                field[x + 24] = roll(v, 64)[:, 0:48]
                v = r0[at, :] - step * left0[at, :]
                resid[x] = v[:, 0:48]
                resid[x + 24] = roll(v, 64)[:, 0:48]
            return carry

        lax.fori_loop(0, size // 2, body, 0)
        for q, (src, dst) in enumerate(((field, field_out), (resid, resid_out))):
            for h in range(2):
                at = pl.ds(p * size + 24 * h, size)
                c = pltpu.make_async_copy(src.at[at], dst.at[at], sems.at[4 * p + 2 * q + h])
                c.start()
                copies.append(c)
    for c in copies:
        c.wait()


def solution(mesh):
    sizes = tuple(mesh.shape[a] for a in ("gx", "gy", "gz"))
    n3, n4 = 24 * sizes[2] + 2 * GUARD, 3 * sizes[2]
    scratch = [pltpu.VMEM((48, 48, 48), F32)] * 3 + [pltpu.SemaphoreType.DMA((3,))]
    scratch += [pltpu.VMEM((L0.total, 128), F32)] * 4
    scratch += [pltpu.VMEM((L1.total, 128), F32)] * 6
    scratch += [pltpu.VMEM((L2.total, 128), F32)] * 6
    scratch += [pltpu.VMEM((n3, 128), F32)] * 6
    scratch += [pltpu.VMEM((n4, 128), F32), pltpu.VMEM((n4 + 2 * GUARD, 128), F32)]
    scratch += [pltpu.VMEM((128, 128), BF16)] * 2 + [pltpu.VMEM((16 * 56, 128), F32)]
    scratch += [pltpu.VMEM((128, 128), F32)] * 2
    scratch += [pltpu.VMEM((3, 128, 128), F32), pltpu.VMEM((40, 128), F32)]
    groups = [p.scratch() for p in PLANS] + [gather_scratch(sizes)] * 2
    devices = sizes[0] * sizes[1] * sizes[2]
    groups += [[pltpu.VMEM((devices, 1, 128), F32)] + [pltpu.SemaphoreType.DMA((1,))] * 2]
    for g in groups:
        scratch += g
    counts = tuple(len(g) for g in groups)
    vmem = pl.BlockSpec(memory_space=pltpu.VMEM)

    anywhere = pl.BlockSpec(memory_space=pl.ANY)

    def body(right_side, start_guess, reaction):
        whole = pltpu.VMEM((L0.total, 128), F32)
        parts = pl.pallas_call(
            functools.partial(kernel, sizes, counts),
            out_shape=[whole] * 4 + [pltpu.VMEM((8, 128), F32)],
            in_specs=[anywhere] * 3,
            out_specs=[vmem] * 5,
            scratch_shapes=scratch,
            compiler_params=pltpu.CompilerParams(
                collective_id=0, has_side_effects=True, vmem_limit_bytes=60 * 2**20
            ),
        )(right_side, start_guess, reaction)
        shape = jax.ShapeDtypeStruct(right_side.shape, F32)
        return tuple(
            pl.pallas_call(
                finish,
                out_shape=[shape, shape],
                in_specs=[vmem] * 5,
                out_specs=[anywhere] * 2,
                scratch_shapes=[pltpu.VMEM(right_side.shape, F32)] * 2 + [pltpu.SemaphoreType.DMA((16,))],
                compiler_params=pltpu.CompilerParams(vmem_limit_bytes=16 * 2**20),
            )(*parts)
        )

    placed = P("gx", "gy", "gz")
    return jax.shard_map(
        body, mesh=mesh, in_specs=(placed,) * 3, out_specs=(placed,) * 2, check_vma=False
    )
```

```python
import functools

import jax
import jax.numpy as jnp
from jax import lax
from jax.experimental import pallas as pl
from jax.experimental.pallas import tpu as pltpu
from jax.sharding import PartitionSpec as P

MESH = pl.DeviceIdType.MESH
F32 = jnp.float32
BF16 = jnp.bfloat16
DAMP = 6.0 / 7.0
GUARD = 8
BOTTOM_ITERS = 6


class Geo:
    def __init__(self, nx, ny, nz, halo, rows, y0, depth, unroll):
        self.nx, self.ny, self.nz, self.halo, self.R, self.y0 = nx, ny, nz, halo, rows, y0
        self.factor = 0.25**depth
        self.unroll = unroll
        self.total = 2 * GUARD + (nx + 2 * halo) * rows

    def row(self, x, y):
        return GUARD + (self.halo + x) * self.R + self.y0 + y


L0 = Geo(24, 48, 48, 4, 56, 4, 0, 28)
L1 = Geo(12, 24, 24, 6, 40, 8, 1, 24)
L2 = Geo(6, 12, 12, 5, 24, 6, 2, 16)
FACTOR3 = 0.25**3
FACTOR4 = 0.25**4


def lanes(rows):
    return lax.broadcasted_iota(jnp.int32, (rows, 128), 1)


def iota2(shape, dim):
    return lax.broadcasted_iota(jnp.int32, shape, dim)


def tree(terms):
    while len(terms) > 1:
        terms = [sum(terms[k + 1 : k + 2], terms[k]) for k in range(0, len(terms), 2)]
    return terms[0]


def roll(v, shift):
    shift = shift % 128
    return v if shift == 0 else pltpu.roll(v, shift, 1)


def split3(a):
    hi = a.astype(BF16)
    rest = a - hi.astype(F32)
    mid = rest.astype(BF16)
    low = (rest - mid.astype(F32)).astype(BF16)
    return hi, mid, low


def mm(a, b):
    parts = split3(a)
    out = [jnp.dot(p, b, preferred_element_type=F32) for p in parts]
    return out[0] + (out[1] + out[2])


def beside_of(ref, r, R):
    c = ref[pl.ds(r, R), :]
    b = ref[pl.ds(r + R, R), :] + ref[pl.ds(r - R, R), :]
    b = b + (ref[pl.ds(r + 1, R), :] + ref[pl.ds(r - 1, R), :])
    b = b + (roll(c, 1) + roll(c, -1))
    return c, b


def image_of(ref, s_ref, g, r):
    c, b = beside_of(ref, r, g.R)
    return c, g.factor * (6.0 * c - b) + s_ref[pl.ds(r, g.R), :] * c


def planes(g, a, b, body):
    unroll = g.unroll

    def group(start, count):
        todo = []
        for k in range(count):
            r = start + k * g.R
            r = r if isinstance(r, int) else pl.multiple_of(r, 8)
            todo.append((r, body(r)))
        for r, pairs in todo:
            for ref, value in pairs:
                ref[pl.ds(r, g.R), :] = value

    trips = (b - a) // unroll
    origin = GUARD + (g.halo + a) * g.R
    if trips == 1:
        group(origin, unroll)
    elif trips:

        def step(i, carry):
            group(pl.multiple_of(origin + i * (unroll * g.R), 8), unroll)
            return carry

        lax.fori_loop(0, trips, step, 0)
    if (b - a) % unroll:
        group(origin + trips * unroll * g.R, (b - a) % unroll)


def inverse(s, factor):
    return jnp.where(s > 0.0, DAMP / (6.0 * factor + s), 0.0)


def relax(g, src, dst, f, s, inv, a, b):
    def body(r):
        c, image = image_of(src, s, g, r)
        at = pl.ds(r, g.R)
        return [(dst, c + inv[at, :] * (f[at, :] - image))]

    planes(g, a, b, body)


def first(g, dst, f, inv, a, b):
    def body(r):
        at = pl.ds(r, g.R)
        return [(dst, inv[at, :] * f[at, :])]

    planes(g, a, b, body)


def leftover(g, src, dst, f, s, a, b):
    def body(r):
        c, image = image_of(src, s, g, r)
        return [(dst, f[pl.ds(r, g.R), :] - image)]

    planes(g, a, b, body)


def restrict(src, gs, dst, gd, x0, x1, y0, count, matrix, tmp):
    step = -(-count // 8) * 8
    for x in range(x0, x1):
        r = gs.row(2 * x, 2 * y0)
        t = src[pl.ds(r, count, stride=2), :] + src[pl.ds(r + 1, count, stride=2), :]
        r = r + gs.R
        t = t + (src[pl.ds(r, count, stride=2), :] + src[pl.ds(r + 1, count, stride=2), :])
        tmp[pl.ds((x - x0) * step, count), :] = t
    for x in range(x0, x1):
        out = mm(tmp[pl.ds((x - x0) * step, step), :], matrix[...])
        dst[pl.ds(gd.row(x, y0), count), :] = out[0:count]


def prolong(src, gc, dst, gf, x0, x1, y0, count, matrix, tmp):
    for x in range(x0, x1):
        o = (x - x0) * 56
        u = mm(src[pl.ds(gc.row(x, y0), count), :], matrix[...])
        tmp[pl.ds(o, count, stride=2), :] = u
        tmp[pl.ds(o + 1, count, stride=2), :] = u
    for x in range(x0, x1):
        o = (x - x0) * 56
        v = tmp[pl.ds(o, 2 * count), :]
        for k in range(2):
            at = pl.ds(gf.row(2 * x + k, 2 * y0), 2 * count)
            dst[at, :] = dst[at, :] + v


class Item:
    def __init__(self, geo, w):
        self.g, self.w = geo, w


class Plan:
    def __init__(self, items):
        self.items = items
        self.yrows = sum(it.g.nx * it.w for it in items)
        self.yrows = -(-self.yrows // 8) * 8
        self.tiles = []
        for k, it in enumerate(items):
            for x in range(it.g.nx):
                for t in self.tiles:
                    if t[0] is it.g and t[1] + it.w <= 64:
                        break
                else:
                    t = [it.g, 0, []]
                    self.tiles.append(t)
                t[2].append((k, x, t[1]))
                t[1] += it.w
        self.zrows = sum(t[0].ny for t in self.tiles)
        self.zrows = -(-self.zrows // 8) * 8
        self.drows = max(it.g.nx for it in items)
        self.drows = -(-self.drows // 8) * 8
        assert sum(it.w * it.w for it in items) <= 64

        self.z0 = [0, self.zrows]
        self.d0 = [2 * self.zrows + q * self.drows for q in range(4)]
        self.y0 = [2 * self.zrows + 4 * self.drows + q * self.yrows for q in range(2)]
        self.total = 2 * (self.zrows + self.yrows) + 4 * self.drows
        self.xtotal = sum(it.w * it.g.R for it in items)

    def scratch(self):
        return [
            pltpu.VMEM((self.xtotal, 128), F32),
            pltpu.VMEM((self.total, 128), F32),
            pltpu.VMEM((self.total, 128), F32),
            pltpu.SemaphoreType.DMA((2,)),
            pltpu.SemaphoreType.DMA((2,)),
        ]


class Exchange:
    def __init__(self, plan, refs, scratch, place):
        self.plan, self.refs, self.place = plan, refs, place
        self.xr, self.sent, self.got, self.ss, self.rs = scratch
        gx, gy, gz = place.me
        self.partner = (1 - gx, gy, gz)
        self.x_copies = []
        o = 0
        for k, it in enumerate(plan.items):
            g = it.g
            start = jnp.where(gx == 0, g.nx - it.w, 0)
            r = pl.multiple_of(GUARD + (g.halo + start) * g.R, 8)
            n = it.w * g.R
            self.x_copies.append(self.copy(refs[k].at[pl.ds(r, n), :], self.xr.at[pl.ds(o, n), :], 0, self.partner))
            o += n
        at = {}
        for d in range(2):
            at[1 - 2 * d, 0] = plan.y0[d]
            at[0, 1 - 2 * d] = plan.z0[d]
            for e in range(2):
                at[1 - 2 * d, 1 - 2 * e] = plan.d0[2 * d + e]
        self.y_copies, self.z_copies, self.d_copies = [], [], []
        for d in (1, -1):
            self.y_copies.append(self.segment(at, d, 0, plan.yrows))
            self.z_copies.append(self.segment(at, 0, d, plan.zrows))
            for e in (1, -1):
                self.d_copies.append(self.segment(at, d, e, plan.drows))

    def segment(self, at, dy, dz, n):
        there = self.place.exists(dy, dz)
        peer = self.place.beside(0, dy, dz)
        peer = tuple(jnp.where(there, p, q) for p, q in zip(peer, self.partner))
        target = pl.multiple_of(jnp.where(there, at[dy, dz], at[-dy, -dz]), 8)
        return self.copy(self.sent.at[pl.ds(at[dy, dz], n), :], self.got.at[pl.ds(target, n), :], 1, peer)

    def copy(self, src, dst, k, peer):
        return pltpu.make_async_remote_copy(
            src_ref=src, dst_ref=dst, send_sem=self.ss.at[k], recv_sem=self.rs.at[k],
            device_id=peer, device_id_type=MESH,
        )

    def x_send(self):
        for c in self.x_copies:
            c.start()

    def x_fill(self):
        self.copy(self.xr, self.xr, 0, self.partner).wait()
        m0, m1 = self.place.x_masks
        o = 0
        for k, it in enumerate(self.plan.items):
            g, w, ref = it.g, it.w, self.refs[k]
            upper = ((lanes(g.R) + 8) & 127) >= 64
            for j in range(w):
                got = self.xr[pl.ds(o + j * g.R, g.R), :]
                top = ref[pl.ds(GUARD + (g.halo + g.nx - w + j) * g.R, g.R), :]
                low = ref[pl.ds(GUARD + (g.halo + j) * g.R, g.R), :]
                ref[pl.ds(GUARD + (g.halo - w + j) * g.R, g.R), :] = roll(jnp.where(upper, got * m1, top), 64)
                ref[pl.ds(GUARD + (g.halo + g.nx + j) * g.R, g.R), :] = roll(jnp.where(upper, low, got * m0), 64)
            o += w * g.R

    def pack_send(self):
        self.pack(True)
        for c in self.d_copies + self.y_copies:
            c.start()

    def send(self):
        for c in self.z_copies + self.d_copies + self.y_copies:
            c.start()

    def pack(self, early=False):
        zo = 0
        for g, _, slots in self.plan.tiles:
            lane = lanes(g.ny) & 63
            acc = [None, None]
            for k, x, at in slots:
                w = self.plan.items[k].w
                v = self.refs[k][pl.ds(g.row(x, 0), g.ny), :]
                for q, z in enumerate((g.nz - w, 0)):
                    moved = roll(v, at - z)
                    acc[q] = moved if acc[q] is None else jnp.where(lane >= at, moved, acc[q])
            for q in range(2):
                self.sent[pl.ds(self.plan.z0[q] + zo, g.ny), :] = acc[q]
            zo += g.ny
        if early:
            for c in self.z_copies:
                c.start()
        yo, co = 0, 0
        corner = [None] * 4
        for k, it in enumerate(self.plan.items):
            g, w, ref = it.g, it.w, self.refs[k]
            n = g.nx
            lane = lanes(self.plan.drows) & 63
            for d in range(1, w + 1):
                at = co + (d - 1) * w
                for e, y in enumerate((g.ny - d, d - 1)):
                    v = ref[pl.ds(g.row(0, y), n, stride=g.R), :]
                    self.sent[pl.ds(self.plan.y0[e] + yo, n), :] = v
                    if n < self.plan.drows:
                        v = jnp.concatenate([v, jnp.zeros((self.plan.drows - n, 128), F32)], axis=0)
                    for q, z in enumerate((g.nz - w, 0)):
                        moved = roll(v, at - z)
                        old = corner[2 * e + q]
                        corner[2 * e + q] = moved if old is None else jnp.where(lane >= at, moved, old)
                yo += n
            co += w * w
        for q in range(4):
            self.sent[pl.ds(self.plan.d0[q], self.plan.drows), :] = corner[q]

    def unpack(self):
        my, mz = self.place.y_masks, self.place.z_masks
        self.copy(self.sent, self.got, 1, self.partner).wait()
        zo = 0
        for g, _, slots in self.plan.tiles:
            lane = lanes(g.ny) & 63
            got = [self.got[pl.ds(self.plan.z0[q] + zo, g.ny), :] * mz[q] for q in range(2)]
            for k, x, at in slots:
                w = self.plan.items[k].w
                rows = pl.ds(g.row(x, 0), g.ny)
                v = self.refs[k][rows, :]
                v = jnp.where(lane >= 64 - w, roll(got[0], -w - at), v)
                v = jnp.where((lane >= g.nz) & (lane < g.nz + w), roll(got[1], g.nz - at), v)
                self.refs[k][rows, :] = v
            zo += g.ny
        yo, co = 0, 0
        for k, it in enumerate(self.plan.items):
            g, w, ref = it.g, it.w, self.refs[k]
            n = g.nx
            lane = lanes(n) & 63
            into = (lane >= 64 - w, (lane >= g.nz) & (lane < g.nz + w))
            for d in range(1, w + 1):
                at = co + (d - 1) * w
                for e, y in enumerate((-d, g.ny + d - 1)):
                    v = self.got[pl.ds(self.plan.y0[e] + yo, n), :]
                    for q, z in enumerate((-w, g.nz)):
                        got = self.got[pl.ds(self.plan.d0[2 * e + q], n), :] * mz[q]
                        v = jnp.where(into[q], roll(got, z - at), v)
                    ref[pl.ds(g.row(0, y), n, stride=g.R), :] = v * my[e]
                yo += n
            co += w * w


class Place:
    def __init__(self, sizes):
        self.sizes = sizes
        self.me = tuple(lax.axis_index(a) for a in ("gx", "gy", "gz"))
        gx, gy, gz = self.me
        one = lambda c: jnp.where(c, 1.0, 0.0).astype(F32)
        self.x_masks = (one(gx == 0), one(gx == 1))
        self.y_masks = (one(gy > 0), one(gy < sizes[1] - 1))
        self.z_masks = (one(gz > 0), one(gz < sizes[2] - 1))

    def exists(self, dy, dz):
        gx, gy, gz = self.me
        y, z = gy + dy, gz + dz
        return (y >= 0) & (y < self.sizes[1]) & (z >= 0) & (z < self.sizes[2])

    def beside(self, dx, dy, dz):
        return tuple(
            lax.rem(m + d % n, n) if d % n else m for m, d, n in zip(self.me, (dx, dy, dz), self.sizes)
        )


class Gather:
    rows = 24

    def __init__(self, place, scratch, whole):
        self.place, self.whole = place, whole
        self.mine, self.got, self.sum, self.ss, self.rs = scratch
        n = place.sizes
        self.near = [(a, b) for a in range(n[0]) for b in range(n[1])][1:]
        self.at = pl.ds(pl.multiple_of(GUARD + self.rows * place.me[2], 8), self.rows)

    def copy(self, src, dst, k, peer):
        return pltpu.make_async_remote_copy(
            src_ref=src, dst_ref=dst, send_sem=self.ss.at[k], recv_sem=self.rs.at[k],
            device_id=peer, device_id_type=MESH,
        )

    def send(self):
        for k, (a, b) in enumerate(self.near):
            self.copy(self.mine, self.got.at[k], 0, self.place.beside(a, b, 0)).start()

    def relay(self):
        self.copy(self.got, self.got, 0, self.place.beside(1, 0, 0)).wait()
        total = self.mine[...]
        for k in range(len(self.near)):
            total = total + self.got[k]
        self.sum[...] = total
        for c in range(1, self.place.sizes[2]):
            self.copy(self.sum, self.whole.at[self.at, :], 1, self.place.beside(0, 0, c)).start()
        self.whole[self.at, :] = total

    def finish(self):
        most = self.whole.at[pl.ds(GUARD, self.rows * (self.place.sizes[2] - 1)), :]
        self.copy(most, most, 1, self.place.beside(1, 0, 0)).wait()


def gather_scratch(sizes):
    return [
        pltpu.VMEM((24, 128), F32),
        pltpu.VMEM((sizes[0] * sizes[1] - 1, 24, 128), F32),
        pltpu.VMEM((24, 128), F32),
        pltpu.SemaphoreType.DMA((2,)),
        pltpu.SemaphoreType.DMA((2,)),
    ]


def to_level3(src, mine, square, turned, place):
    g = L2
    gx, gy, gz = place.me
    for i in range(3):
        r = g.row(2 * i, 0)
        t = src[pl.ds(r, 6, stride=2), :] + src[pl.ds(r + 1, 6, stride=2), :]
        r = r + g.R
        t = t + (src[pl.ds(r, 6, stride=2), :] + src[pl.ds(r + 1, 6, stride=2), :])
        square[pl.ds(8 * i, 6), :] = t
    turned[...] = jnp.transpose(square[...])
    a = turned[pl.ds(0, 8, stride=2), :] + turned[pl.ds(1, 8, stride=2), :]
    b = turned[pl.ds(64, 8, stride=2), :] + turned[pl.ds(65, 8, stride=2), :]
    a = (a + roll(b, 64)) * 0.125
    r = iota2((128, 384), 0)
    l = iota2((128, 384), 1)
    x = 6 * gx + 3 * (r >> 6) + ((r & 63) >> 3)
    y = 6 * gy + (r & 7)
    hit = (x == (l >> 5)) & (y == (l & 31)) & ((r & 7) < 6) & ((r & 63) < 24)
    out = mm(a, jnp.where(hit, 1.0, 0.0).astype(BF16))
    for k in range(3):
        mine[pl.ds(k, 6, stride=4), :] = out[0:6, 128 * k : 128 * k + 128]


def image3(ref, s_ref, r, n):
    lane = lanes(n)
    c = ref[pl.ds(r, n), :]
    b = ref[pl.ds(r + 4, n), :] + ref[pl.ds(r - 4, n), :]
    b = b + (roll(c, 1) + roll(c, -1))
    b = b + roll(jnp.where(lane < 32, ref[pl.ds(r + 1, n), :], c), -32)
    b = b + roll(jnp.where(lane >= 96, ref[pl.ds(r - 1, n), :], c), 32)
    return c, FACTOR3 * (6.0 * c - b) + s_ref[pl.ds(r, n), :] * c


def chunks3(rows, ref, body):
    n = min(rows, 384)

    def step(i, carry):
        r = pl.multiple_of(GUARD + i * n, 8)
        ref[pl.ds(r, n), :] = body(r, n)
        return carry

    lax.fori_loop(0, rows // n, step, 0)


def match4(k, shape, coarse_dim, ny):
    c = iota2(shape, coarse_dim)
    l = iota2(shape, 1 - coarse_dim)
    return ((c >> 4) == 2 * k + (l >> 6)) & ((c & 15) == ((l & 31) >> 1)) & ((l & 31) < ny)


def restrict4(src, n, ny):
    total = None
    for k in range(3):
        t = src[pl.ds(GUARD + k, n, stride=8), :] + src[pl.ds(GUARD + k + 4, n, stride=8), :]
        part = mm(t, jnp.where(match4(k, (128, 128), 1, ny), 0.125, 0.0).astype(BF16))
        total = part if total is None else total + part
    return total


def dot_all(a, b):
    return jnp.sum(jnp.sum(a * b, axis=0, keepdims=True), axis=1, keepdims=True)


def bottom(source, s4, p4, n, ny):
    estimate = jnp.zeros_like(source)
    left = source
    inside = (lanes(n) < 96) & ((lanes(n) & 15) < ny)
    shifted = 6.0 * FACTOR4 + s4[...]
    for it in range(BOTTOM_ITERS):
        p4[pl.ds(GUARD, n), :] = left
        b = p4[pl.ds(GUARD + 1, n), :] + p4[pl.ds(GUARD - 1, n), :]
        b = b + (roll(left, 1) + roll(left, -1))
        b = b + (roll(left, 16) + roll(left, -16))
        image = shifted * left - FACTOR4 * jnp.where(inside, b, 0.0)
        now = dot_all(left, left)
        bent = dot_all(left, image)
        if it == 0:
            step = now / bent
            direction, turned = left, image
        else:
            ratio = now / before
            step = now / (bent - ratio * now / step)
            direction = left + ratio * direction
            turned = image + ratio * turned
        before = now
        estimate = estimate + step * direction
        if it < BOTTOM_ITERS - 1:
            left = left - step * turned
    return estimate


PLAN_A = Plan([Item(L0, 3), Item(L0, 2), Item(L0, 2)])
PLAN_S = Plan([Item(L1, 6), Item(L2, 5)])
PLAN_B = Plan([Item(L1, 6)])
PLAN_C = Plan([Item(L0, 3)])
PLAN_D = Plan([Item(L2, 5)])
PLANS = (PLAN_A, PLAN_S, PLAN_B, PLAN_C, PLAN_D)


def far(p, sizes):
    ring = lambda d, n: min(d % n, -d % n)
    return p[0] + ring(p[1], sizes[1]) + ring(p[2], 4) + ring(p[2] // 4, 4)


def kernel(sizes, counts, right_in, guess_in, react_in, guess, r0, eb0, left0, step_out, *scratch):
    scratch = list(scratch)

    def take(n):
        out = scratch[:n]
        del scratch[:n]
        return out

    raw = take(3)
    (in_sems,) = take(1)
    right, react, inv0, ea0 = take(4)
    f1, s1, inv1, ea1, eb1, left1 = take(6)
    f2, s2, inv2, ea2, eb2, left2 = take(6)
    f3, s3, inv3, ea3, eb3, left3 = take(6)
    s4, p4, down_m, up_m, tmp, square, turned, spread, slab = take(9)
    scr = [take(n) for n in counts]
    place = Place(sizes)
    gx, gy, gz = place.me
    n3, n4, ny3 = 24 * sizes[2], 3 * sizes[2], 6 * sizes[1]

    inputs = (guess_in, right_in, react_in)
    for k in range(3):
        for q in range(4):
            at = pl.ds(12 * q, 12)
            pltpu.make_async_copy(inputs[k].at[at], raw[k].at[at], in_sems.at[k]).start()

    def clear(ref):
        n = ref.shape[0]
        size = next(k for k in (128, 122 * 8, 80, 8) if n % k == 0) if n > 128 else n
        size = {1808: 904, 976: 488}.get(n, size)

        def step(i, carry):
            ref[pl.ds(pl.multiple_of(i * size, 8), size), :] = jnp.zeros((size, 128), F32)
            return carry

        lax.fori_loop(0, n // size, step, 0)

    peers = [(a, b, c) for a in range(sizes[0]) for b in range(sizes[1]) for c in range(sizes[2])][1:]
    peers.sort(key=lambda p: -far(p, sizes))
    barrier = pltpu.get_barrier_semaphore()
    for p in peers:
        pl.semaphore_signal(barrier, inc=1, device_id=place.beside(*p), device_id_type=MESH)
    for ref in (guess, right, react, f1, s1, ea1, eb1, f2, s2, ea2, eb2, ea3, eb3, p4, square):
        clear(ref)
    spread[...] = jnp.zeros_like(spread)
    for ref in (f3, s3):
        for r in (0, GUARD + n3):
            ref[pl.ds(r, GUARD), :] = jnp.zeros((GUARD, 128), F32)

    a = iota2((128, 128), 0)
    b = iota2((128, 128), 1)
    signed = lambda v: ((v + 8) & 63) - 8
    base = lambda v: ((v + 8) & 127) & 64
    zb = signed(b)
    hit = ((a == ((base(b) + 2 * zb) & 127)) | (a == ((base(b) + 2 * zb + 1) & 127))) & (zb >= -8) & (zb < 24)
    down_m[...] = jnp.where(hit, 0.125, 0.0).astype(BF16)
    hit = a == ((base(b) + (zb >> 1)) & 127)
    up_m[...] = jnp.where(hit, 1.0, 0.0).astype(BF16)

    for k, dst in enumerate((guess, right, react)):
        pltpu.make_async_copy(inputs[k], raw[k], in_sems.at[k]).wait()

        for i in range(24):
            dst[pl.ds(L0.row(i, 0), 48), 0:48] = raw[k][i]
            dst[pl.ds(L0.row(i, 0), 48), 64:112] = raw[k][i + 24]

    ex_a = Exchange(PLAN_A, (guess, right, react), scr[0], place)
    ex_s = Exchange(PLAN_S, (s1, s2), scr[1], place)
    ex_b = Exchange(PLAN_B, (f1,), scr[2], place)
    ex_c = Exchange(PLAN_C, (eb0,), scr[3], place)
    ex_d = Exchange(PLAN_D, (f2,), scr[4], place)
    ga_s = Gather(place, scr[5], s3)
    ga_f = Gather(place, scr[6], f3)
    reduced, red_send, red_recv = scr[7]

    ex_a.pack()
    pl.semaphore_wait(barrier, len(peers))
    ex_a.send()

    restrict(react, L0, s1, L1, 0, 12, 0, 24, down_m, tmp)
    restrict(s1, L1, s2, L2, 0, 6, 0, 12, down_m, tmp)
    ex_s.pack_send()
    ga_s.mine[...] = jnp.zeros((24, 128), F32)
    ga_f.mine[...] = jnp.zeros((24, 128), F32)
    to_level3(s2, ga_s.mine, square, turned, place)
    ga_s.send()

    def start(r):
        at = pl.ds(r, L0.R)
        c, image = image_of(guess, react, L0, r)
        res = right[at, :] - image
        inv = inverse(react[at, :], 1.0)
        return [(r0, res), (inv0, inv), (ea0, inv * res)]

    ex_a.unpack()
    ex_a.x_send()
    planes(L0, 1, 23, start)
    ex_a.x_fill()
    planes(L0, -2, 1, start)
    planes(L0, 23, 26, start)
    relax(L0, ea0, eb0, r0, react, inv0, -1, 25)
    leftover(L0, eb0, left0, r0, react, 0, 24)
    restrict(left0, L0, f1, L1, 0, 12, 0, 24, down_m, tmp)
    ex_b.pack_send()

    ex_s.unpack()
    ex_s.x_send()
    ex_c.pack_send()
    ex_s.x_fill()
    for g, sh, inv in ((L1, s1, inv1), (L2, s2, inv2)):
        planes(g, -g.halo, g.nx + g.halo, lambda r: [(inv, inverse(sh[pl.ds(r, g.R), :], g.factor))])
    ga_s.relay()

    ex_b.unpack()
    ex_b.x_send()
    first(L1, ea1, f1, inv1, 0, 12)
    relax(L1, ea1, eb1, f1, s1, inv1, 1, 11)
    ex_b.x_fill()
    first(L1, ea1, f1, inv1, -6, 0)
    first(L1, ea1, f1, inv1, 12, 18)
    relax(L1, ea1, eb1, f1, s1, inv1, -5, 1)
    relax(L1, ea1, eb1, f1, s1, inv1, 11, 17)
    leftover(L1, eb1, left1, f1, s1, -4, 16)
    restrict(left1, L1, f2, L2, -2, 8, -2, 16, down_m, tmp)
    first(L2, ea2, f2, inv2, -2, 8)
    relax(L2, ea2, eb2, f2, s2, inv2, -1, 7)
    leftover(L2, eb2, left2, f2, s2, 0, 6)
    to_level3(left2, ga_f.mine, square, turned, place)
    ga_f.send()
    ex_d.pack_send()

    ex_c.unpack()
    ex_c.x_send()
    ga_s.finish()
    chunks3(n3, inv3, lambda r, n: inverse(s3[pl.ds(r, n), :], FACTOR3))
    s4[...] = restrict4(s3, n4, ny3)

    ga_f.relay()
    ex_d.unpack()
    ex_d.x_send()
    ex_c.x_fill()
    ex_d.x_fill()
    first(L2, ea2, f2, inv2, -5, 11)
    relax(L2, ea2, eb2, f2, s2, inv2, -4, 10)
    ga_f.finish()

    def relax3(src, dst):
        def body(r, n):
            c, image = image3(src, s3, r, n)
            at = pl.ds(r, n)
            return c + inv3[at, :] * (f3[at, :] - image)

        chunks3(n3, dst, body)

    chunks3(n3, ea3, lambda r, n: inv3[pl.ds(r, n), :] * f3[pl.ds(r, n), :])
    relax3(ea3, eb3)
    chunks3(n3, left3, lambda r, n: f3[pl.ds(r, n), :] - image3(eb3, s3, r, n)[1])
    e4 = bottom(restrict4(left3, n4, ny3), s4, p4, n4, ny3 // 2)
    for k in range(3):
        u = mm(e4, jnp.where(match4(k, (128, 128), 0, ny3), 1.0, 0.0).astype(BF16))
        for q in (k, k + 4):
            at = pl.ds(GUARD + q, n4, stride=8)
            eb3[at, :] = eb3[at, :] + u
    relax3(eb3, ea3)
    relax3(ea3, eb3)

    slab[...] = eb3[pl.ds(pl.multiple_of(24 * gz, 8), 40), :]
    for k in range(3):
        v = slab[pl.ds(k, 10, stride=4), :]
        for h in range(2):
            for q in range(2):
                spread[k, pl.ds(64 * h + q, 10, stride=2), :] = v
    wide = [jnp.concatenate(p, axis=1) for p in zip(*[split3(spread[k]) for k in range(3)])]
    coarse = []
    for h in range(2):
        r = iota2((112, 384), 0)
        l = iota2((112, 384), 1)
        hit = (6 * gx + 3 * h + (r >> 4) - 2 == (l >> 5)) & (6 * gy + (r & 15) - 2 == (l & 31)) & ((r & 15) < 10)
        pick = jnp.where(hit, 1.0, 0.0).astype(BF16)
        parts = [
            lax.dot_general(pick, p, (((1,), (1,)), ((), ())), preferred_element_type=F32) for p in wide
        ]
        coarse.append(parts[0] + (parts[1] + parts[2]))
    fine = roll(jnp.where(lanes(112) < 64, coarse[0], coarse[1]), -4)
    for i in range(7):
        u = fine[16 * i : 16 * i + 10]
        tmp[pl.ds(24 * i, 10, stride=2), :] = u
        tmp[pl.ds(24 * i + 1, 10, stride=2), :] = u
    for i in range(7):
        v = tmp[pl.ds(24 * i, 20), :]
        for q in range(2):
            at = pl.ds(L2.row(2 * (i - 2) + q, -4), 20)
            eb2[at, :] = eb2[at, :] + v
    relax(L2, eb2, ea2, f2, s2, inv2, -3, 9)
    relax(L2, ea2, eb2, f2, s2, inv2, -2, 8)
    prolong(eb2, L2, eb1, L1, -2, 8, -2, 16, up_m, tmp)
    relax(L1, eb1, ea1, f1, s1, inv1, -3, 15)
    relax(L1, ea1, eb1, f1, s1, inv1, -2, 14)
    prolong(eb1, L1, eb0, L0, -2, 14, -2, 28, up_m, tmp)
    relax(L0, eb0, ea0, r0, react, inv0, -2, 26)
    relax(L0, ea0, eb0, r0, react, inv0, -1, 25)

    row = iota2((L0.R, 128), 0)
    inside = ((lanes(L0.R) & 63) < 48) & (row >= L0.y0) & (row < L0.y0 + 48)

    upper, lower = [], []
    for i in range(24):
        r = GUARD + (L0.halo + i) * L0.R
        c, image = image_of(eb0, react, L0, r)
        left0[pl.ds(r, L0.R), :] = image
        upper.append(c * r0[pl.ds(r, L0.R), :])
        lower.append(c * image)
    upper = jnp.where(inside, tree(upper), 0.0)
    lower = jnp.where(inside, tree(lower), 0.0)
    upper = jnp.sum(upper, axis=0, keepdims=True)
    lower = jnp.sum(lower, axis=0, keepdims=True)
    half = lanes(1) < 64
    number = (gx * sizes[1] + gy) * sizes[2] + gz
    reduced[number] = jnp.where(half, upper + roll(upper, 64), lower + roll(lower, 64))
    own = reduced.at[number]

    def summed(src, dst, p):
        return pltpu.make_async_remote_copy(
            src_ref=src, dst_ref=dst, send_sem=red_send.at[0], recv_sem=red_recv.at[0],
            device_id=place.beside(*p), device_id_type=MESH,
        )

    for p in peers:
        summed(own, own, p).start()
    most = reduced.at[pl.ds(0, len(peers))]
    summed(most, most, peers[0]).wait()
    sums = [reduced[k] for k in range(8)]
    for k in range(8, len(peers) + 1):
        sums[k % 8] = sums[k % 8] + reduced[k]
    total = tree(sums)
    upper = jnp.sum(jnp.where(half, total, 0.0), axis=1, keepdims=True)
    lower = jnp.sum(jnp.where(half, 0.0, total), axis=1, keepdims=True)
    step_out[...] = jnp.broadcast_to(upper / lower, (8, 128))


def finish(guess, r0, eb0, left0, step_ref, field_out, resid_out, field, resid, sems):
    step = step_ref[0:1, :]
    copies = []
    parts, size = 4, 6
    for p in range(parts):
        for x in range(p * size, p * size + size):
            at = pl.ds(L0.row(x, 0), 48)
            v = guess[at, :] + step * eb0[at, :]
            field[x] = v[:, 0:48]
            field[x + 24] = roll(v, 64)[:, 0:48]
            v = r0[at, :] - step * left0[at, :]
            resid[x] = v[:, 0:48]
            resid[x + 24] = roll(v, 64)[:, 0:48]
        for q, (src, dst) in enumerate(((field, field_out), (resid, resid_out))):
            for h in range(2):
                at = pl.ds(p * size + 24 * h, size)
                c = pltpu.make_async_copy(src.at[at], dst.at[at], sems.at[4 * p + 2 * q + h])
                c.start()
                copies.append(c)
    for c in copies:
        c.wait()


def solution(mesh):
    sizes = tuple(mesh.shape[a] for a in ("gx", "gy", "gz"))
    n3, n4 = 24 * sizes[2] + 2 * GUARD, 3 * sizes[2]
    scratch = [pltpu.VMEM((48, 48, 48), F32)] * 3 + [pltpu.SemaphoreType.DMA((3,))]
    scratch += [pltpu.VMEM((L0.total, 128), F32)] * 4
    scratch += [pltpu.VMEM((L1.total, 128), F32)] * 6
    scratch += [pltpu.VMEM((L2.total, 128), F32)] * 6
    scratch += [pltpu.VMEM((n3, 128), F32)] * 6
    scratch += [pltpu.VMEM((n4, 128), F32), pltpu.VMEM((n4 + 2 * GUARD, 128), F32)]
    scratch += [pltpu.VMEM((128, 128), BF16)] * 2 + [pltpu.VMEM((16 * 56, 128), F32)]
    scratch += [pltpu.VMEM((128, 128), F32)] * 2
    scratch += [pltpu.VMEM((3, 128, 128), F32), pltpu.VMEM((40, 128), F32)]
    groups = [p.scratch() for p in PLANS] + [gather_scratch(sizes)] * 2
    devices = sizes[0] * sizes[1] * sizes[2]
    groups += [[pltpu.VMEM((devices, 1, 128), F32)] + [pltpu.SemaphoreType.DMA((1,))] * 2]
    for g in groups:
        scratch += g
    counts = tuple(len(g) for g in groups)
    vmem = pl.BlockSpec(memory_space=pltpu.VMEM)

    anywhere = pl.BlockSpec(memory_space=pl.ANY)

    def body(right_side, start_guess, reaction):
        whole = pltpu.VMEM((L0.total, 128), F32)
        parts = pl.pallas_call(
            functools.partial(kernel, sizes, counts),
            out_shape=[whole] * 4 + [pltpu.VMEM((8, 128), F32)],
            in_specs=[anywhere] * 3,
            out_specs=[vmem] * 5,
            scratch_shapes=scratch,
            compiler_params=pltpu.CompilerParams(
                collective_id=0, has_side_effects=True, vmem_limit_bytes=60 * 2**20
            ),
        )(right_side, start_guess, reaction)
        shape = jax.ShapeDtypeStruct(right_side.shape, F32)
        return tuple(
            pl.pallas_call(
                finish,
                out_shape=[shape, shape],
                in_specs=[vmem] * 5,
                out_specs=[anywhere] * 2,
                scratch_shapes=[pltpu.VMEM(right_side.shape, F32)] * 2 + [pltpu.SemaphoreType.DMA((16,))],
                compiler_params=pltpu.CompilerParams(vmem_limit_bytes=16 * 2**20),
            )(*parts)
        )

    placed = P("gx", "gy", "gz")
    return jax.shard_map(
        body, mesh=mesh, in_specs=(placed,) * 3, out_specs=(placed,) * 2, check_vma=False
    )
```

```python
import functools

import jax
import jax.numpy as jnp
from jax import lax
from jax.experimental import pallas as pl
from jax.experimental.pallas import tpu as pltpu
from jax.sharding import PartitionSpec as P

MESH = pl.DeviceIdType.MESH
F32 = jnp.float32
BF16 = jnp.bfloat16
DAMP = 6.0 / 7.0
GUARD = 8
GUARD3 = 16
BOTTOM_ITERS = 6


class Geo:
    def __init__(self, nx, ny, nz, halo, rows, y0, depth, unroll):
        self.nx, self.ny, self.nz, self.halo, self.R, self.y0 = nx, ny, nz, halo, rows, y0
        self.factor = 0.25**depth
        self.unroll = unroll
        self.total = 2 * GUARD + (nx + 2 * halo) * rows

    def row(self, x, y):
        return GUARD + (self.halo + x) * self.R + self.y0 + y


L0 = Geo(24, 48, 48, 4, 56, 4, 0, 28)
L1 = Geo(12, 24, 24, 6, 40, 8, 1, 24)
L2 = Geo(6, 12, 12, 5, 24, 6, 2, 16)
FACTOR3 = 0.25**3
FACTOR4 = 0.25**4


def lanes(rows):
    return lax.broadcasted_iota(jnp.int32, (rows, 128), 1)


def iota2(shape, dim):
    return lax.broadcasted_iota(jnp.int32, shape, dim)


def tree(terms):
    while len(terms) > 1:
        terms = [sum(terms[k + 1 : k + 2], terms[k]) for k in range(0, len(terms), 2)]
    return terms[0]


def roll(v, shift):
    shift = shift % 128
    return v if shift == 0 else pltpu.roll(v, shift, 1)


def split(a):
    hi = a.astype(BF16)
    return hi, (a - hi.astype(F32)).astype(BF16)


def mm(a, b):
    hi, low = split(a)
    return jnp.dot(hi, b, preferred_element_type=F32) + jnp.dot(low, b, preferred_element_type=F32)


def beside_of(ref, r, R):
    c = ref[pl.ds(r, R), :]
    b = ref[pl.ds(r + R, R), :] + ref[pl.ds(r - R, R), :]
    b = b + (ref[pl.ds(r + 1, R), :] + ref[pl.ds(r - 1, R), :])
    b = b + (roll(c, 1) + roll(c, -1))
    return c, b


def image_of(ref, s_ref, g, r):
    c, b = beside_of(ref, r, g.R)
    return c, g.factor * (6.0 * c - b) + s_ref[pl.ds(r, g.R), :] * c


def planes(g, a, b, body):
    unroll = g.unroll

    def group(start, count):
        todo = []
        for k in range(count):
            r = start + k * g.R
            r = r if isinstance(r, int) else pl.multiple_of(r, 8)
            todo.append((r, body(r)))
        for r, pairs in todo:
            for ref, value in pairs:
                ref[pl.ds(r, g.R), :] = value

    trips = (b - a) // unroll
    origin = GUARD + (g.halo + a) * g.R
    if trips == 1:
        group(origin, unroll)
    elif trips:

        def step(i, carry):
            group(pl.multiple_of(origin + i * (unroll * g.R), 8), unroll)
            return carry

        lax.fori_loop(0, trips, step, 0)
    if (b - a) % unroll:
        group(origin + trips * unroll * g.R, (b - a) % unroll)


def inverse(s, factor):
    return jnp.where(s > 0.0, DAMP / (6.0 * factor + s), 0.0)


def relax(g, src, dst, f, s, inv, a, b):
    def body(r):
        c, image = image_of(src, s, g, r)
        at = pl.ds(r, g.R)
        return [(dst, c + inv[at, :] * (f[at, :] - image))]

    planes(g, a, b, body)


def first(g, dst, f, inv, a, b):
    def body(r):
        at = pl.ds(r, g.R)
        return [(dst, inv[at, :] * f[at, :])]

    planes(g, a, b, body)


def leftover(g, src, dst, f, s, a, b):
    def body(r):
        c, image = image_of(src, s, g, r)
        return [(dst, f[pl.ds(r, g.R), :] - image)]

    planes(g, a, b, body)


def restrict(src, gs, dst, gd, x0, x1, y0, count, matrix, tmp):
    step = -(-count // 8) * 8
    for x in range(x0, x1):
        r = gs.row(2 * x, 2 * y0)
        t = src[pl.ds(r, count, stride=2), :] + src[pl.ds(r + 1, count, stride=2), :]
        r = r + gs.R
        t = t + (src[pl.ds(r, count, stride=2), :] + src[pl.ds(r + 1, count, stride=2), :])
        tmp[pl.ds((x - x0) * step, count), :] = t
    for x in range(x0, x1):
        out = mm(tmp[pl.ds((x - x0) * step, step), :], matrix[...])
        dst[pl.ds(gd.row(x, y0), count), :] = out[0:count]


def prolong(src, gc, dst, gf, x0, x1, y0, count, matrix, tmp):
    for x in range(x0, x1):
        o = (x - x0) * 56
        u = mm(src[pl.ds(gc.row(x, y0), count), :], matrix[...])
        tmp[pl.ds(o, count, stride=2), :] = u
        tmp[pl.ds(o + 1, count, stride=2), :] = u
    for x in range(x0, x1):
        o = (x - x0) * 56
        v = tmp[pl.ds(o, 2 * count), :]
        for k in range(2):
            at = pl.ds(gf.row(2 * x + k, 2 * y0), 2 * count)
            dst[at, :] = dst[at, :] + v


class Item:
    def __init__(self, geo, w):
        self.g, self.w = geo, w


class Plan:
    def __init__(self, items):
        self.items = items
        self.yrows = sum(it.g.nx * it.w for it in items)
        self.yrows = -(-self.yrows // 8) * 8
        self.tiles = []
        for k, it in enumerate(items):
            for x in range(it.g.nx):
                for t in self.tiles:
                    if t[0] is it.g and t[1] + it.w <= 64:
                        break
                else:
                    t = [it.g, 0, []]
                    self.tiles.append(t)
                t[2].append((k, x, t[1]))
                t[1] += it.w
        self.zrows = sum(t[0].ny for t in self.tiles)
        self.zrows = -(-self.zrows // 8) * 8
        self.drows = max(it.g.nx for it in items)
        self.drows = -(-self.drows // 8) * 8
        assert sum(it.w * it.w for it in items) <= 64

        self.z0 = [0, self.zrows]
        self.d0 = [2 * self.zrows + q * self.drows for q in range(4)]
        self.y0 = [2 * self.zrows + 4 * self.drows + q * self.yrows for q in range(2)]
        self.total = 2 * (self.zrows + self.yrows) + 4 * self.drows
        self.xtotal = sum(it.w * it.g.R for it in items)

    def scratch(self):
        return [
            pltpu.VMEM((self.xtotal, 128), F32),
            pltpu.VMEM((self.total, 128), F32),
            pltpu.VMEM((self.total, 128), F32),
            pltpu.SemaphoreType.DMA((2,)),
            pltpu.SemaphoreType.DMA((2,)),
        ]


class Exchange:
    def __init__(self, plan, refs, scratch, place):
        self.plan, self.refs, self.place = plan, refs, place
        self.xr, self.sent, self.got, self.ss, self.rs = scratch
        gx, gy, gz = place.me
        self.partner = (1 - gx, gy, gz)
        self.x_copies = []
        o = 0
        for k, it in enumerate(plan.items):
            g = it.g
            start = jnp.where(gx == 0, g.nx - it.w, 0)
            r = pl.multiple_of(GUARD + (g.halo + start) * g.R, 8)
            n = it.w * g.R
            self.x_copies.append(self.copy(refs[k].at[pl.ds(r, n), :], self.xr.at[pl.ds(o, n), :], 0, self.partner))
            o += n
        at = {}
        for d in range(2):
            at[1 - 2 * d, 0] = plan.y0[d]
            at[0, 1 - 2 * d] = plan.z0[d]
            for e in range(2):
                at[1 - 2 * d, 1 - 2 * e] = plan.d0[2 * d + e]
        self.y_copies, self.z_copies, self.d_copies = [], [], []
        for d in (1, -1):
            self.y_copies.append(self.segment(at, d, 0, plan.yrows))
            self.z_copies.append(self.segment(at, 0, d, plan.zrows))
            for e in (1, -1):
                self.d_copies.append(self.segment(at, d, e, plan.drows))

    def segment(self, at, dy, dz, n):
        there = self.place.exists(dy, dz)
        peer = self.place.beside(0, dy, dz)
        peer = tuple(jnp.where(there, p, q) for p, q in zip(peer, self.partner))
        target = pl.multiple_of(jnp.where(there, at[dy, dz], at[-dy, -dz]), 8)
        return self.copy(self.sent.at[pl.ds(at[dy, dz], n), :], self.got.at[pl.ds(target, n), :], 1, peer)

    def copy(self, src, dst, k, peer):
        return pltpu.make_async_remote_copy(
            src_ref=src, dst_ref=dst, send_sem=self.ss.at[k], recv_sem=self.rs.at[k],
            device_id=peer, device_id_type=MESH,
        )

    def x_send(self):
        for c in self.x_copies:
            c.start()

    def x_fill(self):
        self.copy(self.xr, self.xr, 0, self.partner).wait()
        m0, m1 = self.place.x_masks
        o = 0
        for k, it in enumerate(self.plan.items):
            g, w, ref = it.g, it.w, self.refs[k]
            upper = ((lanes(g.R) + 8) & 127) >= 64
            for j in range(w):
                got = self.xr[pl.ds(o + j * g.R, g.R), :]
                top = ref[pl.ds(GUARD + (g.halo + g.nx - w + j) * g.R, g.R), :]
                low = ref[pl.ds(GUARD + (g.halo + j) * g.R, g.R), :]
                ref[pl.ds(GUARD + (g.halo - w + j) * g.R, g.R), :] = roll(jnp.where(upper, got * m1, top), 64)
                ref[pl.ds(GUARD + (g.halo + g.nx + j) * g.R, g.R), :] = roll(jnp.where(upper, low, got * m0), 64)
            o += w * g.R

    def pack_send(self):
        self.pack(True)
        for c in self.d_copies + self.y_copies:
            c.start()

    def send(self):
        for c in self.z_copies + self.d_copies + self.y_copies:
            c.start()

    def pack(self, early=False):
        zo = 0
        for g, _, slots in self.plan.tiles:
            lane = lanes(g.ny) & 63
            acc = [None, None]
            for k, x, at in slots:
                w = self.plan.items[k].w
                v = self.refs[k][pl.ds(g.row(x, 0), g.ny), :]
                for q, z in enumerate((g.nz - w, 0)):
                    moved = roll(v, at - z)
                    acc[q] = moved if acc[q] is None else jnp.where(lane >= at, moved, acc[q])
            for q in range(2):
                self.sent[pl.ds(self.plan.z0[q] + zo, g.ny), :] = acc[q]
            zo += g.ny
        if early:
            for c in self.z_copies:
                c.start()
        yo, co = 0, 0
        corner = [None] * 4
        for k, it in enumerate(self.plan.items):
            g, w, ref = it.g, it.w, self.refs[k]
            n = g.nx
            lane = lanes(self.plan.drows) & 63
            for d in range(1, w + 1):
                at = co + (d - 1) * w
                for e, y in enumerate((g.ny - d, d - 1)):
                    v = ref[pl.ds(g.row(0, y), n, stride=g.R), :]
                    self.sent[pl.ds(self.plan.y0[e] + yo, n), :] = v
                    if n < self.plan.drows:
                        v = jnp.concatenate([v, jnp.zeros((self.plan.drows - n, 128), F32)], axis=0)
                    for q, z in enumerate((g.nz - w, 0)):
                        moved = roll(v, at - z)
                        old = corner[2 * e + q]
                        corner[2 * e + q] = moved if old is None else jnp.where(lane >= at, moved, old)
                yo += n
            co += w * w
        for q in range(4):
            self.sent[pl.ds(self.plan.d0[q], self.plan.drows), :] = corner[q]

    def unpack(self):
        my, mz = self.place.y_masks, self.place.z_masks
        self.copy(self.sent, self.got, 1, self.partner).wait()
        yo, co = 0, 0
        for k, it in enumerate(self.plan.items):
            g, w, ref = it.g, it.w, self.refs[k]
            n = g.nx
            lane = lanes(n) & 63
            into = (lane >= 64 - w, (lane >= g.nz) & (lane < g.nz + w))
            for d in range(1, w + 1):
                at = co + (d - 1) * w
                for e, y in enumerate((-d, g.ny + d - 1)):
                    v = self.got[pl.ds(self.plan.y0[e] + yo, n), :]
                    for q, z in enumerate((-w, g.nz)):
                        got = self.got[pl.ds(self.plan.d0[2 * e + q], n), :] * mz[q]
                        v = jnp.where(into[q], roll(got, z - at), v)
                    ref[pl.ds(g.row(0, y), n, stride=g.R), :] = v * my[e]
                yo += n
            co += w * w
        self.unpack_z(True)

    def unpack_rest(self):
        self.unpack_z(False)

    def unpack_z(self, edge):
        mz = self.place.z_masks
        zo = 0
        for g, _, slots in self.plan.tiles:
            lane = lanes(g.ny) & 63
            got = [self.got[pl.ds(self.plan.z0[q] + zo, g.ny), :] * mz[q] for q in range(2)]
            for k, x, at in slots:
                w = self.plan.items[k].w
                if (x < w or x >= g.nx - w) != edge:
                    continue
                rows = pl.ds(g.row(x, 0), g.ny)
                v = self.refs[k][rows, :]
                v = jnp.where(lane >= 64 - w, roll(got[0], -w - at), v)
                v = jnp.where((lane >= g.nz) & (lane < g.nz + w), roll(got[1], g.nz - at), v)
                self.refs[k][rows, :] = v
            zo += g.ny


class Place:
    def __init__(self, sizes):
        self.sizes = sizes
        self.me = tuple(lax.axis_index(a) for a in ("gx", "gy", "gz"))
        gx, gy, gz = self.me
        one = lambda c: jnp.where(c, 1.0, 0.0).astype(F32)
        self.x_masks = (one(gx == 0), one(gx == 1))
        self.y_masks = (one(gy > 0), one(gy < sizes[1] - 1))
        self.z_masks = (one(gz > 0), one(gz < sizes[2] - 1))

    def exists(self, dy, dz):
        gx, gy, gz = self.me
        y, z = gy + dy, gz + dz
        return (y >= 0) & (y < self.sizes[1]) & (z >= 0) & (z < self.sizes[2])

    def beside(self, dx, dy, dz):
        return tuple(
            lax.rem(m + d % n, n) if d % n else m for m, d, n in zip(self.me, (dx, dy, dz), self.sizes)
        )


class Gather:
    rows = 24

    def __init__(self, place, scratch, whole):
        self.place, self.whole = place, whole
        self.mine, self.got, self.sum, self.ss, self.rs = scratch
        n = place.sizes
        self.near = [(a, b) for a in range(n[0]) for b in range(n[1])][1:]
        self.near.sort(key=lambda p: -far((p[0], p[1], 0), n))
        self.line = sorted(range(1, n[2]), key=lambda c: -far((0, 0, c), n))
        self.at = pl.ds(pl.multiple_of(GUARD3 + self.rows * place.me[2], 8), self.rows)

    def copy(self, src, dst, k, peer):
        return pltpu.make_async_remote_copy(
            src_ref=src, dst_ref=dst, send_sem=self.ss.at[k], recv_sem=self.rs.at[k],
            device_id=peer, device_id_type=MESH,
        )

    def send(self):
        for k, (a, b) in enumerate(self.near):
            self.copy(self.mine, self.got.at[k], 0, self.place.beside(a, b, 0)).start()

    def relay(self):
        self.copy(self.got, self.got, 0, self.place.beside(1, 0, 0)).wait()
        total = self.mine[...]
        for k in range(len(self.near)):
            total = total + self.got[k]
        self.sum[...] = total
        for c in self.line:
            self.copy(self.sum, self.whole.at[self.at, :], 1, self.place.beside(0, 0, c)).start()
        self.whole[self.at, :] = total

    def finish(self):
        most = self.whole.at[pl.ds(GUARD3, self.rows * (self.place.sizes[2] - 1)), :]
        self.copy(most, most, 1, self.place.beside(1, 0, 0)).wait()


def gather_scratch(sizes):
    return [
        pltpu.VMEM((24, 128), F32),
        pltpu.VMEM((sizes[0] * sizes[1] - 1, 24, 128), F32),
        pltpu.VMEM((24, 128), F32),
        pltpu.SemaphoreType.DMA((2,)),
        pltpu.SemaphoreType.DMA((2,)),
    ]


def to_level3(src, mine, square, turned, place):
    g = L2
    gx, gy, gz = place.me
    for i in range(3):
        r = g.row(2 * i, 0)
        t = src[pl.ds(r, 6, stride=2), :] + src[pl.ds(r + 1, 6, stride=2), :]
        r = r + g.R
        t = t + (src[pl.ds(r, 6, stride=2), :] + src[pl.ds(r + 1, 6, stride=2), :])
        square[pl.ds(8 * i, 6), :] = t
    turned[...] = jnp.transpose(square[...])
    a = turned[pl.ds(0, 8, stride=2), :] + turned[pl.ds(1, 8, stride=2), :]
    b = turned[pl.ds(64, 8, stride=2), :] + turned[pl.ds(65, 8, stride=2), :]
    a = (a + roll(b, 64)) * 0.125
    r = iota2((128, 384), 0)
    l = iota2((128, 384), 1)
    x = 6 * gx + 3 * (r >> 6) + ((r & 63) >> 3)
    y = 6 * gy + (r & 7)
    hit = (x == (l >> 5)) & (y == (l & 31)) & ((r & 7) < 6) & ((r & 63) < 24)
    out = mm(a, jnp.where(hit, 1.0, 0.0).astype(BF16))
    for k in range(3):
        mine[pl.ds(k, 6, stride=4), :] = out[0:6, 128 * k : 128 * k + 128]


def image3(ref, s_ref, r, n):
    lane = lanes(n)
    c = ref[pl.ds(r, n), :]
    b = ref[pl.ds(r + 4, n), :] + ref[pl.ds(r - 4, n), :]
    b = b + (roll(c, 1) + roll(c, -1))
    b = b + roll(jnp.where(lane < 32, ref[pl.ds(r + 1, n), :], c), -32)
    b = b + roll(jnp.where(lane >= 96, ref[pl.ds(r - 1, n), :], c), 32)
    return c, FACTOR3 * (6.0 * c - b) + s_ref[pl.ds(r, n), :] * c


def chunks3(rows, ref, body):
    n = min(rows, 384)

    def step(i, carry):
        r = pl.multiple_of(GUARD3 + i * n, 8)
        ref[pl.ds(r, n), :] = body(r, n)
        return carry

    lax.fori_loop(0, rows // n, step, 0)


def match4(k, shape, coarse_dim, ny):
    c = iota2(shape, coarse_dim)
    l = iota2(shape, 1 - coarse_dim)
    return ((c >> 4) == 2 * k + (l >> 6)) & ((c & 15) == ((l & 31) >> 1)) & ((l & 31) < ny)


def restrict4(src, n, ny):
    total = None
    for k in range(3):
        t = src[pl.ds(GUARD3 + k, n, stride=8), :] + src[pl.ds(GUARD3 + k + 4, n, stride=8), :]
        part = mm(t, jnp.where(match4(k, (128, 128), 1, ny), 0.125, 0.0).astype(BF16))
        total = part if total is None else total + part
    return total


def dot_all(a, b):
    return jnp.sum(jnp.sum(a * b, axis=0, keepdims=True), axis=1, keepdims=True)


def bottom(source, s4, p4, n, ny):
    estimate = jnp.zeros_like(source)
    left = source
    inside = (lanes(n) < 96) & ((lanes(n) & 15) < ny)
    shifted = 6.0 * FACTOR4 + s4[...]
    for it in range(BOTTOM_ITERS):
        p4[pl.ds(GUARD, n), :] = left
        b = p4[pl.ds(GUARD + 1, n), :] + p4[pl.ds(GUARD - 1, n), :]
        b = b + (roll(left, 1) + roll(left, -1))
        b = b + (roll(left, 16) + roll(left, -16))
        image = shifted * left - FACTOR4 * jnp.where(inside, b, 0.0)
        now = dot_all(left, left)
        bent = dot_all(left, image)
        if it == 0:
            denom = bent
            direction, turned = left, image
        else:
            ratio = now * inv_before
            denom = bent - ratio * ratio * denom
            direction = left + ratio * direction
            turned = image + ratio * turned
        step = now / denom
        inv_before = 1.0 / now
        estimate = estimate + step * direction
        if it < BOTTOM_ITERS - 1:
            left = left - step * turned
    return estimate


PLAN_A = Plan([Item(L0, 3), Item(L0, 2), Item(L0, 2)])
PLAN_S = Plan([Item(L1, 6), Item(L2, 5)])
PLAN_B = Plan([Item(L1, 6)])
PLAN_C = Plan([Item(L0, 3)])
PLAN_D = Plan([Item(L2, 5)])
PLANS = (PLAN_A, PLAN_S, PLAN_B, PLAN_C, PLAN_D)


def far(p, sizes):
    ring = lambda d, n: min(d % n, -d % n)
    return p[0] + ring(p[1], sizes[1]) + ring(p[2], 4) + ring(p[2] // 4, 4)


def kernel(sizes, counts, right_in, guess_in, react_in, guess, r0, eb0, left0, step_out, *scratch):
    scratch = list(scratch)

    def take(n):
        out = scratch[:n]
        del scratch[:n]
        return out

    raw = take(3)
    (in_sems,) = take(1)
    right, react, inv0, ea0 = take(4)
    f1, s1, inv1, ea1, eb1, left1 = take(6)
    f2, s2, inv2, ea2, eb2, left2 = take(6)
    f3, s3, inv3, ea3, eb3, left3 = take(6)
    s4, p4, down_m, up_m, tmp, square, turned, spread, slab = take(9)
    scr = [take(n) for n in counts]
    place = Place(sizes)
    gx, gy, gz = place.me
    n3, n4, ny3 = 24 * sizes[2], 3 * sizes[2], 6 * sizes[1]

    inputs = (guess_in, right_in, react_in)
    for k in range(3):
        for q in range(4):
            at = pl.ds(12 * q, 12)
            pltpu.make_async_copy(inputs[k].at[at], raw[k].at[at], in_sems.at[k]).start()

    def clear(ref):
        n = ref.shape[0]
        size = next(k for k in (128, 122 * 8, 80, 8) if n % k == 0) if n > 128 else n
        size = {1808: 904, 976: 488, 416: 208}.get(n, size)

        def step(i, carry):
            ref[pl.ds(pl.multiple_of(i * size, 8), size), :] = jnp.zeros((size, 128), F32)
            return carry

        lax.fori_loop(0, n // size, step, 0)

    peers = [(a, b, c) for a in range(sizes[0]) for b in range(sizes[1]) for c in range(sizes[2])][1:]
    peers.sort(key=lambda p: -far(p, sizes))
    barrier = pltpu.get_barrier_semaphore()
    for p in peers:
        pl.semaphore_signal(barrier, inc=1, device_id=place.beside(*p), device_id_type=MESH)
    for ref in (guess, right, react, f1, s1, ea1, eb1, f2, s2, ea2, eb2, ea3, eb3, p4, square):
        clear(ref)
    spread[...] = jnp.zeros_like(spread)
    for ref in (f3, s3, inv3):
        for r in (0, GUARD3 + n3):
            ref[pl.ds(r, GUARD3), :] = jnp.zeros((GUARD3, 128), F32)

    a = iota2((128, 128), 0)
    b = iota2((128, 128), 1)
    signed = lambda v: ((v + 8) & 63) - 8
    base = lambda v: ((v + 8) & 127) & 64
    zb = signed(b)
    hit = ((a == ((base(b) + 2 * zb) & 127)) | (a == ((base(b) + 2 * zb + 1) & 127))) & (zb >= -8) & (zb < 24)
    down_m[...] = jnp.where(hit, 0.125, 0.0).astype(BF16)
    hit = a == ((base(b) + (zb >> 1)) & 127)
    up_m[...] = jnp.where(hit, 1.0, 0.0).astype(BF16)

    for k, dst in enumerate((guess, right, react)):
        pltpu.make_async_copy(inputs[k], raw[k], in_sems.at[k]).wait()

        for i in range(24):
            dst[pl.ds(L0.row(i, 0), 48), 0:48] = raw[k][i]
            dst[pl.ds(L0.row(i, 0), 48), 64:112] = raw[k][i + 24]

    ex_a = Exchange(PLAN_A, (guess, right, react), scr[0], place)
    ex_s = Exchange(PLAN_S, (s1, s2), scr[1], place)
    ex_b = Exchange(PLAN_B, (f1,), scr[2], place)
    ex_c = Exchange(PLAN_C, (eb0,), scr[3], place)
    ex_d = Exchange(PLAN_D, (f2,), scr[4], place)
    ga_s = Gather(place, scr[5], s3)
    ga_f = Gather(place, scr[6], f3)
    reduced, red_send, red_recv = scr[7]

    ex_a.pack()
    pl.semaphore_wait(barrier, len(peers))
    ex_a.send()

    restrict(react, L0, s1, L1, 0, 12, 0, 24, down_m, tmp)
    restrict(s1, L1, s2, L2, 0, 6, 0, 12, down_m, tmp)
    ex_s.pack_send()
    ga_s.mine[...] = jnp.zeros((24, 128), F32)
    ga_f.mine[...] = jnp.zeros((24, 128), F32)
    to_level3(s2, ga_s.mine, square, turned, place)
    ga_s.send()

    def start(r):
        at = pl.ds(r, L0.R)
        c, image = image_of(guess, react, L0, r)
        res = right[at, :] - image
        inv = inverse(react[at, :], 1.0)
        return [(r0, res), (inv0, inv), (ea0, inv * res)]

    ex_a.unpack()
    ex_a.x_send()
    ex_a.unpack_rest()
    planes(L0, 1, 23, start)
    ex_a.x_fill()
    planes(L0, -2, 1, start)
    planes(L0, 23, 26, start)
    relax(L0, ea0, eb0, r0, react, inv0, -1, 25)
    leftover(L0, eb0, left0, r0, react, 0, 24)
    restrict(left0, L0, f1, L1, 0, 12, 0, 24, down_m, tmp)
    ex_b.pack_send()

    ex_s.unpack()
    ex_s.x_send()
    ex_c.pack_send()
    ex_s.x_fill()
    for g, sh, inv in ((L1, s1, inv1), (L2, s2, inv2)):
        planes(g, -g.halo, g.nx + g.halo, lambda r: [(inv, inverse(sh[pl.ds(r, g.R), :], g.factor))])
    ga_s.relay()

    ex_b.unpack()
    ex_b.x_send()
    first(L1, ea1, f1, inv1, 0, 12)
    relax(L1, ea1, eb1, f1, s1, inv1, 1, 11)
    ex_b.x_fill()
    first(L1, ea1, f1, inv1, -6, 0)
    first(L1, ea1, f1, inv1, 12, 18)
    relax(L1, ea1, eb1, f1, s1, inv1, -5, 1)
    relax(L1, ea1, eb1, f1, s1, inv1, 11, 17)
    leftover(L1, eb1, left1, f1, s1, -4, 16)
    restrict(left1, L1, f2, L2, -2, 8, -2, 16, down_m, tmp)
    first(L2, ea2, f2, inv2, -2, 8)
    relax(L2, ea2, eb2, f2, s2, inv2, -1, 7)
    leftover(L2, eb2, left2, f2, s2, 0, 6)
    to_level3(left2, ga_f.mine, square, turned, place)
    ga_f.send()
    ex_d.pack_send()

    ex_c.unpack()
    ex_c.x_send()
    ex_c.unpack_rest()
    ga_s.finish()
    chunks3(n3, inv3, lambda r, n: inverse(s3[pl.ds(r, n), :], FACTOR3))
    s4[...] = restrict4(s3, n4, ny3)

    ga_f.relay()
    ex_d.unpack()
    ex_d.x_send()
    ex_c.x_fill()
    ex_d.x_fill()
    first(L2, ea2, f2, inv2, -5, 11)
    relax(L2, ea2, eb2, f2, s2, inv2, -4, 10)
    ga_f.finish()

    def relax3(src, dst):
        def body(r, n):
            c, image = image3(src, s3, r, n)
            at = pl.ds(r, n)
            return c + inv3[at, :] * (f3[at, :] - image)

        chunks3(n3, dst, body)

    chunks3(n3, ea3, lambda r, n: inv3[pl.ds(r, n), :] * f3[pl.ds(r, n), :])
    relax3(ea3, eb3)
    chunks3(n3, left3, lambda r, n: f3[pl.ds(r, n), :] - image3(eb3, s3, r, n)[1])
    e4 = bottom(restrict4(left3, n4, ny3), s4, p4, n4, ny3 // 2)
    for k in range(3):
        u = mm(e4, jnp.where(match4(k, (128, 128), 0, ny3), 1.0, 0.0).astype(BF16))
        for q in (k, k + 4):
            at = pl.ds(GUARD3 + q, n4, stride=8)
            eb3[at, :] = eb3[at, :] + u
    for src, dst, n in ((eb3, ea3, 48), (ea3, slab, 40)):
        r = pl.multiple_of(GUARD3 + 24 * gz - (n - 24) // 2, 4)
        c, image = image3(src, s3, r, n)
        at = pl.ds(r, n)
        dst[at if n == 48 else pl.ds(0, n), :] = c + inv3[at, :] * (f3[at, :] - image)
    for k in range(3):
        v = slab[pl.ds(k, 10, stride=4), :]
        for h in range(2):
            for q in range(2):
                spread[k, pl.ds(64 * h + q, 10, stride=2), :] = v
    wide = [jnp.concatenate(p, axis=1) for p in zip(*[split(spread[k]) for k in range(3)])]
    coarse = []
    for h in range(2):
        r = iota2((112, 384), 0)
        l = iota2((112, 384), 1)
        hit = (6 * gx + 3 * h + (r >> 4) - 2 == (l >> 5)) & (6 * gy + (r & 15) - 2 == (l & 31)) & ((r & 15) < 10)
        pick = jnp.where(hit, 1.0, 0.0).astype(BF16)
        parts = [
            lax.dot_general(pick, p, (((1,), (1,)), ((), ())), preferred_element_type=F32) for p in wide
        ]
        coarse.append(parts[0] + parts[1])
    fine = roll(jnp.where(lanes(112) < 64, coarse[0], coarse[1]), -4)
    for i in range(7):
        u = fine[16 * i : 16 * i + 10]
        tmp[pl.ds(24 * i, 10, stride=2), :] = u
        tmp[pl.ds(24 * i + 1, 10, stride=2), :] = u
    for i in range(7):
        v = tmp[pl.ds(24 * i, 20), :]
        for q in range(2):
            at = pl.ds(L2.row(2 * (i - 2) + q, -4), 20)
            eb2[at, :] = eb2[at, :] + v
    relax(L2, eb2, ea2, f2, s2, inv2, -3, 9)
    relax(L2, ea2, eb2, f2, s2, inv2, -2, 8)
    prolong(eb2, L2, eb1, L1, -2, 8, -2, 16, up_m, tmp)
    relax(L1, eb1, ea1, f1, s1, inv1, -3, 15)
    relax(L1, ea1, eb1, f1, s1, inv1, -2, 14)
    prolong(eb1, L1, eb0, L0, -2, 14, -2, 28, up_m, tmp)
    relax(L0, eb0, ea0, r0, react, inv0, -2, 26)
    relax(L0, ea0, eb0, r0, react, inv0, -1, 25)

    row = iota2((L0.R, 128), 0)
    inside = ((lanes(L0.R) & 63) < 48) & (row >= L0.y0) & (row < L0.y0 + 48)

    upper, lower = [], []
    for i in range(24):
        r = GUARD + (L0.halo + i) * L0.R
        c, image = image_of(eb0, react, L0, r)
        left0[pl.ds(r, L0.R), :] = image
        upper.append(c * r0[pl.ds(r, L0.R), :])
        lower.append(c * image)
    upper = jnp.where(inside, tree(upper), 0.0)
    lower = jnp.where(inside, tree(lower), 0.0)
    upper = jnp.sum(upper, axis=0, keepdims=True)
    lower = jnp.sum(lower, axis=0, keepdims=True)
    half = lanes(1) < 64
    number = (gx * sizes[1] + gy) * sizes[2] + gz
    reduced[number] = jnp.where(half, upper + roll(upper, 64), lower + roll(lower, 64))
    own = reduced.at[number]

    def summed(src, dst, p):
        return pltpu.make_async_remote_copy(
            src_ref=src, dst_ref=dst, send_sem=red_send.at[0], recv_sem=red_recv.at[0],
            device_id=place.beside(*p), device_id_type=MESH,
        )

    for p in peers:
        summed(own, own, p).start()
    most = reduced.at[pl.ds(0, len(peers))]
    summed(most, most, peers[0]).wait()
    sums = [reduced[k] for k in range(8)]
    for k in range(8, len(peers) + 1):
        sums[k % 8] = sums[k % 8] + reduced[k]
    total = tree(sums)
    upper = jnp.sum(jnp.where(half, total, 0.0), axis=1, keepdims=True)
    lower = jnp.sum(jnp.where(half, 0.0, total), axis=1, keepdims=True)
    step_out[...] = jnp.broadcast_to(upper / lower, (8, 128))


def finish(guess, r0, eb0, left0, step_ref, field_out, resid_out, field, resid, sems):
    step = step_ref[0:1, :]
    copies = []
    parts, size = 4, 6
    for p in range(parts):
        for x in range(p * size, p * size + size):
            at = pl.ds(L0.row(x, 0), 48)
            v = guess[at, :] + step * eb0[at, :]
            field[x] = v[:, 0:48]
            field[x + 24] = roll(v, 64)[:, 0:48]
            v = r0[at, :] - step * left0[at, :]
            resid[x] = v[:, 0:48]
            resid[x + 24] = roll(v, 64)[:, 0:48]
        for q, (src, dst) in enumerate(((field, field_out), (resid, resid_out))):
            for h in range(2):
                at = pl.ds(p * size + 24 * h, size)
                c = pltpu.make_async_copy(src.at[at], dst.at[at], sems.at[4 * p + 2 * q + h])
                c.start()
                copies.append(c)
    for c in copies:
        c.wait()


def solution(mesh):
    sizes = tuple(mesh.shape[a] for a in ("gx", "gy", "gz"))
    n3, n4 = 24 * sizes[2] + 2 * GUARD3, 3 * sizes[2]
    scratch = [pltpu.VMEM((48, 48, 48), F32)] * 3 + [pltpu.SemaphoreType.DMA((3,))]
    scratch += [pltpu.VMEM((L0.total, 128), F32)] * 4
    scratch += [pltpu.VMEM((L1.total, 128), F32)] * 6
    scratch += [pltpu.VMEM((L2.total, 128), F32)] * 6
    scratch += [pltpu.VMEM((n3, 128), F32)] * 6
    scratch += [pltpu.VMEM((n4, 128), F32), pltpu.VMEM((n4 + 2 * GUARD, 128), F32)]
    scratch += [pltpu.VMEM((128, 128), BF16)] * 2 + [pltpu.VMEM((16 * 56, 128), F32)]
    scratch += [pltpu.VMEM((128, 128), F32)] * 2
    scratch += [pltpu.VMEM((3, 128, 128), F32), pltpu.VMEM((40, 128), F32)]
    groups = [p.scratch() for p in PLANS] + [gather_scratch(sizes)] * 2
    devices = sizes[0] * sizes[1] * sizes[2]
    groups += [[pltpu.VMEM((devices, 1, 128), F32)] + [pltpu.SemaphoreType.DMA((1,))] * 2]
    for g in groups:
        scratch += g
    counts = tuple(len(g) for g in groups)
    vmem = pl.BlockSpec(memory_space=pltpu.VMEM)

    anywhere = pl.BlockSpec(memory_space=pl.ANY)

    def body(right_side, start_guess, reaction):
        whole = pltpu.VMEM((L0.total, 128), F32)
        parts = pl.pallas_call(
            functools.partial(kernel, sizes, counts),
            out_shape=[whole] * 4 + [pltpu.VMEM((8, 128), F32)],
            in_specs=[anywhere] * 3,
            out_specs=[vmem] * 5,
            scratch_shapes=scratch,
            compiler_params=pltpu.CompilerParams(
                collective_id=0, has_side_effects=True, vmem_limit_bytes=60 * 2**20
            ),
        )(right_side, start_guess, reaction)
        shape = jax.ShapeDtypeStruct(right_side.shape, F32)
        return tuple(
            pl.pallas_call(
                finish,
                out_shape=[shape, shape],
                in_specs=[vmem] * 5,
                out_specs=[anywhere] * 2,
                scratch_shapes=[pltpu.VMEM(right_side.shape, F32)] * 2 + [pltpu.SemaphoreType.DMA((16,))],
                compiler_params=pltpu.CompilerParams(vmem_limit_bytes=16 * 2**20),
            )(*parts)
        )

    placed = P("gx", "gy", "gz")
    return jax.shard_map(
        body, mesh=mesh, in_specs=(placed,) * 3, out_specs=(placed,) * 2, check_vma=False
    )
```

```python
import functools

import jax
import jax.numpy as jnp
from jax import lax
from jax.experimental import pallas as pl
from jax.experimental.pallas import tpu as pltpu
from jax.sharding import PartitionSpec as P

MESH = pl.DeviceIdType.MESH
F32 = jnp.float32
BF16 = jnp.bfloat16
DAMP = 6.0 / 7.0
GUARD = 8
GUARD3 = 16
BOTTOM_ITERS = 6


class Geo:
    def __init__(self, nx, ny, nz, halo, rows, y0, depth, unroll):
        self.nx, self.ny, self.nz, self.halo, self.R, self.y0 = nx, ny, nz, halo, rows, y0
        self.factor = 0.25**depth
        self.unroll = unroll
        self.total = 2 * GUARD + (nx + 2 * halo) * rows

    def row(self, x, y):
        return GUARD + (self.halo + x) * self.R + self.y0 + y


L0 = Geo(24, 48, 48, 4, 56, 4, 0, 28)
L1 = Geo(12, 24, 24, 6, 40, 8, 1, 24)
L2 = Geo(6, 12, 12, 5, 24, 6, 2, 16)
FACTOR3 = 0.25**3
FACTOR4 = 0.25**4


def lanes(rows):
    return lax.broadcasted_iota(jnp.int32, (rows, 128), 1)


def iota2(shape, dim):
    return lax.broadcasted_iota(jnp.int32, shape, dim)


def tree(terms):
    while len(terms) > 1:
        terms = [sum(terms[k + 1 : k + 2], terms[k]) for k in range(0, len(terms), 2)]
    return terms[0]


def roll(v, shift):
    shift = shift % 128
    return v if shift == 0 else pltpu.roll(v, shift, 1)


def split(a):
    hi = a.astype(BF16)
    return hi, (a - hi.astype(F32)).astype(BF16)


def mm(a, b):
    hi, low = split(a)
    return jnp.dot(hi, b, preferred_element_type=F32) + jnp.dot(low, b, preferred_element_type=F32)


def beside_of(ref, r, R):
    c = ref[pl.ds(r, R), :]
    b = ref[pl.ds(r + R, R), :] + ref[pl.ds(r - R, R), :]
    b = b + (ref[pl.ds(r + 1, R), :] + ref[pl.ds(r - 1, R), :])
    b = b + (roll(c, 1) + roll(c, -1))
    return c, b


def image_of(ref, s_ref, g, r):
    c, b = beside_of(ref, r, g.R)
    return c, g.factor * (6.0 * c - b) + s_ref[pl.ds(r, g.R), :] * c


def planes(g, a, b, body):
    unroll = g.unroll

    def group(start, count):
        todo = []
        for k in range(count):
            r = start + k * g.R
            r = r if isinstance(r, int) else pl.multiple_of(r, 8)
            todo.append((r, body(r)))
        for r, pairs in todo:
            for ref, value in pairs:
                ref[pl.ds(r, g.R), :] = value

    trips = (b - a) // unroll
    origin = GUARD + (g.halo + a) * g.R
    if trips == 1:
        group(origin, unroll)
    elif trips:

        def step(i, carry):
            group(pl.multiple_of(origin + i * (unroll * g.R), 8), unroll)
            return carry

        lax.fori_loop(0, trips, step, 0)
    if (b - a) % unroll:
        group(origin + trips * unroll * g.R, (b - a) % unroll)


def inverse(s, factor):
    return jnp.where(s > 0.0, DAMP / (6.0 * factor + s), 0.0)


def relax(g, src, dst, f, s, inv, a, b):
    def body(r):
        c, image = image_of(src, s, g, r)
        at = pl.ds(r, g.R)
        return [(dst, c + inv[at, :] * (f[at, :] - image))]

    planes(g, a, b, body)


def first(g, dst, f, inv, a, b):
    def body(r):
        at = pl.ds(r, g.R)
        return [(dst, inv[at, :] * f[at, :])]

    planes(g, a, b, body)


def leftover(g, src, dst, f, s, a, b):
    def body(r):
        c, image = image_of(src, s, g, r)
        return [(dst, f[pl.ds(r, g.R), :] - image)]

    planes(g, a, b, body)


def restrict(src, gs, dst, gd, x0, x1, y0, count, matrix, tmp):
    step = -(-count // 8) * 8
    for x in range(x0, x1):
        r = gs.row(2 * x, 2 * y0)
        t = src[pl.ds(r, count, stride=2), :] + src[pl.ds(r + 1, count, stride=2), :]
        r = r + gs.R
        t = t + (src[pl.ds(r, count, stride=2), :] + src[pl.ds(r + 1, count, stride=2), :])
        tmp[pl.ds((x - x0) * step, count), :] = t
    for x in range(x0, x1):
        out = mm(tmp[pl.ds((x - x0) * step, step), :], matrix[...])
        dst[pl.ds(gd.row(x, y0), count), :] = out[0:count]


def prolong(src, gc, dst, gf, x0, x1, y0, count, matrix, tmp):
    for x in range(x0, x1):
        o = (x - x0) * 56
        u = mm(src[pl.ds(gc.row(x, y0), count), :], matrix[...])
        tmp[pl.ds(o, count, stride=2), :] = u
        tmp[pl.ds(o + 1, count, stride=2), :] = u
    for x in range(x0, x1):
        o = (x - x0) * 56
        v = tmp[pl.ds(o, 2 * count), :]
        for k in range(2):
            at = pl.ds(gf.row(2 * x + k, 2 * y0), 2 * count)
            dst[at, :] = dst[at, :] + v


class Item:
    def __init__(self, geo, w):
        self.g, self.w = geo, w


class Plan:
    def __init__(self, items):
        self.items = items
        self.yrows = sum(it.g.nx * it.w for it in items)
        self.yrows = -(-self.yrows // 8) * 8
        self.tiles = []
        for k, it in enumerate(items):
            for x in range(it.g.nx):
                for t in self.tiles:
                    if t[0] is it.g and t[1] + it.w <= 64:
                        break
                else:
                    t = [it.g, 0, []]
                    self.tiles.append(t)
                t[2].append((k, x, t[1]))
                t[1] += it.w
        self.zrows = sum(t[0].ny for t in self.tiles)
        self.zrows = -(-self.zrows // 8) * 8
        self.drows = max(it.g.nx for it in items)
        self.drows = -(-self.drows // 8) * 8
        assert sum(it.w * it.w for it in items) <= 64

        self.z0 = [0, self.zrows]
        self.d0 = [2 * self.zrows + q * self.drows for q in range(4)]
        self.y0 = [2 * self.zrows + 4 * self.drows + q * self.yrows for q in range(2)]
        self.total = 2 * (self.zrows + self.yrows) + 4 * self.drows
        self.xtotal = sum(it.w * it.g.R for it in items)

    def scratch(self):
        return [
            pltpu.VMEM((self.xtotal, 128), F32),
            pltpu.VMEM((self.total, 128), F32),
            pltpu.VMEM((self.total, 128), F32),
            pltpu.SemaphoreType.DMA((2,)),
            pltpu.SemaphoreType.DMA((2,)),
        ]


class Exchange:
    def __init__(self, plan, refs, scratch, place):
        self.plan, self.refs, self.place = plan, refs, place
        self.xr, self.sent, self.got, self.ss, self.rs = scratch
        gx, gy, gz = place.me
        self.partner = (1 - gx, gy, gz)
        self.x_copies = []
        o = 0
        for k, it in enumerate(plan.items):
            g = it.g
            start = jnp.where(gx == 0, g.nx - it.w, 0)
            r = pl.multiple_of(GUARD + (g.halo + start) * g.R, 8)
            n = it.w * g.R
            self.x_copies.append(self.copy(refs[k].at[pl.ds(r, n), :], self.xr.at[pl.ds(o, n), :], 0, self.partner))
            o += n
        at = {}
        for d in range(2):
            at[1 - 2 * d, 0] = plan.y0[d]
            at[0, 1 - 2 * d] = plan.z0[d]
            for e in range(2):
                at[1 - 2 * d, 1 - 2 * e] = plan.d0[2 * d + e]
        self.y_copies, self.z_copies, self.d_copies = [], [], []
        for d in (1, -1):
            self.y_copies.append(self.segment(at, d, 0, plan.yrows))
            self.z_copies.append(self.segment(at, 0, d, plan.zrows))
            for e in (1, -1):
                self.d_copies.append(self.segment(at, d, e, plan.drows))

    def segment(self, at, dy, dz, n):
        there = self.place.exists(dy, dz)
        peer = self.place.beside(0, dy, dz)
        peer = tuple(jnp.where(there, p, q) for p, q in zip(peer, self.partner))
        target = pl.multiple_of(jnp.where(there, at[dy, dz], at[-dy, -dz]), 8)
        return self.copy(self.sent.at[pl.ds(at[dy, dz], n), :], self.got.at[pl.ds(target, n), :], 1, peer)

    def copy(self, src, dst, k, peer):
        return pltpu.make_async_remote_copy(
            src_ref=src, dst_ref=dst, send_sem=self.ss.at[k], recv_sem=self.rs.at[k],
            device_id=peer, device_id_type=MESH,
        )

    def x_send(self):
        for c in self.x_copies:
            c.start()

    def settle(self):
        self.copy(self.xr, self.xr, 0, self.partner).wait_send()
        self.copy(self.sent, self.got, 1, self.partner).wait_send()

    def x_fill(self):
        self.copy(self.xr, self.xr, 0, self.partner).wait_recv()
        m0, m1 = self.place.x_masks
        o = 0
        for k, it in enumerate(self.plan.items):
            g, w, ref = it.g, it.w, self.refs[k]
            upper = ((lanes(g.R) + 8) & 127) >= 64
            for j in range(w):
                got = self.xr[pl.ds(o + j * g.R, g.R), :]
                top = ref[pl.ds(GUARD + (g.halo + g.nx - w + j) * g.R, g.R), :]
                low = ref[pl.ds(GUARD + (g.halo + j) * g.R, g.R), :]
                ref[pl.ds(GUARD + (g.halo - w + j) * g.R, g.R), :] = roll(jnp.where(upper, got * m1, top), 64)
                ref[pl.ds(GUARD + (g.halo + g.nx + j) * g.R, g.R), :] = roll(jnp.where(upper, low, got * m0), 64)
            o += w * g.R

    def pack_send(self):
        self.pack_sides()
        for c in self.d_copies:
            c.start()
        self.pack_z()
        for c in self.z_copies + self.y_copies:
            c.start()

    def pack(self):
        self.pack_sides()
        self.pack_z()

    def send(self):
        for c in self.d_copies + self.z_copies + self.y_copies:
            c.start()

    def pack_z(self):
        zo = 0
        for g, _, slots in self.plan.tiles:
            lane = lanes(g.ny)
            acc = [None, None]
            for k, x, at in slots:
                w = self.plan.items[k].w
                moved = roll(self.refs[k][pl.ds(g.row(x, 0), g.ny), :], at)
                for q, past in enumerate((g.nz - self.plan.items[k].w, 0)):
                    here = ((lane - past) & 63 >= at) & ((lane - past) & 63 < at + w)
                    acc[q] = moved if acc[q] is None else jnp.where(here, moved, acc[q])
            for q in range(2):
                self.sent[pl.ds(self.plan.z0[q] + zo, g.ny), :] = acc[q]
            zo += g.ny

    def pack_sides(self):
        yo, co = 0, 0
        corner = [None] * 4
        for k, it in enumerate(self.plan.items):
            g, w, ref = it.g, it.w, self.refs[k]
            n = g.nx
            lane = lanes(self.plan.drows) & 63
            for d in range(1, w + 1):
                at = co + (d - 1) * w
                for e, y in enumerate((g.ny - d, d - 1)):
                    v = ref[pl.ds(g.row(0, y), n, stride=g.R), :]
                    self.sent[pl.ds(self.plan.y0[e] + yo, n), :] = v
                    if n < self.plan.drows:
                        v = jnp.concatenate([v, jnp.zeros((self.plan.drows - n, 128), F32)], axis=0)
                    for q, z in enumerate((g.nz - w, 0)):
                        moved = roll(v, at - z)
                        old = corner[2 * e + q]
                        corner[2 * e + q] = moved if old is None else jnp.where(lane >= at, moved, old)
                yo += n
            co += w * w
        for q in range(4):
            self.sent[pl.ds(self.plan.d0[q], self.plan.drows), :] = corner[q]

    def unpack(self):
        my, mz = self.place.y_masks, self.place.z_masks
        self.copy(self.sent, self.got, 1, self.partner).wait_recv()
        yo, co = 0, 0
        for k, it in enumerate(self.plan.items):
            g, w, ref = it.g, it.w, self.refs[k]
            n = g.nx
            lane = lanes(n) & 63
            into = (lane >= 64 - w, (lane >= g.nz) & (lane < g.nz + w))
            for d in range(1, w + 1):
                at = co + (d - 1) * w
                for e, y in enumerate((-d, g.ny + d - 1)):
                    v = self.got[pl.ds(self.plan.y0[e] + yo, n), :]
                    for q, z in enumerate((-w, g.nz)):
                        got = self.got[pl.ds(self.plan.d0[2 * e + q], n), :] * mz[q]
                        v = jnp.where(into[q], roll(got, z - at), v)
                    ref[pl.ds(g.row(0, y), n, stride=g.R), :] = v * my[e]
                yo += n
            co += w * w
        self.unpack_z(True)

    def unpack_rest(self):
        self.unpack_z(False)

    def unpack_z(self, edge):
        mz = self.place.z_masks
        zo = 0
        for g, _, slots in self.plan.tiles:
            lane = lanes(g.ny) & 63
            got = [self.got[pl.ds(self.plan.z0[q] + zo, g.ny), :] * mz[q] for q in range(2)]
            for k, x, at in slots:
                w = self.plan.items[k].w
                if (x < w or x >= g.nx - w) != edge:
                    continue
                rows = pl.ds(g.row(x, 0), g.ny)
                v = self.refs[k][rows, :]
                v = jnp.where(lane >= 64 - w, roll(got[0], -g.nz - at), v)
                v = jnp.where((lane >= g.nz) & (lane < g.nz + w), roll(got[1], g.nz - at), v)
                self.refs[k][rows, :] = v
            zo += g.ny


class Place:
    def __init__(self, sizes):
        self.sizes = sizes
        self.me = tuple(lax.axis_index(a) for a in ("gx", "gy", "gz"))
        gx, gy, gz = self.me
        one = lambda c: jnp.where(c, 1.0, 0.0).astype(F32)
        self.x_masks = (one(gx == 0), one(gx == 1))
        self.y_masks = (one(gy > 0), one(gy < sizes[1] - 1))
        self.z_masks = (one(gz > 0), one(gz < sizes[2] - 1))

    def exists(self, dy, dz):
        gx, gy, gz = self.me
        y, z = gy + dy, gz + dz
        return (y >= 0) & (y < self.sizes[1]) & (z >= 0) & (z < self.sizes[2])

    def beside(self, dx, dy, dz):
        return tuple(
            lax.rem(m + d % n, n) if d % n else m for m, d, n in zip(self.me, (dx, dy, dz), self.sizes)
        )


class Gather:
    rows = 24

    def __init__(self, place, scratch, whole):
        self.place, self.whole = place, whole
        self.mine, self.got, self.sum, self.ss, self.rs = scratch
        n = place.sizes
        self.near = [(a, b) for a in range(n[0]) for b in range(n[1])][1:]
        self.near.sort(key=lambda p: -far((p[0], p[1], 0), n))
        self.line = sorted(range(1, n[2]), key=lambda c: -far((0, 0, c), n))
        self.at = pl.ds(pl.multiple_of(GUARD3 + self.rows * place.me[2], 8), self.rows)

    def copy(self, src, dst, k, peer):
        return pltpu.make_async_remote_copy(
            src_ref=src, dst_ref=dst, send_sem=self.ss.at[k], recv_sem=self.rs.at[k],
            device_id=peer, device_id_type=MESH,
        )

    def send(self):
        for k, (a, b) in enumerate(self.near):
            self.copy(self.mine, self.got.at[k], 0, self.place.beside(a, b, 0)).start()

    def relay(self):
        self.copy(self.got, self.got, 0, self.place.beside(1, 0, 0)).wait_recv()
        total = self.mine[...]
        for k in range(len(self.near)):
            total = total + self.got[k]
        self.sum[...] = total
        for c in self.line:
            self.copy(self.sum, self.whole.at[self.at, :], 1, self.place.beside(0, 0, c)).start()
        self.whole[self.at, :] = total

    def finish(self):
        self.most().wait_recv()

    def most(self):
        most = self.whole.at[pl.ds(GUARD3, self.rows * (self.place.sizes[2] - 1)), :]
        return self.copy(most, most, 1, self.place.beside(1, 0, 0))

    def settle(self):
        self.copy(self.got, self.got, 0, self.place.beside(1, 0, 0)).wait_send()
        self.most().wait_send()


def gather_scratch(sizes):
    return [
        pltpu.VMEM((24, 128), F32),
        pltpu.VMEM((sizes[0] * sizes[1] - 1, 24, 128), F32),
        pltpu.VMEM((24, 128), F32),
        pltpu.SemaphoreType.DMA((2,)),
        pltpu.SemaphoreType.DMA((2,)),
    ]


def to_level3(src, mine, square, turned, place):
    g = L2
    gx, gy, gz = place.me
    for i in range(3):
        r = g.row(2 * i, 0)
        t = src[pl.ds(r, 6, stride=2), :] + src[pl.ds(r + 1, 6, stride=2), :]
        r = r + g.R
        t = t + (src[pl.ds(r, 6, stride=2), :] + src[pl.ds(r + 1, 6, stride=2), :])
        square[pl.ds(8 * i, 6), :] = t
    turned[...] = jnp.transpose(square[...])
    a = turned[pl.ds(0, 8, stride=2), :] + turned[pl.ds(1, 8, stride=2), :]
    b = turned[pl.ds(64, 8, stride=2), :] + turned[pl.ds(65, 8, stride=2), :]
    a = (a + roll(b, 64)) * 0.125
    r = iota2((128, 384), 0)
    l = iota2((128, 384), 1)
    x = 6 * gx + 3 * (r >> 6) + ((r & 63) >> 3)
    y = 6 * gy + (r & 7)
    hit = (x == (l >> 5)) & (y == (l & 31)) & ((r & 7) < 6) & ((r & 63) < 24)
    out = mm(a, jnp.where(hit, 1.0, 0.0).astype(BF16))
    for k in range(3):
        mine[pl.ds(k, 6, stride=4), :] = out[0:6, 128 * k : 128 * k + 128]


def image3(ref, s_ref, r, n):
    lane = lanes(n)
    c = ref[pl.ds(r, n), :]
    b = ref[pl.ds(r + 4, n), :] + ref[pl.ds(r - 4, n), :]
    b = b + (roll(c, 1) + roll(c, -1))
    b = b + roll(jnp.where(lane < 32, ref[pl.ds(r + 1, n), :], c), -32)
    b = b + roll(jnp.where(lane >= 96, ref[pl.ds(r - 1, n), :], c), 32)
    return c, FACTOR3 * (6.0 * c - b) + s_ref[pl.ds(r, n), :] * c


def chunks3(rows, ref, body):
    n = min(rows, 384)

    def step(i, carry):
        r = pl.multiple_of(GUARD3 + i * n, 8)
        ref[pl.ds(r, n), :] = body(r, n)
        return carry

    lax.fori_loop(0, rows // n, step, 0)


def match4(k, shape, coarse_dim, ny):
    c = iota2(shape, coarse_dim)
    l = iota2(shape, 1 - coarse_dim)
    return ((c >> 4) == 2 * k + (l >> 6)) & ((c & 15) == ((l & 31) >> 1)) & ((l & 31) < ny)


def restrict4(src, n, ny):
    total = None
    for k in range(3):
        t = src[pl.ds(GUARD3 + k, n, stride=8), :] + src[pl.ds(GUARD3 + k + 4, n, stride=8), :]
        part = mm(t, jnp.where(match4(k, (128, 128), 1, ny), 0.125, 0.0).astype(BF16))
        total = part if total is None else total + part
    return total


def dot_all(a, b):
    return jnp.sum(jnp.sum(a * b, axis=0, keepdims=True), axis=1, keepdims=True)


def bottom(source, s4, p4, n, ny):
    estimate = jnp.zeros_like(source)
    left = source
    inside = (lanes(n) < 96) & ((lanes(n) & 15) < ny)
    shifted = 6.0 * FACTOR4 + s4[...]
    for it in range(BOTTOM_ITERS):
        p4[pl.ds(GUARD, n), :] = left
        b = p4[pl.ds(GUARD + 1, n), :] + p4[pl.ds(GUARD - 1, n), :]
        b = b + (roll(left, 1) + roll(left, -1))
        b = b + (roll(left, 16) + roll(left, -16))
        image = shifted * left - FACTOR4 * jnp.where(inside, b, 0.0)
        now = dot_all(left, left)
        bent = dot_all(left, image)
        if it == 0:
            denom = bent
            direction, turned = left, image
        else:
            ratio = now * inv_before
            denom = bent - ratio * ratio * denom
            direction = left + ratio * direction
            turned = image + ratio * turned
        step = now / denom
        inv_before = 1.0 / now
        estimate = estimate + step * direction
        if it < BOTTOM_ITERS - 1:
            left = left - step * turned
    return estimate


PLAN_A = Plan([Item(L0, 3), Item(L0, 2), Item(L0, 2)])
PLAN_S = Plan([Item(L1, 6), Item(L2, 5)])
PLAN_B = Plan([Item(L1, 6)])
PLAN_C = Plan([Item(L0, 3)])
PLAN_D = Plan([Item(L2, 5)])
PLANS = (PLAN_A, PLAN_S, PLAN_B, PLAN_C, PLAN_D)


def far(p, sizes):
    ring = lambda d, n: min(d % n, -d % n)
    return p[0] + ring(p[1], sizes[1]) + ring(p[2], 4) + ring(p[2] // 4, 4)


def kernel(sizes, counts, right_in, guess_in, react_in, guess, r0, eb0, left0, step_out, *scratch):
    scratch = list(scratch)

    def take(n):
        out = scratch[:n]
        del scratch[:n]
        return out

    raw = take(3)
    (in_sems,) = take(1)
    right, react, inv0, ea0 = take(4)
    f1, s1, inv1, ea1, eb1, left1 = take(6)
    f2, s2, inv2, ea2, eb2, left2 = take(6)
    f3, s3, inv3, ea3, eb3, left3 = take(6)
    s4, p4, down_m, up_m, tmp, square, turned, spread, slab = take(9)
    scr = [take(n) for n in counts]
    place = Place(sizes)
    gx, gy, gz = place.me
    n3, n4, ny3 = 24 * sizes[2], 3 * sizes[2], 6 * sizes[1]

    inputs = (guess_in, right_in, react_in)
    for k in range(3):
        for q in range(4):
            at = pl.ds(12 * q, 12)
            pltpu.make_async_copy(inputs[k].at[at], raw[k].at[at], in_sems.at[k]).start()

    def clear(ref):
        n = ref.shape[0]
        size = next(k for k in (128, 122 * 8, 80, 8) if n % k == 0) if n > 128 else n
        size = {1808: 904, 976: 488, 416: 208}.get(n, size)

        def step(i, carry):
            ref[pl.ds(pl.multiple_of(i * size, 8), size), :] = jnp.zeros((size, 128), F32)
            return carry

        lax.fori_loop(0, n // size, step, 0)

    peers = [(a, b, c) for a in range(sizes[0]) for b in range(sizes[1]) for c in range(sizes[2])][1:]
    peers.sort(key=lambda p: -far(p, sizes))
    barrier = pltpu.get_barrier_semaphore()
    for p in peers:
        pl.semaphore_signal(barrier, inc=1, device_id=place.beside(*p), device_id_type=MESH)
    for ref in (guess, right, react, f1, s1, ea1, eb1, f2, s2, ea2, eb2, ea3, eb3, p4, square):
        clear(ref)
    spread[...] = jnp.zeros_like(spread)
    for ref in (f3, s3, inv3):
        for r in (0, GUARD3 + n3):
            ref[pl.ds(r, GUARD3), :] = jnp.zeros((GUARD3, 128), F32)

    a = iota2((128, 128), 0)
    b = iota2((128, 128), 1)
    signed = lambda v: ((v + 8) & 63) - 8
    base = lambda v: ((v + 8) & 127) & 64
    zb = signed(b)
    hit = ((a == ((base(b) + 2 * zb) & 127)) | (a == ((base(b) + 2 * zb + 1) & 127))) & (zb >= -8) & (zb < 24)
    down_m[...] = jnp.where(hit, 0.125, 0.0).astype(BF16)
    hit = a == ((base(b) + (zb >> 1)) & 127)
    up_m[...] = jnp.where(hit, 1.0, 0.0).astype(BF16)

    for k, dst in enumerate((guess, right, react)):
        pltpu.make_async_copy(inputs[k], raw[k], in_sems.at[k]).wait()

        for i in range(24):
            dst[pl.ds(L0.row(i, 0), 48), 0:48] = raw[k][i]
            dst[pl.ds(L0.row(i, 0), 48), 64:112] = raw[k][i + 24]

    ex_a = Exchange(PLAN_A, (guess, right, react), scr[0], place)
    ex_s = Exchange(PLAN_S, (s1, s2), scr[1], place)
    ex_b = Exchange(PLAN_B, (f1,), scr[2], place)
    ex_c = Exchange(PLAN_C, (eb0,), scr[3], place)
    ex_d = Exchange(PLAN_D, (f2,), scr[4], place)
    ga_s = Gather(place, scr[5], s3)
    ga_f = Gather(place, scr[6], f3)
    reduced, red_send, red_recv = scr[7]

    ex_a.pack()
    pl.semaphore_wait(barrier, len(peers))
    ex_a.send()

    restrict(react, L0, s1, L1, 0, 12, 0, 24, down_m, tmp)
    restrict(s1, L1, s2, L2, 0, 6, 0, 12, down_m, tmp)
    ex_s.pack_send()
    ga_s.mine[...] = jnp.zeros((24, 128), F32)
    ga_f.mine[...] = jnp.zeros((24, 128), F32)
    to_level3(s2, ga_s.mine, square, turned, place)
    ga_s.send()

    def start(r):
        at = pl.ds(r, L0.R)
        c, image = image_of(guess, react, L0, r)
        res = right[at, :] - image
        inv = inverse(react[at, :], 1.0)
        return [(r0, res), (inv0, inv), (ea0, inv * res)]

    ex_a.unpack()
    ex_a.x_send()
    ex_a.unpack_rest()
    planes(L0, 1, 23, start)
    ex_a.x_fill()
    planes(L0, -2, 1, start)
    planes(L0, 23, 26, start)
    relax(L0, ea0, eb0, r0, react, inv0, -1, 25)
    leftover(L0, eb0, left0, r0, react, 0, 24)
    restrict(left0, L0, f1, L1, 0, 12, 0, 24, down_m, tmp)
    ex_b.pack_send()

    ex_s.unpack()
    ex_s.x_send()
    ex_c.pack_send()
    ex_s.x_fill()
    for g, sh, inv in ((L1, s1, inv1), (L2, s2, inv2)):
        planes(g, -g.halo, g.nx + g.halo, lambda r: [(inv, inverse(sh[pl.ds(r, g.R), :], g.factor))])
    ga_s.relay()

    ex_b.unpack()
    ex_b.x_send()
    first(L1, ea1, f1, inv1, 0, 12)
    relax(L1, ea1, eb1, f1, s1, inv1, 1, 11)
    ex_b.x_fill()
    first(L1, ea1, f1, inv1, -6, 0)
    first(L1, ea1, f1, inv1, 12, 18)
    relax(L1, ea1, eb1, f1, s1, inv1, -5, 1)
    relax(L1, ea1, eb1, f1, s1, inv1, 11, 17)
    leftover(L1, eb1, left1, f1, s1, -4, 16)
    restrict(left1, L1, f2, L2, -2, 8, -2, 16, down_m, tmp)
    first(L2, ea2, f2, inv2, -2, 8)
    relax(L2, ea2, eb2, f2, s2, inv2, -1, 7)
    leftover(L2, eb2, left2, f2, s2, 0, 6)
    to_level3(left2, ga_f.mine, square, turned, place)
    ga_f.send()
    ex_d.pack_send()

    ex_c.unpack()
    ex_c.x_send()
    ex_c.unpack_rest()
    ga_s.finish()
    chunks3(n3, inv3, lambda r, n: inverse(s3[pl.ds(r, n), :], FACTOR3))
    s4[...] = restrict4(s3, n4, ny3)

    ga_f.relay()
    ex_d.unpack()
    ex_d.x_send()
    ex_c.x_fill()
    ex_d.x_fill()
    first(L2, ea2, f2, inv2, -5, 11)
    relax(L2, ea2, eb2, f2, s2, inv2, -4, 10)
    for e in (ex_a, ex_s, ex_b, ex_c, ex_d, ga_s):
        e.settle()
    ga_f.finish()

    def relax3(src, dst):
        def body(r, n):
            c, image = image3(src, s3, r, n)
            at = pl.ds(r, n)
            return c + inv3[at, :] * (f3[at, :] - image)

        chunks3(n3, dst, body)

    chunks3(n3, ea3, lambda r, n: inv3[pl.ds(r, n), :] * f3[pl.ds(r, n), :])
    relax3(ea3, eb3)
    chunks3(n3, left3, lambda r, n: f3[pl.ds(r, n), :] - image3(eb3, s3, r, n)[1])
    e4 = bottom(restrict4(left3, n4, ny3), s4, p4, n4, ny3 // 2)
    for k in range(3):
        u = mm(e4, jnp.where(match4(k, (128, 128), 0, ny3), 1.0, 0.0).astype(BF16))
        for q in (k, k + 4):
            at = pl.ds(GUARD3 + q, n4, stride=8)
            eb3[at, :] = eb3[at, :] + u
    for src, dst, n in ((eb3, ea3, 48), (ea3, slab, 40)):
        r = pl.multiple_of(GUARD3 + 24 * gz - (n - 24) // 2, 4)
        c, image = image3(src, s3, r, n)
        at = pl.ds(r, n)
        dst[at if n == 48 else pl.ds(0, n), :] = c + inv3[at, :] * (f3[at, :] - image)
    for k in range(3):
        v = slab[pl.ds(k, 10, stride=4), :]
        for h in range(2):
            for q in range(2):
                spread[k, pl.ds(64 * h + q, 10, stride=2), :] = v
    wide = [jnp.concatenate(p, axis=1) for p in zip(*[split(spread[k]) for k in range(3)])]
    coarse = []
    for h in range(2):
        r = iota2((112, 384), 0)
        l = iota2((112, 384), 1)
        hit = (6 * gx + 3 * h + (r >> 4) - 2 == (l >> 5)) & (6 * gy + (r & 15) - 2 == (l & 31)) & ((r & 15) < 10)
        pick = jnp.where(hit, 1.0, 0.0).astype(BF16)
        parts = [
            lax.dot_general(pick, p, (((1,), (1,)), ((), ())), preferred_element_type=F32) for p in wide
        ]
        coarse.append(parts[0] + parts[1])
    fine = roll(jnp.where(lanes(112) < 64, coarse[0], coarse[1]), -4)
    for i in range(7):
        u = fine[16 * i : 16 * i + 10]
        tmp[pl.ds(24 * i, 10, stride=2), :] = u
        tmp[pl.ds(24 * i + 1, 10, stride=2), :] = u
    for i in range(7):
        v = tmp[pl.ds(24 * i, 20), :]
        for q in range(2):
            at = pl.ds(L2.row(2 * (i - 2) + q, -4), 20)
            eb2[at, :] = eb2[at, :] + v
    relax(L2, eb2, ea2, f2, s2, inv2, -3, 9)
    relax(L2, ea2, eb2, f2, s2, inv2, -2, 8)
    prolong(eb2, L2, eb1, L1, -2, 8, -2, 16, up_m, tmp)
    relax(L1, eb1, ea1, f1, s1, inv1, -3, 15)
    relax(L1, ea1, eb1, f1, s1, inv1, -2, 14)
    prolong(eb1, L1, eb0, L0, -2, 14, -2, 28, up_m, tmp)
    relax(L0, eb0, ea0, r0, react, inv0, -2, 26)
    relax(L0, ea0, eb0, r0, react, inv0, -1, 25)

    row = iota2((L0.R, 128), 0)
    inside = ((lanes(L0.R) & 63) < 48) & (row >= L0.y0) & (row < L0.y0 + 48)

    upper, lower = [], []
    for i in range(24):
        r = GUARD + (L0.halo + i) * L0.R
        c, image = image_of(eb0, react, L0, r)
        left0[pl.ds(r, L0.R), :] = image
        upper.append(c * r0[pl.ds(r, L0.R), :])
        lower.append(c * image)
    upper = jnp.where(inside, tree(upper), 0.0)
    lower = jnp.where(inside, tree(lower), 0.0)
    upper = jnp.sum(upper, axis=0, keepdims=True)
    lower = jnp.sum(lower, axis=0, keepdims=True)
    half = lanes(1) < 64
    number = (gx * sizes[1] + gy) * sizes[2] + gz
    reduced[number] = jnp.where(half, upper + roll(upper, 64), lower + roll(lower, 64))
    own = reduced.at[number]

    def summed(src, dst, p):
        return pltpu.make_async_remote_copy(
            src_ref=src, dst_ref=dst, send_sem=red_send.at[0], recv_sem=red_recv.at[0],
            device_id=place.beside(*p), device_id_type=MESH,
        )

    for p in peers:
        summed(own, own, p).start()
    ga_f.settle()
    most = reduced.at[pl.ds(0, len(peers))]
    summed(most, most, peers[0]).wait()
    sums = [reduced[k] for k in range(8)]
    for k in range(8, len(peers) + 1):
        sums[k % 8] = sums[k % 8] + reduced[k]
    total = tree(sums)
    upper = jnp.sum(jnp.where(half, total, 0.0), axis=1, keepdims=True)
    lower = jnp.sum(jnp.where(half, 0.0, total), axis=1, keepdims=True)
    step_out[...] = jnp.broadcast_to(upper / lower, (8, 128))


def finish(guess, r0, eb0, left0, step_ref, field_out, resid_out, field, resid, sems):
    step = step_ref[0:1, :]
    copies = []
    parts, size = 4, 6
    for p in range(parts):
        for x in range(p * size, p * size + size):
            at = pl.ds(L0.row(x, 0), 48)
            v = guess[at, :] + step * eb0[at, :]
            field[x] = v[:, 0:48]
            field[x + 24] = roll(v, 64)[:, 0:48]
            v = r0[at, :] - step * left0[at, :]
            resid[x] = v[:, 0:48]
            resid[x + 24] = roll(v, 64)[:, 0:48]
        for q, (src, dst) in enumerate(((field, field_out), (resid, resid_out))):
            for h in range(2):
                at = pl.ds(p * size + 24 * h, size)
                c = pltpu.make_async_copy(src.at[at], dst.at[at], sems.at[4 * p + 2 * q + h])
                c.start()
                copies.append(c)
    for c in copies:
        c.wait()


def solution(mesh):
    sizes = tuple(mesh.shape[a] for a in ("gx", "gy", "gz"))
    n3, n4 = 24 * sizes[2] + 2 * GUARD3, 3 * sizes[2]
    scratch = [pltpu.VMEM((48, 48, 48), F32)] * 3 + [pltpu.SemaphoreType.DMA((3,))]
    scratch += [pltpu.VMEM((L0.total, 128), F32)] * 4
    scratch += [pltpu.VMEM((L1.total, 128), F32)] * 6
    scratch += [pltpu.VMEM((L2.total, 128), F32)] * 6
    scratch += [pltpu.VMEM((n3, 128), F32)] * 6
    scratch += [pltpu.VMEM((n4, 128), F32), pltpu.VMEM((n4 + 2 * GUARD, 128), F32)]
    scratch += [pltpu.VMEM((128, 128), BF16)] * 2 + [pltpu.VMEM((16 * 56, 128), F32)]
    scratch += [pltpu.VMEM((128, 128), F32)] * 2
    scratch += [pltpu.VMEM((3, 128, 128), F32), pltpu.VMEM((40, 128), F32)]
    groups = [p.scratch() for p in PLANS] + [gather_scratch(sizes)] * 2
    devices = sizes[0] * sizes[1] * sizes[2]
    groups += [[pltpu.VMEM((devices, 1, 128), F32)] + [pltpu.SemaphoreType.DMA((1,))] * 2]
    for g in groups:
        scratch += g
    counts = tuple(len(g) for g in groups)
    vmem = pl.BlockSpec(memory_space=pltpu.VMEM)

    anywhere = pl.BlockSpec(memory_space=pl.ANY)

    def body(right_side, start_guess, reaction):
        whole = pltpu.VMEM((L0.total, 128), F32)
        parts = pl.pallas_call(
            functools.partial(kernel, sizes, counts),
            out_shape=[whole] * 4 + [pltpu.VMEM((8, 128), F32)],
            in_specs=[anywhere] * 3,
            out_specs=[vmem] * 5,
            scratch_shapes=scratch,
            compiler_params=pltpu.CompilerParams(
                collective_id=0, has_side_effects=True, vmem_limit_bytes=60 * 2**20
            ),
        )(right_side, start_guess, reaction)
        shape = jax.ShapeDtypeStruct(right_side.shape, F32)
        return tuple(
            pl.pallas_call(
                finish,
                out_shape=[shape, shape],
                in_specs=[vmem] * 5,
                out_specs=[anywhere] * 2,
                scratch_shapes=[pltpu.VMEM(right_side.shape, F32)] * 2 + [pltpu.SemaphoreType.DMA((16,))],
                compiler_params=pltpu.CompilerParams(vmem_limit_bytes=16 * 2**20),
            )(*parts)
        )

    placed = P("gx", "gy", "gz")
    return jax.shard_map(
        body, mesh=mesh, in_specs=(placed,) * 3, out_specs=(placed,) * 2, check_vma=False
    )
```

```python
import functools

import jax
import jax.numpy as jnp
from jax import lax
from jax.experimental import pallas as pl
from jax.experimental.pallas import tpu as pltpu
from jax.sharding import PartitionSpec as P

MESH = pl.DeviceIdType.MESH
F32 = jnp.float32
BF16 = jnp.bfloat16
DAMP = 6.0 / 7.0
GUARD = 8
GUARD3 = 16
BOTTOM_ITERS = 6


class Geo:
    def __init__(self, nx, ny, nz, halo, rows, y0, depth, unroll):
        self.nx, self.ny, self.nz, self.halo, self.R, self.y0 = nx, ny, nz, halo, rows, y0
        self.factor = 0.25**depth
        self.unroll = unroll
        self.total = 2 * GUARD + (nx + 2 * halo) * rows

    def row(self, x, y):
        return GUARD + (self.halo + x) * self.R + self.y0 + y


L0 = Geo(24, 48, 48, 4, 56, 4, 0, 28)
L1 = Geo(12, 24, 24, 6, 40, 8, 1, 24)
L2 = Geo(6, 12, 12, 5, 24, 6, 2, 16)
FACTOR3 = 0.25**3
FACTOR4 = 0.25**4


def lanes(rows):
    return lax.broadcasted_iota(jnp.int32, (rows, 128), 1)


def iota2(shape, dim):
    return lax.broadcasted_iota(jnp.int32, shape, dim)


def tree(terms):
    while len(terms) > 1:
        terms = [sum(terms[k + 1 : k + 2], terms[k]) for k in range(0, len(terms), 2)]
    return terms[0]


def roll(v, shift):
    shift = shift % 128
    return v if shift == 0 else pltpu.roll(v, shift, 1)


def split(a):
    hi = a.astype(BF16)
    return hi, (a - hi.astype(F32)).astype(BF16)


def mm(a, b):
    hi, low = split(a)
    return jnp.dot(hi, b, preferred_element_type=F32) + jnp.dot(low, b, preferred_element_type=F32)


def beside_of(ref, r, R):
    c = ref[pl.ds(r, R), :]
    b = ref[pl.ds(r + R, R), :] + ref[pl.ds(r - R, R), :]
    b = b + (ref[pl.ds(r + 1, R), :] + ref[pl.ds(r - 1, R), :])
    b = b + (roll(c, 1) + roll(c, -1))
    return c, b


def image_of(ref, s_ref, g, r):
    c, b = beside_of(ref, r, g.R)
    return c, g.factor * (6.0 * c - b) + s_ref[pl.ds(r, g.R), :] * c


def planes(g, a, b, body):
    unroll = g.unroll

    def group(start, count):
        todo = []
        for k in range(count):
            r = start + k * g.R
            r = r if isinstance(r, int) else pl.multiple_of(r, 8)
            todo.append((r, body(r)))
        for r, pairs in todo:
            for ref, value in pairs:
                ref[pl.ds(r, g.R), :] = value

    trips = (b - a) // unroll
    origin = GUARD + (g.halo + a) * g.R
    if trips == 1:
        group(origin, unroll)
    elif trips:

        def step(i, carry):
            group(pl.multiple_of(origin + i * (unroll * g.R), 8), unroll)
            return carry

        lax.fori_loop(0, trips, step, 0)
    if (b - a) % unroll:
        group(origin + trips * unroll * g.R, (b - a) % unroll)


def inverse(s, factor):
    return jnp.where(s > 0.0, DAMP / (6.0 * factor + s), 0.0)


def relax(g, src, dst, f, s, inv, a, b):
    def body(r):
        c, image = image_of(src, s, g, r)
        at = pl.ds(r, g.R)
        return [(dst, c + inv[at, :] * (f[at, :] - image))]

    planes(g, a, b, body)


def first(g, dst, f, inv, a, b):
    def body(r):
        at = pl.ds(r, g.R)
        return [(dst, inv[at, :] * f[at, :])]

    planes(g, a, b, body)


def leftover(g, src, dst, f, s, a, b):
    def body(r):
        c, image = image_of(src, s, g, r)
        return [(dst, f[pl.ds(r, g.R), :] - image)]

    planes(g, a, b, body)


def restrict(src, gs, dst, gd, x0, x1, y0, count, matrix, tmp):
    step = -(-count // 8) * 8
    for x in range(x0, x1):
        r = gs.row(2 * x, 2 * y0)
        t = src[pl.ds(r, count, stride=2), :] + src[pl.ds(r + 1, count, stride=2), :]
        r = r + gs.R
        t = t + (src[pl.ds(r, count, stride=2), :] + src[pl.ds(r + 1, count, stride=2), :])
        tmp[pl.ds((x - x0) * step, count), :] = t
    for x in range(x0, x1):
        out = mm(tmp[pl.ds((x - x0) * step, step), :], matrix[...])
        dst[pl.ds(gd.row(x, y0), count), :] = out[0:count]


def prolong(src, gc, dst, gf, x0, x1, y0, count, matrix, tmp):
    for x in range(x0, x1):
        o = (x - x0) * 56
        u = mm(src[pl.ds(gc.row(x, y0), count), :], matrix[...])
        tmp[pl.ds(o, count, stride=2), :] = u
        tmp[pl.ds(o + 1, count, stride=2), :] = u
    for x in range(x0, x1):
        o = (x - x0) * 56
        v = tmp[pl.ds(o, 2 * count), :]
        for k in range(2):
            at = pl.ds(gf.row(2 * x + k, 2 * y0), 2 * count)
            dst[at, :] = dst[at, :] + v


class Item:
    def __init__(self, geo, w):
        self.g, self.w = geo, w


class Plan:
    def __init__(self, items, cross=False):
        self.items, self.cross = items, cross
        self.counts = [it.w if cross else it.g.nx for it in items]
        self.yrows = sum(n * it.w for n, it in zip(self.counts, items))
        self.yrows = -(-self.yrows // 8) * 8
        self.tiles = []
        for k, it in enumerate(items):
            for x in range(self.counts[k]):
                for t in self.tiles:
                    if t[0] is it.g and t[1] + it.w <= 64:
                        break
                else:
                    t = [it.g, 0, []]
                    self.tiles.append(t)
                t[2].append((k, x, t[1]))
                t[1] += it.w
        self.zrows = sum(t[0].ny for t in self.tiles)
        self.zrows = -(-self.zrows // 8) * 8
        self.drows = max(self.counts)
        self.drows = -(-self.drows // 8) * 8
        assert sum(it.w * it.w for it in items) <= 64

        self.z0 = [0, self.zrows]
        self.d0 = [2 * self.zrows + q * self.drows for q in range(4)]
        self.y0 = [2 * self.zrows + 4 * self.drows + q * self.yrows for q in range(2)]
        self.total = 2 * (self.zrows + self.yrows) + 4 * self.drows
        self.xtotal = sum(it.w * it.g.R for it in items)

    def scratch(self):
        x = [] if self.cross else [pltpu.VMEM((self.xtotal, 128), F32)]
        return x + [
            pltpu.VMEM((self.total, 128), F32),
            pltpu.VMEM((self.total, 128), F32),
            pltpu.SemaphoreType.DMA((2,)),
            pltpu.SemaphoreType.DMA((2,)),
        ]


class Exchange:
    def __init__(self, plan, refs, scratch, place):
        self.plan, self.refs, self.place = plan, refs, place
        self.xr, self.sent, self.got, self.ss, self.rs = scratch
        gx, gy, gz = place.me
        self.partner = (1 - gx, gy, gz)
        self.x_copies = []
        o = 0
        for k, it in enumerate(plan.items):
            r = pl.multiple_of(GUARD + (it.g.halo + self.edge(it)) * it.g.R, 8)
            n = it.w * it.g.R
            self.x_copies.append(self.copy(refs[k].at[pl.ds(r, n), :], self.xr.at[pl.ds(o, n), :], 0, self.partner))
            o += n
        self.segments(0)

    def edge(self, it):
        return jnp.where(self.place.me[0] == 0, it.g.nx - it.w, 0)

    def source(self, k, x, y):
        return self.plan.items[k].g.row(x, y)

    def target(self, k, x, y):
        return self.refs[k], self.plan.items[k].g.row(x, y)

    def segments(self, dx):
        plan = self.plan
        at = {}
        for d in range(2):
            at[1 - 2 * d, 0] = plan.y0[d]
            at[0, 1 - 2 * d] = plan.z0[d]
            for e in range(2):
                at[1 - 2 * d, 1 - 2 * e] = plan.d0[2 * d + e]
        self.y_copies, self.z_copies, self.d_copies = [], [], []
        for d in (1, -1):
            self.y_copies.append(self.segment(at, dx, d, 0, plan.yrows))
            self.z_copies.append(self.segment(at, dx, 0, d, plan.zrows))
            for e in (1, -1):
                self.d_copies.append(self.segment(at, dx, d, e, plan.drows))

    def segment(self, at, dx, dy, dz, n):
        there = self.place.exists(dy, dz)
        peer = self.place.beside(dx, dy, dz)
        peer = tuple(jnp.where(there, p, q) for p, q in zip(peer, self.partner))
        target = pl.multiple_of(jnp.where(there, at[dy, dz], at[-dy, -dz]), 8)
        return self.copy(self.sent.at[pl.ds(at[dy, dz], n), :], self.got.at[pl.ds(target, n), :], 1, peer)

    def copy(self, src, dst, k, peer):
        return pltpu.make_async_remote_copy(
            src_ref=src, dst_ref=dst, send_sem=self.ss.at[k], recv_sem=self.rs.at[k],
            device_id=peer, device_id_type=MESH,
        )

    def x_send(self):
        for c in self.x_copies:
            c.start()

    def settle(self, x=True):
        if x:
            self.x_sent()
        self.copy(self.sent, self.got, 1, self.partner).wait_send()

    def x_sent(self):
        self.copy(self.xr, self.xr, 0, self.partner).wait_send()

    def x_wait(self):
        self.copy(self.xr, self.xr, 0, self.partner).wait_recv()

    def x_fill(self):
        m0, m1 = self.place.x_masks
        o = 0
        for k, it in enumerate(self.plan.items):
            g, w, ref = it.g, it.w, self.refs[k]
            upper = ((lanes(g.R) + 8) & 127) >= 64
            for j in range(w):
                got = self.xr[pl.ds(o + j * g.R, g.R), :]
                top = ref[pl.ds(GUARD + (g.halo + g.nx - w + j) * g.R, g.R), :]
                low = ref[pl.ds(GUARD + (g.halo + j) * g.R, g.R), :]
                ref[pl.ds(GUARD + (g.halo - w + j) * g.R, g.R), :] = roll(jnp.where(upper, got * m1, top), 64)
                ref[pl.ds(GUARD + (g.halo + g.nx + j) * g.R, g.R), :] = roll(jnp.where(upper, low, got * m0), 64)
            o += w * g.R

    def pack_send(self):
        self.pack_sides()
        for c in self.d_copies:
            c.start()
        self.pack_z()
        for c in self.z_copies + self.y_copies:
            c.start()

    def pack(self):
        self.pack_sides()
        self.pack_z()

    def send(self):
        for c in self.d_copies + self.z_copies + self.y_copies:
            c.start()

    def pack_z(self):
        zo = 0
        for g, _, slots in self.plan.tiles:
            lane = lanes(g.ny)
            acc = [None, None]
            for k, x, at in slots:
                w = self.plan.items[k].w
                moved = roll(self.refs[k][pl.ds(self.source(k, x, 0), g.ny), :], at)
                for q, past in enumerate((g.nz - self.plan.items[k].w, 0)):
                    here = ((lane - past) & 63 >= at) & ((lane - past) & 63 < at + w)
                    acc[q] = moved if acc[q] is None else jnp.where(here, moved, acc[q])
            for q in range(2):
                self.sent[pl.ds(self.plan.z0[q] + zo, g.ny), :] = acc[q]
            zo += g.ny

    def pack_sides(self):
        yo, co = 0, 0
        corner = [None] * 4
        for k, it in enumerate(self.plan.items):
            g, w, ref = it.g, it.w, self.refs[k]
            n = self.plan.counts[k]
            lane = lanes(self.plan.drows) & 63
            for d in range(1, w + 1):
                at = co + (d - 1) * w
                for e, y in enumerate((g.ny - d, d - 1)):
                    v = ref[pl.ds(self.source(k, 0, y), n, stride=g.R), :]
                    self.sent[pl.ds(self.plan.y0[e] + yo, n), :] = v
                    if n < self.plan.drows:
                        v = jnp.concatenate([v, jnp.zeros((self.plan.drows - n, 128), F32)], axis=0)
                    for q, z in enumerate((g.nz - w, 0)):
                        moved = roll(v, at - z)
                        old = corner[2 * e + q]
                        corner[2 * e + q] = moved if old is None else jnp.where(lane >= at, moved, old)
                yo += n
            co += w * w
        for q in range(4):
            self.sent[pl.ds(self.plan.d0[q], self.plan.drows), :] = corner[q]

    def unpack(self):
        my, mz = self.place.y_masks, self.place.z_masks
        self.copy(self.sent, self.got, 1, self.partner).wait_recv()
        yo, co = 0, 0
        for k, it in enumerate(self.plan.items):
            g, w = it.g, it.w
            n = self.plan.counts[k]
            lane = lanes(n) & 63
            into = (lane >= 64 - w, (lane >= g.nz) & (lane < g.nz + w))
            for d in range(1, w + 1):
                at = co + (d - 1) * w
                for e, y in enumerate((-d, g.ny + d - 1)):
                    v = self.got[pl.ds(self.plan.y0[e] + yo, n), :]
                    for q, z in enumerate((-w, g.nz)):
                        got = self.got[pl.ds(self.plan.d0[2 * e + q], n), :] * mz[q]
                        v = jnp.where(into[q], roll(got, z - at), v)
                    ref, r = self.target(k, 0, y)
                    ref[pl.ds(r, n, stride=g.R), :] = v * my[e]
                yo += n
            co += w * w
        self.unpack_z(True)

    def unpack_rest(self):
        self.unpack_z(False)

    def unpack_z(self, edge):
        mz = self.place.z_masks
        zo = 0
        for g, _, slots in self.plan.tiles:
            lane = lanes(g.ny) & 63
            got = [self.got[pl.ds(self.plan.z0[q] + zo, g.ny), :] * mz[q] for q in range(2)]
            for k, x, at in slots:
                w = self.plan.items[k].w
                if (x < w or x >= g.nx - w) != edge:
                    continue
                ref, r = self.target(k, x, 0)
                rows = pl.ds(r, g.ny)
                v = ref[rows, :]
                v = jnp.where(lane >= 64 - w, roll(got[0], -g.nz - at), v)
                v = jnp.where((lane >= g.nz) & (lane < g.nz + w), roll(got[1], g.nz - at), v)
                ref[rows, :] = v
            zo += g.ny


class Cross(Exchange):
    def __init__(self, plan, main, scratch, place):
        self.plan, self.main, self.refs, self.place = plan, main, main.refs, place
        self.sent, self.got, self.ss, self.rs = scratch
        self.partner = main.partner
        self.segments(1)

    def source(self, k, x, y):
        it = self.plan.items[k]
        return GUARD + (it.g.halo + self.edge(it) + x) * it.g.R + it.g.y0 + y

    def target(self, k, x, y):
        o = sum(it.w * it.g.R for it in self.plan.items[:k])
        g = self.plan.items[k].g
        return self.main.xr, o + x * g.R + g.y0 + y


class Place:
    def __init__(self, sizes):
        self.sizes = sizes
        self.me = tuple(lax.axis_index(a) for a in ("gx", "gy", "gz"))
        gx, gy, gz = self.me
        one = lambda c: jnp.where(c, 1.0, 0.0).astype(F32)
        self.x_masks = (one(gx == 0), one(gx == 1))
        self.y_masks = (one(gy > 0), one(gy < sizes[1] - 1))
        self.z_masks = (one(gz > 0), one(gz < sizes[2] - 1))

    def exists(self, dy, dz):
        gx, gy, gz = self.me
        y, z = gy + dy, gz + dz
        return (y >= 0) & (y < self.sizes[1]) & (z >= 0) & (z < self.sizes[2])

    def beside(self, dx, dy, dz):
        return tuple(
            lax.rem(m + d % n, n) if d % n else m for m, d, n in zip(self.me, (dx, dy, dz), self.sizes)
        )


class Gather:
    rows = 24

    def __init__(self, place, scratch, whole):
        self.place, self.whole = place, whole
        self.mine, self.got, self.sum, self.ss, self.rs = scratch
        n = place.sizes
        self.near = [(a, b) for a in range(n[0]) for b in range(n[1])][1:]
        self.near.sort(key=lambda p: -far((p[0], p[1], 0), n))
        self.line = sorted(range(1, n[2]), key=lambda c: -far((0, 0, c), n))
        self.at = pl.ds(pl.multiple_of(GUARD3 + self.rows * place.me[2], 8), self.rows)

    def copy(self, src, dst, k, peer):
        return pltpu.make_async_remote_copy(
            src_ref=src, dst_ref=dst, send_sem=self.ss.at[k], recv_sem=self.rs.at[k],
            device_id=peer, device_id_type=MESH,
        )

    def send(self):
        for k, (a, b) in enumerate(self.near):
            self.copy(self.mine, self.got.at[k], 0, self.place.beside(a, b, 0)).start()

    def relay(self):
        self.copy(self.got, self.got, 0, self.place.beside(1, 0, 0)).wait_recv()
        total = self.mine[...]
        for k in range(len(self.near)):
            total = total + self.got[k]
        self.sum[...] = total
        for c in self.line:
            self.copy(self.sum, self.whole.at[self.at, :], 1, self.place.beside(0, 0, c)).start()
        self.whole[self.at, :] = total

    def finish(self):
        self.most().wait_recv()

    def most(self):
        most = self.whole.at[pl.ds(GUARD3, self.rows * (self.place.sizes[2] - 1)), :]
        return self.copy(most, most, 1, self.place.beside(1, 0, 0))

    def settle(self):
        self.copy(self.got, self.got, 0, self.place.beside(1, 0, 0)).wait_send()
        self.most().wait_send()


def gather_scratch(sizes):
    return [
        pltpu.VMEM((24, 128), F32),
        pltpu.VMEM((sizes[0] * sizes[1] - 1, 24, 128), F32),
        pltpu.VMEM((24, 128), F32),
        pltpu.SemaphoreType.DMA((2,)),
        pltpu.SemaphoreType.DMA((2,)),
    ]


def to_level3(src, mine, square, turned, place):
    g = L2
    gx, gy, gz = place.me
    for i in range(3):
        r = g.row(2 * i, 0)
        t = src[pl.ds(r, 6, stride=2), :] + src[pl.ds(r + 1, 6, stride=2), :]
        r = r + g.R
        t = t + (src[pl.ds(r, 6, stride=2), :] + src[pl.ds(r + 1, 6, stride=2), :])
        square[pl.ds(8 * i, 6), :] = t
    turned[...] = jnp.transpose(square[...])
    a = turned[pl.ds(0, 8, stride=2), :] + turned[pl.ds(1, 8, stride=2), :]
    b = turned[pl.ds(64, 8, stride=2), :] + turned[pl.ds(65, 8, stride=2), :]
    a = (a + roll(b, 64)) * 0.125
    r = iota2((128, 384), 0)
    l = iota2((128, 384), 1)
    x = 6 * gx + 3 * (r >> 6) + ((r & 63) >> 3)
    y = 6 * gy + (r & 7)
    hit = (x == (l >> 5)) & (y == (l & 31)) & ((r & 7) < 6) & ((r & 63) < 24)
    out = mm(a, jnp.where(hit, 1.0, 0.0).astype(BF16))
    for k in range(3):
        mine[pl.ds(k, 6, stride=4), :] = out[0:6, 128 * k : 128 * k + 128]


def image3(ref, s_ref, r, n):
    lane = lanes(n)
    c = ref[pl.ds(r, n), :]
    b = ref[pl.ds(r + 4, n), :] + ref[pl.ds(r - 4, n), :]
    b = b + (roll(c, 1) + roll(c, -1))
    b = b + roll(jnp.where(lane < 32, ref[pl.ds(r + 1, n), :], c), -32)
    b = b + roll(jnp.where(lane >= 96, ref[pl.ds(r - 1, n), :], c), 32)
    return c, FACTOR3 * (6.0 * c - b) + s_ref[pl.ds(r, n), :] * c


def chunks3(rows, ref, body):
    n = min(rows, 384)

    def step(i, carry):
        r = pl.multiple_of(GUARD3 + i * n, 8)
        ref[pl.ds(r, n), :] = body(r, n)
        return carry

    lax.fori_loop(0, rows // n, step, 0)


def match4(k, shape, coarse_dim, ny):
    c = iota2(shape, coarse_dim)
    l = iota2(shape, 1 - coarse_dim)
    return ((c >> 4) == 2 * k + (l >> 6)) & ((c & 15) == ((l & 31) >> 1)) & ((l & 31) < ny)


def restrict4(src, n, ny):
    total = None
    for k in range(3):
        t = src[pl.ds(GUARD3 + k, n, stride=8), :] + src[pl.ds(GUARD3 + k + 4, n, stride=8), :]
        part = mm(t, jnp.where(match4(k, (128, 128), 1, ny), 0.125, 0.0).astype(BF16))
        total = part if total is None else total + part
    return total


def dot_all(a, b):
    return jnp.sum(jnp.sum(a * b, axis=0, keepdims=True), axis=1, keepdims=True)


def bottom(source, s4, p4, n, ny):
    estimate = jnp.zeros_like(source)
    left = source
    inside = (lanes(n) < 96) & ((lanes(n) & 15) < ny)
    shifted = 6.0 * FACTOR4 + s4[...]
    for it in range(BOTTOM_ITERS):
        p4[pl.ds(GUARD, n), :] = left
        b = p4[pl.ds(GUARD + 1, n), :] + p4[pl.ds(GUARD - 1, n), :]
        b = b + (roll(left, 1) + roll(left, -1))
        b = b + (roll(left, 16) + roll(left, -16))
        image = shifted * left - FACTOR4 * jnp.where(inside, b, 0.0)
        now = dot_all(left, left)
        bent = dot_all(left, image)
        if it == 0:
            denom = bent
            direction, turned = left, image
        else:
            ratio = now * inv_before
            denom = bent - ratio * ratio * denom
            direction = left + ratio * direction
            turned = image + ratio * turned
        step = now / denom
        inv_before = 1.0 / now
        estimate = estimate + step * direction
        if it < BOTTOM_ITERS - 1:
            left = left - step * turned
    return estimate


PLAN_A = Plan([Item(L0, 3), Item(L0, 2), Item(L0, 2)])
PLAN_S = Plan([Item(L1, 6), Item(L2, 5)])
PLAN_B = Plan([Item(L1, 6)])
PLAN_BX = Plan([Item(L1, 6)], True)
PLAN_C = Plan([Item(L0, 3)])
PLAN_D = Plan([Item(L2, 5)])
PLANS = (PLAN_A, PLAN_S, PLAN_B, PLAN_C, PLAN_D, PLAN_BX)


def far(p, sizes):
    ring = lambda d, n: min(d % n, -d % n)
    return p[0] + ring(p[1], sizes[1]) + ring(p[2], 4) + ring(p[2] // 4, 4)


def kernel(sizes, counts, right_in, guess_in, react_in, guess, r0, eb0, left0, step_out, *scratch):
    scratch = list(scratch)

    def take(n):
        out = scratch[:n]
        del scratch[:n]
        return out

    raw = take(3)
    (in_sems,) = take(1)
    right, react, inv0, ea0 = take(4)
    f1, s1, inv1, ea1, eb1, left1 = take(6)
    f2, s2, inv2, ea2, eb2, left2 = take(6)
    f3, s3, inv3, ea3, eb3, left3 = take(6)
    s4, p4, down_m, up_m, tmp, square, turned, spread, slab = take(9)
    scr = [take(n) for n in counts]
    place = Place(sizes)
    gx, gy, gz = place.me
    n3, n4, ny3 = 24 * sizes[2], 3 * sizes[2], 6 * sizes[1]

    inputs = (guess_in, right_in, react_in)
    for k in range(3):
        for q in range(4):
            at = pl.ds(12 * q, 12)
            pltpu.make_async_copy(inputs[k].at[at], raw[k].at[at], in_sems.at[k]).start()

    def clear(ref):
        n = ref.shape[0]
        size = next(k for k in (128, 122 * 8, 80, 8) if n % k == 0) if n > 128 else n
        size = {1808: 904, 976: 488, 416: 208}.get(n, size)

        def step(i, carry):
            ref[pl.ds(pl.multiple_of(i * size, 8), size), :] = jnp.zeros((size, 128), F32)
            return carry

        lax.fori_loop(0, n // size, step, 0)

    peers = [(a, b, c) for a in range(sizes[0]) for b in range(sizes[1]) for c in range(sizes[2])][1:]
    peers.sort(key=lambda p: -far(p, sizes))
    barrier = pltpu.get_barrier_semaphore()
    for p in peers:
        pl.semaphore_signal(barrier, inc=1, device_id=place.beside(*p), device_id_type=MESH)
    for ref in (guess, right, react, f1, s1, ea1, eb1, f2, s2, ea2, eb2, ea3, eb3, p4, square):
        clear(ref)
    spread[...] = jnp.zeros_like(spread)
    for ref in (f3, s3, inv3):
        for r in (0, GUARD3 + n3):
            ref[pl.ds(r, GUARD3), :] = jnp.zeros((GUARD3, 128), F32)

    a = iota2((128, 128), 0)
    b = iota2((128, 128), 1)
    signed = lambda v: ((v + 8) & 63) - 8
    base = lambda v: ((v + 8) & 127) & 64
    zb = signed(b)
    hit = ((a == ((base(b) + 2 * zb) & 127)) | (a == ((base(b) + 2 * zb + 1) & 127))) & (zb >= -8) & (zb < 24)
    down_m[...] = jnp.where(hit, 0.125, 0.0).astype(BF16)
    hit = a == ((base(b) + (zb >> 1)) & 127)
    up_m[...] = jnp.where(hit, 1.0, 0.0).astype(BF16)

    for k, dst in enumerate((guess, right, react)):
        pltpu.make_async_copy(inputs[k], raw[k], in_sems.at[k]).wait()

        for i in range(24):
            dst[pl.ds(L0.row(i, 0), 48), 0:48] = raw[k][i]
            dst[pl.ds(L0.row(i, 0), 48), 64:112] = raw[k][i + 24]

    ex_a = Exchange(PLAN_A, (guess, right, react), scr[0], place)
    ex_s = Exchange(PLAN_S, (s1, s2), scr[1], place)
    ex_b = Exchange(PLAN_B, (f1,), scr[2], place)
    ex_c = Exchange(PLAN_C, (eb0,), scr[3], place)
    ex_d = Exchange(PLAN_D, (f2,), scr[4], place)
    cx_b = Cross(PLAN_BX, ex_b, scr[5], place)
    ga_s = Gather(place, scr[6], s3)
    ga_f = Gather(place, scr[7], f3)
    reduced, red_send, red_recv = scr[8]

    ex_a.pack()
    pl.semaphore_wait(barrier, len(peers))
    ex_a.send()

    restrict(react, L0, s1, L1, 0, 12, 0, 24, down_m, tmp)
    restrict(s1, L1, s2, L2, 0, 6, 0, 12, down_m, tmp)
    ex_s.pack_send()
    ga_s.mine[...] = jnp.zeros((24, 128), F32)
    ga_f.mine[...] = jnp.zeros((24, 128), F32)
    to_level3(s2, ga_s.mine, square, turned, place)
    ga_s.send()

    def start(r):
        at = pl.ds(r, L0.R)
        c, image = image_of(guess, react, L0, r)
        res = right[at, :] - image
        inv = inverse(react[at, :], 1.0)
        return [(r0, res), (inv0, inv), (ea0, inv * res)]

    ex_a.unpack()
    ex_a.x_send()
    ex_a.unpack_rest()
    planes(L0, 1, 23, start)
    ex_a.x_wait()
    ex_a.x_fill()
    planes(L0, -2, 1, start)
    planes(L0, 23, 26, start)
    relax(L0, ea0, eb0, r0, react, inv0, -1, 25)
    leftover(L0, eb0, left0, r0, react, 0, 24)
    restrict(left0, L0, f1, L1, 0, 12, 0, 24, down_m, tmp)
    ex_b.pack_send()
    cx_b.pack_send()
    ex_b.x_send()

    ex_s.unpack()
    ex_s.x_send()
    ex_c.pack_send()
    ex_s.x_wait()
    ex_s.x_fill()
    for g, sh, inv in ((L1, s1, inv1), (L2, s2, inv2)):
        planes(g, -g.halo, g.nx + g.halo, lambda r: [(inv, inverse(sh[pl.ds(r, g.R), :], g.factor))])
    ga_s.relay()

    ex_b.x_sent()
    ex_b.unpack()
    first(L1, ea1, f1, inv1, 0, 12)
    relax(L1, ea1, eb1, f1, s1, inv1, 1, 11)
    ex_b.x_wait()
    cx_b.unpack()
    ex_b.x_fill()
    first(L1, ea1, f1, inv1, -6, 0)
    first(L1, ea1, f1, inv1, 12, 18)
    relax(L1, ea1, eb1, f1, s1, inv1, -5, 1)
    relax(L1, ea1, eb1, f1, s1, inv1, 11, 17)
    leftover(L1, eb1, left1, f1, s1, -4, 16)
    restrict(left1, L1, f2, L2, -2, 8, -2, 16, down_m, tmp)
    first(L2, ea2, f2, inv2, -2, 8)
    relax(L2, ea2, eb2, f2, s2, inv2, -1, 7)
    leftover(L2, eb2, left2, f2, s2, 0, 6)
    to_level3(left2, ga_f.mine, square, turned, place)
    ga_f.send()
    ex_d.pack_send()

    ex_c.unpack()
    ex_c.x_send()
    ex_c.unpack_rest()
    ga_s.finish()
    chunks3(n3, inv3, lambda r, n: inverse(s3[pl.ds(r, n), :], FACTOR3))
    s4[...] = restrict4(s3, n4, ny3)

    ga_f.relay()
    ex_d.unpack()
    ex_d.x_send()
    ex_c.x_wait()
    ex_c.x_fill()
    ex_d.x_wait()
    ex_d.x_fill()
    first(L2, ea2, f2, inv2, -5, 11)
    relax(L2, ea2, eb2, f2, s2, inv2, -4, 10)
    for e in (ex_a, ex_s, ex_c, ex_d, ga_s):
        e.settle()
    for e in (ex_b, cx_b):
        e.settle(False)
    ga_f.finish()

    def relax3(src, dst):
        def body(r, n):
            c, image = image3(src, s3, r, n)
            at = pl.ds(r, n)
            return c + inv3[at, :] * (f3[at, :] - image)

        chunks3(n3, dst, body)

    chunks3(n3, ea3, lambda r, n: inv3[pl.ds(r, n), :] * f3[pl.ds(r, n), :])
    relax3(ea3, eb3)
    chunks3(n3, left3, lambda r, n: f3[pl.ds(r, n), :] - image3(eb3, s3, r, n)[1])
    e4 = bottom(restrict4(left3, n4, ny3), s4, p4, n4, ny3 // 2)
    for k in range(3):
        u = mm(e4, jnp.where(match4(k, (128, 128), 0, ny3), 1.0, 0.0).astype(BF16))
        for q in (k, k + 4):
            at = pl.ds(GUARD3 + q, n4, stride=8)
            eb3[at, :] = eb3[at, :] + u
    for src, dst, n in ((eb3, ea3, 48), (ea3, slab, 40)):
        r = pl.multiple_of(GUARD3 + 24 * gz - (n - 24) // 2, 4)
        c, image = image3(src, s3, r, n)
        at = pl.ds(r, n)
        dst[at if n == 48 else pl.ds(0, n), :] = c + inv3[at, :] * (f3[at, :] - image)
    for k in range(3):
        v = slab[pl.ds(k, 10, stride=4), :]
        for h in range(2):
            for q in range(2):
                spread[k, pl.ds(64 * h + q, 10, stride=2), :] = v
    wide = [jnp.concatenate(p, axis=1) for p in zip(*[split(spread[k]) for k in range(3)])]
    coarse = []
    for h in range(2):
        r = iota2((112, 384), 0)
        l = iota2((112, 384), 1)
        hit = (6 * gx + 3 * h + (r >> 4) - 2 == (l >> 5)) & (6 * gy + (r & 15) - 2 == (l & 31)) & ((r & 15) < 10)
        pick = jnp.where(hit, 1.0, 0.0).astype(BF16)
        parts = [
            lax.dot_general(pick, p, (((1,), (1,)), ((), ())), preferred_element_type=F32) for p in wide
        ]
        coarse.append(parts[0] + parts[1])
    fine = roll(jnp.where(lanes(112) < 64, coarse[0], coarse[1]), -4)
    for i in range(7):
        u = fine[16 * i : 16 * i + 10]
        tmp[pl.ds(24 * i, 10, stride=2), :] = u
        tmp[pl.ds(24 * i + 1, 10, stride=2), :] = u
    for i in range(7):
        v = tmp[pl.ds(24 * i, 20), :]
        for q in range(2):
            at = pl.ds(L2.row(2 * (i - 2) + q, -4), 20)
            eb2[at, :] = eb2[at, :] + v
    relax(L2, eb2, ea2, f2, s2, inv2, -3, 9)
    relax(L2, ea2, eb2, f2, s2, inv2, -2, 8)
    prolong(eb2, L2, eb1, L1, -2, 8, -2, 16, up_m, tmp)
    relax(L1, eb1, ea1, f1, s1, inv1, -3, 15)
    relax(L1, ea1, eb1, f1, s1, inv1, -2, 14)
    prolong(eb1, L1, eb0, L0, -2, 14, -2, 28, up_m, tmp)
    relax(L0, eb0, ea0, r0, react, inv0, -2, 26)
    relax(L0, ea0, eb0, r0, react, inv0, -1, 25)

    row = iota2((L0.R, 128), 0)
    inside = ((lanes(L0.R) & 63) < 48) & (row >= L0.y0) & (row < L0.y0 + 48)

    upper, lower = [], []
    for i in range(24):
        r = GUARD + (L0.halo + i) * L0.R
        c, image = image_of(eb0, react, L0, r)
        left0[pl.ds(r, L0.R), :] = image
        upper.append(c * r0[pl.ds(r, L0.R), :])
        lower.append(c * image)
    upper = jnp.where(inside, tree(upper), 0.0)
    lower = jnp.where(inside, tree(lower), 0.0)
    upper = jnp.sum(upper, axis=0, keepdims=True)
    lower = jnp.sum(lower, axis=0, keepdims=True)
    half = lanes(1) < 64
    number = (gx * sizes[1] + gy) * sizes[2] + gz
    reduced[number] = jnp.where(half, upper + roll(upper, 64), lower + roll(lower, 64))
    own = reduced.at[number]

    def summed(src, dst, p):
        return pltpu.make_async_remote_copy(
            src_ref=src, dst_ref=dst, send_sem=red_send.at[0], recv_sem=red_recv.at[0],
            device_id=place.beside(*p), device_id_type=MESH,
        )

    for p in peers:
        summed(own, own, p).start()
    ga_f.settle()
    most = reduced.at[pl.ds(0, len(peers))]
    summed(most, most, peers[0]).wait()
    sums = [reduced[k] for k in range(8)]
    for k in range(8, len(peers) + 1):
        sums[k % 8] = sums[k % 8] + reduced[k]
    total = tree(sums)
    upper = jnp.sum(jnp.where(half, total, 0.0), axis=1, keepdims=True)
    lower = jnp.sum(jnp.where(half, 0.0, total), axis=1, keepdims=True)
    step_out[...] = jnp.broadcast_to(upper / lower, (8, 128))


def finish(guess, r0, eb0, left0, step_ref, field_out, resid_out, field, resid, sems):
    step = step_ref[0:1, :]
    copies = []
    parts, size = 4, 6
    for p in range(parts):
        for x in range(p * size, p * size + size):
            at = pl.ds(L0.row(x, 0), 48)
            v = guess[at, :] + step * eb0[at, :]
            field[x] = v[:, 0:48]
            field[x + 24] = roll(v, 64)[:, 0:48]
            v = r0[at, :] - step * left0[at, :]
            resid[x] = v[:, 0:48]
            resid[x + 24] = roll(v, 64)[:, 0:48]
        for q, (src, dst) in enumerate(((field, field_out), (resid, resid_out))):
            for h in range(2):
                at = pl.ds(p * size + 24 * h, size)
                c = pltpu.make_async_copy(src.at[at], dst.at[at], sems.at[4 * p + 2 * q + h])
                c.start()
                copies.append(c)
    for c in copies:
        c.wait()


def solution(mesh):
    sizes = tuple(mesh.shape[a] for a in ("gx", "gy", "gz"))
    n3, n4 = 24 * sizes[2] + 2 * GUARD3, 3 * sizes[2]
    scratch = [pltpu.VMEM((48, 48, 48), F32)] * 3 + [pltpu.SemaphoreType.DMA((3,))]
    scratch += [pltpu.VMEM((L0.total, 128), F32)] * 4
    scratch += [pltpu.VMEM((L1.total, 128), F32)] * 6
    scratch += [pltpu.VMEM((L2.total, 128), F32)] * 6
    scratch += [pltpu.VMEM((n3, 128), F32)] * 6
    scratch += [pltpu.VMEM((n4, 128), F32), pltpu.VMEM((n4 + 2 * GUARD, 128), F32)]
    scratch += [pltpu.VMEM((128, 128), BF16)] * 2 + [pltpu.VMEM((16 * 56, 128), F32)]
    scratch += [pltpu.VMEM((128, 128), F32)] * 2
    scratch += [pltpu.VMEM((3, 128, 128), F32), pltpu.VMEM((40, 128), F32)]
    groups = [p.scratch() for p in PLANS] + [gather_scratch(sizes)] * 2
    devices = sizes[0] * sizes[1] * sizes[2]
    groups += [[pltpu.VMEM((devices, 1, 128), F32)] + [pltpu.SemaphoreType.DMA((1,))] * 2]
    for g in groups:
        scratch += g
    counts = tuple(len(g) for g in groups)
    vmem = pl.BlockSpec(memory_space=pltpu.VMEM)

    anywhere = pl.BlockSpec(memory_space=pl.ANY)

    def body(right_side, start_guess, reaction):
        whole = pltpu.VMEM((L0.total, 128), F32)
        parts = pl.pallas_call(
            functools.partial(kernel, sizes, counts),
            out_shape=[whole] * 4 + [pltpu.VMEM((8, 128), F32)],
            in_specs=[anywhere] * 3,
            out_specs=[vmem] * 5,
            scratch_shapes=scratch,
            compiler_params=pltpu.CompilerParams(
                collective_id=0, has_side_effects=True, vmem_limit_bytes=60 * 2**20
            ),
        )(right_side, start_guess, reaction)
        shape = jax.ShapeDtypeStruct(right_side.shape, F32)
        return tuple(
            pl.pallas_call(
                finish,
                out_shape=[shape, shape],
                in_specs=[vmem] * 5,
                out_specs=[anywhere] * 2,
                scratch_shapes=[pltpu.VMEM(right_side.shape, F32)] * 2 + [pltpu.SemaphoreType.DMA((16,))],
                compiler_params=pltpu.CompilerParams(vmem_limit_bytes=16 * 2**20),
            )(*parts)
        )

    placed = P("gx", "gy", "gz")
    return jax.shard_map(
        body, mesh=mesh, in_specs=(placed,) * 3, out_specs=(placed,) * 2, check_vma=False
    )
```

```python
import functools

import jax
import jax.numpy as jnp
from jax import lax
from jax.experimental import pallas as pl
from jax.experimental.pallas import tpu as pltpu
from jax.sharding import PartitionSpec as P

MESH = pl.DeviceIdType.MESH
F32 = jnp.float32
BF16 = jnp.bfloat16
DAMP = 6.0 / 7.0
GUARD = 8
GUARD3 = 16
BOTTOM_ITERS = 6


class Geo:
    def __init__(self, nx, ny, nz, halo, rows, y0, depth, unroll):
        self.nx, self.ny, self.nz, self.halo, self.R, self.y0 = nx, ny, nz, halo, rows, y0
        self.factor = 0.25**depth
        self.unroll = unroll
        self.total = 2 * GUARD + (nx + 2 * halo) * rows

    def row(self, x, y):
        return GUARD + (self.halo + x) * self.R + self.y0 + y


L0 = Geo(24, 48, 48, 4, 56, 4, 0, 28)
L1 = Geo(12, 24, 24, 6, 40, 8, 1, 24)
L2 = Geo(6, 12, 12, 5, 24, 6, 2, 16)
FACTOR3 = 0.25**3
FACTOR4 = 0.25**4


def lanes(rows):
    return lax.broadcasted_iota(jnp.int32, (rows, 128), 1)


def iota2(shape, dim):
    return lax.broadcasted_iota(jnp.int32, shape, dim)


def tree(terms):
    while len(terms) > 1:
        terms = [sum(terms[k + 1 : k + 2], terms[k]) for k in range(0, len(terms), 2)]
    return terms[0]


def roll(v, shift):
    shift = shift % 128
    return v if shift == 0 else pltpu.roll(v, shift, 1)


def split(a):
    hi = a.astype(BF16)
    return hi, (a - hi.astype(F32)).astype(BF16)


def mm(a, b):
    hi, low = split(a)
    return jnp.dot(hi, b, preferred_element_type=F32) + jnp.dot(low, b, preferred_element_type=F32)


def beside_of(ref, r, R):
    c = ref[pl.ds(r, R), :]
    b = ref[pl.ds(r + R, R), :] + ref[pl.ds(r - R, R), :]
    b = b + (ref[pl.ds(r + 1, R), :] + ref[pl.ds(r - 1, R), :])
    b = b + (roll(c, 1) + roll(c, -1))
    return c, b


def image_of(ref, s_ref, g, r):
    c, b = beside_of(ref, r, g.R)
    return c, g.factor * (6.0 * c - b) + s_ref[pl.ds(r, g.R), :] * c


def planes(g, a, b, body):
    unroll = g.unroll

    def group(start, count):
        todo = []
        for k in range(count):
            r = start + k * g.R
            r = r if isinstance(r, int) else pl.multiple_of(r, 8)
            todo.append((r, body(r)))
        for r, pairs in todo:
            for ref, value in pairs:
                ref[pl.ds(r, g.R), :] = value

    trips = (b - a) // unroll
    origin = GUARD + (g.halo + a) * g.R
    if trips == 1:
        group(origin, unroll)
    elif trips:

        def step(i, carry):
            group(pl.multiple_of(origin + i * (unroll * g.R), 8), unroll)
            return carry

        lax.fori_loop(0, trips, step, 0)
    if (b - a) % unroll:
        group(origin + trips * unroll * g.R, (b - a) % unroll)


def inverse(s, factor):
    return jnp.where(s > 0.0, DAMP / (6.0 * factor + s), 0.0)


def relax(g, src, dst, f, s, inv, a, b):
    def body(r):
        c, image = image_of(src, s, g, r)
        at = pl.ds(r, g.R)
        return [(dst, c + inv[at, :] * (f[at, :] - image))]

    planes(g, a, b, body)


def first(g, dst, f, inv, a, b):
    def body(r):
        at = pl.ds(r, g.R)
        return [(dst, inv[at, :] * f[at, :])]

    planes(g, a, b, body)


def leftover(g, src, dst, f, s, a, b):
    def body(r):
        c, image = image_of(src, s, g, r)
        return [(dst, f[pl.ds(r, g.R), :] - image)]

    planes(g, a, b, body)


def restrict(src, gs, dst, gd, x0, x1, y0, count, matrix, tmp):
    step = -(-count // 8) * 8
    for x in range(x0, x1):
        r = gs.row(2 * x, 2 * y0)
        t = src[pl.ds(r, count, stride=2), :] + src[pl.ds(r + 1, count, stride=2), :]
        r = r + gs.R
        t = t + (src[pl.ds(r, count, stride=2), :] + src[pl.ds(r + 1, count, stride=2), :])
        tmp[pl.ds((x - x0) * step, count), :] = t
    for x in range(x0, x1):
        out = mm(tmp[pl.ds((x - x0) * step, step), :], matrix[...])
        dst[pl.ds(gd.row(x, y0), count), :] = out[0:count]


def prolong(src, gc, dst, gf, x0, x1, y0, count, matrix, tmp):
    for x in range(x0, x1):
        o = (x - x0) * 56
        u = mm(src[pl.ds(gc.row(x, y0), count), :], matrix[...])
        tmp[pl.ds(o, count, stride=2), :] = u
        tmp[pl.ds(o + 1, count, stride=2), :] = u
    for x in range(x0, x1):
        o = (x - x0) * 56
        v = tmp[pl.ds(o, 2 * count), :]
        for k in range(2):
            at = pl.ds(gf.row(2 * x + k, 2 * y0), 2 * count)
            dst[at, :] = dst[at, :] + v


class Item:
    def __init__(self, geo, w):
        self.g, self.w = geo, w


class Plan:
    def __init__(self, items, cross=False):
        self.items, self.cross = items, cross
        self.counts = [it.w if cross else it.g.nx for it in items]
        self.yrows = sum(n * it.w for n, it in zip(self.counts, items))
        self.yrows = -(-self.yrows // 8) * 8
        self.tiles = []
        for k, it in enumerate(items):
            for x in range(self.counts[k]):
                for t in self.tiles:
                    if t[0] is it.g and t[1] + it.w <= 64:
                        break
                else:
                    t = [it.g, 0, []]
                    self.tiles.append(t)
                t[2].append((k, x, t[1]))
                t[1] += it.w
        self.zrows = sum(t[0].ny for t in self.tiles)
        self.zrows = -(-self.zrows // 8) * 8
        self.drows = max(self.counts)
        self.drows = -(-self.drows // 8) * 8
        assert sum(it.w * it.w for it in items) <= 64

        self.z0 = [0, self.zrows]
        self.d0 = [2 * self.zrows + q * self.drows for q in range(4)]
        self.y0 = [2 * self.zrows + 4 * self.drows + q * self.yrows for q in range(2)]
        self.total = 2 * (self.zrows + self.yrows) + 4 * self.drows
        self.xtotal = sum(it.w * it.g.R for it in items)

    def scratch(self):
        x = [] if self.cross else [pltpu.VMEM((self.xtotal, 128), F32)]
        return x + [
            pltpu.VMEM((self.total, 128), F32),
            pltpu.VMEM((self.total, 128), F32),
            pltpu.SemaphoreType.DMA((2,)),
            pltpu.SemaphoreType.DMA((2,)),
        ]


class Exchange:
    def __init__(self, plan, refs, scratch, place):
        self.plan, self.refs, self.place = plan, refs, place
        self.xr, self.sent, self.got, self.ss, self.rs = scratch
        gx, gy, gz = place.me
        self.partner = (1 - gx, gy, gz)
        self.x_copies = []
        o = 0
        for k, it in enumerate(plan.items):
            r = pl.multiple_of(GUARD + (it.g.halo + self.edge(it)) * it.g.R, 8)
            n = it.w * it.g.R
            self.x_copies.append(self.copy(refs[k].at[pl.ds(r, n), :], self.xr.at[pl.ds(o, n), :], 0, self.partner))
            o += n
        self.segments(0)

    def edge(self, it):
        return jnp.where(self.place.me[0] == 0, it.g.nx - it.w, 0)

    def source(self, k, x, y):
        return self.plan.items[k].g.row(x, y)

    def target(self, k, x, y):
        return self.refs[k], self.plan.items[k].g.row(x, y)

    def segments(self, dx):
        plan = self.plan
        at = {}
        for d in range(2):
            at[1 - 2 * d, 0] = plan.y0[d]
            at[0, 1 - 2 * d] = plan.z0[d]
            for e in range(2):
                at[1 - 2 * d, 1 - 2 * e] = plan.d0[2 * d + e]
        self.y_copies, self.z_copies, self.d_copies = [], [], []
        for d in (1, -1):
            self.y_copies.append(self.segment(at, dx, d, 0, plan.yrows))
            self.z_copies.append(self.segment(at, dx, 0, d, plan.zrows))
            for e in (1, -1):
                self.d_copies.append(self.segment(at, dx, d, e, plan.drows))

    def segment(self, at, dx, dy, dz, n):
        there = self.place.exists(dy, dz)
        peer = self.place.beside(dx, dy, dz)
        peer = tuple(jnp.where(there, p, q) for p, q in zip(peer, self.partner))
        target = pl.multiple_of(jnp.where(there, at[dy, dz], at[-dy, -dz]), 8)
        return self.copy(self.sent.at[pl.ds(at[dy, dz], n), :], self.got.at[pl.ds(target, n), :], 1, peer)

    def copy(self, src, dst, k, peer):
        return pltpu.make_async_remote_copy(
            src_ref=src, dst_ref=dst, send_sem=self.ss.at[k], recv_sem=self.rs.at[k],
            device_id=peer, device_id_type=MESH,
        )

    def x_send(self):
        for c in self.x_copies:
            c.start()

    def settle(self, x=True):
        if x:
            self.x_sent()
        self.copy(self.sent, self.got, 1, self.partner).wait_send()

    def x_sent(self):
        self.copy(self.xr, self.xr, 0, self.partner).wait_send()

    def x_wait(self):
        self.copy(self.xr, self.xr, 0, self.partner).wait_recv()

    def x_fill(self):
        m0, m1 = self.place.x_masks
        o = 0
        for k, it in enumerate(self.plan.items):
            g, w, ref = it.g, it.w, self.refs[k]
            upper = ((lanes(g.R) + 8) & 127) >= 64
            for j in range(w):
                got = self.xr[pl.ds(o + j * g.R, g.R), :]
                top = ref[pl.ds(GUARD + (g.halo + g.nx - w + j) * g.R, g.R), :]
                low = ref[pl.ds(GUARD + (g.halo + j) * g.R, g.R), :]
                ref[pl.ds(GUARD + (g.halo - w + j) * g.R, g.R), :] = roll(jnp.where(upper, got * m1, top), 64)
                ref[pl.ds(GUARD + (g.halo + g.nx + j) * g.R, g.R), :] = roll(jnp.where(upper, low, got * m0), 64)
            o += w * g.R

    def pack_send(self):
        self.pack_sides()
        for c in self.d_copies:
            c.start()
        self.pack_z()
        for c in self.z_copies + self.y_copies:
            c.start()

    def pack(self):
        self.pack_sides()
        self.pack_z()

    def send(self):
        for c in self.d_copies + self.z_copies + self.y_copies:
            c.start()

    def pack_z(self):
        zo = 0
        for g, _, slots in self.plan.tiles:
            lane = lanes(g.ny)
            acc = [None, None]
            for k, x, at in slots:
                w = self.plan.items[k].w
                moved = roll(self.refs[k][pl.ds(self.source(k, x, 0), g.ny), :], at)
                for q, past in enumerate((g.nz - self.plan.items[k].w, 0)):
                    here = ((lane - past) & 63 >= at) & ((lane - past) & 63 < at + w)
                    acc[q] = moved if acc[q] is None else jnp.where(here, moved, acc[q])
            for q in range(2):
                self.sent[pl.ds(self.plan.z0[q] + zo, g.ny), :] = acc[q]
            zo += g.ny

    def pack_sides(self):
        yo, co = 0, 0
        corner = [None] * 4
        for k, it in enumerate(self.plan.items):
            g, w, ref = it.g, it.w, self.refs[k]
            n = self.plan.counts[k]
            lane = lanes(self.plan.drows) & 63
            for d in range(1, w + 1):
                at = co + (d - 1) * w
                for e, y in enumerate((g.ny - d, d - 1)):
                    v = ref[pl.ds(self.source(k, 0, y), n, stride=g.R), :]
                    self.sent[pl.ds(self.plan.y0[e] + yo, n), :] = v
                    if n < self.plan.drows:
                        v = jnp.concatenate([v, jnp.zeros((self.plan.drows - n, 128), F32)], axis=0)
                    for q, z in enumerate((g.nz - w, 0)):
                        moved = roll(v, at - z)
                        old = corner[2 * e + q]
                        corner[2 * e + q] = moved if old is None else jnp.where(lane >= at, moved, old)
                yo += n
            co += w * w
        for q in range(4):
            self.sent[pl.ds(self.plan.d0[q], self.plan.drows), :] = corner[q]

    def unpack(self):
        my, mz = self.place.y_masks, self.place.z_masks
        self.copy(self.sent, self.got, 1, self.partner).wait_recv()
        yo, co = 0, 0
        for k, it in enumerate(self.plan.items):
            g, w = it.g, it.w
            n = self.plan.counts[k]
            lane = lanes(n) & 63
            into = (lane >= 64 - w, (lane >= g.nz) & (lane < g.nz + w))
            for d in range(1, w + 1):
                at = co + (d - 1) * w
                for e, y in enumerate((-d, g.ny + d - 1)):
                    v = self.got[pl.ds(self.plan.y0[e] + yo, n), :]
                    for q, z in enumerate((-w, g.nz)):
                        got = self.got[pl.ds(self.plan.d0[2 * e + q], n), :] * mz[q]
                        v = jnp.where(into[q], roll(got, z - at), v)
                    ref, r = self.target(k, 0, y)
                    ref[pl.ds(r, n, stride=g.R), :] = v * my[e]
                yo += n
            co += w * w
        self.unpack_z(True)

    def unpack_rest(self):
        self.unpack_z(False)

    def unpack_z(self, edge):
        mz = self.place.z_masks
        zo = 0
        for g, _, slots in self.plan.tiles:
            lane = lanes(g.ny) & 63
            got = [self.got[pl.ds(self.plan.z0[q] + zo, g.ny), :] * mz[q] for q in range(2)]
            for k, x, at in slots:
                w = self.plan.items[k].w
                if (x < w or x >= g.nx - w) != edge:
                    continue
                ref, r = self.target(k, x, 0)
                rows = pl.ds(r, g.ny)
                v = ref[rows, :]
                v = jnp.where(lane >= 64 - w, roll(got[0], -g.nz - at), v)
                v = jnp.where((lane >= g.nz) & (lane < g.nz + w), roll(got[1], g.nz - at), v)
                ref[rows, :] = v
            zo += g.ny


class Cross(Exchange):
    def __init__(self, plan, main, scratch, place):
        self.plan, self.main, self.refs, self.place = plan, main, main.refs, place
        self.sent, self.got, self.ss, self.rs = scratch
        self.partner = main.partner
        self.segments(1)

    def source(self, k, x, y):
        it = self.plan.items[k]
        return GUARD + (it.g.halo + self.edge(it) + x) * it.g.R + it.g.y0 + y

    def target(self, k, x, y):
        o = sum(it.w * it.g.R for it in self.plan.items[:k])
        g = self.plan.items[k].g
        return self.main.xr, o + x * g.R + g.y0 + y


class Place:
    def __init__(self, sizes):
        self.sizes = sizes
        self.me = tuple(lax.axis_index(a) for a in ("gx", "gy", "gz"))
        gx, gy, gz = self.me
        one = lambda c: jnp.where(c, 1.0, 0.0).astype(F32)
        self.x_masks = (one(gx == 0), one(gx == 1))
        self.y_masks = (one(gy > 0), one(gy < sizes[1] - 1))
        self.z_masks = (one(gz > 0), one(gz < sizes[2] - 1))

    def exists(self, dy, dz):
        gx, gy, gz = self.me
        y, z = gy + dy, gz + dz
        return (y >= 0) & (y < self.sizes[1]) & (z >= 0) & (z < self.sizes[2])

    def beside(self, dx, dy, dz):
        return tuple(
            lax.rem(m + d % n, n) if d % n else m for m, d, n in zip(self.me, (dx, dy, dz), self.sizes)
        )


class Gather:
    rows = 24

    def __init__(self, place, scratch, whole):
        self.place, self.whole = place, whole
        self.mine, self.got, self.sum, self.ss, self.rs = scratch
        n = place.sizes
        self.near = [(a, b) for a in range(n[0]) for b in range(n[1])][1:]
        self.near.sort(key=lambda p: -far((p[0], p[1], 0), n))
        self.line = sorted(range(1, n[2]), key=lambda c: -far((0, 0, c), n))
        self.at = pl.ds(pl.multiple_of(GUARD3 + self.rows * place.me[2], 8), self.rows)

    def copy(self, src, dst, k, peer):
        return pltpu.make_async_remote_copy(
            src_ref=src, dst_ref=dst, send_sem=self.ss.at[k], recv_sem=self.rs.at[k],
            device_id=peer, device_id_type=MESH,
        )

    def send(self):
        for k, (a, b) in enumerate(self.near):
            self.copy(self.mine, self.got.at[k], 0, self.place.beside(a, b, 0)).start()

    def relay(self):
        self.copy(self.got, self.got, 0, self.place.beside(1, 0, 0)).wait_recv()
        total = self.mine[...]
        for k in range(len(self.near)):
            total = total + self.got[k]
        self.sum[...] = total
        for c in self.line:
            self.copy(self.sum, self.whole.at[self.at, :], 1, self.place.beside(0, 0, c)).start()
        self.whole[self.at, :] = total

    def finish(self):
        self.most().wait_recv()

    def most(self):
        most = self.whole.at[pl.ds(GUARD3, self.rows * (self.place.sizes[2] - 1)), :]
        return self.copy(most, most, 1, self.place.beside(1, 0, 0))

    def settle(self):
        self.copy(self.got, self.got, 0, self.place.beside(1, 0, 0)).wait_send()
        self.most().wait_send()


def gather_scratch(sizes):
    return [
        pltpu.VMEM((24, 128), F32),
        pltpu.VMEM((sizes[0] * sizes[1] - 1, 24, 128), F32),
        pltpu.VMEM((24, 128), F32),
        pltpu.SemaphoreType.DMA((2,)),
        pltpu.SemaphoreType.DMA((2,)),
    ]


def to_level3(src, mine, square, turned, place):
    g = L2
    gx, gy, gz = place.me
    for i in range(3):
        r = g.row(2 * i, 0)
        t = src[pl.ds(r, 6, stride=2), :] + src[pl.ds(r + 1, 6, stride=2), :]
        r = r + g.R
        t = t + (src[pl.ds(r, 6, stride=2), :] + src[pl.ds(r + 1, 6, stride=2), :])
        square[pl.ds(8 * i, 6), :] = t
    turned[...] = jnp.transpose(square[...])
    a = turned[pl.ds(0, 8, stride=2), :] + turned[pl.ds(1, 8, stride=2), :]
    b = turned[pl.ds(64, 8, stride=2), :] + turned[pl.ds(65, 8, stride=2), :]
    a = (a + roll(b, 64)) * 0.125
    r = iota2((128, 384), 0)
    l = iota2((128, 384), 1)
    x = 6 * gx + 3 * (r >> 6) + ((r & 63) >> 3)
    y = 6 * gy + (r & 7)
    hit = (x == (l >> 5)) & (y == (l & 31)) & ((r & 7) < 6) & ((r & 63) < 24)
    out = mm(a, jnp.where(hit, 1.0, 0.0).astype(BF16))
    for k in range(3):
        mine[pl.ds(k, 6, stride=4), :] = out[0:6, 128 * k : 128 * k + 128]


def image3(ref, s_ref, r, n):
    lane = lanes(n)
    c = ref[pl.ds(r, n), :]
    b = ref[pl.ds(r + 4, n), :] + ref[pl.ds(r - 4, n), :]
    b = b + (roll(c, 1) + roll(c, -1))
    b = b + roll(jnp.where(lane < 32, ref[pl.ds(r + 1, n), :], c), -32)
    b = b + roll(jnp.where(lane >= 96, ref[pl.ds(r - 1, n), :], c), 32)
    return c, FACTOR3 * (6.0 * c - b) + s_ref[pl.ds(r, n), :] * c


def chunks3(rows, ref, body):
    n = min(rows, 384)

    def step(i, carry):
        r = pl.multiple_of(GUARD3 + i * n, 8)
        ref[pl.ds(r, n), :] = body(r, n)
        return carry

    lax.fori_loop(0, rows // n, step, 0)


def match4(k, shape, coarse_dim, ny):
    c = iota2(shape, coarse_dim)
    l = iota2(shape, 1 - coarse_dim)
    return ((c >> 4) == 2 * k + (l >> 6)) & ((c & 15) == ((l & 31) >> 1)) & ((l & 31) < ny)


def restrict4(src, n, ny):
    total = None
    for k in range(3):
        t = src[pl.ds(GUARD3 + k, n, stride=8), :] + src[pl.ds(GUARD3 + k + 4, n, stride=8), :]
        part = mm(t, jnp.where(match4(k, (128, 128), 1, ny), 0.125, 0.0).astype(BF16))
        total = part if total is None else total + part
    return total


def dot_all(a, b):
    return jnp.sum(jnp.sum(a * b, axis=0, keepdims=True), axis=1, keepdims=True)


def bottom(source, s4, p4, n, ny):
    estimate = jnp.zeros_like(source)
    left = source
    inside = (lanes(n) < 96) & ((lanes(n) & 15) < ny)
    shifted = 6.0 * FACTOR4 + s4[...]
    for it in range(BOTTOM_ITERS):
        p4[pl.ds(GUARD, n), :] = left
        b = p4[pl.ds(GUARD + 1, n), :] + p4[pl.ds(GUARD - 1, n), :]
        b = b + (roll(left, 1) + roll(left, -1))
        b = b + (roll(left, 16) + roll(left, -16))
        image = shifted * left - FACTOR4 * jnp.where(inside, b, 0.0)
        now = dot_all(left, left)
        bent = dot_all(left, image)
        if it == 0:
            denom = bent
            direction, turned = left, image
        else:
            ratio = now * inv_before
            denom = bent - ratio * ratio * denom
            direction = left + ratio * direction
            turned = image + ratio * turned
        step = now / denom
        inv_before = 1.0 / now
        estimate = estimate + step * direction
        if it < BOTTOM_ITERS - 1:
            left = left - step * turned
    return estimate


PLAN_A = Plan([Item(L0, 3), Item(L0, 2), Item(L0, 2)])
PLAN_S = Plan([Item(L1, 6), Item(L2, 5)])
PLAN_B = Plan([Item(L1, 6)])
PLAN_BX = Plan([Item(L1, 6)], True)
PLAN_C = Plan([Item(L0, 3)])
PLAN_D = Plan([Item(L2, 5)])
PLANS = (PLAN_A, PLAN_S, PLAN_B, PLAN_C, PLAN_D, PLAN_BX)


def far(p, sizes):
    ring = lambda d, n: min(d % n, -d % n)
    return p[0] + ring(p[1], sizes[1]) + ring(p[2], 4) + ring(p[2] // 4, 4)


def kernel(sizes, counts, right_in, guess_in, react_in, guess, r0, eb0, left0, step_out, *scratch):
    scratch = list(scratch)

    def take(n):
        out = scratch[:n]
        del scratch[:n]
        return out

    raw = take(3)
    (in_sems,) = take(1)
    right, react, inv0, ea0 = take(4)
    f1, s1, inv1, ea1, eb1, left1 = take(6)
    f2, s2, inv2, ea2, eb2, left2 = take(6)
    f3, s3, inv3, ea3, eb3, left3 = take(6)
    s4, p4, down_m, up_m, tmp, square, turned, spread, slab = take(9)
    scr = [take(n) for n in counts]
    place = Place(sizes)
    gx, gy, gz = place.me
    n3, n4, ny3 = 24 * sizes[2], 3 * sizes[2], 6 * sizes[1]

    inputs = (guess_in, right_in, react_in)
    for k in range(3):
        for q in range(4):
            at = pl.ds(12 * q, 12)
            pltpu.make_async_copy(inputs[k].at[at], raw[k].at[at], in_sems.at[k]).start()

    def clear(ref):
        n = ref.shape[0]
        size = next(k for k in (128, 122 * 8, 80, 8) if n % k == 0) if n > 128 else n
        size = {1808: 904, 976: 488, 416: 208}.get(n, size)

        def step(i, carry):
            ref[pl.ds(pl.multiple_of(i * size, 8), size), :] = jnp.zeros((size, 128), F32)
            return carry

        lax.fori_loop(0, n // size, step, 0)

    peers = [(a, b, c) for a in range(sizes[0]) for b in range(sizes[1]) for c in range(sizes[2])][1:]
    peers.sort(key=lambda p: -far(p, sizes))
    beside = {(a, b % sizes[1], c % sizes[2]) for a in range(2) for b in (1, -1) for c in (1, -1)}
    beside |= {(1, 0, c % sizes[2]) for c in (1, -1)}
    greeted = [p for p in peers if p[2] == 0 or p[:2] == (0, 0) or p in beside]
    barrier = pltpu.get_barrier_semaphore()
    for p in greeted:
        pl.semaphore_signal(barrier, inc=1, device_id=place.beside(*p), device_id_type=MESH)
    for ref in (guess, right, react, f1, s1, ea1, eb1, f2, s2, ea2, eb2, ea3, eb3, p4, square):
        clear(ref)
    spread[...] = jnp.zeros_like(spread)
    for ref in (f3, s3, inv3):
        for r in (0, GUARD3 + n3):
            ref[pl.ds(r, GUARD3), :] = jnp.zeros((GUARD3, 128), F32)

    a = iota2((128, 128), 0)
    b = iota2((128, 128), 1)
    signed = lambda v: ((v + 8) & 63) - 8
    base = lambda v: ((v + 8) & 127) & 64
    zb = signed(b)
    hit = ((a == ((base(b) + 2 * zb) & 127)) | (a == ((base(b) + 2 * zb + 1) & 127))) & (zb >= -8) & (zb < 24)
    down_m[...] = jnp.where(hit, 0.125, 0.0).astype(BF16)
    hit = a == ((base(b) + (zb >> 1)) & 127)
    up_m[...] = jnp.where(hit, 1.0, 0.0).astype(BF16)

    for k, dst in enumerate((guess, right, react)):
        pltpu.make_async_copy(inputs[k], raw[k], in_sems.at[k]).wait()

        for i in range(24):
            dst[pl.ds(L0.row(i, 0), 48), 0:48] = raw[k][i]
            dst[pl.ds(L0.row(i, 0), 48), 64:112] = raw[k][i + 24]

    ex_a = Exchange(PLAN_A, (guess, right, react), scr[0], place)
    ex_s = Exchange(PLAN_S, (s1, s2), scr[1], place)
    ex_b = Exchange(PLAN_B, (f1,), scr[2], place)
    ex_c = Exchange(PLAN_C, (eb0,), scr[3], place)
    ex_d = Exchange(PLAN_D, (f2,), scr[4], place)
    cx_b = Cross(PLAN_BX, ex_b, scr[5], place)
    ga_s = Gather(place, scr[6], s3)
    ga_f = Gather(place, scr[7], f3)
    reduced, red_send, red_recv = scr[8]

    ex_a.pack()
    pl.semaphore_wait(barrier, len(greeted))
    ex_a.send()

    restrict(react, L0, s1, L1, 0, 12, 0, 24, down_m, tmp)
    restrict(s1, L1, s2, L2, 0, 6, 0, 12, down_m, tmp)
    ex_s.pack_send()
    ga_s.mine[...] = jnp.zeros((24, 128), F32)
    ga_f.mine[...] = jnp.zeros((24, 128), F32)
    to_level3(s2, ga_s.mine, square, turned, place)
    ga_s.send()

    def start(r):
        at = pl.ds(r, L0.R)
        c, image = image_of(guess, react, L0, r)
        res = right[at, :] - image
        inv = inverse(react[at, :], 1.0)
        return [(r0, res), (inv0, inv), (ea0, inv * res)]

    ex_a.unpack()
    ex_a.x_send()
    ex_a.unpack_rest()
    planes(L0, 1, 23, start)
    ex_a.x_wait()
    ex_a.x_fill()
    planes(L0, -2, 1, start)
    planes(L0, 23, 26, start)
    relax(L0, ea0, eb0, r0, react, inv0, -1, 25)
    leftover(L0, eb0, left0, r0, react, 0, 24)
    restrict(left0, L0, f1, L1, 0, 12, 0, 24, down_m, tmp)
    ex_b.pack_send()
    cx_b.pack_send()
    ex_b.x_send()

    ex_s.unpack()
    ex_s.x_send()
    ex_c.pack_send()
    ex_s.x_wait()
    ex_s.x_fill()
    for g, sh, inv in ((L1, s1, inv1), (L2, s2, inv2)):
        planes(g, -g.halo, g.nx + g.halo, lambda r: [(inv, inverse(sh[pl.ds(r, g.R), :], g.factor))])
    ga_s.relay()

    ex_b.x_sent()
    ex_b.unpack()
    first(L1, ea1, f1, inv1, 0, 12)
    relax(L1, ea1, eb1, f1, s1, inv1, 1, 11)
    ex_b.x_wait()
    cx_b.unpack()
    ex_b.x_fill()
    first(L1, ea1, f1, inv1, -6, 0)
    first(L1, ea1, f1, inv1, 12, 18)
    relax(L1, ea1, eb1, f1, s1, inv1, -5, 1)
    relax(L1, ea1, eb1, f1, s1, inv1, 11, 17)
    leftover(L1, eb1, left1, f1, s1, -4, 16)
    restrict(left1, L1, f2, L2, -2, 8, -2, 16, down_m, tmp)
    first(L2, ea2, f2, inv2, -2, 8)
    relax(L2, ea2, eb2, f2, s2, inv2, -1, 7)
    leftover(L2, eb2, left2, f2, s2, 0, 6)
    to_level3(left2, ga_f.mine, square, turned, place)
    ga_f.send()
    ex_d.pack_send()

    ex_c.unpack()
    ex_c.x_send()
    ex_c.unpack_rest()
    ga_s.finish()
    chunks3(n3, inv3, lambda r, n: inverse(s3[pl.ds(r, n), :], FACTOR3))
    s4[...] = restrict4(s3, n4, ny3)

    ga_f.relay()
    ex_d.unpack()
    ex_d.x_send()
    ex_c.x_wait()
    ex_c.x_fill()
    ex_d.x_wait()
    ex_d.x_fill()
    first(L2, ea2, f2, inv2, -5, 11)
    relax(L2, ea2, eb2, f2, s2, inv2, -4, 10)
    for e in (ex_a, ex_s, ex_c, ex_d, ga_s):
        e.settle()
    for e in (ex_b, cx_b):
        e.settle(False)
    ga_f.finish()

    def relax3(src, dst):
        def body(r, n):
            c, image = image3(src, s3, r, n)
            at = pl.ds(r, n)
            return c + inv3[at, :] * (f3[at, :] - image)

        chunks3(n3, dst, body)

    chunks3(n3, ea3, lambda r, n: inv3[pl.ds(r, n), :] * f3[pl.ds(r, n), :])
    relax3(ea3, eb3)
    chunks3(n3, left3, lambda r, n: f3[pl.ds(r, n), :] - image3(eb3, s3, r, n)[1])
    e4 = bottom(restrict4(left3, n4, ny3), s4, p4, n4, ny3 // 2)
    for k in range(3):
        u = mm(e4, jnp.where(match4(k, (128, 128), 0, ny3), 1.0, 0.0).astype(BF16))
        for q in (k, k + 4):
            at = pl.ds(GUARD3 + q, n4, stride=8)
            eb3[at, :] = eb3[at, :] + u
    for src, dst, n in ((eb3, ea3, 48), (ea3, slab, 40)):
        r = pl.multiple_of(GUARD3 + 24 * gz - (n - 24) // 2, 4)
        c, image = image3(src, s3, r, n)
        at = pl.ds(r, n)
        dst[at if n == 48 else pl.ds(0, n), :] = c + inv3[at, :] * (f3[at, :] - image)
    for k in range(3):
        v = slab[pl.ds(k, 10, stride=4), :]
        for h in range(2):
            for q in range(2):
                spread[k, pl.ds(64 * h + q, 10, stride=2), :] = v
    wide = [jnp.concatenate(p, axis=1) for p in zip(*[split(spread[k]) for k in range(3)])]
    coarse = []
    for h in range(2):
        r = iota2((112, 384), 0)
        l = iota2((112, 384), 1)
        hit = (6 * gx + 3 * h + (r >> 4) - 2 == (l >> 5)) & (6 * gy + (r & 15) - 2 == (l & 31)) & ((r & 15) < 10)
        pick = jnp.where(hit, 1.0, 0.0).astype(BF16)
        parts = [
            lax.dot_general(pick, p, (((1,), (1,)), ((), ())), preferred_element_type=F32) for p in wide
        ]
        coarse.append(parts[0] + parts[1])
    fine = roll(jnp.where(lanes(112) < 64, coarse[0], coarse[1]), -4)
    for i in range(7):
        u = fine[16 * i : 16 * i + 10]
        tmp[pl.ds(24 * i, 10, stride=2), :] = u
        tmp[pl.ds(24 * i + 1, 10, stride=2), :] = u
    for i in range(7):
        v = tmp[pl.ds(24 * i, 20), :]
        for q in range(2):
            at = pl.ds(L2.row(2 * (i - 2) + q, -4), 20)
            eb2[at, :] = eb2[at, :] + v
    relax(L2, eb2, ea2, f2, s2, inv2, -3, 9)
    relax(L2, ea2, eb2, f2, s2, inv2, -2, 8)
    prolong(eb2, L2, eb1, L1, -2, 8, -2, 16, up_m, tmp)
    relax(L1, eb1, ea1, f1, s1, inv1, -3, 15)
    relax(L1, ea1, eb1, f1, s1, inv1, -2, 14)
    prolong(eb1, L1, eb0, L0, -2, 14, -2, 28, up_m, tmp)
    relax(L0, eb0, ea0, r0, react, inv0, -2, 26)
    relax(L0, ea0, eb0, r0, react, inv0, -1, 25)

    row = iota2((L0.R, 128), 0)
    inside = ((lanes(L0.R) & 63) < 48) & (row >= L0.y0) & (row < L0.y0 + 48)

    upper, lower = [], []
    for i in range(24):
        r = GUARD + (L0.halo + i) * L0.R
        c, image = image_of(eb0, react, L0, r)
        left0[pl.ds(r, L0.R), :] = image
        upper.append(c * r0[pl.ds(r, L0.R), :])
        lower.append(c * image)
    upper = jnp.where(inside, tree(upper), 0.0)
    lower = jnp.where(inside, tree(lower), 0.0)
    upper = jnp.sum(upper, axis=0, keepdims=True)
    lower = jnp.sum(lower, axis=0, keepdims=True)
    half = lanes(1) < 64
    number = (gx * sizes[1] + gy) * sizes[2] + gz
    reduced[number] = jnp.where(half, upper + roll(upper, 64), lower + roll(lower, 64))
    own = reduced.at[number]

    def summed(src, dst, p):
        return pltpu.make_async_remote_copy(
            src_ref=src, dst_ref=dst, send_sem=red_send.at[0], recv_sem=red_recv.at[0],
            device_id=place.beside(*p), device_id_type=MESH,
        )

    for p in peers:
        summed(own, own, p).start()
    ga_f.settle()
    most = reduced.at[pl.ds(0, len(peers))]
    summed(most, most, peers[0]).wait()
    sums = [reduced[k] for k in range(8)]
    for k in range(8, len(peers) + 1):
        sums[k % 8] = sums[k % 8] + reduced[k]
    total = tree(sums)
    upper = jnp.sum(jnp.where(half, total, 0.0), axis=1, keepdims=True)
    lower = jnp.sum(jnp.where(half, 0.0, total), axis=1, keepdims=True)
    step_out[...] = jnp.broadcast_to(upper / lower, (8, 128))


def finish(guess, r0, eb0, left0, step_ref, field_out, resid_out, field, resid, sems):
    step = step_ref[0:1, :]
    copies = []
    parts, size = 4, 6
    for p in range(parts):
        for x in range(p * size, p * size + size):
            at = pl.ds(L0.row(x, 0), 48)
            v = guess[at, :] + step * eb0[at, :]
            field[x] = v[:, 0:48]
            field[x + 24] = roll(v, 64)[:, 0:48]
            v = r0[at, :] - step * left0[at, :]
            resid[x] = v[:, 0:48]
            resid[x + 24] = roll(v, 64)[:, 0:48]
        for q, (src, dst) in enumerate(((field, field_out), (resid, resid_out))):
            for h in range(2):
                at = pl.ds(p * size + 24 * h, size)
                c = pltpu.make_async_copy(src.at[at], dst.at[at], sems.at[4 * p + 2 * q + h])
                c.start()
                copies.append(c)
    for c in copies:
        c.wait()


def solution(mesh):
    sizes = tuple(mesh.shape[a] for a in ("gx", "gy", "gz"))
    n3, n4 = 24 * sizes[2] + 2 * GUARD3, 3 * sizes[2]
    scratch = [pltpu.VMEM((48, 48, 48), F32)] * 3 + [pltpu.SemaphoreType.DMA((3,))]
    scratch += [pltpu.VMEM((L0.total, 128), F32)] * 4
    scratch += [pltpu.VMEM((L1.total, 128), F32)] * 6
    scratch += [pltpu.VMEM((L2.total, 128), F32)] * 6
    scratch += [pltpu.VMEM((n3, 128), F32)] * 6
    scratch += [pltpu.VMEM((n4, 128), F32), pltpu.VMEM((n4 + 2 * GUARD, 128), F32)]
    scratch += [pltpu.VMEM((128, 128), BF16)] * 2 + [pltpu.VMEM((16 * 56, 128), F32)]
    scratch += [pltpu.VMEM((128, 128), F32)] * 2
    scratch += [pltpu.VMEM((3, 128, 128), F32), pltpu.VMEM((40, 128), F32)]
    groups = [p.scratch() for p in PLANS] + [gather_scratch(sizes)] * 2
    devices = sizes[0] * sizes[1] * sizes[2]
    groups += [[pltpu.VMEM((devices, 1, 128), F32)] + [pltpu.SemaphoreType.DMA((1,))] * 2]
    for g in groups:
        scratch += g
    counts = tuple(len(g) for g in groups)
    vmem = pl.BlockSpec(memory_space=pltpu.VMEM)

    anywhere = pl.BlockSpec(memory_space=pl.ANY)

    def body(right_side, start_guess, reaction):
        whole = pltpu.VMEM((L0.total, 128), F32)
        parts = pl.pallas_call(
            functools.partial(kernel, sizes, counts),
            out_shape=[whole] * 4 + [pltpu.VMEM((8, 128), F32)],
            in_specs=[anywhere] * 3,
            out_specs=[vmem] * 5,
            scratch_shapes=scratch,
            compiler_params=pltpu.CompilerParams(
                collective_id=0, has_side_effects=True, vmem_limit_bytes=60 * 2**20
            ),
        )(right_side, start_guess, reaction)
        shape = jax.ShapeDtypeStruct(right_side.shape, F32)
        return tuple(
            pl.pallas_call(
                finish,
                out_shape=[shape, shape],
                in_specs=[vmem] * 5,
                out_specs=[anywhere] * 2,
                scratch_shapes=[pltpu.VMEM(right_side.shape, F32)] * 2 + [pltpu.SemaphoreType.DMA((16,))],
                compiler_params=pltpu.CompilerParams(vmem_limit_bytes=16 * 2**20),
            )(*parts)
        )

    placed = P("gx", "gy", "gz")
    return jax.shard_map(
        body, mesh=mesh, in_specs=(placed,) * 3, out_specs=(placed,) * 2, check_vma=False
    )
```

```python
import functools

import jax
import jax.numpy as jnp
from jax import lax
from jax.experimental import pallas as pl
from jax.experimental.pallas import tpu as pltpu
from jax.sharding import PartitionSpec as P

MESH = pl.DeviceIdType.MESH
F32 = jnp.float32
BF16 = jnp.bfloat16
DAMP = 6.0 / 7.0
GUARD = 8
GUARD3 = 16
BOTTOM_ITERS = 6


class Geo:
    def __init__(self, nx, ny, nz, halo, rows, y0, depth, unroll):
        self.nx, self.ny, self.nz, self.halo, self.R, self.y0 = nx, ny, nz, halo, rows, y0
        self.factor = 0.25**depth
        self.unroll = unroll
        self.total = 2 * GUARD + (nx + 2 * halo) * rows

    def row(self, x, y):
        return GUARD + (self.halo + x) * self.R + self.y0 + y


L0 = Geo(24, 48, 48, 4, 56, 4, 0, 28)
L1 = Geo(12, 24, 24, 6, 40, 8, 1, 24)
L2 = Geo(6, 12, 12, 5, 24, 6, 2, 16)
FACTOR3 = 0.25**3
FACTOR4 = 0.25**4


def lanes(rows):
    return lax.broadcasted_iota(jnp.int32, (rows, 128), 1)


def iota2(shape, dim):
    return lax.broadcasted_iota(jnp.int32, shape, dim)


def tree(terms):
    while len(terms) > 1:
        terms = [sum(terms[k + 1 : k + 2], terms[k]) for k in range(0, len(terms), 2)]
    return terms[0]


def roll(v, shift):
    shift = shift % 128
    return v if shift == 0 else pltpu.roll(v, shift, 1)


def split(a):
    hi = a.astype(BF16)
    return hi, (a - hi.astype(F32)).astype(BF16)


def mm(a, b):
    hi, low = split(a)
    return jnp.dot(hi, b, preferred_element_type=F32) + jnp.dot(low, b, preferred_element_type=F32)


def beside_of(ref, r, R):
    c = ref[pl.ds(r, R), :]
    b = ref[pl.ds(r + R, R), :] + ref[pl.ds(r - R, R), :]
    b = b + (ref[pl.ds(r + 1, R), :] + ref[pl.ds(r - 1, R), :])
    b = b + (roll(c, 1) + roll(c, -1))
    return c, b


def image_of(ref, s_ref, g, r):
    c, b = beside_of(ref, r, g.R)
    return c, g.factor * (6.0 * c - b) + s_ref[pl.ds(r, g.R), :] * c


def planes(g, a, b, body):
    unroll = g.unroll

    def group(start, count):
        todo = []
        for k in range(count):
            r = start + k * g.R
            r = r if isinstance(r, int) else pl.multiple_of(r, 8)
            todo.append((r, body(r)))
        for r, pairs in todo:
            for ref, value in pairs:
                ref[pl.ds(r, g.R), :] = value

    trips = (b - a) // unroll
    origin = GUARD + (g.halo + a) * g.R
    if trips == 1:
        group(origin, unroll)
    elif trips:

        def step(i, carry):
            group(pl.multiple_of(origin + i * (unroll * g.R), 8), unroll)
            return carry

        lax.fori_loop(0, trips, step, 0)
    if (b - a) % unroll:
        group(origin + trips * unroll * g.R, (b - a) % unroll)


def inverse(s, factor):
    return jnp.where(s > 0.0, DAMP / (6.0 * factor + s), 0.0)


def relax(g, src, dst, f, s, inv, a, b):
    def body(r):
        c, image = image_of(src, s, g, r)
        at = pl.ds(r, g.R)
        return [(dst, c + inv[at, :] * (f[at, :] - image))]

    planes(g, a, b, body)


def first(g, dst, f, inv, a, b):
    def body(r):
        at = pl.ds(r, g.R)
        return [(dst, inv[at, :] * f[at, :])]

    planes(g, a, b, body)


def leftover(g, src, dst, f, s, a, b):
    def body(r):
        c, image = image_of(src, s, g, r)
        return [(dst, f[pl.ds(r, g.R), :] - image)]

    planes(g, a, b, body)


def restrict(src, gs, dst, gd, x0, x1, y0, count, matrix, tmp):
    step = -(-count // 8) * 8
    for x in range(x0, x1):
        r = gs.row(2 * x, 2 * y0)
        t = src[pl.ds(r, count, stride=2), :] + src[pl.ds(r + 1, count, stride=2), :]
        r = r + gs.R
        t = t + (src[pl.ds(r, count, stride=2), :] + src[pl.ds(r + 1, count, stride=2), :])
        tmp[pl.ds((x - x0) * step, count), :] = t
    for x in range(x0, x1):
        out = mm(tmp[pl.ds((x - x0) * step, step), :], matrix[...])
        dst[pl.ds(gd.row(x, y0), count), :] = out[0:count]


def prolong(src, gc, dst, gf, x0, x1, y0, count, matrix, tmp):
    for x in range(x0, x1):
        o = (x - x0) * 56
        u = mm(src[pl.ds(gc.row(x, y0), count), :], matrix[...])
        tmp[pl.ds(o, count, stride=2), :] = u
        tmp[pl.ds(o + 1, count, stride=2), :] = u
    for x in range(x0, x1):
        o = (x - x0) * 56
        v = tmp[pl.ds(o, 2 * count), :]
        for k in range(2):
            at = pl.ds(gf.row(2 * x + k, 2 * y0), 2 * count)
            dst[at, :] = dst[at, :] + v


class Item:
    def __init__(self, geo, w):
        self.g, self.w = geo, w


class Plan:
    def __init__(self, items, cross=False):
        self.items, self.cross = items, cross
        self.counts = [it.w if cross else it.g.nx for it in items]
        self.yrows = sum(n * it.w for n, it in zip(self.counts, items))
        self.yrows = -(-self.yrows // 8) * 8
        self.tiles = []
        for k, it in enumerate(items):
            for x in range(self.counts[k]):
                for t in self.tiles:
                    if t[0] is it.g and t[1] + it.w <= 64:
                        break
                else:
                    t = [it.g, 0, []]
                    self.tiles.append(t)
                t[2].append((k, x, t[1]))
                t[1] += it.w
        self.zrows = sum(t[0].ny for t in self.tiles)
        self.zrows = -(-self.zrows // 8) * 8
        self.drows = max(self.counts)
        self.drows = -(-self.drows // 8) * 8
        assert sum(it.w * it.w for it in items) <= 64

        self.z0 = [0, self.zrows]
        self.d0 = [2 * self.zrows + q * self.drows for q in range(4)]
        self.y0 = [2 * self.zrows + 4 * self.drows + q * self.yrows for q in range(2)]
        self.total = 2 * (self.zrows + self.yrows) + 4 * self.drows
        self.xtotal = sum(it.w * it.g.R for it in items)

    def scratch(self):
        x = [] if self.cross else [pltpu.VMEM((self.xtotal, 128), F32)]
        return x + [
            pltpu.VMEM((self.total, 128), F32),
            pltpu.VMEM((self.total, 128), F32),
            pltpu.SemaphoreType.DMA((2,)),
            pltpu.SemaphoreType.DMA((2,)),
        ]


class Exchange:
    def __init__(self, plan, refs, scratch, place):
        self.plan, self.refs, self.place = plan, refs, place
        self.xr, self.sent, self.got, self.ss, self.rs = scratch
        gx, gy, gz = place.me
        self.partner = (1 - gx, gy, gz)
        self.x_copies = []
        o = 0
        for k, it in enumerate(plan.items):
            r = pl.multiple_of(GUARD + (it.g.halo + self.edge(it)) * it.g.R, 8)
            n = it.w * it.g.R
            self.x_copies.append(self.copy(refs[k].at[pl.ds(r, n), :], self.xr.at[pl.ds(o, n), :], 0, self.partner))
            o += n
        self.segments(0)

    def edge(self, it):
        return jnp.where(self.place.me[0] == 0, it.g.nx - it.w, 0)

    def source(self, k, x, y):
        return self.plan.items[k].g.row(x, y)

    def target(self, k, x, y):
        return self.refs[k], self.plan.items[k].g.row(x, y)

    def segments(self, dx):
        plan = self.plan
        at = {}
        for d in range(2):
            at[1 - 2 * d, 0] = plan.y0[d]
            at[0, 1 - 2 * d] = plan.z0[d]
            for e in range(2):
                at[1 - 2 * d, 1 - 2 * e] = plan.d0[2 * d + e]
        self.y_copies, self.z_copies, self.d_copies = [], [], []
        for d in (1, -1):
            self.y_copies.append(self.segment(at, dx, d, 0, plan.yrows))
            self.z_copies.append(self.segment(at, dx, 0, d, plan.zrows))
            for e in (1, -1):
                self.d_copies.append(self.segment(at, dx, d, e, plan.drows))

    def segment(self, at, dx, dy, dz, n):
        there = self.place.exists(dy, dz)
        peer = self.place.beside(dx, dy, dz)
        peer = tuple(jnp.where(there, p, q) for p, q in zip(peer, self.partner))
        target = pl.multiple_of(jnp.where(there, at[dy, dz], at[-dy, -dz]), 8)
        return self.copy(self.sent.at[pl.ds(at[dy, dz], n), :], self.got.at[pl.ds(target, n), :], 1, peer)

    def copy(self, src, dst, k, peer):
        return pltpu.make_async_remote_copy(
            src_ref=src, dst_ref=dst, send_sem=self.ss.at[k], recv_sem=self.rs.at[k],
            device_id=peer, device_id_type=MESH,
        )

    def x_send(self):
        for c in self.x_copies:
            c.start()

    def settle(self, x=True):
        if x:
            self.x_sent()
        self.copy(self.sent, self.got, 1, self.partner).wait_send()

    def x_sent(self):
        self.copy(self.xr, self.xr, 0, self.partner).wait_send()

    def x_wait(self):
        self.copy(self.xr, self.xr, 0, self.partner).wait_recv()

    def x_fill(self):
        m0, m1 = self.place.x_masks
        o = 0
        for k, it in enumerate(self.plan.items):
            g, w, ref = it.g, it.w, self.refs[k]
            upper = ((lanes(g.R) + 8) & 127) >= 64
            for j in range(w):
                got = self.xr[pl.ds(o + j * g.R, g.R), :]
                top = ref[pl.ds(GUARD + (g.halo + g.nx - w + j) * g.R, g.R), :]
                low = ref[pl.ds(GUARD + (g.halo + j) * g.R, g.R), :]
                ref[pl.ds(GUARD + (g.halo - w + j) * g.R, g.R), :] = roll(jnp.where(upper, got * m1, top), 64)
                ref[pl.ds(GUARD + (g.halo + g.nx + j) * g.R, g.R), :] = roll(jnp.where(upper, low, got * m0), 64)
            o += w * g.R

    def pack_send(self):
        self.pack_sides()
        for c in self.d_copies:
            c.start()
        self.pack_z()
        for c in self.z_copies + self.y_copies:
            c.start()

    def pack(self):
        self.pack_sides()
        self.pack_z()

    def send(self):
        for c in self.d_copies + self.z_copies + self.y_copies:
            c.start()

    def pack_z(self):
        zo = 0
        for g, _, slots in self.plan.tiles:
            lane = lanes(g.ny)
            acc = [None, None]
            for k, x, at in slots:
                w = self.plan.items[k].w
                moved = roll(self.refs[k][pl.ds(self.source(k, x, 0), g.ny), :], at)
                for q, past in enumerate((g.nz - self.plan.items[k].w, 0)):
                    here = ((lane - past) & 63 >= at) & ((lane - past) & 63 < at + w)
                    acc[q] = moved if acc[q] is None else jnp.where(here, moved, acc[q])
            for q in range(2):
                self.sent[pl.ds(self.plan.z0[q] + zo, g.ny), :] = acc[q]
            zo += g.ny

    def pack_sides(self):
        yo, co = 0, 0
        corner = [None] * 4
        for k, it in enumerate(self.plan.items):
            g, w, ref = it.g, it.w, self.refs[k]
            n = self.plan.counts[k]
            lane = lanes(self.plan.drows) & 63
            for d in range(1, w + 1):
                at = co + (d - 1) * w
                for e, y in enumerate((g.ny - d, d - 1)):
                    v = ref[pl.ds(self.source(k, 0, y), n, stride=g.R), :]
                    self.sent[pl.ds(self.plan.y0[e] + yo, n), :] = v
                    if n < self.plan.drows:
                        v = jnp.concatenate([v, jnp.zeros((self.plan.drows - n, 128), F32)], axis=0)
                    for q, z in enumerate((g.nz - w, 0)):
                        moved = roll(v, at - z)
                        old = corner[2 * e + q]
                        corner[2 * e + q] = moved if old is None else jnp.where(lane >= at, moved, old)
                yo += n
            co += w * w
        for q in range(4):
            self.sent[pl.ds(self.plan.d0[q], self.plan.drows), :] = corner[q]

    def unpack(self):
        my, mz = self.place.y_masks, self.place.z_masks
        self.copy(self.sent, self.got, 1, self.partner).wait_recv()
        yo, co = 0, 0
        for k, it in enumerate(self.plan.items):
            g, w = it.g, it.w
            n = self.plan.counts[k]
            lane = lanes(n) & 63
            into = (lane >= 64 - w, (lane >= g.nz) & (lane < g.nz + w))
            for d in range(1, w + 1):
                at = co + (d - 1) * w
                for e, y in enumerate((-d, g.ny + d - 1)):
                    v = self.got[pl.ds(self.plan.y0[e] + yo, n), :]
                    for q, z in enumerate((-w, g.nz)):
                        got = self.got[pl.ds(self.plan.d0[2 * e + q], n), :] * mz[q]
                        v = jnp.where(into[q], roll(got, z - at), v)
                    ref, r = self.target(k, 0, y)
                    ref[pl.ds(r, n, stride=g.R), :] = v * my[e]
                yo += n
            co += w * w
        self.unpack_z(True)

    def unpack_rest(self):
        self.unpack_z(False)

    def unpack_z(self, edge):
        mz = self.place.z_masks
        zo = 0
        for g, _, slots in self.plan.tiles:
            lane = lanes(g.ny) & 63
            got = [self.got[pl.ds(self.plan.z0[q] + zo, g.ny), :] * mz[q] for q in range(2)]
            for k, x, at in slots:
                w = self.plan.items[k].w
                if (x < w or x >= g.nx - w) != edge:
                    continue
                ref, r = self.target(k, x, 0)
                rows = pl.ds(r, g.ny)
                v = ref[rows, :]
                v = jnp.where(lane >= 64 - w, roll(got[0], -g.nz - at), v)
                v = jnp.where((lane >= g.nz) & (lane < g.nz + w), roll(got[1], g.nz - at), v)
                ref[rows, :] = v
            zo += g.ny


class Cross(Exchange):
    def __init__(self, plan, main, scratch, place):
        self.plan, self.main, self.refs, self.place = plan, main, main.refs, place
        self.sent, self.got, self.ss, self.rs = scratch
        self.partner = main.partner
        self.segments(1)

    def source(self, k, x, y):
        it = self.plan.items[k]
        return GUARD + (it.g.halo + self.edge(it) + x) * it.g.R + it.g.y0 + y

    def target(self, k, x, y):
        o = sum(it.w * it.g.R for it in self.plan.items[:k])
        g = self.plan.items[k].g
        return self.main.xr, o + x * g.R + g.y0 + y


class Place:
    def __init__(self, sizes):
        self.sizes = sizes
        self.me = tuple(lax.axis_index(a) for a in ("gx", "gy", "gz"))
        gx, gy, gz = self.me
        one = lambda c: jnp.where(c, 1.0, 0.0).astype(F32)
        self.x_masks = (one(gx == 0), one(gx == 1))
        self.y_masks = (one(gy > 0), one(gy < sizes[1] - 1))
        self.z_masks = (one(gz > 0), one(gz < sizes[2] - 1))

    def exists(self, dy, dz):
        gx, gy, gz = self.me
        y, z = gy + dy, gz + dz
        return (y >= 0) & (y < self.sizes[1]) & (z >= 0) & (z < self.sizes[2])

    def beside(self, dx, dy, dz):
        return tuple(
            lax.rem(m + d % n, n) if d % n else m for m, d, n in zip(self.me, (dx, dy, dz), self.sizes)
        )


class Gather:
    rows = 24

    def __init__(self, place, scratch, whole):
        self.place, self.whole = place, whole
        self.mine, self.got, self.sum, self.ss, self.rs = scratch
        n = place.sizes
        self.near = [(a, b) for a in range(n[0]) for b in range(n[1])][1:]
        self.near.sort(key=lambda p: -far((p[0], p[1], 0), n))
        self.line = sorted(range(1, n[2]), key=lambda c: -far((0, 0, c), n))
        self.at = pl.ds(pl.multiple_of(GUARD3 + self.rows * place.me[2], 8), self.rows)

    def copy(self, src, dst, k, peer):
        return pltpu.make_async_remote_copy(
            src_ref=src, dst_ref=dst, send_sem=self.ss.at[k], recv_sem=self.rs.at[k],
            device_id=peer, device_id_type=MESH,
        )

    def send(self):
        for k, (a, b) in enumerate(self.near):
            self.copy(self.mine, self.got.at[k], 0, self.place.beside(a, b, 0)).start()

    def relay(self):
        self.copy(self.got, self.got, 0, self.place.beside(1, 0, 0)).wait_recv()
        total = self.mine[...]
        for k in range(len(self.near)):
            total = total + self.got[k]
        self.sum[...] = total
        for c in self.line:
            self.copy(self.sum, self.whole.at[self.at, :], 1, self.place.beside(0, 0, c)).start()
        self.whole[self.at, :] = total

    def finish(self):
        self.most().wait_recv()

    def most(self):
        most = self.whole.at[pl.ds(GUARD3, self.rows * (self.place.sizes[2] - 1)), :]
        return self.copy(most, most, 1, self.place.beside(1, 0, 0))

    def settle(self):
        self.copy(self.got, self.got, 0, self.place.beside(1, 0, 0)).wait_send()
        self.most().wait_send()


def gather_scratch(sizes):
    return [
        pltpu.VMEM((24, 128), F32),
        pltpu.VMEM((sizes[0] * sizes[1] - 1, 24, 128), F32),
        pltpu.VMEM((24, 128), F32),
        pltpu.SemaphoreType.DMA((2,)),
        pltpu.SemaphoreType.DMA((2,)),
    ]


def to_level3(src, mine, square, turned, place):
    g = L2
    gx, gy, gz = place.me
    for i in range(3):
        r = g.row(2 * i, 0)
        t = src[pl.ds(r, 6, stride=2), :] + src[pl.ds(r + 1, 6, stride=2), :]
        r = r + g.R
        t = t + (src[pl.ds(r, 6, stride=2), :] + src[pl.ds(r + 1, 6, stride=2), :])
        square[pl.ds(8 * i, 6), :] = t
    turned[...] = jnp.transpose(square[...])
    a = turned[pl.ds(0, 8, stride=2), :] + turned[pl.ds(1, 8, stride=2), :]
    b = turned[pl.ds(64, 8, stride=2), :] + turned[pl.ds(65, 8, stride=2), :]
    a = (a + roll(b, 64)) * 0.125
    r = iota2((128, 384), 0)
    l = iota2((128, 384), 1)
    x = 6 * gx + 3 * (r >> 6) + ((r & 63) >> 3)
    y = 6 * gy + (r & 7)
    hit = (x == (l >> 5)) & (y == (l & 31)) & ((r & 7) < 6) & ((r & 63) < 24)
    out = mm(a, jnp.where(hit, 1.0, 0.0).astype(BF16))
    for k in range(3):
        mine[pl.ds(k, 6, stride=4), :] = out[0:6, 128 * k : 128 * k + 128]


def image3(ref, s_ref, r, n):
    lane = lanes(n)
    c = ref[pl.ds(r, n), :]
    b = ref[pl.ds(r + 4, n), :] + ref[pl.ds(r - 4, n), :]
    b = b + (roll(c, 1) + roll(c, -1))
    b = b + roll(jnp.where(lane < 32, ref[pl.ds(r + 1, n), :], c), -32)
    b = b + roll(jnp.where(lane >= 96, ref[pl.ds(r - 1, n), :], c), 32)
    return c, FACTOR3 * (6.0 * c - b) + s_ref[pl.ds(r, n), :] * c


def chunks3(rows, ref, body):
    n = min(rows, 384)

    def step(i, carry):
        r = pl.multiple_of(GUARD3 + i * n, 8)
        ref[pl.ds(r, n), :] = body(r, n)
        return carry

    lax.fori_loop(0, rows // n, step, 0)


def match4(k, shape, coarse_dim, ny):
    c = iota2(shape, coarse_dim)
    l = iota2(shape, 1 - coarse_dim)
    return ((c >> 4) == 2 * k + (l >> 6)) & ((c & 15) == ((l & 31) >> 1)) & ((l & 31) < ny)


def restrict4(src, n, ny):
    total = None
    for k in range(3):
        t = src[pl.ds(GUARD3 + k, n, stride=8), :] + src[pl.ds(GUARD3 + k + 4, n, stride=8), :]
        part = mm(t, jnp.where(match4(k, (128, 128), 1, ny), 0.125, 0.0).astype(BF16))
        total = part if total is None else total + part
    return total


def dot_all(a, b):
    return jnp.sum(jnp.sum(a * b, axis=0, keepdims=True), axis=1, keepdims=True)


def bottom(source, s4, p4, n, ny):
    estimate = jnp.zeros_like(source)
    left = source
    inside = (lanes(n) < 96) & ((lanes(n) & 15) < ny)
    shifted = 6.0 * FACTOR4 + s4[...]
    for it in range(BOTTOM_ITERS):
        p4[pl.ds(GUARD, n), :] = left
        b = p4[pl.ds(GUARD + 1, n), :] + p4[pl.ds(GUARD - 1, n), :]
        b = b + (roll(left, 1) + roll(left, -1))
        b = b + (roll(left, 16) + roll(left, -16))
        image = shifted * left - FACTOR4 * jnp.where(inside, b, 0.0)
        now = dot_all(left, left)
        bent = dot_all(left, image)
        if it == 0:
            denom = bent
            direction, turned = left, image
        else:
            ratio = now * inv_before
            denom = bent - ratio * ratio * denom
            direction = left + ratio * direction
            turned = image + ratio * turned
        step = now / denom
        inv_before = 1.0 / now
        estimate = estimate + step * direction
        if it < BOTTOM_ITERS - 1:
            left = left - step * turned
    return estimate


PLAN_A = Plan([Item(L0, 3), Item(L0, 2), Item(L0, 2)])
PLAN_S = Plan([Item(L1, 6), Item(L2, 5)])
PLAN_B = Plan([Item(L1, 6)])
PLAN_BX = Plan([Item(L1, 6)], True)
PLAN_C = Plan([Item(L0, 3)])
PLAN_D = Plan([Item(L2, 5)])
PLANS = (PLAN_A, PLAN_S, PLAN_B, PLAN_C, PLAN_D, PLAN_BX)


def far(p, sizes):
    ring = lambda d, n: min(d % n, -d % n)
    return p[0] + ring(p[1], sizes[1]) + ring(p[2], 4) + ring(p[2] // 4, 4)


def kernel(sizes, counts, right_in, guess_in, react_in, guess, r0, eb0, left0, step_out, *scratch):
    scratch = list(scratch)

    def take(n):
        out = scratch[:n]
        del scratch[:n]
        return out

    raw = take(3)
    (in_sems,) = take(1)
    right, react, inv0, ea0 = take(4)
    f1, s1, inv1, ea1, eb1, left1 = take(6)
    f2, s2, inv2, ea2, eb2, left2 = take(6)
    f3, s3, inv3, ea3, eb3, left3 = take(6)
    s4, p4, down_m, up_m, tmp, square, turned, spread, slab = take(9)
    scr = [take(n) for n in counts]
    place = Place(sizes)
    gx, gy, gz = place.me
    n3, n4, ny3 = 24 * sizes[2], 3 * sizes[2], 6 * sizes[1]

    inputs = (guess_in, right_in, react_in)
    for k in range(3):
        for q in range(4):
            at = pl.ds(12 * q, 12)
            pltpu.make_async_copy(inputs[k].at[at], raw[k].at[at], in_sems.at[k]).start()

    def clear(ref):
        n = ref.shape[0]
        size = next(k for k in (128, 122 * 8, 80, 8) if n % k == 0) if n > 128 else n
        size = {1808: 904, 976: 488, 416: 208}.get(n, size)

        def step(i, carry):
            ref[pl.ds(pl.multiple_of(i * size, 8), size), :] = jnp.zeros((size, 128), F32)
            return carry

        lax.fori_loop(0, n // size, step, 0)

    peers = [(a, b, c) for a in range(sizes[0]) for b in range(sizes[1]) for c in range(sizes[2])][1:]
    peers.sort(key=lambda p: -far(p, sizes))
    beside = {(a, b % sizes[1], c % sizes[2]) for a in range(2) for b in (1, -1) for c in (1, -1)}
    beside |= {(1, 0, c % sizes[2]) for c in (1, -1)}
    greeted = [p for p in peers if p[2] == 0 or p[:2] == (0, 0) or p in beside]
    barrier = pltpu.get_barrier_semaphore()
    for p in greeted:
        pl.semaphore_signal(barrier, inc=1, device_id=place.beside(*p), device_id_type=MESH)
    for ref in (guess, right, react, f1, s1, ea1, eb1, f2, s2, ea2, eb2, ea3, eb3, p4, square):
        clear(ref)
    spread[...] = jnp.zeros_like(spread)
    for ref in (f3, s3, inv3):
        for r in (0, GUARD3 + n3):
            ref[pl.ds(r, GUARD3), :] = jnp.zeros((GUARD3, 128), F32)

    a = iota2((128, 128), 0)
    b = iota2((128, 128), 1)
    signed = lambda v: ((v + 8) & 63) - 8
    base = lambda v: ((v + 8) & 127) & 64
    zb = signed(b)
    hit = ((a == ((base(b) + 2 * zb) & 127)) | (a == ((base(b) + 2 * zb + 1) & 127))) & (zb >= -8) & (zb < 24)
    down_m[...] = jnp.where(hit, 0.125, 0.0).astype(BF16)
    hit = a == ((base(b) + (zb >> 1)) & 127)
    up_m[...] = jnp.where(hit, 1.0, 0.0).astype(BF16)

    for k, dst in enumerate((guess, right, react)):
        pltpu.make_async_copy(inputs[k], raw[k], in_sems.at[k]).wait()

        for i in range(24):
            dst[pl.ds(L0.row(i, 0), 48), 0:48] = raw[k][i]
            dst[pl.ds(L0.row(i, 0), 48), 64:112] = raw[k][i + 24]

    ex_a = Exchange(PLAN_A, (guess, right, react), scr[0], place)
    ex_s = Exchange(PLAN_S, (s1, s2), scr[1], place)
    ex_b = Exchange(PLAN_B, (f1,), scr[2], place)
    ex_c = Exchange(PLAN_C, (eb0,), scr[3], place)
    ex_d = Exchange(PLAN_D, (f2,), scr[4], place)
    cx_b = Cross(PLAN_BX, ex_b, scr[5], place)
    ga_s = Gather(place, scr[6], s3)
    ga_f = Gather(place, scr[7], f3)
    reduced, red_send, red_recv = scr[8]

    ex_a.pack()
    pl.semaphore_wait(barrier, len(greeted))
    ex_a.send()

    restrict(react, L0, s1, L1, 0, 12, 0, 24, down_m, tmp)
    restrict(s1, L1, s2, L2, 0, 6, 0, 12, down_m, tmp)
    ex_s.pack()
    ga_s.mine[...] = jnp.zeros((24, 128), F32)
    ga_f.mine[...] = jnp.zeros((24, 128), F32)
    to_level3(s2, ga_s.mine, square, turned, place)

    def start(r):
        at = pl.ds(r, L0.R)
        c, image = image_of(guess, react, L0, r)
        res = right[at, :] - image
        inv = inverse(react[at, :], 1.0)
        return [(r0, res), (inv0, inv), (ea0, inv * res)]

    ex_a.unpack()
    ex_a.x_send()
    ex_s.send()
    ga_s.send()
    ex_a.unpack_rest()
    planes(L0, 1, 23, start)
    ex_a.x_wait()
    ex_a.x_fill()
    planes(L0, -2, 1, start)
    planes(L0, 23, 26, start)
    relax(L0, ea0, eb0, r0, react, inv0, -1, 25)
    leftover(L0, eb0, left0, r0, react, 0, 24)
    restrict(left0, L0, f1, L1, 0, 12, 0, 24, down_m, tmp)
    ex_b.pack_send()
    cx_b.pack_send()
    ex_b.x_send()

    ex_c.pack()
    ex_s.unpack()
    ex_s.x_send()
    ex_s.x_wait()
    ex_s.x_fill()
    for g, sh, inv in ((L1, s1, inv1), (L2, s2, inv2)):
        planes(g, -g.halo, g.nx + g.halo, lambda r: [(inv, inverse(sh[pl.ds(r, g.R), :], g.factor))])
    ga_s.relay()

    ex_b.x_sent()
    ex_b.unpack()
    ex_c.send()
    first(L1, ea1, f1, inv1, 0, 12)
    relax(L1, ea1, eb1, f1, s1, inv1, 1, 11)
    ex_b.x_wait()
    cx_b.unpack()
    ex_b.x_fill()
    first(L1, ea1, f1, inv1, -6, 0)
    first(L1, ea1, f1, inv1, 12, 18)
    relax(L1, ea1, eb1, f1, s1, inv1, -5, 1)
    relax(L1, ea1, eb1, f1, s1, inv1, 11, 17)
    leftover(L1, eb1, left1, f1, s1, -4, 16)
    restrict(left1, L1, f2, L2, -2, 8, -2, 16, down_m, tmp)
    first(L2, ea2, f2, inv2, -2, 8)
    relax(L2, ea2, eb2, f2, s2, inv2, -1, 7)
    leftover(L2, eb2, left2, f2, s2, 0, 6)
    to_level3(left2, ga_f.mine, square, turned, place)
    ga_f.send()
    ex_d.pack_send()

    ex_c.unpack()
    ex_c.x_send()
    ex_c.unpack_rest()
    ga_f.relay()
    ex_d.unpack()
    ex_d.x_send()
    ex_c.x_wait()
    ex_c.x_fill()
    ex_d.x_wait()
    ex_d.x_fill()
    first(L2, ea2, f2, inv2, -5, 11)
    relax(L2, ea2, eb2, f2, s2, inv2, -4, 10)
    ga_s.finish()
    chunks3(n3, inv3, lambda r, n: inverse(s3[pl.ds(r, n), :], FACTOR3))
    s4[...] = restrict4(s3, n4, ny3)
    for e in (ex_a, ex_s, ex_c, ex_d, ga_s):
        e.settle()
    for e in (ex_b, cx_b):
        e.settle(False)
    ga_f.finish()

    def relax3(src, dst):
        def body(r, n):
            c, image = image3(src, s3, r, n)
            at = pl.ds(r, n)
            return c + inv3[at, :] * (f3[at, :] - image)

        chunks3(n3, dst, body)

    chunks3(n3, ea3, lambda r, n: inv3[pl.ds(r, n), :] * f3[pl.ds(r, n), :])
    relax3(ea3, eb3)
    chunks3(n3, left3, lambda r, n: f3[pl.ds(r, n), :] - image3(eb3, s3, r, n)[1])
    e4 = bottom(restrict4(left3, n4, ny3), s4, p4, n4, ny3 // 2)
    for k in range(3):
        u = mm(e4, jnp.where(match4(k, (128, 128), 0, ny3), 1.0, 0.0).astype(BF16))
        for q in (k, k + 4):
            at = pl.ds(GUARD3 + q, n4, stride=8)
            eb3[at, :] = eb3[at, :] + u
    for src, dst, n in ((eb3, ea3, 48), (ea3, slab, 40)):
        r = pl.multiple_of(GUARD3 + 24 * gz - (n - 24) // 2, 4)
        c, image = image3(src, s3, r, n)
        at = pl.ds(r, n)
        dst[at if n == 48 else pl.ds(0, n), :] = c + inv3[at, :] * (f3[at, :] - image)
    for k in range(3):
        v = slab[pl.ds(k, 10, stride=4), :]
        for h in range(2):
            for q in range(2):
                spread[k, pl.ds(64 * h + q, 10, stride=2), :] = v
    wide = [jnp.concatenate(p, axis=1) for p in zip(*[split(spread[k]) for k in range(3)])]
    coarse = []
    for h in range(2):
        r = iota2((112, 384), 0)
        l = iota2((112, 384), 1)
        hit = (6 * gx + 3 * h + (r >> 4) - 2 == (l >> 5)) & (6 * gy + (r & 15) - 2 == (l & 31)) & ((r & 15) < 10)
        pick = jnp.where(hit, 1.0, 0.0).astype(BF16)
        parts = [
            lax.dot_general(pick, p, (((1,), (1,)), ((), ())), preferred_element_type=F32) for p in wide
        ]
        coarse.append(parts[0] + parts[1])
    fine = roll(jnp.where(lanes(112) < 64, coarse[0], coarse[1]), -4)
    for i in range(7):
        u = fine[16 * i : 16 * i + 10]
        tmp[pl.ds(24 * i, 10, stride=2), :] = u
        tmp[pl.ds(24 * i + 1, 10, stride=2), :] = u
    for i in range(7):
        v = tmp[pl.ds(24 * i, 20), :]
        for q in range(2):
            at = pl.ds(L2.row(2 * (i - 2) + q, -4), 20)
            eb2[at, :] = eb2[at, :] + v
    relax(L2, eb2, ea2, f2, s2, inv2, -3, 9)
    relax(L2, ea2, eb2, f2, s2, inv2, -2, 8)
    prolong(eb2, L2, eb1, L1, -2, 8, -2, 16, up_m, tmp)
    relax(L1, eb1, ea1, f1, s1, inv1, -3, 15)
    relax(L1, ea1, eb1, f1, s1, inv1, -2, 14)
    prolong(eb1, L1, eb0, L0, -2, 14, -2, 28, up_m, tmp)
    relax(L0, eb0, ea0, r0, react, inv0, -2, 26)
    relax(L0, ea0, eb0, r0, react, inv0, -1, 25)

    row = iota2((L0.R, 128), 0)
    inside = ((lanes(L0.R) & 63) < 48) & (row >= L0.y0) & (row < L0.y0 + 48)

    upper, lower = [], []
    for i in range(24):
        r = GUARD + (L0.halo + i) * L0.R
        c, image = image_of(eb0, react, L0, r)
        left0[pl.ds(r, L0.R), :] = image
        upper.append(c * r0[pl.ds(r, L0.R), :])
        lower.append(c * image)
    upper = jnp.where(inside, tree(upper), 0.0)
    lower = jnp.where(inside, tree(lower), 0.0)
    upper = jnp.sum(upper, axis=0, keepdims=True)
    lower = jnp.sum(lower, axis=0, keepdims=True)
    half = lanes(1) < 64
    number = (gx * sizes[1] + gy) * sizes[2] + gz
    reduced[number] = jnp.where(half, upper + roll(upper, 64), lower + roll(lower, 64))
    own = reduced.at[number]

    def summed(src, dst, p):
        return pltpu.make_async_remote_copy(
            src_ref=src, dst_ref=dst, send_sem=red_send.at[0], recv_sem=red_recv.at[0],
            device_id=place.beside(*p), device_id_type=MESH,
        )

    for p in peers:
        summed(own, own, p).start()
    ga_f.settle()
    most = reduced.at[pl.ds(0, len(peers))]
    summed(most, most, peers[0]).wait()
    sums = [reduced[k] for k in range(8)]
    for k in range(8, len(peers) + 1):
        sums[k % 8] = sums[k % 8] + reduced[k]
    total = tree(sums)
    upper = jnp.sum(jnp.where(half, total, 0.0), axis=1, keepdims=True)
    lower = jnp.sum(jnp.where(half, 0.0, total), axis=1, keepdims=True)
    step_out[...] = jnp.broadcast_to(upper / lower, (8, 128))


def finish(guess, r0, eb0, left0, step_ref, field_out, resid_out, field, resid, sems):
    step = step_ref[0:1, :]
    copies = []
    parts, size = 4, 6
    for p in range(parts):
        for x in range(p * size, p * size + size):
            at = pl.ds(L0.row(x, 0), 48)
            v = guess[at, :] + step * eb0[at, :]
            field[x] = v[:, 0:48]
            field[x + 24] = roll(v, 64)[:, 0:48]
            v = r0[at, :] - step * left0[at, :]
            resid[x] = v[:, 0:48]
            resid[x + 24] = roll(v, 64)[:, 0:48]
        for q, (src, dst) in enumerate(((field, field_out), (resid, resid_out))):
            for h in range(2):
                at = pl.ds(p * size + 24 * h, size)
                c = pltpu.make_async_copy(src.at[at], dst.at[at], sems.at[4 * p + 2 * q + h])
                c.start()
                copies.append(c)
    for c in copies:
        c.wait()


def solution(mesh):
    sizes = tuple(mesh.shape[a] for a in ("gx", "gy", "gz"))
    n3, n4 = 24 * sizes[2] + 2 * GUARD3, 3 * sizes[2]
    scratch = [pltpu.VMEM((48, 48, 48), F32)] * 3 + [pltpu.SemaphoreType.DMA((3,))]
    scratch += [pltpu.VMEM((L0.total, 128), F32)] * 4
    scratch += [pltpu.VMEM((L1.total, 128), F32)] * 6
    scratch += [pltpu.VMEM((L2.total, 128), F32)] * 6
    scratch += [pltpu.VMEM((n3, 128), F32)] * 6
    scratch += [pltpu.VMEM((n4, 128), F32), pltpu.VMEM((n4 + 2 * GUARD, 128), F32)]
    scratch += [pltpu.VMEM((128, 128), BF16)] * 2 + [pltpu.VMEM((16 * 56, 128), F32)]
    scratch += [pltpu.VMEM((128, 128), F32)] * 2
    scratch += [pltpu.VMEM((3, 128, 128), F32), pltpu.VMEM((40, 128), F32)]
    groups = [p.scratch() for p in PLANS] + [gather_scratch(sizes)] * 2
    devices = sizes[0] * sizes[1] * sizes[2]
    groups += [[pltpu.VMEM((devices, 1, 128), F32)] + [pltpu.SemaphoreType.DMA((1,))] * 2]
    for g in groups:
        scratch += g
    counts = tuple(len(g) for g in groups)
    vmem = pl.BlockSpec(memory_space=pltpu.VMEM)

    anywhere = pl.BlockSpec(memory_space=pl.ANY)

    def body(right_side, start_guess, reaction):
        whole = pltpu.VMEM((L0.total, 128), F32)
        parts = pl.pallas_call(
            functools.partial(kernel, sizes, counts),
            out_shape=[whole] * 4 + [pltpu.VMEM((8, 128), F32)],
            in_specs=[anywhere] * 3,
            out_specs=[vmem] * 5,
            scratch_shapes=scratch,
            compiler_params=pltpu.CompilerParams(
                collective_id=0, has_side_effects=True, vmem_limit_bytes=60 * 2**20
            ),
        )(right_side, start_guess, reaction)
        shape = jax.ShapeDtypeStruct(right_side.shape, F32)
        return tuple(
            pl.pallas_call(
                finish,
                out_shape=[shape, shape],
                in_specs=[vmem] * 5,
                out_specs=[anywhere] * 2,
                scratch_shapes=[pltpu.VMEM(right_side.shape, F32)] * 2 + [pltpu.SemaphoreType.DMA((16,))],
                compiler_params=pltpu.CompilerParams(vmem_limit_bytes=16 * 2**20),
            )(*parts)
        )

    placed = P("gx", "gy", "gz")
    return jax.shard_map(
        body, mesh=mesh, in_specs=(placed,) * 3, out_specs=(placed,) * 2, check_vma=False
    )
```

```python
import functools

import jax
import jax.numpy as jnp
from jax import lax
from jax.experimental import pallas as pl
from jax.experimental.pallas import tpu as pltpu
from jax.sharding import PartitionSpec as P

MESH = pl.DeviceIdType.MESH
F32 = jnp.float32
BF16 = jnp.bfloat16
DAMP = 6.0 / 7.0
GUARD = 8
GUARD3 = 16
BOTTOM_ITERS = 6


class Geo:
    def __init__(self, nx, ny, nz, halo, rows, y0, depth, unroll):
        self.nx, self.ny, self.nz, self.halo, self.R, self.y0 = nx, ny, nz, halo, rows, y0
        self.factor = 0.25**depth
        self.unroll = unroll
        self.total = 2 * GUARD + (nx + 2 * halo) * rows

    def row(self, x, y):
        return GUARD + (self.halo + x) * self.R + self.y0 + y


L0 = Geo(24, 48, 48, 4, 56, 4, 0, 28)
L1 = Geo(12, 24, 24, 6, 40, 8, 1, 24)
L2 = Geo(6, 12, 12, 5, 24, 6, 2, 16)
FACTOR3 = 0.25**3
FACTOR4 = 0.25**4


def lanes(rows):
    return lax.broadcasted_iota(jnp.int32, (rows, 128), 1)


def iota2(shape, dim):
    return lax.broadcasted_iota(jnp.int32, shape, dim)


def tree(terms):
    while len(terms) > 1:
        terms = [sum(terms[k + 1 : k + 2], terms[k]) for k in range(0, len(terms), 2)]
    return terms[0]


def roll(v, shift):
    shift = shift % 128
    return v if shift == 0 else pltpu.roll(v, shift, 1)


def split(a):
    hi = a.astype(BF16)
    return hi, (a - hi.astype(F32)).astype(BF16)


def mm(a, b):
    hi, low = split(a)
    return jnp.dot(hi, b, preferred_element_type=F32) + jnp.dot(low, b, preferred_element_type=F32)


def beside_of(ref, r, R):
    c = ref[pl.ds(r, R), :]
    b = ref[pl.ds(r + R, R), :] + ref[pl.ds(r - R, R), :]
    b = b + (ref[pl.ds(r + 1, R), :] + ref[pl.ds(r - 1, R), :])
    b = b + (roll(c, 1) + roll(c, -1))
    return c, b


def image_of(ref, s_ref, g, r):
    c, b = beside_of(ref, r, g.R)
    return c, g.factor * (6.0 * c - b) + s_ref[pl.ds(r, g.R), :] * c


def planes(g, a, b, body):
    unroll = g.unroll

    def group(start, count):
        todo = []
        for k in range(count):
            r = start + k * g.R
            r = r if isinstance(r, int) else pl.multiple_of(r, 8)
            todo.append((r, body(r)))
        for r, pairs in todo:
            for ref, value in pairs:
                ref[pl.ds(r, g.R), :] = value

    trips = (b - a) // unroll
    origin = GUARD + (g.halo + a) * g.R
    if trips == 1:
        group(origin, unroll)
    elif trips:

        def step(i, carry):
            group(pl.multiple_of(origin + i * (unroll * g.R), 8), unroll)
            return carry

        lax.fori_loop(0, trips, step, 0)
    if (b - a) % unroll:
        group(origin + trips * unroll * g.R, (b - a) % unroll)


def inverse(s, factor):
    return jnp.where(s > 0.0, DAMP / (6.0 * factor + s), 0.0)


def relax(g, src, dst, f, s, inv, a, b):
    def body(r):
        c, image = image_of(src, s, g, r)
        at = pl.ds(r, g.R)
        return [(dst, c + inv[at, :] * (f[at, :] - image))]

    planes(g, a, b, body)


def first(g, dst, f, inv, a, b):
    def body(r):
        at = pl.ds(r, g.R)
        return [(dst, inv[at, :] * f[at, :])]

    planes(g, a, b, body)


def leftover(g, src, dst, f, s, a, b):
    def body(r):
        c, image = image_of(src, s, g, r)
        return [(dst, f[pl.ds(r, g.R), :] - image)]

    planes(g, a, b, body)


def restrict(src, gs, dst, gd, x0, x1, y0, count, matrix, tmp):
    step = -(-count // 8) * 8
    for x in range(x0, x1):
        r = gs.row(2 * x, 2 * y0)
        t = src[pl.ds(r, count, stride=2), :] + src[pl.ds(r + 1, count, stride=2), :]
        r = r + gs.R
        t = t + (src[pl.ds(r, count, stride=2), :] + src[pl.ds(r + 1, count, stride=2), :])
        tmp[pl.ds((x - x0) * step, count), :] = t
    for x in range(x0, x1):
        out = mm(tmp[pl.ds((x - x0) * step, step), :], matrix[...])
        dst[pl.ds(gd.row(x, y0), count), :] = out[0:count]


def prolong(src, gc, dst, gf, x0, x1, y0, count, matrix, tmp):
    for x in range(x0, x1):
        o = (x - x0) * 56
        u = mm(src[pl.ds(gc.row(x, y0), count), :], matrix[...])
        tmp[pl.ds(o, count, stride=2), :] = u
        tmp[pl.ds(o + 1, count, stride=2), :] = u
    for x in range(x0, x1):
        o = (x - x0) * 56
        v = tmp[pl.ds(o, 2 * count), :]
        for k in range(2):
            at = pl.ds(gf.row(2 * x + k, 2 * y0), 2 * count)
            dst[at, :] = dst[at, :] + v


class Item:
    def __init__(self, geo, w):
        self.g, self.w = geo, w


class Plan:
    def __init__(self, items, cross=False):
        self.items, self.cross = items, cross
        self.counts = [it.w if cross else it.g.nx for it in items]
        self.yrows = sum(n * it.w for n, it in zip(self.counts, items))
        self.yrows = -(-self.yrows // 8) * 8
        self.tiles = []
        for k, it in enumerate(items):
            for x in range(self.counts[k]):
                for t in self.tiles:
                    if t[0] is it.g and t[1] + it.w <= 64:
                        break
                else:
                    t = [it.g, 0, []]
                    self.tiles.append(t)
                t[2].append((k, x, t[1]))
                t[1] += it.w
        self.zrows = sum(t[0].ny for t in self.tiles)
        self.zrows = -(-self.zrows // 8) * 8
        self.drows = max(self.counts)
        self.drows = -(-self.drows // 8) * 8
        assert sum(it.w * it.w for it in items) <= 64

        self.z0 = [0, self.zrows]
        self.d0 = [2 * self.zrows + q * self.drows for q in range(4)]
        self.y0 = [2 * self.zrows + 4 * self.drows + q * self.yrows for q in range(2)]
        self.total = 2 * (self.zrows + self.yrows) + 4 * self.drows
        self.xtotal = sum(it.w * it.g.R for it in items)

    def scratch(self):
        x = [] if self.cross else [pltpu.VMEM((self.xtotal, 128), F32)]
        return x + [
            pltpu.VMEM((self.total, 128), F32),
            pltpu.VMEM((self.total, 128), F32),
            pltpu.SemaphoreType.DMA((2,)),
            pltpu.SemaphoreType.DMA((2,)),
        ]


class Exchange:
    def __init__(self, plan, refs, scratch, place):
        self.plan, self.refs, self.place = plan, refs, place
        self.xr, self.sent, self.got, self.ss, self.rs = scratch
        gx, gy, gz = place.me
        self.partner = (1 - gx, gy, gz)
        self.x_copies = []
        o = 0
        for k, it in enumerate(plan.items):
            r = pl.multiple_of(GUARD + (it.g.halo + self.edge(it)) * it.g.R, 8)
            n = it.w * it.g.R
            self.x_copies.append(self.copy(refs[k].at[pl.ds(r, n), :], self.xr.at[pl.ds(o, n), :], 0, self.partner))
            o += n
        self.segments(0)

    def edge(self, it):
        return jnp.where(self.place.me[0] == 0, it.g.nx - it.w, 0)

    def source(self, k, x, y):
        return self.plan.items[k].g.row(x, y)

    def target(self, k, x, y):
        return self.refs[k], self.plan.items[k].g.row(x, y)

    def segments(self, dx):
        plan = self.plan
        at = {}
        for d in range(2):
            at[1 - 2 * d, 0] = plan.y0[d]
            at[0, 1 - 2 * d] = plan.z0[d]
            for e in range(2):
                at[1 - 2 * d, 1 - 2 * e] = plan.d0[2 * d + e]
        self.y_copies, self.z_copies, self.d_copies = [], [], []
        for d in (1, -1):
            self.y_copies.append(self.segment(at, dx, d, 0, plan.yrows))
            self.z_copies.append(self.segment(at, dx, 0, d, plan.zrows))
            for e in (1, -1):
                self.d_copies.append(self.segment(at, dx, d, e, plan.drows))

    def segment(self, at, dx, dy, dz, n):
        there = self.place.exists(dy, dz)
        peer = self.place.beside(dx, dy, dz)
        peer = tuple(jnp.where(there, p, q) for p, q in zip(peer, self.partner))
        target = pl.multiple_of(jnp.where(there, at[dy, dz], at[-dy, -dz]), 8)
        return self.copy(self.sent.at[pl.ds(at[dy, dz], n), :], self.got.at[pl.ds(target, n), :], 1, peer)

    def copy(self, src, dst, k, peer):
        return pltpu.make_async_remote_copy(
            src_ref=src, dst_ref=dst, send_sem=self.ss.at[k], recv_sem=self.rs.at[k],
            device_id=peer, device_id_type=MESH,
        )

    def x_send(self):
        for c in self.x_copies:
            c.start()

    def settle(self, x=True):
        if x:
            self.x_sent()
        self.copy(self.sent, self.got, 1, self.partner).wait_send()

    def x_sent(self):
        self.copy(self.xr, self.xr, 0, self.partner).wait_send()

    def x_wait(self):
        self.copy(self.xr, self.xr, 0, self.partner).wait_recv()

    def x_fill(self):
        m0, m1 = self.place.x_masks
        o = 0
        for k, it in enumerate(self.plan.items):
            g, w, ref = it.g, it.w, self.refs[k]
            upper = ((lanes(g.R) + 8) & 127) >= 64
            for j in range(w):
                got = self.xr[pl.ds(o + j * g.R, g.R), :]
                top = ref[pl.ds(GUARD + (g.halo + g.nx - w + j) * g.R, g.R), :]
                low = ref[pl.ds(GUARD + (g.halo + j) * g.R, g.R), :]
                ref[pl.ds(GUARD + (g.halo - w + j) * g.R, g.R), :] = roll(jnp.where(upper, got * m1, top), 64)
                ref[pl.ds(GUARD + (g.halo + g.nx + j) * g.R, g.R), :] = roll(jnp.where(upper, low, got * m0), 64)
            o += w * g.R

    def pack_send(self):
        self.pack()
        self.send()

    def pack(self):
        for k in range(len(self.refs)):
            self.pack_item(k)

    def send(self):
        for c in self.d_copies + self.z_copies + self.y_copies:
            c.start()

    def pack_item(self, k):
        if k == 0:
            self.yo, self.co, self.corner = 0, 0, [None] * 4
        it = self.plan.items[k]
        g, w, ref = it.g, it.w, self.refs[k]
        n = self.plan.counts[k]
        lane = lanes(self.plan.drows) & 63
        for d in range(1, w + 1):
            at = self.co + (d - 1) * w
            for e, y in enumerate((g.ny - d, d - 1)):
                v = ref[pl.ds(self.source(k, 0, y), n, stride=g.R), :]
                self.sent[pl.ds(self.plan.y0[e] + self.yo, n), :] = v
                if n < self.plan.drows:
                    v = jnp.concatenate([v, jnp.zeros((self.plan.drows - n, 128), F32)], axis=0)
                for q, z in enumerate((g.nz - w, 0)):
                    moved = roll(v, at - z)
                    old = self.corner[2 * e + q]
                    self.corner[2 * e + q] = moved if old is None else jnp.where(lane >= at, moved, old)
            self.yo += n
        self.co += w * w
        if k == len(self.refs) - 1:
            for q in range(4):
                self.sent[pl.ds(self.plan.d0[q], self.plan.drows), :] = self.corner[q]
        zo = 0
        for t, _, slots in self.plan.tiles:
            if slots[-1][0] == k:
                self.pack_tile(t, slots, zo)
            zo += t.ny

    def pack_tile(self, g, slots, zo):
        lane = lanes(g.ny)
        acc = [None, None]
        for k, x, at in slots:
            w = self.plan.items[k].w
            moved = roll(self.refs[k][pl.ds(self.source(k, x, 0), g.ny), :], at)
            for q, past in enumerate((g.nz - w, 0)):
                here = ((lane - past) & 63 >= at) & ((lane - past) & 63 < at + w)
                acc[q] = moved if acc[q] is None else jnp.where(here, moved, acc[q])
        for q in range(2):
            self.sent[pl.ds(self.plan.z0[q] + zo, g.ny), :] = acc[q]

    def unpack(self):
        my, mz = self.place.y_masks, self.place.z_masks
        self.copy(self.sent, self.got, 1, self.partner).wait_recv()
        yo, co = 0, 0
        for k, it in enumerate(self.plan.items):
            g, w = it.g, it.w
            n = self.plan.counts[k]
            lane = lanes(n) & 63
            into = (lane >= 64 - w, (lane >= g.nz) & (lane < g.nz + w))
            for d in range(1, w + 1):
                at = co + (d - 1) * w
                for e, y in enumerate((-d, g.ny + d - 1)):
                    v = self.got[pl.ds(self.plan.y0[e] + yo, n), :]
                    for q, z in enumerate((-w, g.nz)):
                        got = self.got[pl.ds(self.plan.d0[2 * e + q], n), :] * mz[q]
                        v = jnp.where(into[q], roll(got, z - at), v)
                    ref, r = self.target(k, 0, y)
                    ref[pl.ds(r, n, stride=g.R), :] = v * my[e]
                yo += n
            co += w * w
        self.unpack_z(True)

    def unpack_rest(self):
        self.unpack_z(False)

    def unpack_z(self, edge):
        mz = self.place.z_masks
        zo = 0
        for g, _, slots in self.plan.tiles:
            lane = lanes(g.ny) & 63
            got = [self.got[pl.ds(self.plan.z0[q] + zo, g.ny), :] * mz[q] for q in range(2)]
            for k, x, at in slots:
                w = self.plan.items[k].w
                if (x < w or x >= g.nx - w) != edge:
                    continue
                ref, r = self.target(k, x, 0)
                rows = pl.ds(r, g.ny)
                v = ref[rows, :]
                v = jnp.where(lane >= 64 - w, roll(got[0], -g.nz - at), v)
                v = jnp.where((lane >= g.nz) & (lane < g.nz + w), roll(got[1], g.nz - at), v)
                ref[rows, :] = v
            zo += g.ny


class Cross(Exchange):
    def __init__(self, plan, main, scratch, place):
        self.plan, self.main, self.refs, self.place = plan, main, main.refs, place
        self.sent, self.got, self.ss, self.rs = scratch
        self.partner = main.partner
        self.segments(1)

    def source(self, k, x, y):
        it = self.plan.items[k]
        return GUARD + (it.g.halo + self.edge(it) + x) * it.g.R + it.g.y0 + y

    def target(self, k, x, y):
        o = sum(it.w * it.g.R for it in self.plan.items[:k])
        g = self.plan.items[k].g
        return self.main.xr, o + x * g.R + g.y0 + y


class Place:
    def __init__(self, sizes):
        self.sizes = sizes
        self.me = tuple(lax.axis_index(a) for a in ("gx", "gy", "gz"))
        gx, gy, gz = self.me
        one = lambda c: jnp.where(c, 1.0, 0.0).astype(F32)
        self.x_masks = (one(gx == 0), one(gx == 1))
        self.y_masks = (one(gy > 0), one(gy < sizes[1] - 1))
        self.z_masks = (one(gz > 0), one(gz < sizes[2] - 1))

    def exists(self, dy, dz):
        gx, gy, gz = self.me
        y, z = gy + dy, gz + dz
        return (y >= 0) & (y < self.sizes[1]) & (z >= 0) & (z < self.sizes[2])

    def beside(self, dx, dy, dz):
        return tuple(
            lax.rem(m + d % n, n) if d % n else m for m, d, n in zip(self.me, (dx, dy, dz), self.sizes)
        )


class Gather:
    rows = 24

    def __init__(self, place, scratch, whole):
        self.place, self.whole = place, whole
        self.mine, self.got, self.sum, self.ss, self.rs = scratch
        n = place.sizes
        self.near = [(a, b) for a in range(n[0]) for b in range(n[1])][1:]
        self.near.sort(key=lambda p: -far((p[0], p[1], 0), n))
        self.line = sorted(range(1, n[2]), key=lambda c: -far((0, 0, c), n))
        self.at = pl.ds(pl.multiple_of(GUARD3 + self.rows * place.me[2], 8), self.rows)

    def copy(self, src, dst, k, peer):
        return pltpu.make_async_remote_copy(
            src_ref=src, dst_ref=dst, send_sem=self.ss.at[k], recv_sem=self.rs.at[k],
            device_id=peer, device_id_type=MESH,
        )

    def send(self):
        for k, (a, b) in enumerate(self.near):
            self.copy(self.mine, self.got.at[k], 0, self.place.beside(a, b, 0)).start()

    def relay(self):
        self.copy(self.got, self.got, 0, self.place.beside(1, 0, 0)).wait_recv()
        total = self.mine[...]
        for k in range(len(self.near)):
            total = total + self.got[k]
        self.sum[...] = total
        for c in self.line:
            self.copy(self.sum, self.whole.at[self.at, :], 1, self.place.beside(0, 0, c)).start()
        self.whole[self.at, :] = total

    def finish(self):
        self.most().wait_recv()

    def most(self):
        most = self.whole.at[pl.ds(GUARD3, self.rows * (self.place.sizes[2] - 1)), :]
        return self.copy(most, most, 1, self.place.beside(1, 0, 0))

    def settle(self):
        self.copy(self.got, self.got, 0, self.place.beside(1, 0, 0)).wait_send()
        self.most().wait_send()


def gather_scratch(sizes):
    return [
        pltpu.VMEM((24, 128), F32),
        pltpu.VMEM((sizes[0] * sizes[1] - 1, 24, 128), F32),
        pltpu.VMEM((24, 128), F32),
        pltpu.SemaphoreType.DMA((2,)),
        pltpu.SemaphoreType.DMA((2,)),
    ]


def to_level3(src, mine, square, turned, place):
    g = L2
    gx, gy, gz = place.me
    for i in range(3):
        r = g.row(2 * i, 0)
        t = src[pl.ds(r, 6, stride=2), :] + src[pl.ds(r + 1, 6, stride=2), :]
        r = r + g.R
        t = t + (src[pl.ds(r, 6, stride=2), :] + src[pl.ds(r + 1, 6, stride=2), :])
        square[pl.ds(8 * i, 6), :] = t
    turned[...] = jnp.transpose(square[...])
    a = turned[pl.ds(0, 8, stride=2), :] + turned[pl.ds(1, 8, stride=2), :]
    b = turned[pl.ds(64, 8, stride=2), :] + turned[pl.ds(65, 8, stride=2), :]
    a = (a + roll(b, 64)) * 0.125
    r = iota2((128, 384), 0)
    l = iota2((128, 384), 1)
    x = 6 * gx + 3 * (r >> 6) + ((r & 63) >> 3)
    y = 6 * gy + (r & 7)
    hit = (x == (l >> 5)) & (y == (l & 31)) & ((r & 7) < 6) & ((r & 63) < 24)
    out = mm(a, jnp.where(hit, 1.0, 0.0).astype(BF16))
    for k in range(3):
        mine[pl.ds(k, 6, stride=4), :] = out[0:6, 128 * k : 128 * k + 128]


def image3(ref, s_ref, r, n):
    lane = lanes(n)
    c = ref[pl.ds(r, n), :]
    b = ref[pl.ds(r + 4, n), :] + ref[pl.ds(r - 4, n), :]
    b = b + (roll(c, 1) + roll(c, -1))
    b = b + roll(jnp.where(lane < 32, ref[pl.ds(r + 1, n), :], c), -32)
    b = b + roll(jnp.where(lane >= 96, ref[pl.ds(r - 1, n), :], c), 32)
    return c, FACTOR3 * (6.0 * c - b) + s_ref[pl.ds(r, n), :] * c


def chunks3(rows, ref, body):
    n = min(rows, 384)

    def step(i, carry):
        r = pl.multiple_of(GUARD3 + i * n, 8)
        ref[pl.ds(r, n), :] = body(r, n)
        return carry

    lax.fori_loop(0, rows // n, step, 0)


def match4(k, shape, coarse_dim, ny):
    c = iota2(shape, coarse_dim)
    l = iota2(shape, 1 - coarse_dim)
    return ((c >> 4) == 2 * k + (l >> 6)) & ((c & 15) == ((l & 31) >> 1)) & ((l & 31) < ny)


def restrict4(src, n, ny):
    total = None
    for k in range(3):
        t = src[pl.ds(GUARD3 + k, n, stride=8), :] + src[pl.ds(GUARD3 + k + 4, n, stride=8), :]
        part = mm(t, jnp.where(match4(k, (128, 128), 1, ny), 0.125, 0.0).astype(BF16))
        total = part if total is None else total + part
    return total


def dot_all(a, b):
    return jnp.sum(jnp.sum(a * b, axis=0, keepdims=True), axis=1, keepdims=True)


def bottom(source, s4, p4, n, ny):
    estimate = jnp.zeros_like(source)
    left = source
    inside = (lanes(n) < 96) & ((lanes(n) & 15) < ny)
    shifted = 6.0 * FACTOR4 + s4[...]
    for it in range(BOTTOM_ITERS):
        p4[pl.ds(GUARD, n), :] = left
        b = p4[pl.ds(GUARD + 1, n), :] + p4[pl.ds(GUARD - 1, n), :]
        b = b + (roll(left, 1) + roll(left, -1))
        b = b + (roll(left, 16) + roll(left, -16))
        image = shifted * left - FACTOR4 * jnp.where(inside, b, 0.0)
        now = dot_all(left, left)
        bent = dot_all(left, image)
        if it == 0:
            denom = bent
            direction, turned = left, image
        else:
            ratio = now * inv_before
            denom = bent - ratio * ratio * denom
            direction = left + ratio * direction
            turned = image + ratio * turned
        step = now / denom
        inv_before = 1.0 / now
        estimate = estimate + step * direction
        if it < BOTTOM_ITERS - 1:
            left = left - step * turned
    return estimate


PLAN_A = Plan([Item(L0, 3), Item(L0, 2), Item(L0, 2)])
PLAN_S = Plan([Item(L1, 6), Item(L2, 5)])
PLAN_B = Plan([Item(L1, 6)])
PLAN_BX = Plan([Item(L1, 6)], True)
PLAN_C = Plan([Item(L0, 3)])
PLAN_D = Plan([Item(L2, 5)])
PLANS = (PLAN_A, PLAN_S, PLAN_B, PLAN_C, PLAN_D, PLAN_BX)


def far(p, sizes):
    ring = lambda d, n: min(d % n, -d % n)
    return p[0] + ring(p[1], sizes[1]) + ring(p[2], 4) + ring(p[2] // 4, 4)


def kernel(sizes, counts, right_in, guess_in, react_in, guess, r0, eb0, left0, step_out, *scratch):
    scratch = list(scratch)

    def take(n):
        out = scratch[:n]
        del scratch[:n]
        return out

    raw = take(3)
    (in_sems,) = take(1)
    right, react, inv0, ea0 = take(4)
    f1, s1, inv1, ea1, eb1, left1 = take(6)
    f2, s2, inv2, ea2, eb2, left2 = take(6)
    f3, s3, inv3, ea3, eb3, left3 = take(6)
    s4, p4, down_m, up_m, tmp, square, turned, spread, slab = take(9)
    scr = [take(n) for n in counts]
    place = Place(sizes)
    gx, gy, gz = place.me
    n3, n4, ny3 = 24 * sizes[2], 3 * sizes[2], 6 * sizes[1]

    inputs = (guess_in, right_in, react_in)
    for k in range(3):
        for q in range(4):
            at = pl.ds(12 * q, 12)
            pltpu.make_async_copy(inputs[k].at[at], raw[k].at[at], in_sems.at[k]).start()

    def clear(ref):
        n = ref.shape[0]
        size = next(k for k in (128, 122 * 8, 80, 8) if n % k == 0) if n > 128 else n
        size = {1808: 904, 976: 488, 416: 208}.get(n, size)

        def step(i, carry):
            ref[pl.ds(pl.multiple_of(i * size, 8), size), :] = jnp.zeros((size, 128), F32)
            return carry

        lax.fori_loop(0, n // size, step, 0)

    peers = [(a, b, c) for a in range(sizes[0]) for b in range(sizes[1]) for c in range(sizes[2])][1:]
    peers.sort(key=lambda p: -far(p, sizes))
    beside = {(a, b % sizes[1], c % sizes[2]) for a in range(2) for b in (1, -1) for c in (1, -1)}
    beside |= {(1, 0, c % sizes[2]) for c in (1, -1)}
    greeted = [p for p in peers if p[2] == 0 or p[:2] == (0, 0) or p in beside]
    barrier = pltpu.get_barrier_semaphore()
    for p in greeted:
        pl.semaphore_signal(barrier, inc=1, device_id=place.beside(*p), device_id_type=MESH)
    for ref in (guess, right, react, f1, s1, ea1, eb1, f2, s2, ea2, eb2, ea3, eb3, p4, square):
        clear(ref)
    spread[...] = jnp.zeros_like(spread)
    for ref in (f3, s3, inv3):
        for r in (0, GUARD3 + n3):
            ref[pl.ds(r, GUARD3), :] = jnp.zeros((GUARD3, 128), F32)

    a = iota2((128, 128), 0)
    b = iota2((128, 128), 1)
    signed = lambda v: ((v + 8) & 63) - 8
    base = lambda v: ((v + 8) & 127) & 64
    zb = signed(b)
    hit = ((a == ((base(b) + 2 * zb) & 127)) | (a == ((base(b) + 2 * zb + 1) & 127))) & (zb >= -8) & (zb < 24)
    down_m[...] = jnp.where(hit, 0.125, 0.0).astype(BF16)
    hit = a == ((base(b) + (zb >> 1)) & 127)
    up_m[...] = jnp.where(hit, 1.0, 0.0).astype(BF16)

    ex_a = Exchange(PLAN_A, (guess, right, react), scr[0], place)
    ex_s = Exchange(PLAN_S, (s1, s2), scr[1], place)
    ex_b = Exchange(PLAN_B, (f1,), scr[2], place)
    ex_c = Exchange(PLAN_C, (eb0,), scr[3], place)
    ex_d = Exchange(PLAN_D, (f2,), scr[4], place)
    cx_b = Cross(PLAN_BX, ex_b, scr[5], place)
    ga_s = Gather(place, scr[6], s3)
    ga_f = Gather(place, scr[7], f3)
    for k, dst in enumerate((guess, right, react)):
        pltpu.make_async_copy(inputs[k], raw[k], in_sems.at[k]).wait()

        for i in range(24):
            dst[pl.ds(L0.row(i, 0), 48), 0:48] = raw[k][i]
            dst[pl.ds(L0.row(i, 0), 48), 64:112] = raw[k][i + 24]
        ex_a.pack_item(k)

    reduced, red_send, red_recv = scr[8]

    pl.semaphore_wait(barrier, len(greeted))
    ex_a.send()

    restrict(react, L0, s1, L1, 0, 12, 0, 24, down_m, tmp)
    restrict(s1, L1, s2, L2, 0, 6, 0, 12, down_m, tmp)
    ex_s.pack()
    ga_s.mine[...] = jnp.zeros((24, 128), F32)
    ga_f.mine[...] = jnp.zeros((24, 128), F32)
    to_level3(s2, ga_s.mine, square, turned, place)

    def start(r):
        at = pl.ds(r, L0.R)
        c, image = image_of(guess, react, L0, r)
        res = right[at, :] - image
        inv = inverse(react[at, :], 1.0)
        return [(r0, res), (inv0, inv), (ea0, inv * res)]

    ex_a.unpack()
    ex_a.x_send()
    ex_s.send()
    ga_s.send()
    ex_a.unpack_rest()
    planes(L0, 1, 23, start)
    ex_a.x_wait()
    ex_a.x_fill()
    planes(L0, -2, 1, start)
    planes(L0, 23, 26, start)
    relax(L0, ea0, eb0, r0, react, inv0, -1, 25)
    leftover(L0, eb0, left0, r0, react, 0, 24)
    restrict(left0, L0, f1, L1, 0, 12, 0, 24, down_m, tmp)
    ex_b.pack_send()
    cx_b.pack_send()
    ex_b.x_send()

    ex_c.pack()
    ex_s.unpack()
    ex_s.x_send()

    def inverse_of(g, sh, inv, first_plane, end):
        planes(g, first_plane, end, lambda r: [(inv, inverse(sh[pl.ds(r, g.R), :], g.factor))])

    inverse_of(L1, s1, inv1, 0, 12)
    ga_s.relay()

    ex_b.x_sent()
    ex_b.unpack()
    ex_c.send()
    first(L1, ea1, f1, inv1, 0, 12)
    relax(L1, ea1, eb1, f1, s1, inv1, 1, 11)
    ex_s.x_wait()
    ex_s.x_fill()
    inverse_of(L1, s1, inv1, -6, 0)
    inverse_of(L1, s1, inv1, 12, 18)
    inverse_of(L2, s2, inv2, -5, 11)
    ex_b.x_wait()
    cx_b.unpack()
    ex_b.x_fill()
    first(L1, ea1, f1, inv1, -6, 0)
    first(L1, ea1, f1, inv1, 12, 18)
    relax(L1, ea1, eb1, f1, s1, inv1, -5, 1)
    relax(L1, ea1, eb1, f1, s1, inv1, 11, 17)
    leftover(L1, eb1, left1, f1, s1, -4, 16)
    restrict(left1, L1, f2, L2, -2, 8, -2, 16, down_m, tmp)
    first(L2, ea2, f2, inv2, -2, 8)
    relax(L2, ea2, eb2, f2, s2, inv2, -1, 7)
    leftover(L2, eb2, left2, f2, s2, 0, 6)
    to_level3(left2, ga_f.mine, square, turned, place)
    ga_f.send()
    ex_d.pack_send()

    ga_f.relay()
    ex_c.unpack()
    ex_c.x_send()
    ex_c.unpack_rest()
    ex_d.unpack()
    ex_d.x_send()
    ex_c.x_wait()
    ex_c.x_fill()
    ex_d.x_wait()
    ex_d.x_fill()
    first(L2, ea2, f2, inv2, -5, 11)
    relax(L2, ea2, eb2, f2, s2, inv2, -4, 10)
    ga_s.finish()
    chunks3(n3, inv3, lambda r, n: inverse(s3[pl.ds(r, n), :], FACTOR3))
    s4[...] = restrict4(s3, n4, ny3)
    for e in (ex_a, ex_s, ex_c, ex_d, ga_s):
        e.settle()
    for e in (ex_b, cx_b):
        e.settle(False)
    ga_f.finish()

    def relax3(src, dst):
        def body(r, n):
            c, image = image3(src, s3, r, n)
            at = pl.ds(r, n)
            return c + inv3[at, :] * (f3[at, :] - image)

        chunks3(n3, dst, body)

    chunks3(n3, ea3, lambda r, n: inv3[pl.ds(r, n), :] * f3[pl.ds(r, n), :])
    relax3(ea3, eb3)
    chunks3(n3, left3, lambda r, n: f3[pl.ds(r, n), :] - image3(eb3, s3, r, n)[1])
    e4 = bottom(restrict4(left3, n4, ny3), s4, p4, n4, ny3 // 2)
    for k in range(3):
        u = mm(e4, jnp.where(match4(k, (128, 128), 0, ny3), 1.0, 0.0).astype(BF16))
        for q in (k, k + 4):
            at = pl.ds(GUARD3 + q, n4, stride=8)
            eb3[at, :] = eb3[at, :] + u
    for src, dst, n in ((eb3, ea3, 48), (ea3, slab, 40)):
        r = pl.multiple_of(GUARD3 + 24 * gz - (n - 24) // 2, 4)
        c, image = image3(src, s3, r, n)
        at = pl.ds(r, n)
        dst[at if n == 48 else pl.ds(0, n), :] = c + inv3[at, :] * (f3[at, :] - image)
    for k in range(3):
        v = slab[pl.ds(k, 10, stride=4), :]
        for h in range(2):
            for q in range(2):
                spread[k, pl.ds(64 * h + q, 10, stride=2), :] = v
    wide = [jnp.concatenate(p, axis=1) for p in zip(*[split(spread[k]) for k in range(3)])]
    coarse = []
    for h in range(2):
        r = iota2((112, 384), 0)
        l = iota2((112, 384), 1)
        hit = (6 * gx + 3 * h + (r >> 4) - 2 == (l >> 5)) & (6 * gy + (r & 15) - 2 == (l & 31)) & ((r & 15) < 10)
        pick = jnp.where(hit, 1.0, 0.0).astype(BF16)
        parts = [
            lax.dot_general(pick, p, (((1,), (1,)), ((), ())), preferred_element_type=F32) for p in wide
        ]
        coarse.append(parts[0] + parts[1])
    fine = roll(jnp.where(lanes(112) < 64, coarse[0], coarse[1]), -4)
    for i in range(7):
        u = fine[16 * i : 16 * i + 10]
        tmp[pl.ds(24 * i, 10, stride=2), :] = u
        tmp[pl.ds(24 * i + 1, 10, stride=2), :] = u
    for i in range(7):
        v = tmp[pl.ds(24 * i, 20), :]
        for q in range(2):
            at = pl.ds(L2.row(2 * (i - 2) + q, -4), 20)
            eb2[at, :] = eb2[at, :] + v
    relax(L2, eb2, ea2, f2, s2, inv2, -3, 9)
    relax(L2, ea2, eb2, f2, s2, inv2, -2, 8)
    prolong(eb2, L2, eb1, L1, -2, 8, -2, 16, up_m, tmp)
    relax(L1, eb1, ea1, f1, s1, inv1, -3, 15)
    relax(L1, ea1, eb1, f1, s1, inv1, -2, 14)
    prolong(eb1, L1, eb0, L0, -2, 14, -2, 28, up_m, tmp)
    relax(L0, eb0, ea0, r0, react, inv0, -2, 26)
    relax(L0, ea0, eb0, r0, react, inv0, -1, 25)

    row = iota2((L0.R, 128), 0)
    inside = ((lanes(L0.R) & 63) < 48) & (row >= L0.y0) & (row < L0.y0 + 48)

    upper, lower = [], []
    for i in range(24):
        r = GUARD + (L0.halo + i) * L0.R
        c, image = image_of(eb0, react, L0, r)
        left0[pl.ds(r, L0.R), :] = image
        upper.append(c * r0[pl.ds(r, L0.R), :])
        lower.append(c * image)
    upper = jnp.where(inside, tree(upper), 0.0)
    lower = jnp.where(inside, tree(lower), 0.0)
    upper = jnp.sum(upper, axis=0, keepdims=True)
    lower = jnp.sum(lower, axis=0, keepdims=True)
    half = lanes(1) < 64
    number = (gx * sizes[1] + gy) * sizes[2] + gz
    reduced[number] = jnp.where(half, upper + roll(upper, 64), lower + roll(lower, 64))
    own = reduced.at[number]

    def summed(src, dst, p):
        return pltpu.make_async_remote_copy(
            src_ref=src, dst_ref=dst, send_sem=red_send.at[0], recv_sem=red_recv.at[0],
            device_id=place.beside(*p), device_id_type=MESH,
        )

    for p in peers:
        summed(own, own, p).start()
    ga_f.settle()
    most = reduced.at[pl.ds(0, len(peers))]
    summed(most, most, peers[0]).wait()
    sums = [reduced[k] for k in range(8)]
    for k in range(8, len(peers) + 1):
        sums[k % 8] = sums[k % 8] + reduced[k]
    total = tree(sums)
    upper = jnp.sum(jnp.where(half, total, 0.0), axis=1, keepdims=True)
    lower = jnp.sum(jnp.where(half, 0.0, total), axis=1, keepdims=True)
    step_out[...] = jnp.broadcast_to(upper / lower, (8, 128))


def finish(guess, r0, eb0, left0, step_ref, field_out, resid_out, field, resid, sems):
    step = step_ref[0:1, :]
    copies = []
    parts, size = 4, 6
    for p in range(parts):
        for x in range(p * size, p * size + size):
            at = pl.ds(L0.row(x, 0), 48)
            v = guess[at, :] + step * eb0[at, :]
            field[x] = v[:, 0:48]
            field[x + 24] = roll(v, 64)[:, 0:48]
            v = r0[at, :] - step * left0[at, :]
            resid[x] = v[:, 0:48]
            resid[x + 24] = roll(v, 64)[:, 0:48]
        for q, (src, dst) in enumerate(((field, field_out), (resid, resid_out))):
            for h in range(2):
                at = pl.ds(p * size + 24 * h, size)
                c = pltpu.make_async_copy(src.at[at], dst.at[at], sems.at[4 * p + 2 * q + h])
                c.start()
                copies.append(c)
    for c in copies:
        c.wait()


def solution(mesh):
    sizes = tuple(mesh.shape[a] for a in ("gx", "gy", "gz"))
    n3, n4 = 24 * sizes[2] + 2 * GUARD3, 3 * sizes[2]
    scratch = [pltpu.VMEM((48, 48, 48), F32)] * 3 + [pltpu.SemaphoreType.DMA((3,))]
    scratch += [pltpu.VMEM((L0.total, 128), F32)] * 4
    scratch += [pltpu.VMEM((L1.total, 128), F32)] * 6
    scratch += [pltpu.VMEM((L2.total, 128), F32)] * 6
    scratch += [pltpu.VMEM((n3, 128), F32)] * 6
    scratch += [pltpu.VMEM((n4, 128), F32), pltpu.VMEM((n4 + 2 * GUARD, 128), F32)]
    scratch += [pltpu.VMEM((128, 128), BF16)] * 2 + [pltpu.VMEM((16 * 56, 128), F32)]
    scratch += [pltpu.VMEM((128, 128), F32)] * 2
    scratch += [pltpu.VMEM((3, 128, 128), F32), pltpu.VMEM((40, 128), F32)]
    groups = [p.scratch() for p in PLANS] + [gather_scratch(sizes)] * 2
    devices = sizes[0] * sizes[1] * sizes[2]
    groups += [[pltpu.VMEM((devices, 1, 128), F32)] + [pltpu.SemaphoreType.DMA((1,))] * 2]
    for g in groups:
        scratch += g
    counts = tuple(len(g) for g in groups)
    vmem = pl.BlockSpec(memory_space=pltpu.VMEM)

    anywhere = pl.BlockSpec(memory_space=pl.ANY)

    def body(right_side, start_guess, reaction):
        whole = pltpu.VMEM((L0.total, 128), F32)
        parts = pl.pallas_call(
            functools.partial(kernel, sizes, counts),
            out_shape=[whole] * 4 + [pltpu.VMEM((8, 128), F32)],
            in_specs=[anywhere] * 3,
            out_specs=[vmem] * 5,
            scratch_shapes=scratch,
            compiler_params=pltpu.CompilerParams(
                collective_id=0, has_side_effects=True, vmem_limit_bytes=60 * 2**20
            ),
        )(right_side, start_guess, reaction)
        shape = jax.ShapeDtypeStruct(right_side.shape, F32)
        return tuple(
            pl.pallas_call(
                finish,
                out_shape=[shape, shape],
                in_specs=[vmem] * 5,
                out_specs=[anywhere] * 2,
                scratch_shapes=[pltpu.VMEM(right_side.shape, F32)] * 2 + [pltpu.SemaphoreType.DMA((16,))],
                compiler_params=pltpu.CompilerParams(vmem_limit_bytes=16 * 2**20),
            )(*parts)
        )

    placed = P("gx", "gy", "gz")
    return jax.shard_map(
        body, mesh=mesh, in_specs=(placed,) * 3, out_specs=(placed,) * 2, check_vma=False
    )
```

```python
import functools

import jax
import jax.numpy as jnp
from jax import lax
from jax.experimental import pallas as pl
from jax.experimental.pallas import tpu as pltpu
from jax.sharding import PartitionSpec as P

MESH = pl.DeviceIdType.MESH
F32 = jnp.float32
BF16 = jnp.bfloat16
DAMP = 6.0 / 7.0
GUARD = 8
GUARD3 = 16
BOTTOM_ITERS = 6


class Geo:
    def __init__(self, nx, ny, nz, halo, rows, y0, depth, unroll):
        self.nx, self.ny, self.nz, self.halo, self.R, self.y0 = nx, ny, nz, halo, rows, y0
        self.factor = 0.25**depth
        self.unroll = unroll
        self.total = 2 * GUARD + (nx + 2 * halo) * rows

    def row(self, x, y):
        return GUARD + (self.halo + x) * self.R + self.y0 + y


L0 = Geo(24, 48, 48, 4, 56, 4, 0, 28)
L1 = Geo(12, 24, 24, 6, 40, 8, 1, 24)
L2 = Geo(6, 12, 12, 5, 24, 6, 2, 16)
FACTOR3 = 0.25**3
FACTOR4 = 0.25**4


def lanes(rows):
    return lax.broadcasted_iota(jnp.int32, (rows, 128), 1)


def iota2(shape, dim):
    return lax.broadcasted_iota(jnp.int32, shape, dim)


def tree(terms):
    while len(terms) > 1:
        terms = [sum(terms[k + 1 : k + 2], terms[k]) for k in range(0, len(terms), 2)]
    return terms[0]


def roll(v, shift):
    shift = shift % 128
    return v if shift == 0 else pltpu.roll(v, shift, 1)


def split(a):
    hi = a.astype(BF16)
    return hi, (a - hi.astype(F32)).astype(BF16)


def mm(a, b):
    hi, low = split(a)
    return jnp.dot(hi, b, preferred_element_type=F32) + jnp.dot(low, b, preferred_element_type=F32)


def beside_of(ref, r, R):
    c = ref[pl.ds(r, R), :]
    b = ref[pl.ds(r + R, R), :] + ref[pl.ds(r - R, R), :]
    b = b + (ref[pl.ds(r + 1, R), :] + ref[pl.ds(r - 1, R), :])
    b = b + (roll(c, 1) + roll(c, -1))
    return c, b


def image_of(ref, s_ref, g, r):
    c, b = beside_of(ref, r, g.R)
    return c, g.factor * (6.0 * c - b) + s_ref[pl.ds(r, g.R), :] * c


def planes(g, a, b, body):
    unroll = g.unroll

    def group(start, count):
        todo = []
        for k in range(count):
            r = start + k * g.R
            r = r if isinstance(r, int) else pl.multiple_of(r, 8)
            todo.append((r, body(r)))
        for r, pairs in todo:
            for ref, value in pairs:
                ref[pl.ds(r, g.R), :] = value

    trips = (b - a) // unroll
    origin = GUARD + (g.halo + a) * g.R
    if trips == 1:
        group(origin, unroll)
    elif trips:

        def step(i, carry):
            group(pl.multiple_of(origin + i * (unroll * g.R), 8), unroll)
            return carry

        lax.fori_loop(0, trips, step, 0)
    if (b - a) % unroll:
        group(origin + trips * unroll * g.R, (b - a) % unroll)


def inverse(s, factor):
    return jnp.where(s > 0.0, DAMP / (6.0 * factor + s), 0.0)


def relax(g, src, dst, f, s, inv, a, b):
    def body(r):
        c, image = image_of(src, s, g, r)
        at = pl.ds(r, g.R)
        return [(dst, c + inv[at, :] * (f[at, :] - image))]

    planes(g, a, b, body)


def first(g, dst, f, inv, a, b):
    def body(r):
        at = pl.ds(r, g.R)
        return [(dst, inv[at, :] * f[at, :])]

    planes(g, a, b, body)


def leftover(g, src, dst, f, s, a, b):
    def body(r):
        c, image = image_of(src, s, g, r)
        return [(dst, f[pl.ds(r, g.R), :] - image)]

    planes(g, a, b, body)


def restrict(src, gs, dst, gd, x0, x1, y0, count, matrix, tmp):
    step = -(-count // 8) * 8
    for x in range(x0, x1):
        r = gs.row(2 * x, 2 * y0)
        t = src[pl.ds(r, count, stride=2), :] + src[pl.ds(r + 1, count, stride=2), :]
        r = r + gs.R
        t = t + (src[pl.ds(r, count, stride=2), :] + src[pl.ds(r + 1, count, stride=2), :])
        tmp[pl.ds((x - x0) * step, count), :] = t
    for x in range(x0, x1):
        out = mm(tmp[pl.ds((x - x0) * step, step), :], matrix[...])
        dst[pl.ds(gd.row(x, y0), count), :] = out[0:count]


def prolong(src, gc, dst, gf, x0, x1, y0, count, matrix, tmp):
    for x in range(x0, x1):
        o = (x - x0) * 56
        u = mm(src[pl.ds(gc.row(x, y0), count), :], matrix[...])
        tmp[pl.ds(o, count, stride=2), :] = u
        tmp[pl.ds(o + 1, count, stride=2), :] = u
    for x in range(x0, x1):
        o = (x - x0) * 56
        v = tmp[pl.ds(o, 2 * count), :]
        for k in range(2):
            at = pl.ds(gf.row(2 * x + k, 2 * y0), 2 * count)
            dst[at, :] = dst[at, :] + v


class Item:
    def __init__(self, geo, w):
        self.g, self.w = geo, w


class Plan:
    def __init__(self, items, cross=False):
        self.items, self.cross = items, cross
        self.counts = [it.w if cross else it.g.nx for it in items]
        self.yrows = sum(n * it.w for n, it in zip(self.counts, items))
        self.yrows = -(-self.yrows // 8) * 8
        self.tiles = []
        for k, it in enumerate(items):
            for x in range(self.counts[k]):
                for t in self.tiles:
                    if t[0] is it.g and t[1] + it.w <= 64:
                        break
                else:
                    t = [it.g, 0, []]
                    self.tiles.append(t)
                t[2].append((k, x, t[1]))
                t[1] += it.w
        self.zrows = sum(t[0].ny for t in self.tiles)
        self.zrows = -(-self.zrows // 8) * 8
        self.drows = max(self.counts)
        self.drows = -(-self.drows // 8) * 8
        assert sum(it.w * it.w for it in items) <= 64

        self.z0 = [0, self.zrows]
        self.d0 = [2 * self.zrows + q * self.drows for q in range(4)]
        self.y0 = [2 * self.zrows + 4 * self.drows + q * self.yrows for q in range(2)]
        self.total = 2 * (self.zrows + self.yrows) + 4 * self.drows
        self.xtotal = sum(it.w * it.g.R for it in items)

    def scratch(self):
        x = [] if self.cross else [pltpu.VMEM((self.xtotal, 128), F32)]
        return x + [
            pltpu.VMEM((self.total, 128), F32),
            pltpu.VMEM((self.total, 128), F32),
            pltpu.SemaphoreType.DMA((2,)),
            pltpu.SemaphoreType.DMA((2,)),
        ]


class Exchange:
    def __init__(self, plan, refs, scratch, place):
        self.plan, self.refs, self.place = plan, refs, place
        self.xr, self.sent, self.got, self.ss, self.rs = scratch
        gx, gy, gz = place.me
        self.partner = (1 - gx, gy, gz)
        self.x_copies = []
        o = 0
        for k, it in enumerate(plan.items):
            r = pl.multiple_of(GUARD + (it.g.halo + self.edge(it)) * it.g.R, 8)
            n = it.w * it.g.R
            self.x_copies.append(self.copy(refs[k].at[pl.ds(r, n), :], self.xr.at[pl.ds(o, n), :], 0, self.partner))
            o += n
        self.segments(0)

    def edge(self, it):
        return jnp.where(self.place.me[0] == 0, it.g.nx - it.w, 0)

    def source(self, k, x, y):
        return self.plan.items[k].g.row(x, y)

    def target(self, k, x, y):
        return self.refs[k], self.plan.items[k].g.row(x, y)

    def segments(self, dx):
        plan = self.plan
        at = {}
        for d in range(2):
            at[1 - 2 * d, 0] = plan.y0[d]
            at[0, 1 - 2 * d] = plan.z0[d]
            for e in range(2):
                at[1 - 2 * d, 1 - 2 * e] = plan.d0[2 * d + e]
        self.y_copies, self.z_copies, self.d_copies = [], [], []
        for d in (1, -1):
            self.y_copies.append(self.segment(at, dx, d, 0, plan.yrows))
            self.z_copies.append(self.segment(at, dx, 0, d, plan.zrows))
            for e in (1, -1):
                self.d_copies.append(self.segment(at, dx, d, e, plan.drows))

    def segment(self, at, dx, dy, dz, n):
        there = self.place.exists(dy, dz)
        peer = self.place.beside(dx, dy, dz)
        peer = tuple(jnp.where(there, p, q) for p, q in zip(peer, self.partner))
        target = pl.multiple_of(jnp.where(there, at[dy, dz], at[-dy, -dz]), 8)
        return self.copy(self.sent.at[pl.ds(at[dy, dz], n), :], self.got.at[pl.ds(target, n), :], 1, peer)

    def copy(self, src, dst, k, peer):
        return pltpu.make_async_remote_copy(
            src_ref=src, dst_ref=dst, send_sem=self.ss.at[k], recv_sem=self.rs.at[k],
            device_id=peer, device_id_type=MESH,
        )

    def x_send(self):
        for c in self.x_copies:
            c.start()

    def settle(self, x=True):
        if x:
            self.x_sent()
        self.copy(self.sent, self.got, 1, self.partner).wait_send()

    def x_sent(self):
        self.copy(self.xr, self.xr, 0, self.partner).wait_send()

    def x_wait(self):
        self.copy(self.xr, self.xr, 0, self.partner).wait_recv()

    def x_fill(self):
        m0, m1 = self.place.x_masks
        o = 0
        for k, it in enumerate(self.plan.items):
            g, w, ref = it.g, it.w, self.refs[k]
            upper = ((lanes(g.R) + 8) & 127) >= 64
            for j in range(w):
                got = self.xr[pl.ds(o + j * g.R, g.R), :]
                top = ref[pl.ds(GUARD + (g.halo + g.nx - w + j) * g.R, g.R), :]
                low = ref[pl.ds(GUARD + (g.halo + j) * g.R, g.R), :]
                ref[pl.ds(GUARD + (g.halo - w + j) * g.R, g.R), :] = roll(jnp.where(upper, got * m1, top), 64)
                ref[pl.ds(GUARD + (g.halo + g.nx + j) * g.R, g.R), :] = roll(jnp.where(upper, low, got * m0), 64)
            o += w * g.R

    def pack_send(self):
        self.pack()
        self.send()

    def pack(self):
        for k in range(len(self.refs)):
            self.pack_item(k)

    def send(self):
        for c in self.d_copies + self.z_copies + self.y_copies:
            c.start()

    def pack_item(self, k):
        if k == 0:
            self.yo, self.co, self.corner = 0, 0, [None] * 4
        it = self.plan.items[k]
        g, w, ref = it.g, it.w, self.refs[k]
        n = self.plan.counts[k]
        lane = lanes(self.plan.drows) & 63
        for d in range(1, w + 1):
            at = self.co + (d - 1) * w
            for e, y in enumerate((g.ny - d, d - 1)):
                v = ref[pl.ds(self.source(k, 0, y), n, stride=g.R), :]
                self.sent[pl.ds(self.plan.y0[e] + self.yo, n), :] = v
                if n < self.plan.drows:
                    v = jnp.concatenate([v, jnp.zeros((self.plan.drows - n, 128), F32)], axis=0)
                for q, z in enumerate((g.nz - w, 0)):
                    moved = roll(v, at - z)
                    old = self.corner[2 * e + q]
                    self.corner[2 * e + q] = moved if old is None else jnp.where(lane >= at, moved, old)
            self.yo += n
        self.co += w * w
        if k == len(self.refs) - 1:
            for q in range(4):
                self.sent[pl.ds(self.plan.d0[q], self.plan.drows), :] = self.corner[q]
        zo = 0
        for t, _, slots in self.plan.tiles:
            if slots[-1][0] == k:
                self.pack_tile(t, slots, zo)
            zo += t.ny

    def pack_tile(self, g, slots, zo):
        lane = lanes(g.ny)
        acc = [None, None]
        for k, x, at in slots:
            w = self.plan.items[k].w
            moved = roll(self.refs[k][pl.ds(self.source(k, x, 0), g.ny), :], at)
            for q, past in enumerate((g.nz - w, 0)):
                here = ((lane - past) & 63 >= at) & ((lane - past) & 63 < at + w)
                acc[q] = moved if acc[q] is None else jnp.where(here, moved, acc[q])
        for q in range(2):
            self.sent[pl.ds(self.plan.z0[q] + zo, g.ny), :] = acc[q]

    def unpack(self):
        my, mz = self.place.y_masks, self.place.z_masks
        self.copy(self.sent, self.got, 1, self.partner).wait_recv()
        yo, co = 0, 0
        for k, it in enumerate(self.plan.items):
            g, w = it.g, it.w
            n = self.plan.counts[k]
            lane = lanes(n) & 63
            into = (lane >= 64 - w, (lane >= g.nz) & (lane < g.nz + w))
            for d in range(1, w + 1):
                at = co + (d - 1) * w
                for e, y in enumerate((-d, g.ny + d - 1)):
                    v = self.got[pl.ds(self.plan.y0[e] + yo, n), :]
                    for q, z in enumerate((-w, g.nz)):
                        got = self.got[pl.ds(self.plan.d0[2 * e + q], n), :] * mz[q]
                        v = jnp.where(into[q], roll(got, z - at), v)
                    ref, r = self.target(k, 0, y)
                    ref[pl.ds(r, n, stride=g.R), :] = v * my[e]
                yo += n
            co += w * w
        self.unpack_z(True)

    def unpack_rest(self):
        self.unpack_z(False)

    def unpack_z(self, edge):
        mz = self.place.z_masks
        zo = 0
        for g, _, slots in self.plan.tiles:
            lane = lanes(g.ny) & 63
            got = [self.got[pl.ds(self.plan.z0[q] + zo, g.ny), :] * mz[q] for q in range(2)]
            for k, x, at in slots:
                w = self.plan.items[k].w
                if (x < w or x >= g.nx - w) != edge:
                    continue
                ref, r = self.target(k, x, 0)
                rows = pl.ds(r, g.ny)
                v = ref[rows, :]
                v = jnp.where(lane >= 64 - w, roll(got[0], -g.nz - at), v)
                v = jnp.where((lane >= g.nz) & (lane < g.nz + w), roll(got[1], g.nz - at), v)
                ref[rows, :] = v
            zo += g.ny


class Cross(Exchange):
    def __init__(self, plan, main, scratch, place):
        self.plan, self.main, self.refs, self.place = plan, main, main.refs, place
        self.sent, self.got, self.ss, self.rs = scratch
        self.partner = main.partner
        self.segments(1)

    def source(self, k, x, y):
        it = self.plan.items[k]
        return GUARD + (it.g.halo + self.edge(it) + x) * it.g.R + it.g.y0 + y

    def target(self, k, x, y):
        o = sum(it.w * it.g.R for it in self.plan.items[:k])
        g = self.plan.items[k].g
        return self.main.xr, o + x * g.R + g.y0 + y


class Place:
    def __init__(self, sizes):
        self.sizes = sizes
        self.me = tuple(lax.axis_index(a) for a in ("gx", "gy", "gz"))
        gx, gy, gz = self.me
        one = lambda c: jnp.where(c, 1.0, 0.0).astype(F32)
        self.x_masks = (one(gx == 0), one(gx == 1))
        self.y_masks = (one(gy > 0), one(gy < sizes[1] - 1))
        self.z_masks = (one(gz > 0), one(gz < sizes[2] - 1))

    def exists(self, dy, dz):
        gx, gy, gz = self.me
        y, z = gy + dy, gz + dz
        return (y >= 0) & (y < self.sizes[1]) & (z >= 0) & (z < self.sizes[2])

    def beside(self, dx, dy, dz):
        return tuple(
            lax.rem(m + d % n, n) if d % n else m for m, d, n in zip(self.me, (dx, dy, dz), self.sizes)
        )


class Gather:
    rows = 24

    def __init__(self, place, scratch, whole):
        self.place, self.whole = place, whole
        self.mine, self.got, self.sum, self.ss, self.rs = scratch
        n = place.sizes
        self.near = [(a, b) for a in range(n[0]) for b in range(n[1])][1:]
        self.near.sort(key=lambda p: -far((p[0], p[1], 0), n))
        self.line = sorted(range(1, n[2]), key=lambda c: -far((0, 0, c), n))
        self.at = pl.ds(pl.multiple_of(GUARD3 + self.rows * place.me[2], 8), self.rows)

    def copy(self, src, dst, k, peer):
        return pltpu.make_async_remote_copy(
            src_ref=src, dst_ref=dst, send_sem=self.ss.at[k], recv_sem=self.rs.at[k],
            device_id=peer, device_id_type=MESH,
        )

    def send(self):
        for k, (a, b) in enumerate(self.near):
            self.copy(self.mine, self.got.at[k], 0, self.place.beside(a, b, 0)).start()

    def relay(self):
        self.copy(self.got, self.got, 0, self.place.beside(1, 0, 0)).wait_recv()
        total = self.mine[...]
        for k in range(len(self.near)):
            total = total + self.got[k]
        self.sum[...] = total
        for c in self.line:
            self.copy(self.sum, self.whole.at[self.at, :], 1, self.place.beside(0, 0, c)).start()
        self.whole[self.at, :] = total

    def finish(self):
        self.most().wait_recv()

    def most(self):
        most = self.whole.at[pl.ds(GUARD3, self.rows * (self.place.sizes[2] - 1)), :]
        return self.copy(most, most, 1, self.place.beside(1, 0, 0))

    def settle(self):
        self.copy(self.got, self.got, 0, self.place.beside(1, 0, 0)).wait_send()
        self.most().wait_send()


def gather_scratch(sizes):
    return [
        pltpu.VMEM((24, 128), F32),
        pltpu.VMEM((sizes[0] * sizes[1] - 1, 24, 128), F32),
        pltpu.VMEM((24, 128), F32),
        pltpu.SemaphoreType.DMA((2,)),
        pltpu.SemaphoreType.DMA((2,)),
    ]


def to_level3(src, mine, square, turned, place):
    g = L2
    gx, gy, gz = place.me
    for i in range(3):
        r = g.row(2 * i, 0)
        t = src[pl.ds(r, 6, stride=2), :] + src[pl.ds(r + 1, 6, stride=2), :]
        r = r + g.R
        t = t + (src[pl.ds(r, 6, stride=2), :] + src[pl.ds(r + 1, 6, stride=2), :])
        square[pl.ds(8 * i, 6), :] = t
    turned[...] = jnp.transpose(square[...])
    a = turned[pl.ds(0, 8, stride=2), :] + turned[pl.ds(1, 8, stride=2), :]
    b = turned[pl.ds(64, 8, stride=2), :] + turned[pl.ds(65, 8, stride=2), :]
    a = (a + roll(b, 64)) * 0.125
    r = iota2((128, 384), 0)
    l = iota2((128, 384), 1)
    x = 6 * gx + 3 * (r >> 6) + ((r & 63) >> 3)
    y = 6 * gy + (r & 7)
    hit = (x == (l >> 5)) & (y == (l & 31)) & ((r & 7) < 6) & ((r & 63) < 24)
    out = mm(a, jnp.where(hit, 1.0, 0.0).astype(BF16))
    for k in range(3):
        mine[pl.ds(k, 6, stride=4), :] = out[0:6, 128 * k : 128 * k + 128]


def image3(ref, s_ref, r, n):
    lane = lanes(n)
    c = ref[pl.ds(r, n), :]
    b = ref[pl.ds(r + 4, n), :] + ref[pl.ds(r - 4, n), :]
    b = b + (roll(c, 1) + roll(c, -1))
    b = b + roll(jnp.where(lane < 32, ref[pl.ds(r + 1, n), :], c), -32)
    b = b + roll(jnp.where(lane >= 96, ref[pl.ds(r - 1, n), :], c), 32)
    return c, FACTOR3 * (6.0 * c - b) + s_ref[pl.ds(r, n), :] * c


def chunks3(rows, ref, body):
    n = min(rows, 384)

    def step(i, carry):
        r = pl.multiple_of(GUARD3 + i * n, 8)
        ref[pl.ds(r, n), :] = body(r, n)
        return carry

    lax.fori_loop(0, rows // n, step, 0)


def match4(k, shape, coarse_dim, ny):
    c = iota2(shape, coarse_dim)
    l = iota2(shape, 1 - coarse_dim)
    return ((c >> 4) == 2 * k + (l >> 6)) & ((c & 15) == ((l & 31) >> 1)) & ((l & 31) < ny)


def restrict4(src, n, ny):
    total = None
    for k in range(3):
        t = src[pl.ds(GUARD3 + k, n, stride=8), :] + src[pl.ds(GUARD3 + k + 4, n, stride=8), :]
        part = mm(t, jnp.where(match4(k, (128, 128), 1, ny), 0.125, 0.0).astype(BF16))
        total = part if total is None else total + part
    return total


def dot_all(a, b):
    return jnp.sum(jnp.sum(a * b, axis=0, keepdims=True), axis=1, keepdims=True)


def bottom(source, s4, p4, n, ny):
    estimate = jnp.zeros_like(source)
    left = source
    inside = (lanes(n) < 96) & ((lanes(n) & 15) < ny)
    shifted = 6.0 * FACTOR4 + s4[...]
    for it in range(BOTTOM_ITERS):
        p4[pl.ds(GUARD, n), :] = left
        b = p4[pl.ds(GUARD + 1, n), :] + p4[pl.ds(GUARD - 1, n), :]
        b = b + (roll(left, 1) + roll(left, -1))
        b = b + (roll(left, 16) + roll(left, -16))
        image = shifted * left - FACTOR4 * jnp.where(inside, b, 0.0)
        now = dot_all(left, left)
        bent = dot_all(left, image)
        if it == 0:
            denom = bent
            direction, turned = left, image
        else:
            ratio = now * inv_before
            denom = bent - ratio * ratio * denom
            direction = left + ratio * direction
            turned = image + ratio * turned
        step = now / denom
        inv_before = 1.0 / now
        estimate = estimate + step * direction
        if it < BOTTOM_ITERS - 1:
            left = left - step * turned
    return estimate


PLAN_A = Plan([Item(L0, 3), Item(L0, 2), Item(L0, 2)])
PLAN_S = Plan([Item(L1, 6), Item(L2, 5)])
PLAN_B = Plan([Item(L1, 6)])
PLAN_BX = Plan([Item(L1, 6)], True)
PLAN_C = Plan([Item(L0, 3)])
PLAN_D = Plan([Item(L2, 5)])
PLANS = (PLAN_A, PLAN_S, PLAN_B, PLAN_C, PLAN_D, PLAN_BX)


def far(p, sizes):
    ring = lambda d, n: min(d % n, -d % n)
    return p[0] + ring(p[1], sizes[1]) + ring(p[2], 4) + ring(p[2] // 4, 4)


def kernel(sizes, counts, right_in, guess_in, react_in, guess, r0, eb0, left0, step_out, *scratch):
    scratch = list(scratch)

    def take(n):
        out = scratch[:n]
        del scratch[:n]
        return out

    raw = take(3)
    (in_sems,) = take(1)
    right, react, inv0, ea0 = take(4)
    f1, s1, inv1, ea1, eb1, left1 = take(6)
    f2, s2, inv2, ea2, eb2, left2 = take(6)
    f3, s3, inv3, ea3, eb3, left3 = take(6)
    s4, p4, down_m, up_m, tmp, square, turned, spread, slab = take(9)
    scr = [take(n) for n in counts]
    place = Place(sizes)
    gx, gy, gz = place.me
    n3, n4, ny3 = 24 * sizes[2], 3 * sizes[2], 6 * sizes[1]

    inputs = (guess_in, right_in, react_in)
    for k in range(3):
        for q in range(4):
            at = pl.ds(12 * q, 12)
            pltpu.make_async_copy(inputs[k].at[at], raw[k].at[at], in_sems.at[k]).start()

    def clear(ref):
        n = ref.shape[0]
        size = next(k for k in (128, 122 * 8, 80, 8) if n % k == 0) if n > 128 else n
        size = {1808: 904, 976: 488, 416: 208}.get(n, size)

        def step(i, carry):
            ref[pl.ds(pl.multiple_of(i * size, 8), size), :] = jnp.zeros((size, 128), F32)
            return carry

        lax.fori_loop(0, n // size, step, 0)

    peers = [(a, b, c) for a in range(sizes[0]) for b in range(sizes[1]) for c in range(sizes[2])][1:]
    peers.sort(key=lambda p: -far(p, sizes))
    beside = {(a, b % sizes[1], c % sizes[2]) for a in range(2) for b in (1, -1) for c in (1, -1)}
    beside |= {(1, 0, c % sizes[2]) for c in (1, -1)}
    greeted = [p for p in peers if p[2] == 0 or p[:2] == (0, 0) or p in beside]
    barrier = pltpu.get_barrier_semaphore()
    for p in greeted:
        pl.semaphore_signal(barrier, inc=1, device_id=place.beside(*p), device_id_type=MESH)
    for ref in (guess, right, react, f1, s1, ea1, eb1, f2, s2, ea2, eb2, ea3, eb3, p4, square):
        clear(ref)
    spread[...] = jnp.zeros_like(spread)
    for ref in (f3, s3, inv3):
        for r in (0, GUARD3 + n3):
            ref[pl.ds(r, GUARD3), :] = jnp.zeros((GUARD3, 128), F32)

    a = iota2((128, 128), 0)
    b = iota2((128, 128), 1)
    signed = lambda v: ((v + 8) & 63) - 8
    base = lambda v: ((v + 8) & 127) & 64
    zb = signed(b)
    hit = ((a == ((base(b) + 2 * zb) & 127)) | (a == ((base(b) + 2 * zb + 1) & 127))) & (zb >= -8) & (zb < 24)
    down_m[...] = jnp.where(hit, 0.125, 0.0).astype(BF16)
    hit = a == ((base(b) + (zb >> 1)) & 127)
    up_m[...] = jnp.where(hit, 1.0, 0.0).astype(BF16)

    ex_a = Exchange(PLAN_A, (guess, right, react), scr[0], place)
    ex_s = Exchange(PLAN_S, (s1, s2), scr[1], place)
    ex_b = Exchange(PLAN_B, (f1,), scr[2], place)
    ex_c = Exchange(PLAN_C, (eb0,), scr[3], place)
    ex_d = Exchange(PLAN_D, (f2,), scr[4], place)
    cx_b = Cross(PLAN_BX, ex_b, scr[5], place)
    ga_s = Gather(place, scr[6], s3)
    ga_f = Gather(place, scr[7], f3)
    for k, dst in enumerate((guess, right, react)):
        pltpu.make_async_copy(inputs[k], raw[k], in_sems.at[k]).wait()

        for i in range(24):
            dst[pl.ds(L0.row(i, 0), 48), 0:48] = raw[k][i]
            dst[pl.ds(L0.row(i, 0), 48), 64:112] = raw[k][i + 24]
        ex_a.pack_item(k)

    reduced, red_send, red_recv = scr[8]

    pl.semaphore_wait(barrier, len(greeted))
    ex_a.send()

    restrict(react, L0, s1, L1, 0, 12, 0, 24, down_m, tmp)
    restrict(s1, L1, s2, L2, 0, 6, 0, 12, down_m, tmp)
    ex_s.pack()
    ga_s.mine[...] = jnp.zeros((24, 128), F32)
    ga_f.mine[...] = jnp.zeros((24, 128), F32)
    to_level3(s2, ga_s.mine, square, turned, place)

    def start(r):
        at = pl.ds(r, L0.R)
        c, image = image_of(guess, react, L0, r)
        res = right[at, :] - image
        inv = inverse(react[at, :], 1.0)
        return [(r0, res), (inv0, inv), (ea0, inv * res)]

    ex_a.unpack()
    ex_a.x_send()
    ex_s.send()
    ga_s.send()
    ex_a.unpack_rest()
    planes(L0, 1, 23, start)
    ex_a.x_wait()
    ex_a.x_fill()
    planes(L0, -2, 1, start)
    planes(L0, 23, 26, start)
    relax(L0, ea0, eb0, r0, react, inv0, -1, 25)
    leftover(L0, eb0, left0, r0, react, 0, 24)
    restrict(left0, L0, f1, L1, 0, 12, 0, 24, down_m, tmp)
    ex_b.pack_send()
    cx_b.pack_send()
    ex_b.x_send()

    ex_c.pack()
    ex_s.unpack()
    ex_s.x_send()

    def inverse_of(g, sh, inv, first_plane, end):
        planes(g, first_plane, end, lambda r: [(inv, inverse(sh[pl.ds(r, g.R), :], g.factor))])

    inverse_of(L1, s1, inv1, 0, 12)

    ex_b.x_sent()
    ex_b.unpack()
    ex_c.send()
    first(L1, ea1, f1, inv1, 0, 12)
    relax(L1, ea1, eb1, f1, s1, inv1, 1, 11)
    ex_s.x_wait()
    ex_s.x_fill()
    inverse_of(L1, s1, inv1, -6, 0)
    inverse_of(L1, s1, inv1, 12, 18)
    inverse_of(L2, s2, inv2, -5, 11)
    ex_b.x_wait()
    cx_b.unpack()
    ex_b.x_fill()
    first(L1, ea1, f1, inv1, -6, 0)
    first(L1, ea1, f1, inv1, 12, 18)
    relax(L1, ea1, eb1, f1, s1, inv1, -5, 1)
    relax(L1, ea1, eb1, f1, s1, inv1, 11, 17)
    leftover(L1, eb1, left1, f1, s1, -4, 16)
    restrict(left1, L1, f2, L2, -2, 8, -2, 16, down_m, tmp)
    first(L2, ea2, f2, inv2, -2, 8)
    relax(L2, ea2, eb2, f2, s2, inv2, -1, 7)
    leftover(L2, eb2, left2, f2, s2, 0, 6)
    to_level3(left2, ga_f.mine, square, turned, place)
    ga_f.send()
    ex_d.pack_send()
    ga_s.relay()

    ga_f.relay()
    ex_c.unpack()
    ex_c.x_send()
    ex_c.unpack_rest()
    ex_d.unpack()
    ex_d.x_send()
    ex_c.x_wait()
    ex_c.x_fill()
    ex_d.x_wait()
    ex_d.x_fill()
    first(L2, ea2, f2, inv2, -5, 11)
    relax(L2, ea2, eb2, f2, s2, inv2, -4, 10)
    ga_s.finish()
    chunks3(n3, inv3, lambda r, n: inverse(s3[pl.ds(r, n), :], FACTOR3))
    s4[...] = restrict4(s3, n4, ny3)
    for e in (ex_a, ex_s, ex_c, ex_d, ga_s):
        e.settle()
    for e in (ex_b, cx_b):
        e.settle(False)
    ga_f.finish()

    def relax3(src, dst):
        def body(r, n):
            c, image = image3(src, s3, r, n)
            at = pl.ds(r, n)
            return c + inv3[at, :] * (f3[at, :] - image)

        chunks3(n3, dst, body)

    chunks3(n3, ea3, lambda r, n: inv3[pl.ds(r, n), :] * f3[pl.ds(r, n), :])
    relax3(ea3, eb3)
    chunks3(n3, left3, lambda r, n: f3[pl.ds(r, n), :] - image3(eb3, s3, r, n)[1])
    e4 = bottom(restrict4(left3, n4, ny3), s4, p4, n4, ny3 // 2)
    for k in range(3):
        u = mm(e4, jnp.where(match4(k, (128, 128), 0, ny3), 1.0, 0.0).astype(BF16))
        for q in (k, k + 4):
            at = pl.ds(GUARD3 + q, n4, stride=8)
            eb3[at, :] = eb3[at, :] + u
    for src, dst, n in ((eb3, ea3, 48), (ea3, slab, 40)):
        r = pl.multiple_of(GUARD3 + 24 * gz - (n - 24) // 2, 4)
        c, image = image3(src, s3, r, n)
        at = pl.ds(r, n)
        dst[at if n == 48 else pl.ds(0, n), :] = c + inv3[at, :] * (f3[at, :] - image)
    for k in range(3):
        v = slab[pl.ds(k, 10, stride=4), :]
        for h in range(2):
            for q in range(2):
                spread[k, pl.ds(64 * h + q, 10, stride=2), :] = v
    wide = [jnp.concatenate(p, axis=1) for p in zip(*[split(spread[k]) for k in range(3)])]
    coarse = []
    for h in range(2):
        r = iota2((112, 384), 0)
        l = iota2((112, 384), 1)
        hit = (6 * gx + 3 * h + (r >> 4) - 2 == (l >> 5)) & (6 * gy + (r & 15) - 2 == (l & 31)) & ((r & 15) < 10)
        pick = jnp.where(hit, 1.0, 0.0).astype(BF16)
        parts = [
            lax.dot_general(pick, p, (((1,), (1,)), ((), ())), preferred_element_type=F32) for p in wide
        ]
        coarse.append(parts[0] + parts[1])
    fine = roll(jnp.where(lanes(112) < 64, coarse[0], coarse[1]), -4)
    for i in range(7):
        u = fine[16 * i : 16 * i + 10]
        tmp[pl.ds(24 * i, 10, stride=2), :] = u
        tmp[pl.ds(24 * i + 1, 10, stride=2), :] = u
    for i in range(7):
        v = tmp[pl.ds(24 * i, 20), :]
        for q in range(2):
            at = pl.ds(L2.row(2 * (i - 2) + q, -4), 20)
            eb2[at, :] = eb2[at, :] + v
    relax(L2, eb2, ea2, f2, s2, inv2, -3, 9)
    relax(L2, ea2, eb2, f2, s2, inv2, -2, 8)
    prolong(eb2, L2, eb1, L1, -2, 8, -2, 16, up_m, tmp)
    relax(L1, eb1, ea1, f1, s1, inv1, -3, 15)
    relax(L1, ea1, eb1, f1, s1, inv1, -2, 14)
    prolong(eb1, L1, eb0, L0, -2, 14, -2, 28, up_m, tmp)
    relax(L0, eb0, ea0, r0, react, inv0, -2, 26)
    relax(L0, ea0, eb0, r0, react, inv0, -1, 25)

    row = iota2((L0.R, 128), 0)
    inside = ((lanes(L0.R) & 63) < 48) & (row >= L0.y0) & (row < L0.y0 + 48)

    upper, lower = [], []
    for i in range(24):
        r = GUARD + (L0.halo + i) * L0.R
        c, image = image_of(eb0, react, L0, r)
        left0[pl.ds(r, L0.R), :] = image
        upper.append(c * r0[pl.ds(r, L0.R), :])
        lower.append(c * image)
    upper = jnp.where(inside, tree(upper), 0.0)
    lower = jnp.where(inside, tree(lower), 0.0)
    upper = jnp.sum(upper, axis=0, keepdims=True)
    lower = jnp.sum(lower, axis=0, keepdims=True)
    half = lanes(1) < 64
    number = (gx * sizes[1] + gy) * sizes[2] + gz
    reduced[number] = jnp.where(half, upper + roll(upper, 64), lower + roll(lower, 64))
    own = reduced.at[number]

    def summed(src, dst, p):
        return pltpu.make_async_remote_copy(
            src_ref=src, dst_ref=dst, send_sem=red_send.at[0], recv_sem=red_recv.at[0],
            device_id=place.beside(*p), device_id_type=MESH,
        )

    for p in peers:
        summed(own, own, p).start()
    ga_f.settle()
    most = reduced.at[pl.ds(0, len(peers))]
    summed(most, most, peers[0]).wait()
    sums = [reduced[k] for k in range(8)]
    for k in range(8, len(peers) + 1):
        sums[k % 8] = sums[k % 8] + reduced[k]
    total = tree(sums)
    upper = jnp.sum(jnp.where(half, total, 0.0), axis=1, keepdims=True)
    lower = jnp.sum(jnp.where(half, 0.0, total), axis=1, keepdims=True)
    step_out[...] = jnp.broadcast_to(upper / lower, (8, 128))


def finish(guess, r0, eb0, left0, step_ref, field_out, resid_out, field, resid, sems):
    step = step_ref[0:1, :]
    copies = []
    parts, size = 4, 6
    for p in range(parts):
        for x in range(p * size, p * size + size):
            at = pl.ds(L0.row(x, 0), 48)
            v = guess[at, :] + step * eb0[at, :]
            field[x] = v[:, 0:48]
            field[x + 24] = roll(v, 64)[:, 0:48]
            v = r0[at, :] - step * left0[at, :]
            resid[x] = v[:, 0:48]
            resid[x + 24] = roll(v, 64)[:, 0:48]
        for q, (src, dst) in enumerate(((field, field_out), (resid, resid_out))):
            for h in range(2):
                at = pl.ds(p * size + 24 * h, size)
                c = pltpu.make_async_copy(src.at[at], dst.at[at], sems.at[4 * p + 2 * q + h])
                c.start()
                copies.append(c)
    for c in copies:
        c.wait()


def solution(mesh):
    sizes = tuple(mesh.shape[a] for a in ("gx", "gy", "gz"))
    n3, n4 = 24 * sizes[2] + 2 * GUARD3, 3 * sizes[2]
    scratch = [pltpu.VMEM((48, 48, 48), F32)] * 3 + [pltpu.SemaphoreType.DMA((3,))]
    scratch += [pltpu.VMEM((L0.total, 128), F32)] * 4
    scratch += [pltpu.VMEM((L1.total, 128), F32)] * 6
    scratch += [pltpu.VMEM((L2.total, 128), F32)] * 6
    scratch += [pltpu.VMEM((n3, 128), F32)] * 6
    scratch += [pltpu.VMEM((n4, 128), F32), pltpu.VMEM((n4 + 2 * GUARD, 128), F32)]
    scratch += [pltpu.VMEM((128, 128), BF16)] * 2 + [pltpu.VMEM((16 * 56, 128), F32)]
    scratch += [pltpu.VMEM((128, 128), F32)] * 2
    scratch += [pltpu.VMEM((3, 128, 128), F32), pltpu.VMEM((40, 128), F32)]
    groups = [p.scratch() for p in PLANS] + [gather_scratch(sizes)] * 2
    devices = sizes[0] * sizes[1] * sizes[2]
    groups += [[pltpu.VMEM((devices, 1, 128), F32)] + [pltpu.SemaphoreType.DMA((1,))] * 2]
    for g in groups:
        scratch += g
    counts = tuple(len(g) for g in groups)
    vmem = pl.BlockSpec(memory_space=pltpu.VMEM)

    anywhere = pl.BlockSpec(memory_space=pl.ANY)

    def body(right_side, start_guess, reaction):
        whole = pltpu.VMEM((L0.total, 128), F32)
        parts = pl.pallas_call(
            functools.partial(kernel, sizes, counts),
            out_shape=[whole] * 4 + [pltpu.VMEM((8, 128), F32)],
            in_specs=[anywhere] * 3,
            out_specs=[vmem] * 5,
            scratch_shapes=scratch,
            compiler_params=pltpu.CompilerParams(
                collective_id=0, has_side_effects=True, vmem_limit_bytes=60 * 2**20
            ),
        )(right_side, start_guess, reaction)
        shape = jax.ShapeDtypeStruct(right_side.shape, F32)
        return tuple(
            pl.pallas_call(
                finish,
                out_shape=[shape, shape],
                in_specs=[vmem] * 5,
                out_specs=[anywhere] * 2,
                scratch_shapes=[pltpu.VMEM(right_side.shape, F32)] * 2 + [pltpu.SemaphoreType.DMA((16,))],
                compiler_params=pltpu.CompilerParams(vmem_limit_bytes=16 * 2**20),
            )(*parts)
        )

    placed = P("gx", "gy", "gz")
    return jax.shard_map(
        body, mesh=mesh, in_specs=(placed,) * 3, out_specs=(placed,) * 2, check_vma=False
    )
```

```python
import functools

import jax
import jax.numpy as jnp
from jax import lax
from jax.experimental import pallas as pl
from jax.experimental.pallas import tpu as pltpu
from jax.sharding import PartitionSpec as P

MESH = pl.DeviceIdType.MESH
F32 = jnp.float32
BF16 = jnp.bfloat16
DAMP = 6.0 / 7.0
GUARD = 8
GUARD3 = 16
BOTTOM_ITERS = 6


class Geo:
    def __init__(self, nx, ny, nz, halo, rows, y0, depth, unroll):
        self.nx, self.ny, self.nz, self.halo, self.R, self.y0 = nx, ny, nz, halo, rows, y0
        self.factor = 0.25**depth
        self.unroll = unroll
        self.total = 2 * GUARD + (nx + 2 * halo) * rows

    def row(self, x, y):
        return GUARD + (self.halo + x) * self.R + self.y0 + y


L0 = Geo(24, 48, 48, 4, 56, 4, 0, 28)
L1 = Geo(12, 24, 24, 6, 40, 8, 1, 24)
L2 = Geo(6, 12, 12, 5, 24, 6, 2, 16)
FACTOR3 = 0.25**3
FACTOR4 = 0.25**4


def lanes(rows):
    return lax.broadcasted_iota(jnp.int32, (rows, 128), 1)


def iota2(shape, dim):
    return lax.broadcasted_iota(jnp.int32, shape, dim)


def tree(terms):
    while len(terms) > 1:
        terms = [sum(terms[k + 1 : k + 2], terms[k]) for k in range(0, len(terms), 2)]
    return terms[0]


def roll(v, shift):
    shift = shift % 128
    return v if shift == 0 else pltpu.roll(v, shift, 1)


def split(a):
    hi = a.astype(BF16)
    return hi, (a - hi.astype(F32)).astype(BF16)


def mm(a, b):
    hi, low = split(a)
    return jnp.dot(hi, b, preferred_element_type=F32) + jnp.dot(low, b, preferred_element_type=F32)


def beside_of(ref, r, R):
    c = ref[pl.ds(r, R), :]
    b = ref[pl.ds(r + R, R), :] + ref[pl.ds(r - R, R), :]
    b = b + (ref[pl.ds(r + 1, R), :] + ref[pl.ds(r - 1, R), :])
    b = b + (roll(c, 1) + roll(c, -1))
    return c, b


def image_of(ref, s_ref, g, r):
    c, b = beside_of(ref, r, g.R)
    return c, g.factor * (6.0 * c - b) + s_ref[pl.ds(r, g.R), :] * c


def planes(g, a, b, body):
    unroll = g.unroll

    def group(start, count):
        todo = []
        for k in range(count):
            r = start + k * g.R
            r = r if isinstance(r, int) else pl.multiple_of(r, 8)
            todo.append((r, body(r)))
        for r, pairs in todo:
            for ref, value in pairs:
                ref[pl.ds(r, g.R), :] = value

    trips = (b - a) // unroll
    origin = GUARD + (g.halo + a) * g.R
    if trips == 1:
        group(origin, unroll)
    elif trips:

        def step(i, carry):
            group(pl.multiple_of(origin + i * (unroll * g.R), 8), unroll)
            return carry

        lax.fori_loop(0, trips, step, 0)
    if (b - a) % unroll:
        group(origin + trips * unroll * g.R, (b - a) % unroll)


def inverse(s, factor):
    return jnp.where(s > 0.0, DAMP / (6.0 * factor + s), 0.0)


def relax(g, src, dst, f, s, inv, a, b):
    def body(r):
        c, image = image_of(src, s, g, r)
        at = pl.ds(r, g.R)
        return [(dst, c + inv[at, :] * (f[at, :] - image))]

    planes(g, a, b, body)


def first(g, dst, f, inv, a, b):
    def body(r):
        at = pl.ds(r, g.R)
        return [(dst, inv[at, :] * f[at, :])]

    planes(g, a, b, body)


def leftover(g, src, dst, f, s, a, b):
    def body(r):
        c, image = image_of(src, s, g, r)
        return [(dst, f[pl.ds(r, g.R), :] - image)]

    planes(g, a, b, body)


def restrict(src, gs, dst, gd, x0, x1, y0, count, matrix, tmp):
    step = -(-count // 8) * 8
    for x in range(x0, x1):
        r = gs.row(2 * x, 2 * y0)
        t = src[pl.ds(r, count, stride=2), :] + src[pl.ds(r + 1, count, stride=2), :]
        r = r + gs.R
        t = t + (src[pl.ds(r, count, stride=2), :] + src[pl.ds(r + 1, count, stride=2), :])
        tmp[pl.ds((x - x0) * step, count), :] = t
    for x in range(x0, x1):
        out = mm(tmp[pl.ds((x - x0) * step, step), :], matrix[...])
        dst[pl.ds(gd.row(x, y0), count), :] = out[0:count]


def prolong(src, gc, dst, gf, x0, x1, y0, count, matrix, tmp):
    for x in range(x0, x1):
        o = (x - x0) * 56
        u = mm(src[pl.ds(gc.row(x, y0), count), :], matrix[...])
        tmp[pl.ds(o, count, stride=2), :] = u
        tmp[pl.ds(o + 1, count, stride=2), :] = u
    for x in range(x0, x1):
        o = (x - x0) * 56
        v = tmp[pl.ds(o, 2 * count), :]
        for k in range(2):
            at = pl.ds(gf.row(2 * x + k, 2 * y0), 2 * count)
            dst[at, :] = dst[at, :] + v


class Item:
    def __init__(self, geo, w):
        self.g, self.w = geo, w


class Plan:
    def __init__(self, items, cross=False):
        self.items, self.cross = items, cross
        self.counts = [it.w if cross else it.g.nx for it in items]
        self.yrows = sum(n * it.w for n, it in zip(self.counts, items))
        self.yrows = -(-self.yrows // 8) * 8
        self.tiles = []
        for k, it in enumerate(items):
            for x in range(self.counts[k]):
                for t in self.tiles:
                    if t[0] is it.g and t[1] + it.w <= 64:
                        break
                else:
                    t = [it.g, 0, []]
                    self.tiles.append(t)
                t[2].append((k, x, t[1]))
                t[1] += it.w
        self.zrows = sum(t[0].ny for t in self.tiles)
        self.zrows = -(-self.zrows // 8) * 8
        self.drows = max(self.counts)
        self.drows = -(-self.drows // 8) * 8
        assert sum(it.w * it.w for it in items) <= 64

        self.z0 = [0, self.zrows]
        self.d0 = [2 * self.zrows + q * self.drows for q in range(4)]
        self.y0 = [2 * self.zrows + 4 * self.drows + q * self.yrows for q in range(2)]
        self.total = 2 * (self.zrows + self.yrows) + 4 * self.drows
        self.xtotal = sum(it.w * it.g.R for it in items)

    def scratch(self):
        x = [] if self.cross else [pltpu.VMEM((self.xtotal, 128), F32)]
        return x + [
            pltpu.VMEM((self.total, 128), F32),
            pltpu.VMEM((self.total, 128), F32),
            pltpu.SemaphoreType.DMA((2,)),
            pltpu.SemaphoreType.DMA((2,)),
        ]


class Exchange:
    def __init__(self, plan, refs, scratch, place):
        self.plan, self.refs, self.place = plan, refs, place
        self.xr, self.sent, self.got, self.ss, self.rs = scratch
        gx, gy, gz = place.me
        self.partner = (1 - gx, gy, gz)
        self.x_copies = []
        o = 0
        for k, it in enumerate(plan.items):
            r = pl.multiple_of(GUARD + (it.g.halo + self.edge(it)) * it.g.R, 8)
            n = it.w * it.g.R
            self.x_copies.append(self.copy(refs[k].at[pl.ds(r, n), :], self.xr.at[pl.ds(o, n), :], 0, self.partner))
            o += n
        self.segments(0)

    def edge(self, it):
        return jnp.where(self.place.me[0] == 0, it.g.nx - it.w, 0)

    def source(self, k, x, y):
        return self.plan.items[k].g.row(x, y)

    def target(self, k, x, y):
        return self.refs[k], self.plan.items[k].g.row(x, y)

    def segments(self, dx):
        plan = self.plan
        at = {}
        for d in range(2):
            at[1 - 2 * d, 0] = plan.y0[d]
            at[0, 1 - 2 * d] = plan.z0[d]
            for e in range(2):
                at[1 - 2 * d, 1 - 2 * e] = plan.d0[2 * d + e]
        self.y_copies, self.z_copies, self.d_copies = [], [], []
        for d in (1, -1):
            self.y_copies.append(self.segment(at, dx, d, 0, plan.yrows))
            self.z_copies.append(self.segment(at, dx, 0, d, plan.zrows))
            for e in (1, -1):
                self.d_copies.append(self.segment(at, dx, d, e, plan.drows))

    def segment(self, at, dx, dy, dz, n):
        there = self.place.exists(dy, dz)
        peer = self.place.beside(dx, dy, dz)
        peer = tuple(jnp.where(there, p, q) for p, q in zip(peer, self.partner))
        target = pl.multiple_of(jnp.where(there, at[dy, dz], at[-dy, -dz]), 8)
        return self.copy(self.sent.at[pl.ds(at[dy, dz], n), :], self.got.at[pl.ds(target, n), :], 1, peer)

    def copy(self, src, dst, k, peer):
        return pltpu.make_async_remote_copy(
            src_ref=src, dst_ref=dst, send_sem=self.ss.at[k], recv_sem=self.rs.at[k],
            device_id=peer, device_id_type=MESH,
        )

    def x_send(self):
        for c in self.x_copies:
            c.start()

    def settle(self, x=True):
        if x:
            self.x_sent()
        self.copy(self.sent, self.got, 1, self.partner).wait_send()

    def x_sent(self):
        self.copy(self.xr, self.xr, 0, self.partner).wait_send()

    def x_wait(self):
        self.copy(self.xr, self.xr, 0, self.partner).wait_recv()

    def x_fill(self):
        m0, m1 = self.place.x_masks
        o = 0
        for k, it in enumerate(self.plan.items):
            g, w, ref = it.g, it.w, self.refs[k]
            upper = ((lanes(g.R) + 8) & 127) >= 64
            for j in range(w):
                got = self.xr[pl.ds(o + j * g.R, g.R), :]
                top = ref[pl.ds(GUARD + (g.halo + g.nx - w + j) * g.R, g.R), :]
                low = ref[pl.ds(GUARD + (g.halo + j) * g.R, g.R), :]
                ref[pl.ds(GUARD + (g.halo - w + j) * g.R, g.R), :] = roll(jnp.where(upper, got * m1, top), 64)
                ref[pl.ds(GUARD + (g.halo + g.nx + j) * g.R, g.R), :] = roll(jnp.where(upper, low, got * m0), 64)
            o += w * g.R

    def pack_send(self):
        self.pack()
        self.send()

    def pack(self):
        for k in range(len(self.refs)):
            self.pack_item(k)

    def send(self):
        for c in self.d_copies + self.z_copies + self.y_copies:
            c.start()

    def pack_item(self, k):
        if k == 0:
            self.yo, self.co, self.corner = 0, 0, [None] * 4
        it = self.plan.items[k]
        g, w, ref = it.g, it.w, self.refs[k]
        n = self.plan.counts[k]
        lane = lanes(self.plan.drows) & 63
        for d in range(1, w + 1):
            at = self.co + (d - 1) * w
            for e, y in enumerate((g.ny - d, d - 1)):
                v = ref[pl.ds(self.source(k, 0, y), n, stride=g.R), :]
                self.sent[pl.ds(self.plan.y0[e] + self.yo, n), :] = v
                if n < self.plan.drows:
                    v = jnp.concatenate([v, jnp.zeros((self.plan.drows - n, 128), F32)], axis=0)
                for q, z in enumerate((g.nz - w, 0)):
                    moved = roll(v, at - z)
                    old = self.corner[2 * e + q]
                    self.corner[2 * e + q] = moved if old is None else jnp.where(lane >= at, moved, old)
            self.yo += n
        self.co += w * w
        if k == len(self.refs) - 1:
            for q in range(4):
                self.sent[pl.ds(self.plan.d0[q], self.plan.drows), :] = self.corner[q]
        zo = 0
        for t, _, slots in self.plan.tiles:
            if slots[-1][0] == k:
                self.pack_tile(t, slots, zo)
            zo += t.ny

    def pack_tile(self, g, slots, zo):
        lane = lanes(g.ny)
        acc = [None, None]
        for k, x, at in slots:
            w = self.plan.items[k].w
            moved = roll(self.refs[k][pl.ds(self.source(k, x, 0), g.ny), :], at)
            for q, past in enumerate((g.nz - w, 0)):
                here = ((lane - past) & 63 >= at) & ((lane - past) & 63 < at + w)
                acc[q] = moved if acc[q] is None else jnp.where(here, moved, acc[q])
        for q in range(2):
            self.sent[pl.ds(self.plan.z0[q] + zo, g.ny), :] = acc[q]

    def unpack(self):
        my, mz = self.place.y_masks, self.place.z_masks
        self.copy(self.sent, self.got, 1, self.partner).wait_recv()
        yo, co = 0, 0
        for k, it in enumerate(self.plan.items):
            g, w = it.g, it.w
            n = self.plan.counts[k]
            lane = lanes(n) & 63
            into = (lane >= 64 - w, (lane >= g.nz) & (lane < g.nz + w))
            for d in range(1, w + 1):
                at = co + (d - 1) * w
                for e, y in enumerate((-d, g.ny + d - 1)):
                    v = self.got[pl.ds(self.plan.y0[e] + yo, n), :]
                    for q, z in enumerate((-w, g.nz)):
                        got = self.got[pl.ds(self.plan.d0[2 * e + q], n), :] * mz[q]
                        v = jnp.where(into[q], roll(got, z - at), v)
                    ref, r = self.target(k, 0, y)
                    ref[pl.ds(r, n, stride=g.R), :] = v * my[e]
                yo += n
            co += w * w
        self.unpack_z(True)

    def unpack_rest(self):
        self.unpack_z(False)

    def unpack_z(self, edge):
        mz = self.place.z_masks
        zo = 0
        for g, _, slots in self.plan.tiles:
            lane = lanes(g.ny) & 63
            got = [self.got[pl.ds(self.plan.z0[q] + zo, g.ny), :] * mz[q] for q in range(2)]
            for k, x, at in slots:
                w = self.plan.items[k].w
                if (x < w or x >= g.nx - w) != edge:
                    continue
                ref, r = self.target(k, x, 0)
                rows = pl.ds(r, g.ny)
                v = ref[rows, :]
                v = jnp.where(lane >= 64 - w, roll(got[0], -g.nz - at), v)
                v = jnp.where((lane >= g.nz) & (lane < g.nz + w), roll(got[1], g.nz - at), v)
                ref[rows, :] = v
            zo += g.ny


class Cross(Exchange):
    def __init__(self, plan, main, scratch, place):
        self.plan, self.main, self.refs, self.place = plan, main, main.refs, place
        self.sent, self.got, self.ss, self.rs = scratch
        self.partner = main.partner
        self.segments(1)

    def source(self, k, x, y):
        it = self.plan.items[k]
        return GUARD + (it.g.halo + self.edge(it) + x) * it.g.R + it.g.y0 + y

    def target(self, k, x, y):
        o = sum(it.w * it.g.R for it in self.plan.items[:k])
        g = self.plan.items[k].g
        return self.main.xr, o + x * g.R + g.y0 + y


class Place:
    def __init__(self, sizes):
        self.sizes = sizes
        self.me = tuple(lax.axis_index(a) for a in ("gx", "gy", "gz"))
        gx, gy, gz = self.me
        one = lambda c: jnp.where(c, 1.0, 0.0).astype(F32)
        self.x_masks = (one(gx == 0), one(gx == 1))
        self.y_masks = (one(gy > 0), one(gy < sizes[1] - 1))
        self.z_masks = (one(gz > 0), one(gz < sizes[2] - 1))

    def exists(self, dy, dz):
        gx, gy, gz = self.me
        y, z = gy + dy, gz + dz
        return (y >= 0) & (y < self.sizes[1]) & (z >= 0) & (z < self.sizes[2])

    def beside(self, dx, dy, dz):
        return tuple(
            lax.rem(m + d % n, n) if d % n else m for m, d, n in zip(self.me, (dx, dy, dz), self.sizes)
        )


class Gather:
    rows = 24

    def __init__(self, place, scratch, whole):
        self.place, self.whole = place, whole
        self.mine, self.got, self.sum, self.ss, self.rs = scratch
        n = place.sizes
        self.near = [(a, b) for a in range(n[0]) for b in range(n[1])][1:]
        self.near.sort(key=lambda p: -far((p[0], p[1], 0), n))
        self.line = sorted(range(1, n[2]), key=lambda c: -far((0, 0, c), n))
        self.at = pl.ds(pl.multiple_of(GUARD3 + self.rows * place.me[2], 8), self.rows)

    def copy(self, src, dst, k, peer):
        return pltpu.make_async_remote_copy(
            src_ref=src, dst_ref=dst, send_sem=self.ss.at[k], recv_sem=self.rs.at[k],
            device_id=peer, device_id_type=MESH,
        )

    def send(self):
        for k, (a, b) in enumerate(self.near):
            self.copy(self.mine, self.got.at[k], 0, self.place.beside(a, b, 0)).start()

    def relay(self):
        self.copy(self.got, self.got, 0, self.place.beside(1, 0, 0)).wait_recv()
        total = self.mine[...]
        for k in range(len(self.near)):
            total = total + self.got[k]
        self.sum[...] = total
        for c in self.line:
            self.copy(self.sum, self.whole.at[self.at, :], 1, self.place.beside(0, 0, c)).start()
        self.whole[self.at, :] = total

    def finish(self):
        self.most().wait_recv()

    def most(self):
        most = self.whole.at[pl.ds(GUARD3, self.rows * (self.place.sizes[2] - 1)), :]
        return self.copy(most, most, 1, self.place.beside(1, 0, 0))

    def settle(self):
        self.copy(self.got, self.got, 0, self.place.beside(1, 0, 0)).wait_send()
        self.most().wait_send()


def gather_scratch(sizes):
    return [
        pltpu.VMEM((24, 128), F32),
        pltpu.VMEM((sizes[0] * sizes[1] - 1, 24, 128), F32),
        pltpu.VMEM((24, 128), F32),
        pltpu.SemaphoreType.DMA((2,)),
        pltpu.SemaphoreType.DMA((2,)),
    ]


def spread_to_level3(place):
    gx, gy, gz = place.me
    r = iota2((128, 384), 0)
    l = iota2((128, 384), 1)
    x = 6 * gx + 3 * (r >> 6) + ((r & 63) >> 3)
    y = 6 * gy + (r & 7)
    hit = (x == (l >> 5)) & (y == (l & 31)) & ((r & 7) < 6) & ((r & 63) < 24)
    return jnp.where(hit, 1.0, 0.0).astype(BF16)


def to_level3(src, mine, square, turned, chosen):
    g = L2
    for i in range(3):
        r = g.row(2 * i, 0)
        t = src[pl.ds(r, 6, stride=2), :] + src[pl.ds(r + 1, 6, stride=2), :]
        r = r + g.R
        t = t + (src[pl.ds(r, 6, stride=2), :] + src[pl.ds(r + 1, 6, stride=2), :])
        square[pl.ds(8 * i, 6), :] = t
    turned[...] = jnp.transpose(square[...])
    a = turned[pl.ds(0, 8, stride=2), :] + turned[pl.ds(1, 8, stride=2), :]
    b = turned[pl.ds(64, 8, stride=2), :] + turned[pl.ds(65, 8, stride=2), :]
    a = (a + roll(b, 64)) * 0.125
    out = mm(a, chosen[...])
    for k in range(3):
        mine[pl.ds(k, 6, stride=4), :] = out[0:6, 128 * k : 128 * k + 128]


def image3(ref, s_ref, r, n):
    lane = lanes(n)
    c = ref[pl.ds(r, n), :]
    b = ref[pl.ds(r + 4, n), :] + ref[pl.ds(r - 4, n), :]
    b = b + (roll(c, 1) + roll(c, -1))
    b = b + roll(jnp.where(lane < 32, ref[pl.ds(r + 1, n), :], c), -32)
    b = b + roll(jnp.where(lane >= 96, ref[pl.ds(r - 1, n), :], c), 32)
    return c, FACTOR3 * (6.0 * c - b) + s_ref[pl.ds(r, n), :] * c


def chunks3(rows, ref, body):
    n = min(rows, 384)

    def step(i, carry):
        r = pl.multiple_of(GUARD3 + i * n, 8)
        ref[pl.ds(r, n), :] = body(r, n)
        return carry

    lax.fori_loop(0, rows // n, step, 0)


def match4(k, shape, coarse_dim, ny):
    c = iota2(shape, coarse_dim)
    l = iota2(shape, 1 - coarse_dim)
    return ((c >> 4) == 2 * k + (l >> 6)) & ((c & 15) == ((l & 31) >> 1)) & ((l & 31) < ny)


def restrict4(src, n, matrix):
    total = None
    for k in range(3):
        t = src[pl.ds(GUARD3 + k, n, stride=8), :] + src[pl.ds(GUARD3 + k + 4, n, stride=8), :]
        part = mm(t, matrix[k])
        total = part if total is None else total + part
    return total


def dot_all(a, b):
    return jnp.sum(jnp.sum(a * b, axis=0, keepdims=True), axis=1, keepdims=True)


def bottom(source, s4, p4, n, ny):
    estimate = jnp.zeros_like(source)
    left = source
    inside = (lanes(n) < 96) & ((lanes(n) & 15) < ny)
    shifted = 6.0 * FACTOR4 + s4[...]
    for it in range(BOTTOM_ITERS):
        p4[pl.ds(GUARD, n), :] = left
        b = p4[pl.ds(GUARD + 1, n), :] + p4[pl.ds(GUARD - 1, n), :]
        b = b + (roll(left, 1) + roll(left, -1))
        b = b + (roll(left, 16) + roll(left, -16))
        image = shifted * left - FACTOR4 * jnp.where(inside, b, 0.0)
        now = dot_all(left, left)
        bent = dot_all(left, image)
        if it == 0:
            denom = bent
            direction, turned = left, image
        else:
            ratio = now * inv_before
            denom = bent - ratio * ratio * denom
            direction = left + ratio * direction
            turned = image + ratio * turned
        step = now / denom
        inv_before = 1.0 / now
        estimate = estimate + step * direction
        if it < BOTTOM_ITERS - 1:
            left = left - step * turned
    return estimate


PLAN_A = Plan([Item(L0, 3), Item(L0, 2), Item(L0, 2)])
PLAN_S = Plan([Item(L1, 6), Item(L2, 5)])
PLAN_B = Plan([Item(L1, 6)])
PLAN_BX = Plan([Item(L1, 6)], True)
PLAN_C = Plan([Item(L0, 3)])
PLAN_D = Plan([Item(L2, 5)])
PLANS = (PLAN_A, PLAN_S, PLAN_B, PLAN_C, PLAN_D, PLAN_BX)


def far(p, sizes):
    ring = lambda d, n: min(d % n, -d % n)
    return p[0] + ring(p[1], sizes[1]) + ring(p[2], 4) + ring(p[2] // 4, 4)


def kernel(sizes, counts, right_in, guess_in, react_in, guess, r0, eb0, left0, step_out, *scratch):
    scratch = list(scratch)

    def take(n):
        out = scratch[:n]
        del scratch[:n]
        return out

    raw = take(3)
    (in_sems,) = take(1)
    right, react, inv0, ea0 = take(4)
    f1, s1, inv1, ea1, eb1, left1 = take(6)
    f2, s2, inv2, ea2, eb2, left2 = take(6)
    f3, s3, inv3, ea3, eb3, left3 = take(6)
    s4, p4, down_m, up_m, tmp, square, turned, spread, slab = take(9)
    chosen, picks, down4, up4 = take(4)
    scr = [take(n) for n in counts]
    place = Place(sizes)
    gx, gy, gz = place.me
    n3, n4, ny3 = 24 * sizes[2], 3 * sizes[2], 6 * sizes[1]

    inputs = (guess_in, right_in, react_in)
    for k in range(3):
        for q in range(4):
            at = pl.ds(12 * q, 12)
            pltpu.make_async_copy(inputs[k].at[at], raw[k].at[at], in_sems.at[k]).start()

    def clear(ref):
        n = ref.shape[0]
        size = next(k for k in (128, 122 * 8, 80, 8) if n % k == 0) if n > 128 else n
        size = {1808: 904, 976: 488, 416: 208}.get(n, size)

        def step(i, carry):
            ref[pl.ds(pl.multiple_of(i * size, 8), size), :] = jnp.zeros((size, 128), F32)
            return carry

        lax.fori_loop(0, n // size, step, 0)

    peers = [(a, b, c) for a in range(sizes[0]) for b in range(sizes[1]) for c in range(sizes[2])][1:]
    peers.sort(key=lambda p: -far(p, sizes))
    beside = {(a, b % sizes[1], c % sizes[2]) for a in range(2) for b in (1, -1) for c in (1, -1)}
    beside |= {(1, 0, c % sizes[2]) for c in (1, -1)}
    greeted = [p for p in peers if p[2] == 0 or p[:2] == (0, 0) or p in beside]
    barrier = pltpu.get_barrier_semaphore()
    for p in greeted:
        pl.semaphore_signal(barrier, inc=1, device_id=place.beside(*p), device_id_type=MESH)
    for ref in (guess, right, react, f1, s1, ea1, eb1, f2, s2, ea2, eb2, ea3, eb3, p4, square):
        clear(ref)
    spread[...] = jnp.zeros_like(spread)
    for ref in (f3, s3, inv3):
        for r in (0, GUARD3 + n3):
            ref[pl.ds(r, GUARD3), :] = jnp.zeros((GUARD3, 128), F32)

    a = iota2((128, 128), 0)
    b = iota2((128, 128), 1)
    signed = lambda v: ((v + 8) & 63) - 8
    base = lambda v: ((v + 8) & 127) & 64
    zb = signed(b)
    hit = ((a == ((base(b) + 2 * zb) & 127)) | (a == ((base(b) + 2 * zb + 1) & 127))) & (zb >= -8) & (zb < 24)
    down_m[...] = jnp.where(hit, 0.125, 0.0).astype(BF16)
    hit = a == ((base(b) + (zb >> 1)) & 127)
    up_m[...] = jnp.where(hit, 1.0, 0.0).astype(BF16)

    ex_a = Exchange(PLAN_A, (guess, right, react), scr[0], place)
    ex_s = Exchange(PLAN_S, (s1, s2), scr[1], place)
    ex_b = Exchange(PLAN_B, (f1,), scr[2], place)
    ex_c = Exchange(PLAN_C, (eb0,), scr[3], place)
    ex_d = Exchange(PLAN_D, (f2,), scr[4], place)
    cx_b = Cross(PLAN_BX, ex_b, scr[5], place)
    ga_s = Gather(place, scr[6], s3)
    ga_f = Gather(place, scr[7], f3)
    for k, dst in enumerate((guess, right, react)):
        pltpu.make_async_copy(inputs[k], raw[k], in_sems.at[k]).wait()

        for i in range(24):
            dst[pl.ds(L0.row(i, 0), 48), 0:48] = raw[k][i]
            dst[pl.ds(L0.row(i, 0), 48), 64:112] = raw[k][i + 24]
        ex_a.pack_item(k)

    reduced, red_send, red_recv = scr[8]

    pl.semaphore_wait(barrier, len(greeted))
    ex_a.send()

    restrict(react, L0, s1, L1, 0, 12, 0, 24, down_m, tmp)
    restrict(s1, L1, s2, L2, 0, 6, 0, 12, down_m, tmp)
    ex_s.pack()
    ga_s.mine[...] = jnp.zeros((24, 128), F32)
    ga_f.mine[...] = jnp.zeros((24, 128), F32)
    chosen[...] = spread_to_level3(place)
    to_level3(s2, ga_s.mine, square, turned, chosen)
    for h in range(2):
        r = iota2((112, 384), 0)
        l = iota2((112, 384), 1)
        hit = (6 * gx + 3 * h + (r >> 4) - 2 == (l >> 5)) & (6 * gy + (r & 15) - 2 == (l & 31)) & ((r & 15) < 10)
        picks[h] = jnp.where(hit, 1.0, 0.0).astype(BF16)
    for k in range(3):
        down4[k] = jnp.where(match4(k, (128, 128), 1, ny3), 0.125, 0.0).astype(BF16)
        up4[k] = jnp.where(match4(k, (128, 128), 0, ny3), 1.0, 0.0).astype(BF16)


    def start(r):
        at = pl.ds(r, L0.R)
        c, image = image_of(guess, react, L0, r)
        res = right[at, :] - image
        inv = inverse(react[at, :], 1.0)
        return [(r0, res), (inv0, inv), (ea0, inv * res)]

    ex_a.unpack()
    ex_a.x_send()
    ex_s.send()
    ga_s.send()
    ex_a.unpack_rest()
    planes(L0, 1, 23, start)
    ex_a.x_wait()
    ex_a.x_fill()
    planes(L0, -2, 1, start)
    planes(L0, 23, 26, start)
    relax(L0, ea0, eb0, r0, react, inv0, -1, 25)
    leftover(L0, eb0, left0, r0, react, 0, 24)
    restrict(left0, L0, f1, L1, 0, 12, 0, 24, down_m, tmp)
    ex_b.pack_send()
    cx_b.pack_send()
    ex_b.x_send()

    ex_c.pack()
    ex_s.unpack()
    ex_s.x_send()

    def inverse_of(g, sh, inv, first_plane, end):
        planes(g, first_plane, end, lambda r: [(inv, inverse(sh[pl.ds(r, g.R), :], g.factor))])

    inverse_of(L1, s1, inv1, 0, 12)

    ex_b.x_sent()
    ex_b.unpack()
    ex_c.send()
    first(L1, ea1, f1, inv1, 0, 12)
    relax(L1, ea1, eb1, f1, s1, inv1, 1, 11)
    ex_s.x_wait()
    ex_s.x_fill()
    inverse_of(L1, s1, inv1, -6, 0)
    inverse_of(L1, s1, inv1, 12, 18)
    inverse_of(L2, s2, inv2, -5, 11)
    ex_b.x_wait()
    cx_b.unpack()
    ex_b.x_fill()
    first(L1, ea1, f1, inv1, -6, 0)
    first(L1, ea1, f1, inv1, 12, 18)
    relax(L1, ea1, eb1, f1, s1, inv1, -5, 1)
    relax(L1, ea1, eb1, f1, s1, inv1, 11, 17)
    leftover(L1, eb1, left1, f1, s1, -4, 16)
    restrict(left1, L1, f2, L2, -2, 8, -2, 16, down_m, tmp)
    first(L2, ea2, f2, inv2, -2, 8)
    relax(L2, ea2, eb2, f2, s2, inv2, -1, 7)
    leftover(L2, eb2, left2, f2, s2, 0, 6)
    to_level3(left2, ga_f.mine, square, turned, chosen)
    ga_f.send()
    ex_d.pack_send()
    ga_s.relay()

    ga_f.relay()
    ex_c.unpack()
    ex_c.x_send()
    ex_c.unpack_rest()
    ex_d.unpack()
    ex_d.x_send()
    ex_c.x_wait()
    ex_c.x_fill()
    ex_d.x_wait()
    ex_d.x_fill()
    first(L2, ea2, f2, inv2, -5, 11)
    relax(L2, ea2, eb2, f2, s2, inv2, -4, 10)
    ga_s.finish()
    chunks3(n3, inv3, lambda r, n: inverse(s3[pl.ds(r, n), :], FACTOR3))
    s4[...] = restrict4(s3, n4, down4)
    for e in (ex_a, ex_s, ex_c, ex_d, ga_s):
        e.settle()
    for e in (ex_b, cx_b):
        e.settle(False)
    ga_f.finish()

    def relax3(src, dst):
        def body(r, n):
            c, image = image3(src, s3, r, n)
            at = pl.ds(r, n)
            return c + inv3[at, :] * (f3[at, :] - image)

        chunks3(n3, dst, body)

    chunks3(n3, ea3, lambda r, n: inv3[pl.ds(r, n), :] * f3[pl.ds(r, n), :])
    relax3(ea3, eb3)
    chunks3(n3, left3, lambda r, n: f3[pl.ds(r, n), :] - image3(eb3, s3, r, n)[1])
    e4 = bottom(restrict4(left3, n4, down4), s4, p4, n4, ny3 // 2)
    for k in range(3):
        u = mm(e4, up4[k])
        for q in (k, k + 4):
            at = pl.ds(GUARD3 + q, n4, stride=8)
            eb3[at, :] = eb3[at, :] + u
    for src, dst, n in ((eb3, ea3, 48), (ea3, slab, 40)):
        r = pl.multiple_of(GUARD3 + 24 * gz - (n - 24) // 2, 4)
        c, image = image3(src, s3, r, n)
        at = pl.ds(r, n)
        dst[at if n == 48 else pl.ds(0, n), :] = c + inv3[at, :] * (f3[at, :] - image)
    for k in range(3):
        v = slab[pl.ds(k, 10, stride=4), :]
        for h in range(2):
            for q in range(2):
                spread[k, pl.ds(64 * h + q, 10, stride=2), :] = v
    wide = [jnp.concatenate(p, axis=1) for p in zip(*[split(spread[k]) for k in range(3)])]
    coarse = []
    for h in range(2):
        pick = picks[h]
        parts = [
            lax.dot_general(pick, p, (((1,), (1,)), ((), ())), preferred_element_type=F32) for p in wide
        ]
        coarse.append(parts[0] + parts[1])
    fine = roll(jnp.where(lanes(112) < 64, coarse[0], coarse[1]), -4)
    for i in range(7):
        u = fine[16 * i : 16 * i + 10]
        tmp[pl.ds(24 * i, 10, stride=2), :] = u
        tmp[pl.ds(24 * i + 1, 10, stride=2), :] = u
    for i in range(7):
        v = tmp[pl.ds(24 * i, 20), :]
        for q in range(2):
            at = pl.ds(L2.row(2 * (i - 2) + q, -4), 20)
            eb2[at, :] = eb2[at, :] + v
    relax(L2, eb2, ea2, f2, s2, inv2, -3, 9)
    relax(L2, ea2, eb2, f2, s2, inv2, -2, 8)
    prolong(eb2, L2, eb1, L1, -2, 8, -2, 16, up_m, tmp)
    relax(L1, eb1, ea1, f1, s1, inv1, -3, 15)
    relax(L1, ea1, eb1, f1, s1, inv1, -2, 14)
    prolong(eb1, L1, eb0, L0, -2, 14, -2, 28, up_m, tmp)
    relax(L0, eb0, ea0, r0, react, inv0, -2, 26)
    relax(L0, ea0, eb0, r0, react, inv0, -1, 25)

    row = iota2((L0.R, 128), 0)
    inside = ((lanes(L0.R) & 63) < 48) & (row >= L0.y0) & (row < L0.y0 + 48)

    upper, lower = [], []
    for i in range(24):
        r = GUARD + (L0.halo + i) * L0.R
        c, image = image_of(eb0, react, L0, r)
        left0[pl.ds(r, L0.R), :] = image
        upper.append(c * r0[pl.ds(r, L0.R), :])
        lower.append(c * image)
    upper = jnp.where(inside, tree(upper), 0.0)
    lower = jnp.where(inside, tree(lower), 0.0)
    upper = jnp.sum(upper, axis=0, keepdims=True)
    lower = jnp.sum(lower, axis=0, keepdims=True)
    half = lanes(1) < 64
    number = (gx * sizes[1] + gy) * sizes[2] + gz
    reduced[number] = jnp.where(half, upper + roll(upper, 64), lower + roll(lower, 64))
    own = reduced.at[number]

    def summed(src, dst, p):
        return pltpu.make_async_remote_copy(
            src_ref=src, dst_ref=dst, send_sem=red_send.at[0], recv_sem=red_recv.at[0],
            device_id=place.beside(*p), device_id_type=MESH,
        )

    for p in peers:
        summed(own, own, p).start()
    ga_f.settle()
    most = reduced.at[pl.ds(0, len(peers))]
    summed(most, most, peers[0]).wait()
    sums = [reduced[k] for k in range(8)]
    for k in range(8, len(peers) + 1):
        sums[k % 8] = sums[k % 8] + reduced[k]
    total = tree(sums)
    upper = jnp.sum(jnp.where(half, total, 0.0), axis=1, keepdims=True)
    lower = jnp.sum(jnp.where(half, 0.0, total), axis=1, keepdims=True)
    step_out[...] = jnp.broadcast_to(upper / lower, (8, 128))


def finish(guess, r0, eb0, left0, step_ref, field_out, resid_out, field, resid, sems):
    step = step_ref[0:1, :]
    copies = []
    parts, size = 4, 6
    for p in range(parts):
        for x in range(p * size, p * size + size):
            at = pl.ds(L0.row(x, 0), 48)
            v = guess[at, :] + step * eb0[at, :]
            field[x] = v[:, 0:48]
            field[x + 24] = roll(v, 64)[:, 0:48]
            v = r0[at, :] - step * left0[at, :]
            resid[x] = v[:, 0:48]
            resid[x + 24] = roll(v, 64)[:, 0:48]
        for q, (src, dst) in enumerate(((field, field_out), (resid, resid_out))):
            for h in range(2):
                at = pl.ds(p * size + 24 * h, size)
                c = pltpu.make_async_copy(src.at[at], dst.at[at], sems.at[4 * p + 2 * q + h])
                c.start()
                copies.append(c)
    for c in copies:
        c.wait()


def solution(mesh):
    sizes = tuple(mesh.shape[a] for a in ("gx", "gy", "gz"))
    n3, n4 = 24 * sizes[2] + 2 * GUARD3, 3 * sizes[2]
    scratch = [pltpu.VMEM((48, 48, 48), F32)] * 3 + [pltpu.SemaphoreType.DMA((3,))]
    scratch += [pltpu.VMEM((L0.total, 128), F32)] * 4
    scratch += [pltpu.VMEM((L1.total, 128), F32)] * 6
    scratch += [pltpu.VMEM((L2.total, 128), F32)] * 6
    scratch += [pltpu.VMEM((n3, 128), F32)] * 6
    scratch += [pltpu.VMEM((n4, 128), F32), pltpu.VMEM((n4 + 2 * GUARD, 128), F32)]
    scratch += [pltpu.VMEM((128, 128), BF16)] * 2 + [pltpu.VMEM((16 * 56, 128), F32)]
    scratch += [pltpu.VMEM((128, 128), F32)] * 2
    scratch += [pltpu.VMEM((3, 128, 128), F32), pltpu.VMEM((40, 128), F32)]
    scratch += [pltpu.VMEM((128, 384), BF16), pltpu.VMEM((2, 112, 384), BF16)]
    scratch += [pltpu.VMEM((3, 128, 128), BF16)] * 2
    groups = [p.scratch() for p in PLANS] + [gather_scratch(sizes)] * 2
    devices = sizes[0] * sizes[1] * sizes[2]
    groups += [[pltpu.VMEM((devices, 1, 128), F32)] + [pltpu.SemaphoreType.DMA((1,))] * 2]
    for g in groups:
        scratch += g
    counts = tuple(len(g) for g in groups)
    vmem = pl.BlockSpec(memory_space=pltpu.VMEM)

    anywhere = pl.BlockSpec(memory_space=pl.ANY)

    def body(right_side, start_guess, reaction):
        whole = pltpu.VMEM((L0.total, 128), F32)
        parts = pl.pallas_call(
            functools.partial(kernel, sizes, counts),
            out_shape=[whole] * 4 + [pltpu.VMEM((8, 128), F32)],
            in_specs=[anywhere] * 3,
            out_specs=[vmem] * 5,
            scratch_shapes=scratch,
            compiler_params=pltpu.CompilerParams(
                collective_id=0, has_side_effects=True, vmem_limit_bytes=60 * 2**20
            ),
        )(right_side, start_guess, reaction)
        shape = jax.ShapeDtypeStruct(right_side.shape, F32)
        return tuple(
            pl.pallas_call(
                finish,
                out_shape=[shape, shape],
                in_specs=[vmem] * 5,
                out_specs=[anywhere] * 2,
                scratch_shapes=[pltpu.VMEM(right_side.shape, F32)] * 2 + [pltpu.SemaphoreType.DMA((16,))],
                compiler_params=pltpu.CompilerParams(vmem_limit_bytes=16 * 2**20),
            )(*parts)
        )

    placed = P("gx", "gy", "gz")
    return jax.shard_map(
        body, mesh=mesh, in_specs=(placed,) * 3, out_specs=(placed,) * 2, check_vma=False
    )
```

```python
import functools

import jax
import jax.numpy as jnp
from jax import lax
from jax.experimental import pallas as pl
from jax.experimental.pallas import tpu as pltpu
from jax.sharding import PartitionSpec as P

MESH = pl.DeviceIdType.MESH
F32 = jnp.float32
BF16 = jnp.bfloat16
DAMP = 6.0 / 7.0
GUARD = 8
GUARD3 = 16
BOTTOM_ITERS = 6


class Geo:
    def __init__(self, nx, ny, nz, halo, rows, y0, depth, unroll):
        self.nx, self.ny, self.nz, self.halo, self.R, self.y0 = nx, ny, nz, halo, rows, y0
        self.factor = 0.25**depth
        self.unroll = unroll
        self.total = 2 * GUARD + (nx + 2 * halo) * rows

    def row(self, x, y):
        return GUARD + (self.halo + x) * self.R + self.y0 + y


L0 = Geo(24, 48, 48, 4, 56, 4, 0, 28)
L1 = Geo(12, 24, 24, 6, 40, 8, 1, 24)
L2 = Geo(6, 12, 12, 5, 24, 6, 2, 16)
FACTOR3 = 0.25**3
FACTOR4 = 0.25**4


def lanes(rows):
    return lax.broadcasted_iota(jnp.int32, (rows, 128), 1)


def iota2(shape, dim):
    return lax.broadcasted_iota(jnp.int32, shape, dim)


def tree(terms):
    while len(terms) > 1:
        terms = [sum(terms[k + 1 : k + 2], terms[k]) for k in range(0, len(terms), 2)]
    return terms[0]


def roll(v, shift):
    shift = shift % 128
    return v if shift == 0 else pltpu.roll(v, shift, 1)


def split(a):
    hi = a.astype(BF16)
    return hi, (a - hi.astype(F32)).astype(BF16)


def mm(a, b):
    hi, low = split(a)
    return jnp.dot(hi, b, preferred_element_type=F32) + jnp.dot(low, b, preferred_element_type=F32)


def beside_of(ref, r, R):
    c = ref[pl.ds(r, R), :]
    b = ref[pl.ds(r + R, R), :] + ref[pl.ds(r - R, R), :]
    b = b + (ref[pl.ds(r + 1, R), :] + ref[pl.ds(r - 1, R), :])
    b = b + (roll(c, 1) + roll(c, -1))
    return c, b


def image_of(ref, s_ref, g, r):
    c, b = beside_of(ref, r, g.R)
    return c, g.factor * (6.0 * c - b) + s_ref[pl.ds(r, g.R), :] * c


def planes(g, a, b, body):
    unroll = g.unroll

    def group(start, count):
        todo = []
        for k in range(count):
            r = start + k * g.R
            r = r if isinstance(r, int) else pl.multiple_of(r, 8)
            todo.append((r, body(r)))
        for r, pairs in todo:
            for ref, value in pairs:
                ref[pl.ds(r, g.R), :] = value

    trips = (b - a) // unroll
    origin = GUARD + (g.halo + a) * g.R
    if trips == 1:
        group(origin, unroll)
    elif trips:

        def step(i, carry):
            group(pl.multiple_of(origin + i * (unroll * g.R), 8), unroll)
            return carry

        lax.fori_loop(0, trips, step, 0)
    if (b - a) % unroll:
        group(origin + trips * unroll * g.R, (b - a) % unroll)


def inverse(s, factor):
    return jnp.where(s > 0.0, DAMP / (6.0 * factor + s), 0.0)


def relax(g, src, dst, f, s, inv, a, b):
    def body(r):
        c, image = image_of(src, s, g, r)
        at = pl.ds(r, g.R)
        return [(dst, c + inv[at, :] * (f[at, :] - image))]

    planes(g, a, b, body)


def first(g, dst, f, inv, a, b):
    def body(r):
        at = pl.ds(r, g.R)
        return [(dst, inv[at, :] * f[at, :])]

    planes(g, a, b, body)


def leftover(g, src, dst, f, s, a, b):
    def body(r):
        c, image = image_of(src, s, g, r)
        return [(dst, f[pl.ds(r, g.R), :] - image)]

    planes(g, a, b, body)


def restrict(src, gs, dst, gd, x0, x1, y0, count, matrix, tmp):
    step = -(-count // 8) * 8
    for x in range(x0, x1):
        r = gs.row(2 * x, 2 * y0)
        t = src[pl.ds(r, count, stride=2), :] + src[pl.ds(r + 1, count, stride=2), :]
        r = r + gs.R
        t = t + (src[pl.ds(r, count, stride=2), :] + src[pl.ds(r + 1, count, stride=2), :])
        tmp[pl.ds((x - x0) * step, count), :] = t
    for x in range(x0, x1):
        out = mm(tmp[pl.ds((x - x0) * step, step), :], matrix[...])
        dst[pl.ds(gd.row(x, y0), count), :] = out[0:count]


def prolong(src, gc, dst, gf, x0, x1, y0, count, matrix, tmp):
    for x in range(x0, x1):
        o = (x - x0) * 56
        u = mm(src[pl.ds(gc.row(x, y0), count), :], matrix[...])
        tmp[pl.ds(o, count, stride=2), :] = u
        tmp[pl.ds(o + 1, count, stride=2), :] = u
    for x in range(x0, x1):
        o = (x - x0) * 56
        v = tmp[pl.ds(o, 2 * count), :]
        for k in range(2):
            at = pl.ds(gf.row(2 * x + k, 2 * y0), 2 * count)
            dst[at, :] = dst[at, :] + v


class Item:
    def __init__(self, geo, w):
        self.g, self.w = geo, w


class Plan:
    def __init__(self, items, cross=False):
        self.items, self.cross = items, cross
        self.counts = [it.w if cross else it.g.nx for it in items]
        self.yrows = sum(n * it.w for n, it in zip(self.counts, items))
        self.yrows = -(-self.yrows // 8) * 8
        self.tiles = []
        for k, it in enumerate(items):
            for x in range(self.counts[k]):
                for t in self.tiles:
                    if t[0] is it.g and t[1] + it.w <= 64:
                        break
                else:
                    t = [it.g, 0, []]
                    self.tiles.append(t)
                t[2].append((k, x, t[1]))
                t[1] += it.w
        self.zrows = sum(t[0].ny for t in self.tiles)
        self.zrows = -(-self.zrows // 8) * 8
        self.drows = max(self.counts)
        self.drows = -(-self.drows // 8) * 8
        assert sum(it.w * it.w for it in items) <= 64

        self.z0 = [0, self.zrows]
        self.d0 = [2 * self.zrows + q * self.drows for q in range(4)]
        self.y0 = [2 * self.zrows + 4 * self.drows + q * self.yrows for q in range(2)]
        self.total = 2 * (self.zrows + self.yrows) + 4 * self.drows
        self.xtotal = sum(it.w * it.g.R for it in items)

    def scratch(self):
        x = [] if self.cross else [pltpu.VMEM((self.xtotal, 128), F32)]
        return x + [
            pltpu.VMEM((self.total, 128), F32),
            pltpu.VMEM((self.total, 128), F32),
            pltpu.SemaphoreType.DMA((2,)),
            pltpu.SemaphoreType.DMA((2,)),
        ]


class Exchange:
    def __init__(self, plan, refs, scratch, place):
        self.plan, self.refs, self.place = plan, refs, place
        self.xr, self.sent, self.got, self.ss, self.rs = scratch
        gx, gy, gz = place.me
        self.partner = (1 - gx, gy, gz)
        self.x_copies = []
        o = 0
        for k, it in enumerate(plan.items):
            r = pl.multiple_of(GUARD + (it.g.halo + self.edge(it)) * it.g.R, 8)
            n = it.w * it.g.R
            self.x_copies.append(self.copy(refs[k].at[pl.ds(r, n), :], self.xr.at[pl.ds(o, n), :], 0, self.partner))
            o += n
        self.segments(0)

    def edge(self, it):
        return jnp.where(self.place.me[0] == 0, it.g.nx - it.w, 0)

    def source(self, k, x, y):
        return self.plan.items[k].g.row(x, y)

    def target(self, k, x, y):
        return self.refs[k], self.plan.items[k].g.row(x, y)

    def segments(self, dx):
        plan = self.plan
        at = {}
        for d in range(2):
            at[1 - 2 * d, 0] = plan.y0[d]
            at[0, 1 - 2 * d] = plan.z0[d]
            for e in range(2):
                at[1 - 2 * d, 1 - 2 * e] = plan.d0[2 * d + e]
        self.y_copies, self.z_copies, self.d_copies = [], [], []
        for d in (1, -1):
            self.y_copies.append(self.segment(at, dx, d, 0, plan.yrows))
            self.z_copies.append(self.segment(at, dx, 0, d, plan.zrows))
            for e in (1, -1):
                self.d_copies.append(self.segment(at, dx, d, e, plan.drows))

    def segment(self, at, dx, dy, dz, n):
        there = self.place.exists(dy, dz)
        peer = self.place.beside(dx, dy, dz)
        peer = tuple(jnp.where(there, p, q) for p, q in zip(peer, self.partner))
        target = pl.multiple_of(jnp.where(there, at[dy, dz], at[-dy, -dz]), 8)
        return self.copy(self.sent.at[pl.ds(at[dy, dz], n), :], self.got.at[pl.ds(target, n), :], 1, peer)

    def copy(self, src, dst, k, peer):
        return pltpu.make_async_remote_copy(
            src_ref=src, dst_ref=dst, send_sem=self.ss.at[k], recv_sem=self.rs.at[k],
            device_id=peer, device_id_type=MESH,
        )

    def x_send(self):
        for c in self.x_copies:
            c.start()

    def settle(self, x=True):
        if x:
            self.x_sent()
        self.copy(self.sent, self.got, 1, self.partner).wait_send()

    def x_sent(self):
        self.copy(self.xr, self.xr, 0, self.partner).wait_send()

    def x_wait(self):
        self.copy(self.xr, self.xr, 0, self.partner).wait_recv()

    def x_fill(self):
        m0, m1 = self.place.x_masks
        o = 0
        for k, it in enumerate(self.plan.items):
            g, w, ref = it.g, it.w, self.refs[k]
            upper = ((lanes(g.R) + 8) & 127) >= 64
            for j in range(w):
                got = self.xr[pl.ds(o + j * g.R, g.R), :]
                top = ref[pl.ds(GUARD + (g.halo + g.nx - w + j) * g.R, g.R), :]
                low = ref[pl.ds(GUARD + (g.halo + j) * g.R, g.R), :]
                ref[pl.ds(GUARD + (g.halo - w + j) * g.R, g.R), :] = roll(jnp.where(upper, got * m1, top), 64)
                ref[pl.ds(GUARD + (g.halo + g.nx + j) * g.R, g.R), :] = roll(jnp.where(upper, low, got * m0), 64)
            o += w * g.R

    def pack_send(self):
        self.pack()
        self.send()

    def pack(self):
        for k in range(len(self.refs)):
            self.pack_item(k)

    def send(self):
        for c in self.d_copies + self.z_copies + self.y_copies:
            c.start()

    def pack_item(self, k):
        if k == 0:
            self.yo, self.co, self.corner = 0, 0, [None] * 4
        it = self.plan.items[k]
        g, w, ref = it.g, it.w, self.refs[k]
        n = self.plan.counts[k]
        lane = lanes(self.plan.drows) & 63
        for d in range(1, w + 1):
            at = self.co + (d - 1) * w
            for e, y in enumerate((g.ny - d, d - 1)):
                v = ref[pl.ds(self.source(k, 0, y), n, stride=g.R), :]
                self.sent[pl.ds(self.plan.y0[e] + self.yo, n), :] = v
                if n < self.plan.drows:
                    v = jnp.concatenate([v, jnp.zeros((self.plan.drows - n, 128), F32)], axis=0)
                for q, z in enumerate((g.nz - w, 0)):
                    moved = roll(v, at - z)
                    old = self.corner[2 * e + q]
                    self.corner[2 * e + q] = moved if old is None else jnp.where(lane >= at, moved, old)
            self.yo += n
        self.co += w * w
        if k == len(self.refs) - 1:
            for q in range(4):
                self.sent[pl.ds(self.plan.d0[q], self.plan.drows), :] = self.corner[q]
        zo = 0
        for t, _, slots in self.plan.tiles:
            if slots[-1][0] == k:
                self.pack_tile(t, slots, zo)
            zo += t.ny

    def pack_tile(self, g, slots, zo):
        lane = lanes(g.ny)
        acc = [None, None]
        for k, x, at in slots:
            w = self.plan.items[k].w
            moved = roll(self.refs[k][pl.ds(self.source(k, x, 0), g.ny), :], at)
            for q, past in enumerate((g.nz - w, 0)):
                here = ((lane - past) & 63 >= at) & ((lane - past) & 63 < at + w)
                acc[q] = moved if acc[q] is None else jnp.where(here, moved, acc[q])
        for q in range(2):
            self.sent[pl.ds(self.plan.z0[q] + zo, g.ny), :] = acc[q]

    def unpack(self):
        my, mz = self.place.y_masks, self.place.z_masks
        self.copy(self.sent, self.got, 1, self.partner).wait_recv()
        yo, co = 0, 0
        for k, it in enumerate(self.plan.items):
            g, w = it.g, it.w
            n = self.plan.counts[k]
            lane = lanes(n) & 63
            into = (lane >= 64 - w, (lane >= g.nz) & (lane < g.nz + w))
            for d in range(1, w + 1):
                at = co + (d - 1) * w
                for e, y in enumerate((-d, g.ny + d - 1)):
                    v = self.got[pl.ds(self.plan.y0[e] + yo, n), :]
                    for q, z in enumerate((-w, g.nz)):
                        got = self.got[pl.ds(self.plan.d0[2 * e + q], n), :] * mz[q]
                        v = jnp.where(into[q], roll(got, z - at), v)
                    ref, r = self.target(k, 0, y)
                    ref[pl.ds(r, n, stride=g.R), :] = v * my[e]
                yo += n
            co += w * w
        self.unpack_z(True)

    def unpack_rest(self):
        self.unpack_z(False)

    def unpack_z(self, edge):
        mz = self.place.z_masks
        zo = 0
        for g, _, slots in self.plan.tiles:
            lane = lanes(g.ny) & 63
            got = [self.got[pl.ds(self.plan.z0[q] + zo, g.ny), :] * mz[q] for q in range(2)]
            for k, x, at in slots:
                w = self.plan.items[k].w
                if (x < w or x >= g.nx - w) != edge:
                    continue
                ref, r = self.target(k, x, 0)
                rows = pl.ds(r, g.ny)
                v = ref[rows, :]
                v = jnp.where(lane >= 64 - w, roll(got[0], -g.nz - at), v)
                v = jnp.where((lane >= g.nz) & (lane < g.nz + w), roll(got[1], g.nz - at), v)
                ref[rows, :] = v
            zo += g.ny


class Cross(Exchange):
    def __init__(self, plan, main, scratch, place):
        self.plan, self.main, self.refs, self.place = plan, main, main.refs, place
        self.sent, self.got, self.ss, self.rs = scratch
        self.partner = main.partner
        self.segments(1)

    def source(self, k, x, y):
        it = self.plan.items[k]
        return GUARD + (it.g.halo + self.edge(it) + x) * it.g.R + it.g.y0 + y

    def target(self, k, x, y):
        o = sum(it.w * it.g.R for it in self.plan.items[:k])
        g = self.plan.items[k].g
        return self.main.xr, o + x * g.R + g.y0 + y


class Place:
    def __init__(self, sizes):
        self.sizes = sizes
        self.me = tuple(lax.axis_index(a) for a in ("gx", "gy", "gz"))
        gx, gy, gz = self.me
        one = lambda c: jnp.where(c, 1.0, 0.0).astype(F32)
        self.x_masks = (one(gx == 0), one(gx == 1))
        self.y_masks = (one(gy > 0), one(gy < sizes[1] - 1))
        self.z_masks = (one(gz > 0), one(gz < sizes[2] - 1))

    def exists(self, dy, dz):
        gx, gy, gz = self.me
        y, z = gy + dy, gz + dz
        return (y >= 0) & (y < self.sizes[1]) & (z >= 0) & (z < self.sizes[2])

    def beside(self, dx, dy, dz):
        return tuple(
            lax.rem(m + d % n, n) if d % n else m for m, d, n in zip(self.me, (dx, dy, dz), self.sizes)
        )


class Gather:
    rows = 24

    def __init__(self, place, scratch, whole):
        self.place, self.whole = place, whole
        self.mine, self.got, self.sum, self.ss, self.rs = scratch
        n = place.sizes
        self.near = [(a, b) for a in range(n[0]) for b in range(n[1])][1:]
        self.near.sort(key=lambda p: -far((p[0], p[1], 0), n))
        self.line = sorted(range(1, n[2]), key=lambda c: -far((0, 0, c), n))
        self.at = pl.ds(pl.multiple_of(GUARD3 + self.rows * place.me[2], 8), self.rows)

    def copy(self, src, dst, k, peer):
        return pltpu.make_async_remote_copy(
            src_ref=src, dst_ref=dst, send_sem=self.ss.at[k], recv_sem=self.rs.at[k],
            device_id=peer, device_id_type=MESH,
        )

    def send(self):
        for k, (a, b) in enumerate(self.near):
            self.copy(self.mine, self.got.at[k], 0, self.place.beside(a, b, 0)).start()

    def relay(self):
        self.copy(self.got, self.got, 0, self.place.beside(1, 0, 0)).wait_recv()
        total = self.mine[...]
        for k in range(len(self.near)):
            total = total + self.got[k]
        self.sum[...] = total
        for c in self.line:
            self.copy(self.sum, self.whole.at[self.at, :], 1, self.place.beside(0, 0, c)).start()
        self.whole[self.at, :] = total

    def finish(self):
        self.most().wait_recv()

    def most(self):
        most = self.whole.at[pl.ds(GUARD3, self.rows * (self.place.sizes[2] - 1)), :]
        return self.copy(most, most, 1, self.place.beside(1, 0, 0))

    def settle(self):
        self.copy(self.got, self.got, 0, self.place.beside(1, 0, 0)).wait_send()
        self.most().wait_send()


def gather_scratch(sizes):
    return [
        pltpu.VMEM((24, 128), F32),
        pltpu.VMEM((sizes[0] * sizes[1] - 1, 24, 128), F32),
        pltpu.VMEM((24, 128), F32),
        pltpu.SemaphoreType.DMA((2,)),
        pltpu.SemaphoreType.DMA((2,)),
    ]


def spread_to_level3(place):
    gx, gy, gz = place.me
    r = iota2((128, 384), 0)
    l = iota2((128, 384), 1)
    x = 6 * gx + 3 * (r >> 6) + ((r & 63) >> 3)
    y = 6 * gy + (r & 7)
    hit = (x == (l >> 5)) & (y == (l & 31)) & ((r & 7) < 6) & ((r & 63) < 24)
    return jnp.where(hit, 1.0, 0.0).astype(BF16)


def to_level3(src, mine, square, turned, chosen):
    g = L2
    for i in range(3):
        r = g.row(2 * i, 0)
        t = src[pl.ds(r, 6, stride=2), :] + src[pl.ds(r + 1, 6, stride=2), :]
        r = r + g.R
        t = t + (src[pl.ds(r, 6, stride=2), :] + src[pl.ds(r + 1, 6, stride=2), :])
        square[pl.ds(8 * i, 6), :] = t
    turned[...] = jnp.transpose(square[...])
    a = turned[pl.ds(0, 8, stride=2), :] + turned[pl.ds(1, 8, stride=2), :]
    b = turned[pl.ds(64, 8, stride=2), :] + turned[pl.ds(65, 8, stride=2), :]
    a = (a + roll(b, 64)) * 0.125
    out = mm(a, chosen[...])
    for k in range(3):
        mine[pl.ds(k, 6, stride=4), :] = out[0:6, 128 * k : 128 * k + 128]


def image3(ref, s_ref, r, n):
    lane = lanes(n)
    c = ref[pl.ds(r, n), :]
    b = ref[pl.ds(r + 4, n), :] + ref[pl.ds(r - 4, n), :]
    b = b + (roll(c, 1) + roll(c, -1))
    b = b + roll(jnp.where(lane < 32, ref[pl.ds(r + 1, n), :], c), -32)
    b = b + roll(jnp.where(lane >= 96, ref[pl.ds(r - 1, n), :], c), 32)
    return c, FACTOR3 * (6.0 * c - b) + s_ref[pl.ds(r, n), :] * c


def chunks3(rows, ref, body):
    n = min(rows, 384)

    def step(i, carry):
        r = pl.multiple_of(GUARD3 + i * n, 8)
        ref[pl.ds(r, n), :] = body(r, n)
        return carry

    lax.fori_loop(0, rows // n, step, 0)


def match4(k, shape, coarse_dim, ny):
    c = iota2(shape, coarse_dim)
    l = iota2(shape, 1 - coarse_dim)
    return ((c >> 4) == 2 * k + (l >> 6)) & ((c & 15) == ((l & 31) >> 1)) & ((l & 31) < ny)


def restrict4(src, n, matrix):
    total = None
    for k in range(3):
        t = src[pl.ds(GUARD3 + k, n, stride=8), :] + src[pl.ds(GUARD3 + k + 4, n, stride=8), :]
        part = mm(t, matrix[k])
        total = part if total is None else total + part
    return total


def dot_all(a, b):
    return jnp.sum(jnp.sum(a * b, axis=0, keepdims=True), axis=1, keepdims=True)


def bottom(source, s4, p4, n, ny):
    estimate = jnp.zeros_like(source)
    left = source
    inside = (lanes(n) < 96) & ((lanes(n) & 15) < ny)
    shifted = 6.0 * FACTOR4 + s4[...]
    for it in range(BOTTOM_ITERS):
        p4[pl.ds(GUARD, n), :] = left
        b = p4[pl.ds(GUARD + 1, n), :] + p4[pl.ds(GUARD - 1, n), :]
        b = b + (roll(left, 1) + roll(left, -1))
        b = b + (roll(left, 16) + roll(left, -16))
        image = shifted * left - FACTOR4 * jnp.where(inside, b, 0.0)
        now = dot_all(left, left)
        bent = dot_all(left, image)
        if it == 0:
            denom = bent
            direction, turned = left, image
        else:
            ratio = now * inv_before
            denom = bent - ratio * ratio * denom
            direction = left + ratio * direction
            turned = image + ratio * turned
        step = now / denom
        inv_before = 1.0 / now
        estimate = estimate + step * direction
        if it < BOTTOM_ITERS - 1:
            left = left - step * turned
    return estimate


PLAN_A = Plan([Item(L0, 3), Item(L0, 2), Item(L0, 2)])
PLAN_S = Plan([Item(L1, 6), Item(L2, 5)])
PLAN_B = Plan([Item(L1, 6)])
PLAN_BX = Plan([Item(L1, 6)], True)
PLAN_C = Plan([Item(L0, 3)])
PLAN_D = Plan([Item(L2, 5)])
PLANS = (PLAN_A, PLAN_S, PLAN_B, PLAN_C, PLAN_D, PLAN_BX)


def far(p, sizes):
    ring = lambda d, n: min(d % n, -d % n)
    return p[0] + ring(p[1], sizes[1]) + ring(p[2], 4) + ring(p[2] // 4, 4)


def kernel(sizes, counts, right_in, guess_in, react_in, guess, r0, eb0, left0, step_out, *scratch):
    scratch = list(scratch)

    def take(n):
        out = scratch[:n]
        del scratch[:n]
        return out

    raw = take(3)
    (in_sems,) = take(1)
    right, react, inv0, ea0 = take(4)
    f1, s1, inv1, ea1, eb1, left1 = take(6)
    f2, s2, inv2, ea2, eb2, left2 = take(6)
    f3, s3, inv3, ea3, eb3, left3 = take(6)
    s4, p4, down_m, up_m, tmp, square, turned, spread, slab = take(9)
    chosen, picks, down4, up4 = take(4)
    scr = [take(n) for n in counts]
    place = Place(sizes)
    gx, gy, gz = place.me
    n3, n4, ny3 = 24 * sizes[2], 3 * sizes[2], 6 * sizes[1]

    inputs = (guess_in, right_in, react_in)
    for k in range(3):
        for q in range(4):
            at = pl.ds(12 * q, 12)
            pltpu.make_async_copy(inputs[k].at[at], raw[k].at[at], in_sems.at[k]).start()

    def clear(ref):
        n = ref.shape[0]
        size = next(k for k in (128, 122 * 8, 80, 8) if n % k == 0) if n > 128 else n
        size = {1808: 904, 976: 488, 416: 208}.get(n, size)

        def step(i, carry):
            ref[pl.ds(pl.multiple_of(i * size, 8), size), :] = jnp.zeros((size, 128), F32)
            return carry

        lax.fori_loop(0, n // size, step, 0)

    peers = [(a, b, c) for a in range(sizes[0]) for b in range(sizes[1]) for c in range(sizes[2])][1:]
    peers.sort(key=lambda p: -far(p, sizes))
    beside = {(a, b % sizes[1], c % sizes[2]) for a in range(2) for b in (1, -1) for c in (1, -1)}
    beside |= {(1, 0, c % sizes[2]) for c in (1, -1)}
    greeted = [p for p in peers if p[2] == 0 or p[:2] == (0, 0) or p in beside]
    barrier = pltpu.get_barrier_semaphore()
    for p in greeted:
        pl.semaphore_signal(barrier, inc=1, device_id=place.beside(*p), device_id_type=MESH)
    for ref in (guess, right, react, f1, s1, ea1, eb1, f2, s2, ea2, eb2, ea3, eb3, p4, square):
        clear(ref)
    spread[...] = jnp.zeros_like(spread)
    for ref in (f3, s3, inv3):
        for r in (0, GUARD3 + n3):
            ref[pl.ds(r, GUARD3), :] = jnp.zeros((GUARD3, 128), F32)

    a = iota2((128, 128), 0)
    b = iota2((128, 128), 1)
    signed = lambda v: ((v + 8) & 63) - 8
    base = lambda v: ((v + 8) & 127) & 64
    zb = signed(b)
    hit = ((a == ((base(b) + 2 * zb) & 127)) | (a == ((base(b) + 2 * zb + 1) & 127))) & (zb >= -8) & (zb < 24)
    down_m[...] = jnp.where(hit, 0.125, 0.0).astype(BF16)
    hit = a == ((base(b) + (zb >> 1)) & 127)
    up_m[...] = jnp.where(hit, 1.0, 0.0).astype(BF16)

    ex_a = Exchange(PLAN_A, (guess, right, react), scr[0], place)
    ex_s = Exchange(PLAN_S, (s1, s2), scr[1], place)
    ex_b = Exchange(PLAN_B, (f1,), scr[2], place)
    ex_c = Exchange(PLAN_C, (eb0,), scr[3], place)
    ex_d = Exchange(PLAN_D, (f2,), scr[4], place)
    cx_b = Cross(PLAN_BX, ex_b, scr[5], place)
    ga_s = Gather(place, scr[6], s3)
    ga_f = Gather(place, scr[7], f3)
    for k, dst in enumerate((guess, right, react)):
        pltpu.make_async_copy(inputs[k], raw[k], in_sems.at[k]).wait()

        for i in range(24):
            dst[pl.ds(L0.row(i, 0), 48), 0:48] = raw[k][i]
            dst[pl.ds(L0.row(i, 0), 48), 64:112] = raw[k][i + 24]
        ex_a.pack_item(k)

    reduced, red_send, red_recv = scr[8]

    pl.semaphore_wait(barrier, len(greeted))
    ex_a.send()

    restrict(react, L0, s1, L1, 0, 12, 0, 24, down_m, tmp)
    restrict(s1, L1, s2, L2, 0, 6, 0, 12, down_m, tmp)
    ex_s.pack()
    ga_s.mine[...] = jnp.zeros((24, 128), F32)
    ga_f.mine[...] = jnp.zeros((24, 128), F32)
    chosen[...] = spread_to_level3(place)
    to_level3(s2, ga_s.mine, square, turned, chosen)
    for h in range(2):
        r = iota2((112, 384), 0)
        l = iota2((112, 384), 1)
        hit = (6 * gx + 3 * h + (r >> 4) - 2 == (l >> 5)) & (6 * gy + (r & 15) - 2 == (l & 31)) & ((r & 15) < 10)
        picks[h] = jnp.where(hit, 1.0, 0.0).astype(BF16)
    for k in range(3):
        down4[k] = jnp.where(match4(k, (128, 128), 1, ny3), 0.125, 0.0).astype(BF16)
        up4[k] = jnp.where(match4(k, (128, 128), 0, ny3), 1.0, 0.0).astype(BF16)


    def start(r):
        at = pl.ds(r, L0.R)
        c, image = image_of(guess, react, L0, r)
        res = right[at, :] - image
        inv = inverse(react[at, :], 1.0)
        return [(r0, res), (inv0, inv), (ea0, inv * res)]

    ex_a.unpack()
    ex_a.x_send()
    ex_s.send()
    ga_s.send()
    ex_a.unpack_rest()
    planes(L0, 1, 23, start)
    ex_a.x_wait()
    ex_a.x_fill()
    planes(L0, -2, 1, start)
    planes(L0, 23, 26, start)
    relax(L0, ea0, eb0, r0, react, inv0, -1, 25)
    leftover(L0, eb0, left0, r0, react, 0, 24)
    restrict(left0, L0, f1, L1, 0, 12, 0, 24, down_m, tmp)
    ex_b.pack_send()
    cx_b.pack_send()
    ex_b.x_send()

    ex_c.pack()
    ex_s.unpack()
    ex_s.x_send()

    def inverse_of(g, sh, inv, first_plane, end):
        planes(g, first_plane, end, lambda r: [(inv, inverse(sh[pl.ds(r, g.R), :], g.factor))])

    inverse_of(L1, s1, inv1, 0, 12)

    ex_c.send()
    ex_b.x_sent()
    ex_b.unpack()
    first(L1, ea1, f1, inv1, 0, 12)
    relax(L1, ea1, eb1, f1, s1, inv1, 1, 11)
    ex_s.x_wait()
    ex_s.x_fill()
    inverse_of(L1, s1, inv1, -6, 0)
    inverse_of(L1, s1, inv1, 12, 18)
    inverse_of(L2, s2, inv2, -5, 11)
    ex_b.x_wait()
    cx_b.unpack()
    ex_b.x_fill()
    first(L1, ea1, f1, inv1, -6, 0)
    first(L1, ea1, f1, inv1, 12, 18)
    relax(L1, ea1, eb1, f1, s1, inv1, -5, 1)
    relax(L1, ea1, eb1, f1, s1, inv1, 11, 17)
    leftover(L1, eb1, left1, f1, s1, -4, 16)
    restrict(left1, L1, f2, L2, -2, 8, -2, 16, down_m, tmp)
    first(L2, ea2, f2, inv2, -2, 8)
    relax(L2, ea2, eb2, f2, s2, inv2, -1, 7)
    leftover(L2, eb2, left2, f2, s2, 0, 6)
    to_level3(left2, ga_f.mine, square, turned, chosen)
    ga_f.send()
    ex_d.pack_send()
    ga_s.relay()

    ga_f.relay()
    ex_c.unpack()
    ex_c.x_send()
    ex_c.unpack_rest()
    ex_d.unpack()
    ex_d.x_send()
    ex_c.x_wait()
    ex_c.x_fill()
    ex_d.x_wait()
    ex_d.x_fill()
    first(L2, ea2, f2, inv2, -5, 11)
    relax(L2, ea2, eb2, f2, s2, inv2, -4, 10)
    ga_s.finish()
    chunks3(n3, inv3, lambda r, n: inverse(s3[pl.ds(r, n), :], FACTOR3))
    s4[...] = restrict4(s3, n4, down4)
    for e in (ex_a, ex_s, ex_c, ex_d, ga_s):
        e.settle()
    for e in (ex_b, cx_b):
        e.settle(False)
    ga_f.finish()

    def relax3(src, dst):
        def body(r, n):
            c, image = image3(src, s3, r, n)
            at = pl.ds(r, n)
            return c + inv3[at, :] * (f3[at, :] - image)

        chunks3(n3, dst, body)

    chunks3(n3, ea3, lambda r, n: inv3[pl.ds(r, n), :] * f3[pl.ds(r, n), :])
    relax3(ea3, eb3)
    chunks3(n3, left3, lambda r, n: f3[pl.ds(r, n), :] - image3(eb3, s3, r, n)[1])
    e4 = bottom(restrict4(left3, n4, down4), s4, p4, n4, ny3 // 2)
    for k in range(3):
        u = mm(e4, up4[k])
        for q in (k, k + 4):
            at = pl.ds(GUARD3 + q, n4, stride=8)
            eb3[at, :] = eb3[at, :] + u
    for src, dst, n in ((eb3, ea3, 48), (ea3, slab, 40)):
        r = pl.multiple_of(GUARD3 + 24 * gz - (n - 24) // 2, 4)
        c, image = image3(src, s3, r, n)
        at = pl.ds(r, n)
        dst[at if n == 48 else pl.ds(0, n), :] = c + inv3[at, :] * (f3[at, :] - image)
    for k in range(3):
        v = slab[pl.ds(k, 10, stride=4), :]
        for h in range(2):
            for q in range(2):
                spread[k, pl.ds(64 * h + q, 10, stride=2), :] = v
    wide = [jnp.concatenate(p, axis=1) for p in zip(*[split(spread[k]) for k in range(3)])]
    coarse = []
    for h in range(2):
        pick = picks[h]
        parts = [
            lax.dot_general(pick, p, (((1,), (1,)), ((), ())), preferred_element_type=F32) for p in wide
        ]
        coarse.append(parts[0] + parts[1])
    fine = roll(jnp.where(lanes(112) < 64, coarse[0], coarse[1]), -4)
    for i in range(7):
        u = fine[16 * i : 16 * i + 10]
        tmp[pl.ds(24 * i, 10, stride=2), :] = u
        tmp[pl.ds(24 * i + 1, 10, stride=2), :] = u
    for i in range(7):
        v = tmp[pl.ds(24 * i, 20), :]
        for q in range(2):
            at = pl.ds(L2.row(2 * (i - 2) + q, -4), 20)
            eb2[at, :] = eb2[at, :] + v
    relax(L2, eb2, ea2, f2, s2, inv2, -3, 9)
    relax(L2, ea2, eb2, f2, s2, inv2, -2, 8)
    prolong(eb2, L2, eb1, L1, -2, 8, -2, 16, up_m, tmp)
    relax(L1, eb1, ea1, f1, s1, inv1, -3, 15)
    relax(L1, ea1, eb1, f1, s1, inv1, -2, 14)
    prolong(eb1, L1, eb0, L0, -2, 14, -2, 28, up_m, tmp)
    relax(L0, eb0, ea0, r0, react, inv0, -2, 26)
    relax(L0, ea0, eb0, r0, react, inv0, -1, 25)

    row = iota2((L0.R, 128), 0)
    inside = ((lanes(L0.R) & 63) < 48) & (row >= L0.y0) & (row < L0.y0 + 48)

    upper, lower = [], []
    for i in range(24):
        r = GUARD + (L0.halo + i) * L0.R
        c, image = image_of(eb0, react, L0, r)
        left0[pl.ds(r, L0.R), :] = image
        upper.append(c * r0[pl.ds(r, L0.R), :])
        lower.append(c * image)
    upper = jnp.where(inside, tree(upper), 0.0)
    lower = jnp.where(inside, tree(lower), 0.0)
    upper = jnp.sum(upper, axis=0, keepdims=True)
    lower = jnp.sum(lower, axis=0, keepdims=True)
    half = lanes(1) < 64
    number = (gx * sizes[1] + gy) * sizes[2] + gz
    reduced[number] = jnp.where(half, upper + roll(upper, 64), lower + roll(lower, 64))
    own = reduced.at[number]

    def summed(src, dst, p):
        return pltpu.make_async_remote_copy(
            src_ref=src, dst_ref=dst, send_sem=red_send.at[0], recv_sem=red_recv.at[0],
            device_id=place.beside(*p), device_id_type=MESH,
        )

    for p in peers:
        summed(own, own, p).start()
    ga_f.settle()
    most = reduced.at[pl.ds(0, len(peers))]
    summed(most, most, peers[0]).wait()
    sums = [reduced[k] for k in range(8)]
    for k in range(8, len(peers) + 1):
        sums[k % 8] = sums[k % 8] + reduced[k]
    total = tree(sums)
    upper = jnp.sum(jnp.where(half, total, 0.0), axis=1, keepdims=True)
    lower = jnp.sum(jnp.where(half, 0.0, total), axis=1, keepdims=True)
    step_out[...] = jnp.broadcast_to(upper / lower, (8, 128))


def finish(guess, r0, eb0, left0, step_ref, field_out, resid_out, field, resid, sems):
    step = step_ref[0:1, :]
    copies = []
    parts, size = 4, 6
    for p in range(parts):
        for x in range(p * size, p * size + size):
            at = pl.ds(L0.row(x, 0), 48)
            v = guess[at, :] + step * eb0[at, :]
            field[x] = v[:, 0:48]
            field[x + 24] = roll(v, 64)[:, 0:48]
            v = r0[at, :] - step * left0[at, :]
            resid[x] = v[:, 0:48]
            resid[x + 24] = roll(v, 64)[:, 0:48]
        for q, (src, dst) in enumerate(((field, field_out), (resid, resid_out))):
            for h in range(2):
                at = pl.ds(p * size + 24 * h, size)
                c = pltpu.make_async_copy(src.at[at], dst.at[at], sems.at[4 * p + 2 * q + h])
                c.start()
                copies.append(c)
    for c in copies:
        c.wait()


def solution(mesh):
    sizes = tuple(mesh.shape[a] for a in ("gx", "gy", "gz"))
    n3, n4 = 24 * sizes[2] + 2 * GUARD3, 3 * sizes[2]
    scratch = [pltpu.VMEM((48, 48, 48), F32)] * 3 + [pltpu.SemaphoreType.DMA((3,))]
    scratch += [pltpu.VMEM((L0.total, 128), F32)] * 4
    scratch += [pltpu.VMEM((L1.total, 128), F32)] * 6
    scratch += [pltpu.VMEM((L2.total, 128), F32)] * 6
    scratch += [pltpu.VMEM((n3, 128), F32)] * 6
    scratch += [pltpu.VMEM((n4, 128), F32), pltpu.VMEM((n4 + 2 * GUARD, 128), F32)]
    scratch += [pltpu.VMEM((128, 128), BF16)] * 2 + [pltpu.VMEM((16 * 56, 128), F32)]
    scratch += [pltpu.VMEM((128, 128), F32)] * 2
    scratch += [pltpu.VMEM((3, 128, 128), F32), pltpu.VMEM((40, 128), F32)]
    scratch += [pltpu.VMEM((128, 384), BF16), pltpu.VMEM((2, 112, 384), BF16)]
    scratch += [pltpu.VMEM((3, 128, 128), BF16)] * 2
    groups = [p.scratch() for p in PLANS] + [gather_scratch(sizes)] * 2
    devices = sizes[0] * sizes[1] * sizes[2]
    groups += [[pltpu.VMEM((devices, 1, 128), F32)] + [pltpu.SemaphoreType.DMA((1,))] * 2]
    for g in groups:
        scratch += g
    counts = tuple(len(g) for g in groups)
    vmem = pl.BlockSpec(memory_space=pltpu.VMEM)

    anywhere = pl.BlockSpec(memory_space=pl.ANY)

    def body(right_side, start_guess, reaction):
        whole = pltpu.VMEM((L0.total, 128), F32)
        parts = pl.pallas_call(
            functools.partial(kernel, sizes, counts),
            out_shape=[whole] * 4 + [pltpu.VMEM((8, 128), F32)],
            in_specs=[anywhere] * 3,
            out_specs=[vmem] * 5,
            scratch_shapes=scratch,
            compiler_params=pltpu.CompilerParams(
                collective_id=0, has_side_effects=True, vmem_limit_bytes=60 * 2**20
            ),
        )(right_side, start_guess, reaction)
        shape = jax.ShapeDtypeStruct(right_side.shape, F32)
        return tuple(
            pl.pallas_call(
                finish,
                out_shape=[shape, shape],
                in_specs=[vmem] * 5,
                out_specs=[anywhere] * 2,
                scratch_shapes=[pltpu.VMEM(right_side.shape, F32)] * 2 + [pltpu.SemaphoreType.DMA((16,))],
                compiler_params=pltpu.CompilerParams(vmem_limit_bytes=16 * 2**20),
            )(*parts)
        )

    placed = P("gx", "gy", "gz")
    return jax.shard_map(
        body, mesh=mesh, in_specs=(placed,) * 3, out_specs=(placed,) * 2, check_vma=False
    )
```

```python
import functools

import jax
import jax.numpy as jnp
from jax import lax
from jax.experimental import pallas as pl
from jax.experimental.pallas import tpu as pltpu
from jax.sharding import PartitionSpec as P

MESH = pl.DeviceIdType.MESH
F32 = jnp.float32
BF16 = jnp.bfloat16
DAMP = 6.0 / 7.0
GUARD = 8
GUARD3 = 16
BOTTOM_ITERS = 6


class Geo:
    def __init__(self, nx, ny, nz, halo, rows, y0, depth, unroll):
        self.nx, self.ny, self.nz, self.halo, self.R, self.y0 = nx, ny, nz, halo, rows, y0
        self.factor = 0.25**depth
        self.unroll = unroll
        self.total = 2 * GUARD + (nx + 2 * halo) * rows

    def row(self, x, y):
        return GUARD + (self.halo + x) * self.R + self.y0 + y


L0 = Geo(24, 48, 48, 4, 56, 4, 0, 28)
L1 = Geo(12, 24, 24, 6, 40, 8, 1, 24)
L2 = Geo(6, 12, 12, 5, 24, 6, 2, 16)
FACTOR3 = 0.25**3
FACTOR4 = 0.25**4


def lanes(rows):
    return lax.broadcasted_iota(jnp.int32, (rows, 128), 1)


def iota2(shape, dim):
    return lax.broadcasted_iota(jnp.int32, shape, dim)


def tree(terms):
    while len(terms) > 1:
        terms = [sum(terms[k + 1 : k + 2], terms[k]) for k in range(0, len(terms), 2)]
    return terms[0]


def roll(v, shift):
    shift = shift % 128
    return v if shift == 0 else pltpu.roll(v, shift, 1)


def split(a):
    hi = a.astype(BF16)
    return hi, (a - hi.astype(F32)).astype(BF16)


def mm(a, b):
    hi, low = split(a)
    return jnp.dot(hi, b, preferred_element_type=F32) + jnp.dot(low, b, preferred_element_type=F32)


def beside_of(ref, r, R):
    c = ref[pl.ds(r, R), :]
    b = ref[pl.ds(r + R, R), :] + ref[pl.ds(r - R, R), :]
    b = b + (ref[pl.ds(r + 1, R), :] + ref[pl.ds(r - 1, R), :])
    b = b + (roll(c, 1) + roll(c, -1))
    return c, b


def image_of(ref, s_ref, g, r):
    c, b = beside_of(ref, r, g.R)
    return c, g.factor * (6.0 * c - b) + s_ref[pl.ds(r, g.R), :] * c


def planes(g, a, b, body):
    unroll = g.unroll

    def group(start, count):
        todo = []
        for k in range(count):
            r = start + k * g.R
            r = r if isinstance(r, int) else pl.multiple_of(r, 8)
            todo.append((r, body(r)))
        for r, pairs in todo:
            for ref, value in pairs:
                ref[pl.ds(r, g.R), :] = value

    trips = (b - a) // unroll
    origin = GUARD + (g.halo + a) * g.R
    if trips == 1:
        group(origin, unroll)
    elif trips:

        def step(i, carry):
            group(pl.multiple_of(origin + i * (unroll * g.R), 8), unroll)
            return carry

        lax.fori_loop(0, trips, step, 0)
    if (b - a) % unroll:
        group(origin + trips * unroll * g.R, (b - a) % unroll)


def inverse(s, factor):
    return jnp.where(s > 0.0, DAMP / (6.0 * factor + s), 0.0)


def relax(g, src, dst, f, s, inv, a, b):
    def body(r):
        c, image = image_of(src, s, g, r)
        at = pl.ds(r, g.R)
        return [(dst, c + inv[at, :] * (f[at, :] - image))]

    planes(g, a, b, body)


def first(g, dst, f, inv, a, b):
    def body(r):
        at = pl.ds(r, g.R)
        return [(dst, inv[at, :] * f[at, :])]

    planes(g, a, b, body)


def leftover(g, src, dst, f, s, a, b):
    def body(r):
        c, image = image_of(src, s, g, r)
        return [(dst, f[pl.ds(r, g.R), :] - image)]

    planes(g, a, b, body)


def restrict(src, gs, dst, gd, x0, x1, y0, count, matrix, tmp):
    step = -(-count // 8) * 8
    for x in range(x0, x1):
        r = gs.row(2 * x, 2 * y0)
        t = src[pl.ds(r, count, stride=2), :] + src[pl.ds(r + 1, count, stride=2), :]
        r = r + gs.R
        t = t + (src[pl.ds(r, count, stride=2), :] + src[pl.ds(r + 1, count, stride=2), :])
        tmp[pl.ds((x - x0) * step, count), :] = t
    for x in range(x0, x1):
        out = mm(tmp[pl.ds((x - x0) * step, step), :], matrix[...])
        dst[pl.ds(gd.row(x, y0), count), :] = out[0:count]


def prolong(src, gc, dst, gf, x0, x1, y0, count, matrix, tmp):
    for x in range(x0, x1):
        o = (x - x0) * 56
        u = mm(src[pl.ds(gc.row(x, y0), count), :], matrix[...])
        tmp[pl.ds(o, count, stride=2), :] = u
        tmp[pl.ds(o + 1, count, stride=2), :] = u
    for x in range(x0, x1):
        o = (x - x0) * 56
        v = tmp[pl.ds(o, 2 * count), :]
        for k in range(2):
            at = pl.ds(gf.row(2 * x + k, 2 * y0), 2 * count)
            dst[at, :] = dst[at, :] + v


class Item:
    def __init__(self, geo, w):
        self.g, self.w = geo, w


class Plan:
    def __init__(self, items, cross=False):
        self.items, self.cross = items, cross
        self.counts = [it.w if cross else it.g.nx for it in items]
        self.yrows = sum(n * it.w for n, it in zip(self.counts, items))
        self.yrows = -(-self.yrows // 8) * 8
        self.tiles = []
        for k, it in enumerate(items):
            for x in range(self.counts[k]):
                for t in self.tiles:
                    if t[0] is it.g and t[1] + it.w <= 64:
                        break
                else:
                    t = [it.g, 0, []]
                    self.tiles.append(t)
                t[2].append((k, x, t[1]))
                t[1] += it.w
        self.zrows = sum(t[0].ny for t in self.tiles)
        self.zrows = -(-self.zrows // 8) * 8
        self.drows = max(self.counts)
        self.drows = -(-self.drows // 8) * 8
        assert sum(it.w * it.w for it in items) <= 64

        self.z0 = [0, self.zrows]
        self.d0 = [2 * self.zrows + q * self.drows for q in range(4)]
        self.y0 = [2 * self.zrows + 4 * self.drows + q * self.yrows for q in range(2)]
        self.total = 2 * (self.zrows + self.yrows) + 4 * self.drows
        self.xtotal = sum(it.w * it.g.R for it in items)

    def scratch(self):
        x = [] if self.cross else [pltpu.VMEM((self.xtotal, 128), F32)]
        return x + [
            pltpu.VMEM((self.total, 128), F32),
            pltpu.VMEM((self.total, 128), F32),
            pltpu.SemaphoreType.DMA((2,)),
            pltpu.SemaphoreType.DMA((2,)),
        ]


class Exchange:
    def __init__(self, plan, refs, scratch, place):
        self.plan, self.refs, self.place = plan, refs, place
        self.xr, self.sent, self.got, self.ss, self.rs = scratch
        gx, gy, gz = place.me
        self.partner = (1 - gx, gy, gz)
        self.x_copies = []
        o = 0
        for k, it in enumerate(plan.items):
            r = pl.multiple_of(GUARD + (it.g.halo + self.edge(it)) * it.g.R, 8)
            n = it.w * it.g.R
            self.x_copies.append(self.copy(refs[k].at[pl.ds(r, n), :], self.xr.at[pl.ds(o, n), :], 0, self.partner))
            o += n
        self.segments(0)

    def edge(self, it):
        return jnp.where(self.place.me[0] == 0, it.g.nx - it.w, 0)

    def source(self, k, x, y):
        return self.plan.items[k].g.row(x, y)

    def target(self, k, x, y):
        return self.refs[k], self.plan.items[k].g.row(x, y)

    def segments(self, dx):
        plan = self.plan
        at = {}
        for d in range(2):
            at[1 - 2 * d, 0] = plan.y0[d]
            at[0, 1 - 2 * d] = plan.z0[d]
            for e in range(2):
                at[1 - 2 * d, 1 - 2 * e] = plan.d0[2 * d + e]
        self.y_copies, self.z_copies, self.d_copies = [], [], []
        for d in (1, -1):
            self.y_copies.append(self.segment(at, dx, d, 0, plan.yrows))
            self.z_copies.append(self.segment(at, dx, 0, d, plan.zrows))
            for e in (1, -1):
                self.d_copies.append(self.segment(at, dx, d, e, plan.drows))

    def segment(self, at, dx, dy, dz, n):
        there = self.place.exists(dy, dz)
        peer = self.place.beside(dx, dy, dz)
        peer = tuple(jnp.where(there, p, q) for p, q in zip(peer, self.partner))
        target = pl.multiple_of(jnp.where(there, at[dy, dz], at[-dy, -dz]), 8)
        return self.copy(self.sent.at[pl.ds(at[dy, dz], n), :], self.got.at[pl.ds(target, n), :], 1, peer)

    def copy(self, src, dst, k, peer):
        return pltpu.make_async_remote_copy(
            src_ref=src, dst_ref=dst, send_sem=self.ss.at[k], recv_sem=self.rs.at[k],
            device_id=peer, device_id_type=MESH,
        )

    def x_send(self):
        for c in self.x_copies:
            c.start()

    def settle(self, x=True):
        if x:
            self.x_sent()
        self.copy(self.sent, self.got, 1, self.partner).wait_send()

    def x_sent(self):
        self.copy(self.xr, self.xr, 0, self.partner).wait_send()

    def x_wait(self):
        self.copy(self.xr, self.xr, 0, self.partner).wait_recv()

    def x_fill(self):
        m0, m1 = self.place.x_masks
        o = 0
        for k, it in enumerate(self.plan.items):
            g, w, ref = it.g, it.w, self.refs[k]
            upper = ((lanes(g.R) + 8) & 127) >= 64
            for j in range(w):
                got = self.xr[pl.ds(o + j * g.R, g.R), :]
                top = ref[pl.ds(GUARD + (g.halo + g.nx - w + j) * g.R, g.R), :]
                low = ref[pl.ds(GUARD + (g.halo + j) * g.R, g.R), :]
                ref[pl.ds(GUARD + (g.halo - w + j) * g.R, g.R), :] = roll(jnp.where(upper, got * m1, top), 64)
                ref[pl.ds(GUARD + (g.halo + g.nx + j) * g.R, g.R), :] = roll(jnp.where(upper, low, got * m0), 64)
            o += w * g.R

    def pack_send(self):
        self.pack()
        self.send()

    def pack(self):
        for k in range(len(self.refs)):
            self.pack_item(k)

    def send(self):
        for c in self.d_copies + self.z_copies + self.y_copies:
            c.start()

    def pack_item(self, k):
        if k == 0:
            self.yo, self.co, self.corner = 0, 0, [None] * 4
        it = self.plan.items[k]
        g, w, ref = it.g, it.w, self.refs[k]
        n = self.plan.counts[k]
        lane = lanes(self.plan.drows) & 63
        for d in range(1, w + 1):
            at = self.co + (d - 1) * w
            for e, y in enumerate((g.ny - d, d - 1)):
                v = ref[pl.ds(self.source(k, 0, y), n, stride=g.R), :]
                self.sent[pl.ds(self.plan.y0[e] + self.yo, n), :] = v
                if n < self.plan.drows:
                    v = jnp.concatenate([v, jnp.zeros((self.plan.drows - n, 128), F32)], axis=0)
                for q, z in enumerate((g.nz - w, 0)):
                    moved = roll(v, at - z)
                    old = self.corner[2 * e + q]
                    self.corner[2 * e + q] = moved if old is None else jnp.where(lane >= at, moved, old)
            self.yo += n
        self.co += w * w
        if k == len(self.refs) - 1:
            for q in range(4):
                self.sent[pl.ds(self.plan.d0[q], self.plan.drows), :] = self.corner[q]
        zo = 0
        for t, _, slots in self.plan.tiles:
            if slots[-1][0] == k:
                self.pack_tile(t, slots, zo)
            zo += t.ny

    def pack_tile(self, g, slots, zo):
        lane = lanes(g.ny)
        acc = [None, None]
        for k, x, at in slots:
            w = self.plan.items[k].w
            moved = roll(self.refs[k][pl.ds(self.source(k, x, 0), g.ny), :], at)
            for q, past in enumerate((g.nz - w, 0)):
                here = ((lane - past) & 63 >= at) & ((lane - past) & 63 < at + w)
                acc[q] = moved if acc[q] is None else jnp.where(here, moved, acc[q])
        for q in range(2):
            self.sent[pl.ds(self.plan.z0[q] + zo, g.ny), :] = acc[q]

    def unpack(self):
        my, mz = self.place.y_masks, self.place.z_masks
        self.copy(self.sent, self.got, 1, self.partner).wait_recv()
        yo, co = 0, 0
        for k, it in enumerate(self.plan.items):
            g, w = it.g, it.w
            n = self.plan.counts[k]
            lane = lanes(n) & 63
            into = (lane >= 64 - w, (lane >= g.nz) & (lane < g.nz + w))
            for d in range(1, w + 1):
                at = co + (d - 1) * w
                for e, y in enumerate((-d, g.ny + d - 1)):
                    v = self.got[pl.ds(self.plan.y0[e] + yo, n), :]
                    for q, z in enumerate((-w, g.nz)):
                        got = self.got[pl.ds(self.plan.d0[2 * e + q], n), :] * mz[q]
                        v = jnp.where(into[q], roll(got, z - at), v)
                    ref, r = self.target(k, 0, y)
                    ref[pl.ds(r, n, stride=g.R), :] = v * my[e]
                yo += n
            co += w * w
        self.unpack_z(True)

    def unpack_rest(self):
        self.unpack_z(False)

    def unpack_z(self, edge):
        mz = self.place.z_masks
        zo = 0
        for g, _, slots in self.plan.tiles:
            lane = lanes(g.ny) & 63
            got = [self.got[pl.ds(self.plan.z0[q] + zo, g.ny), :] * mz[q] for q in range(2)]
            for k, x, at in slots:
                w = self.plan.items[k].w
                if (x < w or x >= g.nx - w) != edge:
                    continue
                ref, r = self.target(k, x, 0)
                rows = pl.ds(r, g.ny)
                v = ref[rows, :]
                v = jnp.where(lane >= 64 - w, roll(got[0], -g.nz - at), v)
                v = jnp.where((lane >= g.nz) & (lane < g.nz + w), roll(got[1], g.nz - at), v)
                ref[rows, :] = v
            zo += g.ny


class Cross(Exchange):
    def __init__(self, plan, main, scratch, place):
        self.plan, self.main, self.refs, self.place = plan, main, main.refs, place
        self.sent, self.got, self.ss, self.rs = scratch
        self.partner = main.partner
        self.segments(1)

    def source(self, k, x, y):
        it = self.plan.items[k]
        return GUARD + (it.g.halo + self.edge(it) + x) * it.g.R + it.g.y0 + y

    def target(self, k, x, y):
        o = sum(it.w * it.g.R for it in self.plan.items[:k])
        g = self.plan.items[k].g
        return self.main.xr, o + x * g.R + g.y0 + y


class Place:
    def __init__(self, sizes):
        self.sizes = sizes
        self.me = tuple(lax.axis_index(a) for a in ("gx", "gy", "gz"))
        gx, gy, gz = self.me
        one = lambda c: jnp.where(c, 1.0, 0.0).astype(F32)
        self.x_masks = (one(gx == 0), one(gx == 1))
        self.y_masks = (one(gy > 0), one(gy < sizes[1] - 1))
        self.z_masks = (one(gz > 0), one(gz < sizes[2] - 1))

    def exists(self, dy, dz):
        gx, gy, gz = self.me
        y, z = gy + dy, gz + dz
        return (y >= 0) & (y < self.sizes[1]) & (z >= 0) & (z < self.sizes[2])

    def beside(self, dx, dy, dz):
        return tuple(
            lax.rem(m + d % n, n) if d % n else m for m, d, n in zip(self.me, (dx, dy, dz), self.sizes)
        )


class Gather:
    rows = 24

    def __init__(self, place, scratch, whole):
        self.place, self.whole = place, whole
        self.mine, self.got, self.sum, self.parts, self.ss, self.rs = scratch
        n = place.sizes
        self.near = [(a, b) for a in range(n[0]) for b in range(n[1])][1:]
        self.near.sort(key=lambda p: -far((p[0], p[1], 0), n))
        self.line = sorted(range(1, n[2]), key=lambda c: -far((0, 0, c), n))
        self.at = pl.ds(pl.multiple_of(GUARD3 + self.rows * place.me[2], 8), self.rows)

    def copy(self, src, dst, k, peer):
        return pltpu.make_async_remote_copy(
            src_ref=src, dst_ref=dst, send_sem=self.ss.at[k], recv_sem=self.rs.at[k],
            device_id=peer, device_id_type=MESH,
        )

    def send(self):
        for k, (a, b) in enumerate(self.near):
            self.copy(self.mine, self.got.at[k], 0, self.place.beside(a, b, 0)).start()

    def relay(self):
        self.copy(self.got, self.got, 0, self.place.beside(1, 0, 0)).wait_recv()
        gx, gy, gz = self.place.me
        ny = self.place.sizes[1]
        lane = lanes(8)
        sums = [[], []], [[], []]
        for k, (a, b) in enumerate([(0, 0)] + self.near):
            tile = self.mine[...] if k == 0 else self.got[k - 1]
            start = 6 * lax.rem(gy + ny - b, ny)
            for h in range(2):
                y = (lane - 16 * h) & 31
                sums[a][h].append(jnp.where((y >= start) & (y < start + 6), tile, 0.0))
        for h in range(2):
            own, other = (roll(tree(sums[a][h]), -16 * h) for a in range(2))
            self.parts[pl.ds(16 * h, 8), :] = jnp.where(gx == 0, own, other)
            self.parts[pl.ds(16 * h + 8, 8), :] = jnp.where(gx == 0, other, own)
        for h in range(2):
            r = 16 * h
            self.sum[pl.ds(12 * h, 3, stride=4), :] = self.parts[pl.ds(r, 3), :]
            self.sum[pl.ds(12 * h + 1, 3, stride=4), :] = self.parts[pl.ds(r + 4, 3), :] + self.parts[pl.ds(r + 8, 3), :]
            self.sum[pl.ds(12 * h + 2, 3, stride=4), :] = self.parts[pl.ds(r + 12, 3), :]
        for c in self.line:
            self.copy(self.sum, self.whole.at[self.at, :], 1, self.place.beside(0, 0, c)).start()
        self.whole[self.at, :] = self.sum[...]

    def finish(self):
        self.most().wait_recv()

    def most(self):
        most = self.whole.at[pl.ds(GUARD3, self.rows * (self.place.sizes[2] - 1)), :]
        return self.copy(most, most, 1, self.place.beside(1, 0, 0))

    def settle(self):
        self.copy(self.got, self.got, 0, self.place.beside(1, 0, 0)).wait_send()
        self.most().wait_send()


def gather_scratch(sizes):
    return [
        pltpu.VMEM((8, 128), F32),
        pltpu.VMEM((sizes[0] * sizes[1] - 1, 8, 128), F32),
        pltpu.VMEM((24, 128), F32),
        pltpu.VMEM((32, 128), F32),
        pltpu.SemaphoreType.DMA((2,)),
        pltpu.SemaphoreType.DMA((2,)),
    ]


def spread_to_level3(place):
    gx, gy, gz = place.me
    r = iota2((128, 256), 0)
    l = iota2((128, 256), 1)
    x = 6 * gx + 3 * (r >> 6) + ((r & 63) >> 3)
    y = 6 * gy + (r & 7)
    hit = (x == (l >> 5) + 4 * gx) & (y == (l & 31)) & ((r & 7) < 6) & ((r & 63) < 24)
    return jnp.where(hit, 1.0, 0.0).astype(BF16)


def to_level3(src, mine, square, turned, chosen):
    g = L2
    for i in range(3):
        r = g.row(2 * i, 0)
        t = src[pl.ds(r, 6, stride=2), :] + src[pl.ds(r + 1, 6, stride=2), :]
        r = r + g.R
        t = t + (src[pl.ds(r, 6, stride=2), :] + src[pl.ds(r + 1, 6, stride=2), :])
        square[pl.ds(8 * i, 6), :] = t
    turned[...] = jnp.transpose(square[...])
    a = turned[pl.ds(0, 8, stride=2), :] + turned[pl.ds(1, 8, stride=2), :]
    b = turned[pl.ds(64, 8, stride=2), :] + turned[pl.ds(65, 8, stride=2), :]
    a = (a + roll(b, 64)) * 0.125
    out = mm(a, chosen[...])
    for k in range(2):
        turned[pl.ds(8 * k, 8), :] = out[:, 128 * k : 128 * k + 128]
    for k in range(2):
        mine[pl.ds(4 * k, 3), :] = turned[pl.ds(8 * k, 3), :] + roll(turned[pl.ds(8 * k + 3, 3), :], 16)


def image3(ref, s_ref, r, n):
    lane = lanes(n)
    c = ref[pl.ds(r, n), :]
    b = ref[pl.ds(r + 4, n), :] + ref[pl.ds(r - 4, n), :]
    b = b + (roll(c, 1) + roll(c, -1))
    b = b + roll(jnp.where(lane < 32, ref[pl.ds(r + 1, n), :], c), -32)
    b = b + roll(jnp.where(lane >= 96, ref[pl.ds(r - 1, n), :], c), 32)
    return c, FACTOR3 * (6.0 * c - b) + s_ref[pl.ds(r, n), :] * c


def chunks3(rows, ref, body):
    n = min(rows, 384)

    def step(i, carry):
        r = pl.multiple_of(GUARD3 + i * n, 8)
        ref[pl.ds(r, n), :] = body(r, n)
        return carry

    lax.fori_loop(0, rows // n, step, 0)


def match4(k, shape, coarse_dim, ny):
    c = iota2(shape, coarse_dim)
    l = iota2(shape, 1 - coarse_dim)
    return ((c >> 4) == 2 * k + (l >> 6)) & ((c & 15) == ((l & 31) >> 1)) & ((l & 31) < ny)


def restrict4(src, n, matrix):
    total = None
    for k in range(3):
        t = src[pl.ds(GUARD3 + k, n, stride=8), :] + src[pl.ds(GUARD3 + k + 4, n, stride=8), :]
        part = mm(t, matrix[k])
        total = part if total is None else total + part
    return total


def dot_all(a, b):
    return jnp.sum(jnp.sum(a * b, axis=0, keepdims=True), axis=1, keepdims=True)


def bottom(source, s4, p4, n, ny):
    estimate = jnp.zeros_like(source)
    left = source
    inside = (lanes(n) < 96) & ((lanes(n) & 15) < ny)
    shifted = 6.0 * FACTOR4 + s4[...]
    for it in range(BOTTOM_ITERS):
        p4[pl.ds(GUARD, n), :] = left
        b = p4[pl.ds(GUARD + 1, n), :] + p4[pl.ds(GUARD - 1, n), :]
        b = b + (roll(left, 1) + roll(left, -1))
        b = b + (roll(left, 16) + roll(left, -16))
        image = shifted * left - FACTOR4 * jnp.where(inside, b, 0.0)
        now = dot_all(left, left)
        bent = dot_all(left, image)
        if it == 0:
            denom = bent
            direction, turned = left, image
        else:
            ratio = now * inv_before
            denom = bent - ratio * ratio * denom
            direction = left + ratio * direction
            turned = image + ratio * turned
        step = now / denom
        inv_before = 1.0 / now
        estimate = estimate + step * direction
        if it < BOTTOM_ITERS - 1:
            left = left - step * turned
    return estimate


PLAN_A = Plan([Item(L0, 3), Item(L0, 2), Item(L0, 2)])
PLAN_S = Plan([Item(L1, 6), Item(L2, 5)])
PLAN_B = Plan([Item(L1, 6)])
PLAN_BX = Plan([Item(L1, 6)], True)
PLAN_C = Plan([Item(L0, 3)])
PLAN_D = Plan([Item(L2, 5)])
PLANS = (PLAN_A, PLAN_S, PLAN_B, PLAN_C, PLAN_D, PLAN_BX)


def far(p, sizes):
    ring = lambda d, n: min(d % n, -d % n)
    return p[0] + ring(p[1], sizes[1]) + ring(p[2], 4) + ring(p[2] // 4, 4)


def kernel(sizes, counts, right_in, guess_in, react_in, guess, r0, eb0, left0, step_out, *scratch):
    scratch = list(scratch)

    def take(n):
        out = scratch[:n]
        del scratch[:n]
        return out

    raw = take(3)
    (in_sems,) = take(1)
    right, react, inv0, ea0 = take(4)
    f1, s1, inv1, ea1, eb1, left1 = take(6)
    f2, s2, inv2, ea2, eb2, left2 = take(6)
    f3, s3, inv3, ea3, eb3, left3 = take(6)
    s4, p4, down_m, up_m, tmp, square, turned, spread, slab = take(9)
    chosen, picks, down4, up4 = take(4)
    scr = [take(n) for n in counts]
    place = Place(sizes)
    gx, gy, gz = place.me
    n3, n4, ny3 = 24 * sizes[2], 3 * sizes[2], 6 * sizes[1]

    inputs = (guess_in, right_in, react_in)
    for k in range(3):
        for q in range(4):
            at = pl.ds(12 * q, 12)
            pltpu.make_async_copy(inputs[k].at[at], raw[k].at[at], in_sems.at[k]).start()

    def clear(ref):
        n = ref.shape[0]
        size = next(k for k in (128, 122 * 8, 80, 8) if n % k == 0) if n > 128 else n
        size = {1808: 904, 976: 488, 416: 208}.get(n, size)

        def step(i, carry):
            ref[pl.ds(pl.multiple_of(i * size, 8), size), :] = jnp.zeros((size, 128), F32)
            return carry

        lax.fori_loop(0, n // size, step, 0)

    peers = [(a, b, c) for a in range(sizes[0]) for b in range(sizes[1]) for c in range(sizes[2])][1:]
    peers.sort(key=lambda p: -far(p, sizes))
    beside = {(a, b % sizes[1], c % sizes[2]) for a in range(2) for b in (1, -1) for c in (1, -1)}
    beside |= {(1, 0, c % sizes[2]) for c in (1, -1)}
    greeted = [p for p in peers if p[2] == 0 or p[:2] == (0, 0) or p in beside]
    barrier = pltpu.get_barrier_semaphore()
    for p in greeted:
        pl.semaphore_signal(barrier, inc=1, device_id=place.beside(*p), device_id_type=MESH)
    for ref in (guess, right, react, f1, s1, ea1, eb1, f2, s2, ea2, eb2, ea3, eb3, p4, square):
        clear(ref)
    spread[...] = jnp.zeros_like(spread)
    for ref in (f3, s3, inv3):
        for r in (0, GUARD3 + n3):
            ref[pl.ds(r, GUARD3), :] = jnp.zeros((GUARD3, 128), F32)

    a = iota2((128, 128), 0)
    b = iota2((128, 128), 1)
    signed = lambda v: ((v + 8) & 63) - 8
    base = lambda v: ((v + 8) & 127) & 64
    zb = signed(b)
    hit = ((a == ((base(b) + 2 * zb) & 127)) | (a == ((base(b) + 2 * zb + 1) & 127))) & (zb >= -8) & (zb < 24)
    down_m[...] = jnp.where(hit, 0.125, 0.0).astype(BF16)
    hit = a == ((base(b) + (zb >> 1)) & 127)
    up_m[...] = jnp.where(hit, 1.0, 0.0).astype(BF16)

    ex_a = Exchange(PLAN_A, (guess, right, react), scr[0], place)
    ex_s = Exchange(PLAN_S, (s1, s2), scr[1], place)
    ex_b = Exchange(PLAN_B, (f1,), scr[2], place)
    ex_c = Exchange(PLAN_C, (eb0,), scr[3], place)
    ex_d = Exchange(PLAN_D, (f2,), scr[4], place)
    cx_b = Cross(PLAN_BX, ex_b, scr[5], place)
    ga_s = Gather(place, scr[6], s3)
    ga_f = Gather(place, scr[7], f3)
    for k, dst in enumerate((guess, right, react)):
        pltpu.make_async_copy(inputs[k], raw[k], in_sems.at[k]).wait()

        for i in range(24):
            dst[pl.ds(L0.row(i, 0), 48), 0:48] = raw[k][i]
            dst[pl.ds(L0.row(i, 0), 48), 64:112] = raw[k][i + 24]
        ex_a.pack_item(k)

    reduced, red_send, red_recv = scr[8]

    pl.semaphore_wait(barrier, len(greeted))
    ex_a.send()

    restrict(react, L0, s1, L1, 0, 12, 0, 24, down_m, tmp)
    restrict(s1, L1, s2, L2, 0, 6, 0, 12, down_m, tmp)
    ex_s.pack()
    for e in (ga_s, ga_f):
        e.mine[...] = jnp.zeros((8, 128), F32)
        e.sum[...] = jnp.zeros((24, 128), F32)
    chosen[...] = spread_to_level3(place)
    to_level3(s2, ga_s.mine, square, turned, chosen)
    for h in range(2):
        r = iota2((112, 384), 0)
        l = iota2((112, 384), 1)
        hit = (6 * gx + 3 * h + (r >> 4) - 2 == (l >> 5)) & (6 * gy + (r & 15) - 2 == (l & 31)) & ((r & 15) < 10)
        picks[h] = jnp.where(hit, 1.0, 0.0).astype(BF16)
    for k in range(3):
        down4[k] = jnp.where(match4(k, (128, 128), 1, ny3), 0.125, 0.0).astype(BF16)
        up4[k] = jnp.where(match4(k, (128, 128), 0, ny3), 1.0, 0.0).astype(BF16)


    def start(r):
        at = pl.ds(r, L0.R)
        c, image = image_of(guess, react, L0, r)
        res = right[at, :] - image
        inv = inverse(react[at, :], 1.0)
        return [(r0, res), (inv0, inv), (ea0, inv * res)]

    ex_a.unpack()
    ex_a.x_send()
    ex_s.send()
    ga_s.send()
    ex_a.unpack_rest()
    planes(L0, 1, 23, start)
    ex_a.x_wait()
    ex_a.x_fill()
    planes(L0, -2, 1, start)
    planes(L0, 23, 26, start)
    relax(L0, ea0, eb0, r0, react, inv0, -1, 25)
    leftover(L0, eb0, left0, r0, react, 0, 24)
    restrict(left0, L0, f1, L1, 0, 12, 0, 24, down_m, tmp)
    ex_b.pack_send()
    cx_b.pack_send()
    ex_b.x_send()

    ex_c.pack()
    ex_s.unpack()
    ex_s.x_send()

    def inverse_of(g, sh, inv, first_plane, end):
        planes(g, first_plane, end, lambda r: [(inv, inverse(sh[pl.ds(r, g.R), :], g.factor))])

    inverse_of(L1, s1, inv1, 0, 12)

    ex_b.x_sent()
    ex_b.unpack()
    ex_c.send()
    first(L1, ea1, f1, inv1, 0, 12)
    relax(L1, ea1, eb1, f1, s1, inv1, 1, 11)
    ex_s.x_wait()
    ex_s.x_fill()
    inverse_of(L1, s1, inv1, -6, 0)
    inverse_of(L1, s1, inv1, 12, 18)
    inverse_of(L2, s2, inv2, -5, 11)
    ex_b.x_wait()
    cx_b.unpack()
    ex_b.x_fill()
    first(L1, ea1, f1, inv1, -6, 0)
    first(L1, ea1, f1, inv1, 12, 18)
    relax(L1, ea1, eb1, f1, s1, inv1, -5, 1)
    relax(L1, ea1, eb1, f1, s1, inv1, 11, 17)
    leftover(L1, eb1, left1, f1, s1, -4, 16)
    restrict(left1, L1, f2, L2, -2, 8, -2, 16, down_m, tmp)
    first(L2, ea2, f2, inv2, -2, 8)
    relax(L2, ea2, eb2, f2, s2, inv2, -1, 7)
    leftover(L2, eb2, left2, f2, s2, 0, 6)
    to_level3(left2, ga_f.mine, square, turned, chosen)
    ga_f.send()
    ex_d.pack_send()
    ga_s.relay()

    ga_f.relay()
    ex_c.unpack()
    ex_c.x_send()
    ex_c.unpack_rest()
    ex_d.unpack()
    ex_d.x_send()
    ex_c.x_wait()
    ex_c.x_fill()
    ex_d.x_wait()
    ex_d.x_fill()
    first(L2, ea2, f2, inv2, -5, 11)
    relax(L2, ea2, eb2, f2, s2, inv2, -4, 10)
    ga_s.finish()
    chunks3(n3, inv3, lambda r, n: inverse(s3[pl.ds(r, n), :], FACTOR3))
    s4[...] = restrict4(s3, n4, down4)
    for e in (ex_a, ex_s, ex_c, ex_d, ga_s):
        e.settle()
    for e in (ex_b, cx_b):
        e.settle(False)
    ga_f.finish()

    def relax3(src, dst):
        def body(r, n):
            c, image = image3(src, s3, r, n)
            at = pl.ds(r, n)
            return c + inv3[at, :] * (f3[at, :] - image)

        chunks3(n3, dst, body)

    chunks3(n3, ea3, lambda r, n: inv3[pl.ds(r, n), :] * f3[pl.ds(r, n), :])
    relax3(ea3, eb3)
    chunks3(n3, left3, lambda r, n: f3[pl.ds(r, n), :] - image3(eb3, s3, r, n)[1])
    e4 = bottom(restrict4(left3, n4, down4), s4, p4, n4, ny3 // 2)
    for k in range(3):
        u = mm(e4, up4[k])
        for q in (k, k + 4):
            at = pl.ds(GUARD3 + q, n4, stride=8)
            eb3[at, :] = eb3[at, :] + u
    for src, dst, n in ((eb3, ea3, 48), (ea3, slab, 40)):
        r = pl.multiple_of(GUARD3 + 24 * gz - (n - 24) // 2, 4)
        c, image = image3(src, s3, r, n)
        at = pl.ds(r, n)
        dst[at if n == 48 else pl.ds(0, n), :] = c + inv3[at, :] * (f3[at, :] - image)
    for k in range(3):
        v = slab[pl.ds(k, 10, stride=4), :]
        for h in range(2):
            for q in range(2):
                spread[k, pl.ds(64 * h + q, 10, stride=2), :] = v
    wide = [jnp.concatenate(p, axis=1) for p in zip(*[split(spread[k]) for k in range(3)])]
    coarse = []
    for h in range(2):
        pick = picks[h]
        parts = [
            lax.dot_general(pick, p, (((1,), (1,)), ((), ())), preferred_element_type=F32) for p in wide
        ]
        coarse.append(parts[0] + parts[1])
    fine = roll(jnp.where(lanes(112) < 64, coarse[0], coarse[1]), -4)
    for i in range(7):
        u = fine[16 * i : 16 * i + 10]
        tmp[pl.ds(24 * i, 10, stride=2), :] = u
        tmp[pl.ds(24 * i + 1, 10, stride=2), :] = u
    for i in range(7):
        v = tmp[pl.ds(24 * i, 20), :]
        for q in range(2):
            at = pl.ds(L2.row(2 * (i - 2) + q, -4), 20)
            eb2[at, :] = eb2[at, :] + v
    relax(L2, eb2, ea2, f2, s2, inv2, -3, 9)
    relax(L2, ea2, eb2, f2, s2, inv2, -2, 8)
    prolong(eb2, L2, eb1, L1, -2, 8, -2, 16, up_m, tmp)
    relax(L1, eb1, ea1, f1, s1, inv1, -3, 15)
    relax(L1, ea1, eb1, f1, s1, inv1, -2, 14)
    prolong(eb1, L1, eb0, L0, -2, 14, -2, 28, up_m, tmp)
    relax(L0, eb0, ea0, r0, react, inv0, -2, 26)
    relax(L0, ea0, eb0, r0, react, inv0, -1, 25)

    row = iota2((L0.R, 128), 0)
    inside = ((lanes(L0.R) & 63) < 48) & (row >= L0.y0) & (row < L0.y0 + 48)

    upper, lower = [], []
    for i in range(24):
        r = GUARD + (L0.halo + i) * L0.R
        c, image = image_of(eb0, react, L0, r)
        left0[pl.ds(r, L0.R), :] = image
        upper.append(c * r0[pl.ds(r, L0.R), :])
        lower.append(c * image)
    upper = jnp.where(inside, tree(upper), 0.0)
    lower = jnp.where(inside, tree(lower), 0.0)
    upper = jnp.sum(upper, axis=0, keepdims=True)
    lower = jnp.sum(lower, axis=0, keepdims=True)
    half = lanes(1) < 64
    number = (gx * sizes[1] + gy) * sizes[2] + gz
    reduced[number] = jnp.where(half, upper + roll(upper, 64), lower + roll(lower, 64))
    own = reduced.at[number]

    def summed(src, dst, p):
        return pltpu.make_async_remote_copy(
            src_ref=src, dst_ref=dst, send_sem=red_send.at[0], recv_sem=red_recv.at[0],
            device_id=place.beside(*p), device_id_type=MESH,
        )

    for p in peers:
        summed(own, own, p).start()
    ga_f.settle()
    most = reduced.at[pl.ds(0, len(peers))]
    summed(most, most, peers[0]).wait()
    sums = [reduced[k] for k in range(8)]
    for k in range(8, len(peers) + 1):
        sums[k % 8] = sums[k % 8] + reduced[k]
    total = tree(sums)
    upper = jnp.sum(jnp.where(half, total, 0.0), axis=1, keepdims=True)
    lower = jnp.sum(jnp.where(half, 0.0, total), axis=1, keepdims=True)
    step_out[...] = jnp.broadcast_to(upper / lower, (8, 128))


def finish(guess, r0, eb0, left0, step_ref, field_out, resid_out, field, resid, sems):
    step = step_ref[0:1, :]
    copies = []
    parts, size = 4, 6
    for p in range(parts):
        for x in range(p * size, p * size + size):
            at = pl.ds(L0.row(x, 0), 48)
            v = guess[at, :] + step * eb0[at, :]
            field[x] = v[:, 0:48]
            field[x + 24] = roll(v, 64)[:, 0:48]
            v = r0[at, :] - step * left0[at, :]
            resid[x] = v[:, 0:48]
            resid[x + 24] = roll(v, 64)[:, 0:48]
        for q, (src, dst) in enumerate(((field, field_out), (resid, resid_out))):
            for h in range(2):
                at = pl.ds(p * size + 24 * h, size)
                c = pltpu.make_async_copy(src.at[at], dst.at[at], sems.at[4 * p + 2 * q + h])
                c.start()
                copies.append(c)
    for c in copies:
        c.wait()


def solution(mesh):
    sizes = tuple(mesh.shape[a] for a in ("gx", "gy", "gz"))
    n3, n4 = 24 * sizes[2] + 2 * GUARD3, 3 * sizes[2]
    scratch = [pltpu.VMEM((48, 48, 48), F32)] * 3 + [pltpu.SemaphoreType.DMA((3,))]
    scratch += [pltpu.VMEM((L0.total, 128), F32)] * 4
    scratch += [pltpu.VMEM((L1.total, 128), F32)] * 6
    scratch += [pltpu.VMEM((L2.total, 128), F32)] * 6
    scratch += [pltpu.VMEM((n3, 128), F32)] * 6
    scratch += [pltpu.VMEM((n4, 128), F32), pltpu.VMEM((n4 + 2 * GUARD, 128), F32)]
    scratch += [pltpu.VMEM((128, 128), BF16)] * 2 + [pltpu.VMEM((16 * 56, 128), F32)]
    scratch += [pltpu.VMEM((128, 128), F32)] * 2
    scratch += [pltpu.VMEM((3, 128, 128), F32), pltpu.VMEM((40, 128), F32)]
    scratch += [pltpu.VMEM((128, 256), BF16), pltpu.VMEM((2, 112, 384), BF16)]
    scratch += [pltpu.VMEM((3, 128, 128), BF16)] * 2
    groups = [p.scratch() for p in PLANS] + [gather_scratch(sizes)] * 2
    devices = sizes[0] * sizes[1] * sizes[2]
    groups += [[pltpu.VMEM((devices, 1, 128), F32)] + [pltpu.SemaphoreType.DMA((1,))] * 2]
    for g in groups:
        scratch += g
    counts = tuple(len(g) for g in groups)
    vmem = pl.BlockSpec(memory_space=pltpu.VMEM)

    anywhere = pl.BlockSpec(memory_space=pl.ANY)

    def body(right_side, start_guess, reaction):
        whole = pltpu.VMEM((L0.total, 128), F32)
        parts = pl.pallas_call(
            functools.partial(kernel, sizes, counts),
            out_shape=[whole] * 4 + [pltpu.VMEM((8, 128), F32)],
            in_specs=[anywhere] * 3,
            out_specs=[vmem] * 5,
            scratch_shapes=scratch,
            compiler_params=pltpu.CompilerParams(
                collective_id=0, has_side_effects=True, vmem_limit_bytes=60 * 2**20
            ),
        )(right_side, start_guess, reaction)
        shape = jax.ShapeDtypeStruct(right_side.shape, F32)
        return tuple(
            pl.pallas_call(
                finish,
                out_shape=[shape, shape],
                in_specs=[vmem] * 5,
                out_specs=[anywhere] * 2,
                scratch_shapes=[pltpu.VMEM(right_side.shape, F32)] * 2 + [pltpu.SemaphoreType.DMA((16,))],
                compiler_params=pltpu.CompilerParams(vmem_limit_bytes=16 * 2**20),
            )(*parts)
        )

    placed = P("gx", "gy", "gz")
    return jax.shard_map(
        body, mesh=mesh, in_specs=(placed,) * 3, out_specs=(placed,) * 2, check_vma=False
    )
```

```python
import functools

import jax
import jax.numpy as jnp
from jax import lax
from jax.experimental import pallas as pl
from jax.experimental.pallas import tpu as pltpu
from jax.sharding import PartitionSpec as P

MESH = pl.DeviceIdType.MESH
F32 = jnp.float32
BF16 = jnp.bfloat16
DAMP = 6.0 / 7.0
GUARD = 8
GUARD3 = 16
BOTTOM_ITERS = 6


class Geo:
    def __init__(self, nx, ny, nz, halo, rows, y0, depth, unroll):
        self.nx, self.ny, self.nz, self.halo, self.R, self.y0 = nx, ny, nz, halo, rows, y0
        self.factor = 0.25**depth
        self.unroll = unroll
        self.total = 2 * GUARD + (nx + 2 * halo) * rows

    def row(self, x, y):
        return GUARD + (self.halo + x) * self.R + self.y0 + y


L0 = Geo(24, 48, 48, 4, 56, 4, 0, 28)
L1 = Geo(12, 24, 24, 6, 40, 8, 1, 24)
L2 = Geo(6, 12, 12, 5, 24, 6, 2, 16)
FACTOR3 = 0.25**3
FACTOR4 = 0.25**4


def lanes(rows):
    return lax.broadcasted_iota(jnp.int32, (rows, 128), 1)


def iota2(shape, dim):
    return lax.broadcasted_iota(jnp.int32, shape, dim)


def tree(terms):
    while len(terms) > 1:
        terms = [sum(terms[k + 1 : k + 2], terms[k]) for k in range(0, len(terms), 2)]
    return terms[0]


def roll(v, shift):
    shift = shift % 128
    return v if shift == 0 else pltpu.roll(v, shift, 1)


def split(a):
    hi = a.astype(BF16)
    return hi, (a - hi.astype(F32)).astype(BF16)


def mm(a, b):
    hi, low = split(a)
    return jnp.dot(hi, b, preferred_element_type=F32) + jnp.dot(low, b, preferred_element_type=F32)


def beside_of(ref, r, R):
    c = ref[pl.ds(r, R), :]
    b = ref[pl.ds(r + R, R), :] + ref[pl.ds(r - R, R), :]
    b = b + (ref[pl.ds(r + 1, R), :] + ref[pl.ds(r - 1, R), :])
    b = b + (roll(c, 1) + roll(c, -1))
    return c, b


def image_of(ref, s_ref, g, r):
    c, b = beside_of(ref, r, g.R)
    return c, g.factor * (6.0 * c - b) + s_ref[pl.ds(r, g.R), :] * c


def planes(g, a, b, body):
    unroll = g.unroll

    def group(start, count):
        todo = []
        for k in range(count):
            r = start + k * g.R
            r = r if isinstance(r, int) else pl.multiple_of(r, 8)
            todo.append((r, body(r)))
        for r, pairs in todo:
            for ref, value in pairs:
                ref[pl.ds(r, g.R), :] = value

    trips = (b - a) // unroll
    origin = GUARD + (g.halo + a) * g.R
    if trips == 1:
        group(origin, unroll)
    elif trips:

        def step(i, carry):
            group(pl.multiple_of(origin + i * (unroll * g.R), 8), unroll)
            return carry

        lax.fori_loop(0, trips, step, 0)
    if (b - a) % unroll:
        group(origin + trips * unroll * g.R, (b - a) % unroll)


def inverse(s, factor):
    return jnp.where(s > 0.0, DAMP / (6.0 * factor + s), 0.0)


def relax(g, src, dst, f, s, inv, a, b):
    def body(r):
        c, image = image_of(src, s, g, r)
        at = pl.ds(r, g.R)
        return [(dst, c + inv[at, :] * (f[at, :] - image))]

    planes(g, a, b, body)


def first(g, dst, f, inv, a, b):
    def body(r):
        at = pl.ds(r, g.R)
        return [(dst, inv[at, :] * f[at, :])]

    planes(g, a, b, body)


def leftover(g, src, dst, f, s, a, b):
    def body(r):
        c, image = image_of(src, s, g, r)
        return [(dst, f[pl.ds(r, g.R), :] - image)]

    planes(g, a, b, body)


def restrict(src, gs, dst, gd, x0, x1, y0, count, matrix, tmp):
    step = -(-count // 8) * 8
    for x in range(x0, x1):
        r = gs.row(2 * x, 2 * y0)
        t = src[pl.ds(r, count, stride=2), :] + src[pl.ds(r + 1, count, stride=2), :]
        r = r + gs.R
        t = t + (src[pl.ds(r, count, stride=2), :] + src[pl.ds(r + 1, count, stride=2), :])
        tmp[pl.ds((x - x0) * step, count), :] = t
    for x in range(x0, x1):
        out = mm(tmp[pl.ds((x - x0) * step, step), :], matrix[...])
        dst[pl.ds(gd.row(x, y0), count), :] = out[0:count]


def prolong(src, gc, dst, gf, x0, x1, y0, count, matrix, tmp):
    for x in range(x0, x1):
        o = (x - x0) * 56
        u = mm(src[pl.ds(gc.row(x, y0), count), :], matrix[...])
        tmp[pl.ds(o, count, stride=2), :] = u
        tmp[pl.ds(o + 1, count, stride=2), :] = u
    for x in range(x0, x1):
        o = (x - x0) * 56
        v = tmp[pl.ds(o, 2 * count), :]
        for k in range(2):
            at = pl.ds(gf.row(2 * x + k, 2 * y0), 2 * count)
            dst[at, :] = dst[at, :] + v


class Item:
    def __init__(self, geo, w):
        self.g, self.w = geo, w


class Plan:
    def __init__(self, items, cross=False):
        self.items, self.cross = items, cross
        self.counts = [it.w if cross else it.g.nx for it in items]
        self.yrows = sum(n * it.w for n, it in zip(self.counts, items))
        self.yrows = -(-self.yrows // 8) * 8
        self.tiles = []
        for k, it in enumerate(items):
            for x in range(self.counts[k]):
                for t in self.tiles:
                    if t[0] is it.g and t[1] + it.w <= 64:
                        break
                else:
                    t = [it.g, 0, []]
                    self.tiles.append(t)
                t[2].append((k, x, t[1]))
                t[1] += it.w
        self.zrows = sum(t[0].ny for t in self.tiles)
        self.zrows = -(-self.zrows // 8) * 8
        self.drows = max(self.counts)
        self.drows = -(-self.drows // 8) * 8
        assert sum(it.w * it.w for it in items) <= 64

        self.z0 = [0, self.zrows]
        self.d0 = [2 * self.zrows + q * self.drows for q in range(4)]
        self.y0 = [2 * self.zrows + 4 * self.drows + q * self.yrows for q in range(2)]
        self.total = 2 * (self.zrows + self.yrows) + 4 * self.drows
        self.xtotal = sum(it.w * it.g.R for it in items)

    def scratch(self):
        x = [] if self.cross else [pltpu.VMEM((self.xtotal, 128), F32)]
        return x + [
            pltpu.VMEM((self.total, 128), F32),
            pltpu.VMEM((self.total, 128), F32),
            pltpu.SemaphoreType.DMA((2,)),
            pltpu.SemaphoreType.DMA((2,)),
        ]


class Exchange:
    def __init__(self, plan, refs, scratch, place):
        self.plan, self.refs, self.place = plan, refs, place
        self.xr, self.sent, self.got, self.ss, self.rs = scratch
        gx, gy, gz = place.me
        self.partner = (1 - gx, gy, gz)
        self.x_copies = []
        o = 0
        for k, it in enumerate(plan.items):
            r = pl.multiple_of(GUARD + (it.g.halo + self.edge(it)) * it.g.R, 8)
            n = it.w * it.g.R
            self.x_copies.append(self.copy(refs[k].at[pl.ds(r, n), :], self.xr.at[pl.ds(o, n), :], 0, self.partner))
            o += n
        self.segments(0)

    def edge(self, it):
        return jnp.where(self.place.me[0] == 0, it.g.nx - it.w, 0)

    def source(self, k, x, y):
        return self.plan.items[k].g.row(x, y)

    def target(self, k, x, y):
        return self.refs[k], self.plan.items[k].g.row(x, y)

    def segments(self, dx):
        plan = self.plan
        at = {}
        for d in range(2):
            at[1 - 2 * d, 0] = plan.y0[d]
            at[0, 1 - 2 * d] = plan.z0[d]
            for e in range(2):
                at[1 - 2 * d, 1 - 2 * e] = plan.d0[2 * d + e]
        self.y_copies, self.z_copies, self.d_copies = [], [], []
        for d in (1, -1):
            self.y_copies.append(self.segment(at, dx, d, 0, plan.yrows))
            self.z_copies.append(self.segment(at, dx, 0, d, plan.zrows))
            for e in (1, -1):
                self.d_copies.append(self.segment(at, dx, d, e, plan.drows))

    def segment(self, at, dx, dy, dz, n):
        there = self.place.exists(dy, dz)
        peer = self.place.beside(dx, dy, dz)
        peer = tuple(jnp.where(there, p, q) for p, q in zip(peer, self.partner))
        target = pl.multiple_of(jnp.where(there, at[dy, dz], at[-dy, -dz]), 8)
        return self.copy(self.sent.at[pl.ds(at[dy, dz], n), :], self.got.at[pl.ds(target, n), :], 1, peer)

    def copy(self, src, dst, k, peer):
        return pltpu.make_async_remote_copy(
            src_ref=src, dst_ref=dst, send_sem=self.ss.at[k], recv_sem=self.rs.at[k],
            device_id=peer, device_id_type=MESH,
        )

    def x_send(self):
        for c in self.x_copies:
            c.start()

    def settle(self, x=True):
        if x:
            self.x_sent()
        self.copy(self.sent, self.got, 1, self.partner).wait_send()

    def x_sent(self):
        self.copy(self.xr, self.xr, 0, self.partner).wait_send()

    def x_wait(self):
        self.copy(self.xr, self.xr, 0, self.partner).wait_recv()

    def x_fill(self):
        m0, m1 = self.place.x_masks
        o = 0
        for k, it in enumerate(self.plan.items):
            g, w, ref = it.g, it.w, self.refs[k]
            upper = ((lanes(g.R) + 8) & 127) >= 64
            for j in range(w):
                got = self.xr[pl.ds(o + j * g.R, g.R), :]
                top = ref[pl.ds(GUARD + (g.halo + g.nx - w + j) * g.R, g.R), :]
                low = ref[pl.ds(GUARD + (g.halo + j) * g.R, g.R), :]
                ref[pl.ds(GUARD + (g.halo - w + j) * g.R, g.R), :] = roll(jnp.where(upper, got * m1, top), 64)
                ref[pl.ds(GUARD + (g.halo + g.nx + j) * g.R, g.R), :] = roll(jnp.where(upper, low, got * m0), 64)
            o += w * g.R

    def pack_send(self):
        self.pack()
        self.send()

    def pack(self):
        for k in range(len(self.refs)):
            self.pack_item(k)

    def send(self):
        for c in self.d_copies + self.z_copies + self.y_copies:
            c.start()

    def pack_item(self, k):
        if k == 0:
            self.yo, self.co, self.corner = 0, 0, [None] * 4
        it = self.plan.items[k]
        g, w, ref = it.g, it.w, self.refs[k]
        n = self.plan.counts[k]
        lane = lanes(self.plan.drows) & 63
        for d in range(1, w + 1):
            at = self.co + (d - 1) * w
            for e, y in enumerate((g.ny - d, d - 1)):
                v = ref[pl.ds(self.source(k, 0, y), n, stride=g.R), :]
                self.sent[pl.ds(self.plan.y0[e] + self.yo, n), :] = v
                if n < self.plan.drows:
                    v = jnp.concatenate([v, jnp.zeros((self.plan.drows - n, 128), F32)], axis=0)
                for q, z in enumerate((g.nz - w, 0)):
                    moved = roll(v, at - z)
                    old = self.corner[2 * e + q]
                    self.corner[2 * e + q] = moved if old is None else jnp.where(lane >= at, moved, old)
            self.yo += n
        self.co += w * w
        if k == len(self.refs) - 1:
            for q in range(4):
                self.sent[pl.ds(self.plan.d0[q], self.plan.drows), :] = self.corner[q]
        zo = 0
        for t, _, slots in self.plan.tiles:
            if slots[-1][0] == k:
                self.pack_tile(t, slots, zo)
            zo += t.ny

    def pack_tile(self, g, slots, zo):
        lane = lanes(g.ny)
        acc = [None, None]
        for k, x, at in slots:
            w = self.plan.items[k].w
            moved = roll(self.refs[k][pl.ds(self.source(k, x, 0), g.ny), :], at)
            for q, past in enumerate((g.nz - w, 0)):
                here = ((lane - past) & 63 >= at) & ((lane - past) & 63 < at + w)
                acc[q] = moved if acc[q] is None else jnp.where(here, moved, acc[q])
        for q in range(2):
            self.sent[pl.ds(self.plan.z0[q] + zo, g.ny), :] = acc[q]

    def unpack(self):
        my, mz = self.place.y_masks, self.place.z_masks
        self.copy(self.sent, self.got, 1, self.partner).wait_recv()
        yo, co = 0, 0
        for k, it in enumerate(self.plan.items):
            g, w = it.g, it.w
            n = self.plan.counts[k]
            lane = lanes(n) & 63
            into = (lane >= 64 - w, (lane >= g.nz) & (lane < g.nz + w))
            for d in range(1, w + 1):
                at = co + (d - 1) * w
                for e, y in enumerate((-d, g.ny + d - 1)):
                    v = self.got[pl.ds(self.plan.y0[e] + yo, n), :]
                    for q, z in enumerate((-w, g.nz)):
                        got = self.got[pl.ds(self.plan.d0[2 * e + q], n), :] * mz[q]
                        v = jnp.where(into[q], roll(got, z - at), v)
                    ref, r = self.target(k, 0, y)
                    ref[pl.ds(r, n, stride=g.R), :] = v * my[e]
                yo += n
            co += w * w
        self.unpack_z(True)

    def unpack_rest(self):
        self.unpack_z(False)

    def unpack_z(self, edge):
        mz = self.place.z_masks
        zo = 0
        for g, _, slots in self.plan.tiles:
            lane = lanes(g.ny) & 63
            got = [self.got[pl.ds(self.plan.z0[q] + zo, g.ny), :] * mz[q] for q in range(2)]
            for k, x, at in slots:
                w = self.plan.items[k].w
                if (x < w or x >= g.nx - w) != edge:
                    continue
                ref, r = self.target(k, x, 0)
                rows = pl.ds(r, g.ny)
                v = ref[rows, :]
                v = jnp.where(lane >= 64 - w, roll(got[0], -g.nz - at), v)
                v = jnp.where((lane >= g.nz) & (lane < g.nz + w), roll(got[1], g.nz - at), v)
                ref[rows, :] = v
            zo += g.ny


class Cross(Exchange):
    def __init__(self, plan, main, scratch, place):
        self.plan, self.main, self.refs, self.place = plan, main, main.refs, place
        self.sent, self.got, self.ss, self.rs = scratch
        self.partner = main.partner
        self.segments(1)

    def source(self, k, x, y):
        it = self.plan.items[k]
        return GUARD + (it.g.halo + self.edge(it) + x) * it.g.R + it.g.y0 + y

    def target(self, k, x, y):
        o = sum(it.w * it.g.R for it in self.plan.items[:k])
        g = self.plan.items[k].g
        return self.main.xr, o + x * g.R + g.y0 + y


class Place:
    def __init__(self, sizes):
        self.sizes = sizes
        self.me = tuple(lax.axis_index(a) for a in ("gx", "gy", "gz"))
        gx, gy, gz = self.me
        one = lambda c: jnp.where(c, 1.0, 0.0).astype(F32)
        self.x_masks = (one(gx == 0), one(gx == 1))
        self.y_masks = (one(gy > 0), one(gy < sizes[1] - 1))
        self.z_masks = (one(gz > 0), one(gz < sizes[2] - 1))

    def exists(self, dy, dz):
        gx, gy, gz = self.me
        y, z = gy + dy, gz + dz
        return (y >= 0) & (y < self.sizes[1]) & (z >= 0) & (z < self.sizes[2])

    def beside(self, dx, dy, dz):
        return tuple(
            lax.rem(m + d % n, n) if d % n else m for m, d, n in zip(self.me, (dx, dy, dz), self.sizes)
        )


class Gather:
    rows = 24

    def __init__(self, place, scratch, whole):
        self.place, self.whole = place, whole
        self.mine, self.got, self.sum, self.parts, self.ss, self.rs = scratch
        n = place.sizes
        self.near = [(a, b) for a in range(n[0]) for b in range(n[1])][1:]
        self.near.sort(key=lambda p: -far((p[0], p[1], 0), n))
        self.line = sorted(range(1, n[2]), key=lambda c: -far((0, 0, c), n))
        self.at = pl.ds(pl.multiple_of(GUARD3 + self.rows * place.me[2], 8), self.rows)

    def copy(self, src, dst, k, peer):
        return pltpu.make_async_remote_copy(
            src_ref=src, dst_ref=dst, send_sem=self.ss.at[k], recv_sem=self.rs.at[k],
            device_id=peer, device_id_type=MESH,
        )

    def send(self):
        for k, (a, b) in enumerate(self.near):
            self.copy(self.mine, self.got.at[k], 0, self.place.beside(a, b, 0)).start()

    def relay(self):
        self.copy(self.got, self.got, 0, self.place.beside(1, 0, 0)).wait_recv()
        gx, gy, gz = self.place.me
        ny = self.place.sizes[1]
        lane = lanes(8)
        sums = [[], []], [[], []]
        for k, (a, b) in enumerate([(0, 0)] + self.near):
            tile = self.mine[...] if k == 0 else self.got[k - 1]
            start = 6 * lax.rem(gy + ny - b, ny)
            for h in range(2):
                y = (lane - 16 * h) & 31
                sums[a][h].append(jnp.where((y >= start) & (y < start + 6), tile, 0.0))
        for h in range(2):
            own, other = (roll(tree(sums[a][h]), -16 * h) for a in range(2))
            self.parts[pl.ds(16 * h, 8), :] = jnp.where(gx == 0, own, other)
            self.parts[pl.ds(16 * h + 8, 8), :] = jnp.where(gx == 0, other, own)
        for h in range(2):
            r = 16 * h
            self.sum[pl.ds(12 * h, 3, stride=4), :] = self.parts[pl.ds(r, 3), :]
            self.sum[pl.ds(12 * h + 1, 3, stride=4), :] = self.parts[pl.ds(r + 4, 3), :] + self.parts[pl.ds(r + 8, 3), :]
            self.sum[pl.ds(12 * h + 2, 3, stride=4), :] = self.parts[pl.ds(r + 12, 3), :]
        for c in self.line:
            self.copy(self.sum, self.whole.at[self.at, :], 1, self.place.beside(0, 0, c)).start()
        self.whole[self.at, :] = self.sum[...]

    def finish(self):
        self.most().wait_recv()

    def most(self):
        most = self.whole.at[pl.ds(GUARD3, self.rows * (self.place.sizes[2] - 1)), :]
        return self.copy(most, most, 1, self.place.beside(1, 0, 0))

    def settle(self):
        self.copy(self.got, self.got, 0, self.place.beside(1, 0, 0)).wait_send()
        self.most().wait_send()


def gather_scratch(sizes):
    return [
        pltpu.VMEM((8, 128), F32),
        pltpu.VMEM((sizes[0] * sizes[1] - 1, 8, 128), F32),
        pltpu.VMEM((24, 128), F32),
        pltpu.VMEM((32, 128), F32),
        pltpu.SemaphoreType.DMA((2,)),
        pltpu.SemaphoreType.DMA((2,)),
    ]


def spread_to_level3(place):
    gx, gy, gz = place.me
    r = iota2((128, 256), 0)
    l = iota2((128, 256), 1)
    x = 6 * gx + 3 * (r >> 6) + ((r & 63) >> 3)
    y = 6 * gy + (r & 7)
    hit = (x == (l >> 5) + 4 * gx) & (y == (l & 31)) & ((r & 7) < 6) & ((r & 63) < 24)
    return jnp.where(hit, 1.0, 0.0).astype(BF16)


def to_level3(src, mine, square, turned, chosen):
    g = L2
    for i in range(3):
        r = g.row(2 * i, 0)
        t = src[pl.ds(r, 6, stride=2), :] + src[pl.ds(r + 1, 6, stride=2), :]
        r = r + g.R
        t = t + (src[pl.ds(r, 6, stride=2), :] + src[pl.ds(r + 1, 6, stride=2), :])
        square[pl.ds(8 * i, 6), :] = t
    turned[...] = jnp.transpose(square[...])
    a = turned[pl.ds(0, 8, stride=2), :] + turned[pl.ds(1, 8, stride=2), :]
    b = turned[pl.ds(64, 8, stride=2), :] + turned[pl.ds(65, 8, stride=2), :]
    a = (a + roll(b, 64)) * 0.125
    out = mm(a, chosen[...])
    for k in range(2):
        turned[pl.ds(8 * k, 8), :] = out[:, 128 * k : 128 * k + 128]
    for k in range(2):
        mine[pl.ds(4 * k, 3), :] = turned[pl.ds(8 * k, 3), :] + roll(turned[pl.ds(8 * k + 3, 3), :], 16)


def image3(ref, s_ref, r, n):
    lane = lanes(n)
    c = ref[pl.ds(r, n), :]
    b = ref[pl.ds(r + 4, n), :] + ref[pl.ds(r - 4, n), :]
    b = b + (roll(c, 1) + roll(c, -1))
    b = b + roll(jnp.where(lane < 32, ref[pl.ds(r + 1, n), :], c), -32)
    b = b + roll(jnp.where(lane >= 96, ref[pl.ds(r - 1, n), :], c), 32)
    return c, FACTOR3 * (6.0 * c - b) + s_ref[pl.ds(r, n), :] * c


def chunks3(rows, ref, body):
    n = min(rows, 384)

    def step(i, carry):
        r = pl.multiple_of(GUARD3 + i * n, 8)
        ref[pl.ds(r, n), :] = body(r, n)
        return carry

    lax.fori_loop(0, rows // n, step, 0)


def match4(k, shape, coarse_dim, ny):
    c = iota2(shape, coarse_dim)
    l = iota2(shape, 1 - coarse_dim)
    return ((c >> 4) == 2 * k + (l >> 6)) & ((c & 15) == ((l & 31) >> 1)) & ((l & 31) < ny)


def restrict4(src, n, matrix):
    total = None
    for k in range(3):
        t = src[pl.ds(GUARD3 + k, n, stride=8), :] + src[pl.ds(GUARD3 + k + 4, n, stride=8), :]
        part = mm(t, matrix[k])
        total = part if total is None else total + part
    return total


def dot_all(a, b):
    return jnp.sum(jnp.sum(a * b, axis=0, keepdims=True), axis=1, keepdims=True)


def bottom(source, s4, p4, n, ny):
    estimate = jnp.zeros_like(source)
    left = source
    inside = (lanes(n) < 96) & ((lanes(n) & 15) < ny)
    shifted = 6.0 * FACTOR4 + s4[...]
    for it in range(BOTTOM_ITERS):
        p4[pl.ds(GUARD, n), :] = left
        b = p4[pl.ds(GUARD + 1, n), :] + p4[pl.ds(GUARD - 1, n), :]
        b = b + (roll(left, 1) + roll(left, -1))
        b = b + (roll(left, 16) + roll(left, -16))
        image = shifted * left - FACTOR4 * jnp.where(inside, b, 0.0)
        now = dot_all(left, left)
        bent = dot_all(left, image)
        if it == 0:
            denom = bent
            direction, turned = left, image
        else:
            ratio = now * inv_before
            denom = bent - ratio * ratio * denom
            direction = left + ratio * direction
            turned = image + ratio * turned
        step = now / denom
        inv_before = 1.0 / now
        estimate = estimate + step * direction
        if it < BOTTOM_ITERS - 1:
            left = left - step * turned
    return estimate


PLAN_A = Plan([Item(L0, 3), Item(L0, 2), Item(L0, 2)])
PLAN_S = Plan([Item(L1, 6), Item(L2, 5)])
PLAN_B = Plan([Item(L1, 6)])
PLAN_BX = Plan([Item(L1, 6)], True)
PLAN_C = Plan([Item(L0, 3)])
PLAN_D = Plan([Item(L2, 5)])
PLANS = (PLAN_A, PLAN_S, PLAN_B, PLAN_C, PLAN_D, PLAN_BX)


def far(p, sizes):
    ring = lambda d, n: min(d % n, -d % n)
    return p[0] + ring(p[1], sizes[1]) + ring(p[2], 4) + ring(p[2] // 4, 4)


def kernel(sizes, counts, right_in, guess_in, react_in, guess, r0, eb0, left0, step_out, *scratch):
    scratch = list(scratch)

    def take(n):
        out = scratch[:n]
        del scratch[:n]
        return out

    raw = take(3)
    (in_sems,) = take(1)
    right, react, inv0, ea0 = take(4)
    f1, s1, inv1, ea1, eb1, left1 = take(6)
    f2, s2, inv2, ea2, eb2, left2 = take(6)
    f3, s3, inv3, ea3, eb3, left3 = take(6)
    s4, p4, down_m, up_m, tmp, square, turned, spread, slab = take(9)
    chosen, picks, down4, up4 = take(4)
    scr = [take(n) for n in counts]
    place = Place(sizes)
    gx, gy, gz = place.me
    n3, n4, ny3 = 24 * sizes[2], 3 * sizes[2], 6 * sizes[1]

    inputs = (guess_in, right_in, react_in)
    for k in range(3):
        for q in range(4):
            at = pl.ds(12 * q, 12)
            pltpu.make_async_copy(inputs[k].at[at], raw[k].at[at], in_sems.at[k]).start()

    def clear(ref):
        n = ref.shape[0]
        size = next(k for k in (128, 122 * 8, 80, 8) if n % k == 0) if n > 128 else n
        size = {1808: 904, 976: 488, 416: 208}.get(n, size)

        def step(i, carry):
            ref[pl.ds(pl.multiple_of(i * size, 8), size), :] = jnp.zeros((size, 128), F32)
            return carry

        lax.fori_loop(0, n // size, step, 0)

    peers = [(a, b, c) for a in range(sizes[0]) for b in range(sizes[1]) for c in range(sizes[2])][1:]
    peers.sort(key=lambda p: -far(p, sizes))
    beside = {(a, b % sizes[1], c % sizes[2]) for a in range(2) for b in (1, -1) for c in (1, -1)}
    beside |= {(1, 0, c % sizes[2]) for c in (1, -1)}
    greeted = [p for p in peers if p[2] == 0 or p[:2] == (0, 0) or p in beside]
    barrier = pltpu.get_barrier_semaphore()
    for p in greeted:
        pl.semaphore_signal(barrier, inc=1, device_id=place.beside(*p), device_id_type=MESH)
    for ref in (guess, right, react):
        ref[...] = jnp.zeros_like(ref)

    ex_a = Exchange(PLAN_A, (guess, right, react), scr[0], place)
    ex_s = Exchange(PLAN_S, (s1, s2), scr[1], place)
    ex_b = Exchange(PLAN_B, (f1,), scr[2], place)
    ex_c = Exchange(PLAN_C, (eb0,), scr[3], place)
    ex_d = Exchange(PLAN_D, (f2,), scr[4], place)
    cx_b = Cross(PLAN_BX, ex_b, scr[5], place)
    ga_s = Gather(place, scr[6], s3)
    ga_f = Gather(place, scr[7], f3)
    for k, dst in enumerate((guess, right, react)):
        pltpu.make_async_copy(inputs[k], raw[k], in_sems.at[k]).wait()

        for i in range(24):
            dst[pl.ds(L0.row(i, 0), 48), 0:48] = raw[k][i]
            dst[pl.ds(L0.row(i, 0), 48), 64:112] = raw[k][i + 24]
        ex_a.pack_item(k)

    reduced, red_send, red_recv = scr[8]

    pl.semaphore_wait(barrier, len(greeted))
    ex_a.send()

    for ref in (f1, s1, ea1, eb1, f2, s2, ea2, eb2, ea3, eb3, p4, square):
        clear(ref)
    spread[...] = jnp.zeros_like(spread)
    for ref in (f3, s3, inv3):
        for r in (0, GUARD3 + n3):
            ref[pl.ds(r, GUARD3), :] = jnp.zeros((GUARD3, 128), F32)

    a = iota2((128, 128), 0)
    b = iota2((128, 128), 1)
    signed = lambda v: ((v + 8) & 63) - 8
    base = lambda v: ((v + 8) & 127) & 64
    zb = signed(b)
    hit = ((a == ((base(b) + 2 * zb) & 127)) | (a == ((base(b) + 2 * zb + 1) & 127))) & (zb >= -8) & (zb < 24)
    down_m[...] = jnp.where(hit, 0.125, 0.0).astype(BF16)
    hit = a == ((base(b) + (zb >> 1)) & 127)
    up_m[...] = jnp.where(hit, 1.0, 0.0).astype(BF16)


    restrict(react, L0, s1, L1, 0, 12, 0, 24, down_m, tmp)
    restrict(s1, L1, s2, L2, 0, 6, 0, 12, down_m, tmp)
    ex_s.pack()
    for e in (ga_s, ga_f):
        e.mine[...] = jnp.zeros((8, 128), F32)
        e.sum[...] = jnp.zeros((24, 128), F32)
    chosen[...] = spread_to_level3(place)
    to_level3(s2, ga_s.mine, square, turned, chosen)
    for h in range(2):
        r = iota2((112, 384), 0)
        l = iota2((112, 384), 1)
        hit = (6 * gx + 3 * h + (r >> 4) - 2 == (l >> 5)) & (6 * gy + (r & 15) - 2 == (l & 31)) & ((r & 15) < 10)
        picks[h] = jnp.where(hit, 1.0, 0.0).astype(BF16)
    for k in range(3):
        down4[k] = jnp.where(match4(k, (128, 128), 1, ny3), 0.125, 0.0).astype(BF16)
        up4[k] = jnp.where(match4(k, (128, 128), 0, ny3), 1.0, 0.0).astype(BF16)


    def start(r):
        at = pl.ds(r, L0.R)
        c, image = image_of(guess, react, L0, r)
        res = right[at, :] - image
        inv = inverse(react[at, :], 1.0)
        return [(r0, res), (inv0, inv), (ea0, inv * res)]

    ex_a.unpack()
    ex_a.x_send()
    ex_s.send()
    ga_s.send()
    ex_a.unpack_rest()
    planes(L0, 1, 23, start)
    ex_a.x_wait()
    ex_a.x_fill()
    planes(L0, -2, 1, start)
    planes(L0, 23, 26, start)
    relax(L0, ea0, eb0, r0, react, inv0, -1, 25)
    leftover(L0, eb0, left0, r0, react, 0, 24)
    restrict(left0, L0, f1, L1, 0, 12, 0, 24, down_m, tmp)
    ex_b.pack_send()
    cx_b.pack_send()
    ex_b.x_send()

    ex_c.pack()
    ex_s.unpack()
    ex_s.x_send()

    def inverse_of(g, sh, inv, first_plane, end):
        planes(g, first_plane, end, lambda r: [(inv, inverse(sh[pl.ds(r, g.R), :], g.factor))])

    inverse_of(L1, s1, inv1, 0, 12)

    ex_b.x_sent()
    ex_b.unpack()
    ex_c.send()
    first(L1, ea1, f1, inv1, 0, 12)
    relax(L1, ea1, eb1, f1, s1, inv1, 1, 11)
    ex_s.x_wait()
    ex_s.x_fill()
    inverse_of(L1, s1, inv1, -6, 0)
    inverse_of(L1, s1, inv1, 12, 18)
    inverse_of(L2, s2, inv2, -5, 11)
    ex_b.x_wait()
    cx_b.unpack()
    ex_b.x_fill()
    first(L1, ea1, f1, inv1, -6, 0)
    first(L1, ea1, f1, inv1, 12, 18)
    relax(L1, ea1, eb1, f1, s1, inv1, -5, 1)
    relax(L1, ea1, eb1, f1, s1, inv1, 11, 17)
    leftover(L1, eb1, left1, f1, s1, -4, 16)
    restrict(left1, L1, f2, L2, -2, 8, -2, 16, down_m, tmp)
    first(L2, ea2, f2, inv2, -2, 8)
    relax(L2, ea2, eb2, f2, s2, inv2, -1, 7)
    leftover(L2, eb2, left2, f2, s2, 0, 6)
    to_level3(left2, ga_f.mine, square, turned, chosen)
    ga_f.send()
    ex_d.pack_send()
    ga_s.relay()

    ga_f.relay()
    ex_c.unpack()
    ex_c.x_send()
    ex_c.unpack_rest()
    ex_d.unpack()
    ex_d.x_send()
    ex_c.x_wait()
    ex_c.x_fill()
    ex_d.x_wait()
    ex_d.x_fill()
    first(L2, ea2, f2, inv2, -5, 11)
    relax(L2, ea2, eb2, f2, s2, inv2, -4, 10)
    ga_s.finish()
    chunks3(n3, inv3, lambda r, n: inverse(s3[pl.ds(r, n), :], FACTOR3))
    s4[...] = restrict4(s3, n4, down4)
    for e in (ex_a, ex_s, ex_c, ex_d, ga_s):
        e.settle()
    for e in (ex_b, cx_b):
        e.settle(False)
    ga_f.finish()

    def relax3(src, dst):
        def body(r, n):
            c, image = image3(src, s3, r, n)
            at = pl.ds(r, n)
            return c + inv3[at, :] * (f3[at, :] - image)

        chunks3(n3, dst, body)

    chunks3(n3, ea3, lambda r, n: inv3[pl.ds(r, n), :] * f3[pl.ds(r, n), :])
    relax3(ea3, eb3)
    chunks3(n3, left3, lambda r, n: f3[pl.ds(r, n), :] - image3(eb3, s3, r, n)[1])
    e4 = bottom(restrict4(left3, n4, down4), s4, p4, n4, ny3 // 2)
    for k in range(3):
        u = mm(e4, up4[k])
        for q in (k, k + 4):
            at = pl.ds(GUARD3 + q, n4, stride=8)
            eb3[at, :] = eb3[at, :] + u
    for src, dst, n in ((eb3, ea3, 48), (ea3, slab, 40)):
        r = pl.multiple_of(GUARD3 + 24 * gz - (n - 24) // 2, 4)
        c, image = image3(src, s3, r, n)
        at = pl.ds(r, n)
        dst[at if n == 48 else pl.ds(0, n), :] = c + inv3[at, :] * (f3[at, :] - image)
    for k in range(3):
        v = slab[pl.ds(k, 10, stride=4), :]
        for h in range(2):
            for q in range(2):
                spread[k, pl.ds(64 * h + q, 10, stride=2), :] = v
    wide = [jnp.concatenate(p, axis=1) for p in zip(*[split(spread[k]) for k in range(3)])]
    coarse = []
    for h in range(2):
        pick = picks[h]
        parts = [
            lax.dot_general(pick, p, (((1,), (1,)), ((), ())), preferred_element_type=F32) for p in wide
        ]
        coarse.append(parts[0] + parts[1])
    fine = roll(jnp.where(lanes(112) < 64, coarse[0], coarse[1]), -4)
    for i in range(7):
        u = fine[16 * i : 16 * i + 10]
        tmp[pl.ds(24 * i, 10, stride=2), :] = u
        tmp[pl.ds(24 * i + 1, 10, stride=2), :] = u
    for i in range(7):
        v = tmp[pl.ds(24 * i, 20), :]
        for q in range(2):
            at = pl.ds(L2.row(2 * (i - 2) + q, -4), 20)
            eb2[at, :] = eb2[at, :] + v
    relax(L2, eb2, ea2, f2, s2, inv2, -3, 9)
    relax(L2, ea2, eb2, f2, s2, inv2, -2, 8)
    prolong(eb2, L2, eb1, L1, -2, 8, -2, 16, up_m, tmp)
    relax(L1, eb1, ea1, f1, s1, inv1, -3, 15)
    relax(L1, ea1, eb1, f1, s1, inv1, -2, 14)
    prolong(eb1, L1, eb0, L0, -2, 14, -2, 28, up_m, tmp)
    relax(L0, eb0, ea0, r0, react, inv0, -2, 26)
    relax(L0, ea0, eb0, r0, react, inv0, -1, 25)

    row = iota2((L0.R, 128), 0)
    inside = ((lanes(L0.R) & 63) < 48) & (row >= L0.y0) & (row < L0.y0 + 48)

    upper, lower = [], []
    for i in range(24):
        r = GUARD + (L0.halo + i) * L0.R
        c, image = image_of(eb0, react, L0, r)
        left0[pl.ds(r, L0.R), :] = image
        upper.append(c * r0[pl.ds(r, L0.R), :])
        lower.append(c * image)
    upper = jnp.where(inside, tree(upper), 0.0)
    lower = jnp.where(inside, tree(lower), 0.0)
    upper = jnp.sum(upper, axis=0, keepdims=True)
    lower = jnp.sum(lower, axis=0, keepdims=True)
    half = lanes(1) < 64
    number = (gx * sizes[1] + gy) * sizes[2] + gz
    reduced[number] = jnp.where(half, upper + roll(upper, 64), lower + roll(lower, 64))
    own = reduced.at[number]

    def summed(src, dst, p):
        return pltpu.make_async_remote_copy(
            src_ref=src, dst_ref=dst, send_sem=red_send.at[0], recv_sem=red_recv.at[0],
            device_id=place.beside(*p), device_id_type=MESH,
        )

    for p in peers:
        summed(own, own, p).start()
    ga_f.settle()
    most = reduced.at[pl.ds(0, len(peers))]
    summed(most, most, peers[0]).wait()
    sums = [reduced[k] for k in range(8)]
    for k in range(8, len(peers) + 1):
        sums[k % 8] = sums[k % 8] + reduced[k]
    total = tree(sums)
    upper = jnp.sum(jnp.where(half, total, 0.0), axis=1, keepdims=True)
    lower = jnp.sum(jnp.where(half, 0.0, total), axis=1, keepdims=True)
    step_out[...] = jnp.broadcast_to(upper / lower, (8, 128))


def finish(guess, r0, eb0, left0, step_ref, field_out, resid_out, field, resid, sems):
    step = step_ref[0:1, :]
    copies = []
    parts, size = 4, 6
    for p in range(parts):
        for x in range(p * size, p * size + size):
            at = pl.ds(L0.row(x, 0), 48)
            v = guess[at, :] + step * eb0[at, :]
            field[x] = v[:, 0:48]
            field[x + 24] = roll(v, 64)[:, 0:48]
            v = r0[at, :] - step * left0[at, :]
            resid[x] = v[:, 0:48]
            resid[x + 24] = roll(v, 64)[:, 0:48]
        for q, (src, dst) in enumerate(((field, field_out), (resid, resid_out))):
            for h in range(2):
                at = pl.ds(p * size + 24 * h, size)
                c = pltpu.make_async_copy(src.at[at], dst.at[at], sems.at[4 * p + 2 * q + h])
                c.start()
                copies.append(c)
    for c in copies:
        c.wait()


def solution(mesh):
    sizes = tuple(mesh.shape[a] for a in ("gx", "gy", "gz"))
    n3, n4 = 24 * sizes[2] + 2 * GUARD3, 3 * sizes[2]
    scratch = [pltpu.VMEM((48, 48, 48), F32)] * 3 + [pltpu.SemaphoreType.DMA((3,))]
    scratch += [pltpu.VMEM((L0.total, 128), F32)] * 4
    scratch += [pltpu.VMEM((L1.total, 128), F32)] * 6
    scratch += [pltpu.VMEM((L2.total, 128), F32)] * 6
    scratch += [pltpu.VMEM((n3, 128), F32)] * 6
    scratch += [pltpu.VMEM((n4, 128), F32), pltpu.VMEM((n4 + 2 * GUARD, 128), F32)]
    scratch += [pltpu.VMEM((128, 128), BF16)] * 2 + [pltpu.VMEM((16 * 56, 128), F32)]
    scratch += [pltpu.VMEM((128, 128), F32)] * 2
    scratch += [pltpu.VMEM((3, 128, 128), F32), pltpu.VMEM((40, 128), F32)]
    scratch += [pltpu.VMEM((128, 256), BF16), pltpu.VMEM((2, 112, 384), BF16)]
    scratch += [pltpu.VMEM((3, 128, 128), BF16)] * 2
    groups = [p.scratch() for p in PLANS] + [gather_scratch(sizes)] * 2
    devices = sizes[0] * sizes[1] * sizes[2]
    groups += [[pltpu.VMEM((devices, 1, 128), F32)] + [pltpu.SemaphoreType.DMA((1,))] * 2]
    for g in groups:
        scratch += g
    counts = tuple(len(g) for g in groups)
    vmem = pl.BlockSpec(memory_space=pltpu.VMEM)

    anywhere = pl.BlockSpec(memory_space=pl.ANY)

    def body(right_side, start_guess, reaction):
        whole = pltpu.VMEM((L0.total, 128), F32)
        parts = pl.pallas_call(
            functools.partial(kernel, sizes, counts),
            out_shape=[whole] * 4 + [pltpu.VMEM((8, 128), F32)],
            in_specs=[anywhere] * 3,
            out_specs=[vmem] * 5,
            scratch_shapes=scratch,
            compiler_params=pltpu.CompilerParams(
                collective_id=0, has_side_effects=True, vmem_limit_bytes=60 * 2**20
            ),
        )(right_side, start_guess, reaction)
        shape = jax.ShapeDtypeStruct(right_side.shape, F32)
        return tuple(
            pl.pallas_call(
                finish,
                out_shape=[shape, shape],
                in_specs=[vmem] * 5,
                out_specs=[anywhere] * 2,
                scratch_shapes=[pltpu.VMEM(right_side.shape, F32)] * 2 + [pltpu.SemaphoreType.DMA((16,))],
                compiler_params=pltpu.CompilerParams(vmem_limit_bytes=16 * 2**20),
            )(*parts)
        )

    placed = P("gx", "gy", "gz")
    return jax.shard_map(
        body, mesh=mesh, in_specs=(placed,) * 3, out_specs=(placed,) * 2, check_vma=False
    )
```

```python
import functools

import jax
import jax.numpy as jnp
from jax import lax
from jax.experimental import pallas as pl
from jax.experimental.pallas import tpu as pltpu
from jax.sharding import PartitionSpec as P

MESH = pl.DeviceIdType.MESH
F32 = jnp.float32
BF16 = jnp.bfloat16
DAMP = 6.0 / 7.0
GUARD = 8
GUARD3 = 16
BOTTOM_ITERS = 6


class Geo:
    def __init__(self, nx, ny, nz, halo, rows, y0, depth, unroll):
        self.nx, self.ny, self.nz, self.halo, self.R, self.y0 = nx, ny, nz, halo, rows, y0
        self.factor = 0.25**depth
        self.unroll = unroll
        self.total = 2 * GUARD + (nx + 2 * halo) * rows

    def row(self, x, y):
        return GUARD + (self.halo + x) * self.R + self.y0 + y


L0 = Geo(24, 48, 48, 4, 56, 4, 0, 28)
L1 = Geo(12, 24, 24, 6, 40, 8, 1, 24)
L2 = Geo(6, 12, 12, 5, 24, 6, 2, 16)
FACTOR3 = 0.25**3
FACTOR4 = 0.25**4


def lanes(rows):
    return lax.broadcasted_iota(jnp.int32, (rows, 128), 1)


def iota2(shape, dim):
    return lax.broadcasted_iota(jnp.int32, shape, dim)


def tree(terms):
    while len(terms) > 1:
        terms = [sum(terms[k + 1 : k + 2], terms[k]) for k in range(0, len(terms), 2)]
    return terms[0]


def roll(v, shift):
    shift = shift % 128
    return v if shift == 0 else pltpu.roll(v, shift, 1)


def split(a):
    hi = a.astype(BF16)
    return hi, (a - hi.astype(F32)).astype(BF16)


def mm(a, b):
    hi, low = split(a)
    return jnp.dot(hi, b, preferred_element_type=F32) + jnp.dot(low, b, preferred_element_type=F32)


def beside_of(ref, r, R):
    c = ref[pl.ds(r, R), :]
    b = ref[pl.ds(r + R, R), :] + ref[pl.ds(r - R, R), :]
    b = b + (ref[pl.ds(r + 1, R), :] + ref[pl.ds(r - 1, R), :])
    b = b + (roll(c, 1) + roll(c, -1))
    return c, b


def image_of(ref, s_ref, g, r):
    c, b = beside_of(ref, r, g.R)
    return c, g.factor * (6.0 * c - b) + s_ref[pl.ds(r, g.R), :] * c


def planes(g, a, b, body):
    unroll = g.unroll

    def group(start, count):
        todo = []
        for k in range(count):
            r = start + k * g.R
            r = r if isinstance(r, int) else pl.multiple_of(r, 8)
            todo.append((r, body(r)))
        for r, pairs in todo:
            for ref, value in pairs:
                ref[pl.ds(r, g.R), :] = value

    trips = (b - a) // unroll
    origin = GUARD + (g.halo + a) * g.R
    if trips == 1:
        group(origin, unroll)
    elif trips:

        def step(i, carry):
            group(pl.multiple_of(origin + i * (unroll * g.R), 8), unroll)
            return carry

        lax.fori_loop(0, trips, step, 0)
    if (b - a) % unroll:
        group(origin + trips * unroll * g.R, (b - a) % unroll)


def inverse(s, factor):
    return jnp.where(s > 0.0, DAMP / (6.0 * factor + s), 0.0)


def relax(g, src, dst, f, s, inv, a, b):
    def body(r):
        c, image = image_of(src, s, g, r)
        at = pl.ds(r, g.R)
        return [(dst, c + inv[at, :] * (f[at, :] - image))]

    planes(g, a, b, body)


def first(g, dst, f, inv, a, b):
    def body(r):
        at = pl.ds(r, g.R)
        return [(dst, inv[at, :] * f[at, :])]

    planes(g, a, b, body)


def leftover(g, src, dst, f, s, a, b):
    def body(r):
        c, image = image_of(src, s, g, r)
        return [(dst, f[pl.ds(r, g.R), :] - image)]

    planes(g, a, b, body)


def restrict(src, gs, dst, gd, x0, x1, y0, count, matrix, tmp):
    step = -(-count // 8) * 8
    for x in range(x0, x1):
        r = gs.row(2 * x, 2 * y0)
        t = src[pl.ds(r, count, stride=2), :] + src[pl.ds(r + 1, count, stride=2), :]
        r = r + gs.R
        t = t + (src[pl.ds(r, count, stride=2), :] + src[pl.ds(r + 1, count, stride=2), :])
        tmp[pl.ds((x - x0) * step, count), :] = t
    for x in range(x0, x1):
        out = mm(tmp[pl.ds((x - x0) * step, step), :], matrix[...])
        dst[pl.ds(gd.row(x, y0), count), :] = out[0:count]


def prolong(src, gc, dst, gf, x0, x1, y0, count, matrix, tmp):
    for x in range(x0, x1):
        o = (x - x0) * 56
        u = mm(src[pl.ds(gc.row(x, y0), count), :], matrix[...])
        tmp[pl.ds(o, count, stride=2), :] = u
        tmp[pl.ds(o + 1, count, stride=2), :] = u
    for x in range(x0, x1):
        o = (x - x0) * 56
        v = tmp[pl.ds(o, 2 * count), :]
        for k in range(2):
            at = pl.ds(gf.row(2 * x + k, 2 * y0), 2 * count)
            dst[at, :] = dst[at, :] + v


class Item:
    def __init__(self, geo, w):
        self.g, self.w = geo, w
        self.deep = w - 1 if geo is L0 else w


class Plan:
    def __init__(self, items, cross=False):
        self.items, self.cross = items, cross
        self.counts = [it.w if cross else it.g.nx for it in items]
        self.yrows = sum(n * it.w for n, it in zip(self.counts, items))
        self.yrows = -(-self.yrows // 8) * 8
        self.tiles = []
        for k, it in enumerate(items):
            for x in range(self.counts[k]):
                for t in self.tiles:
                    if t[0] is it.g and t[1] + it.w <= 64:
                        break
                else:
                    t = [it.g, 0, []]
                    self.tiles.append(t)
                t[2].append((k, x, t[1]))
                t[1] += it.w
        self.zrows = sum(t[0].ny for t in self.tiles)
        self.zrows = -(-self.zrows // 8) * 8
        self.drows = max(self.counts)
        self.drows = -(-self.drows // 8) * 8
        assert sum(it.w * it.w for it in items) <= 64

        self.z0 = [0, self.zrows]
        self.d0 = [2 * self.zrows + q * self.drows for q in range(4)]
        self.y0 = [2 * self.zrows + 4 * self.drows + q * self.yrows for q in range(2)]
        self.total = 2 * (self.zrows + self.yrows) + 4 * self.drows
        self.xtotal = sum(it.w * it.g.R for it in items)

    def scratch(self):
        x = [] if self.cross else [pltpu.VMEM((self.xtotal, 128), F32)]
        return x + [
            pltpu.VMEM((self.total, 128), F32),
            pltpu.VMEM((self.total, 128), F32),
            pltpu.SemaphoreType.DMA((2,)),
            pltpu.SemaphoreType.DMA((2,)),
        ]


class Exchange:
    def __init__(self, plan, refs, scratch, place):
        self.plan, self.refs, self.place = plan, refs, place
        self.xr, self.sent, self.got, self.ss, self.rs = scratch
        gx, gy, gz = place.me
        self.partner = (1 - gx, gy, gz)
        self.x_copies = []
        o = 0
        for k, it in enumerate(plan.items):
            r = pl.multiple_of(GUARD + (it.g.halo + self.edge(it)) * it.g.R, 8)
            n = it.w * it.g.R
            self.x_copies.append(self.copy(refs[k].at[pl.ds(r, n), :], self.xr.at[pl.ds(o, n), :], 0, self.partner))
            o += n
        self.segments(0)

    def edge(self, it):
        return jnp.where(self.place.me[0] == 0, it.g.nx - it.w, 0)

    def source(self, k, x, y):
        return self.plan.items[k].g.row(x, y)

    def target(self, k, x, y):
        return self.refs[k], self.plan.items[k].g.row(x, y)

    def segments(self, dx):
        plan = self.plan
        at = {}
        for d in range(2):
            at[1 - 2 * d, 0] = plan.y0[d]
            at[0, 1 - 2 * d] = plan.z0[d]
            for e in range(2):
                at[1 - 2 * d, 1 - 2 * e] = plan.d0[2 * d + e]
        self.y_copies, self.z_copies, self.d_copies = [], [], []
        for d in (1, -1):
            self.y_copies.append(self.segment(at, dx, d, 0, plan.yrows))
            self.z_copies.append(self.segment(at, dx, 0, d, plan.zrows))
            for e in (1, -1):
                self.d_copies.append(self.segment(at, dx, d, e, plan.drows))

    def segment(self, at, dx, dy, dz, n):
        there = self.place.exists(dy, dz)
        peer = self.place.beside(dx, dy, dz)
        peer = tuple(jnp.where(there, p, q) for p, q in zip(peer, self.partner))
        target = pl.multiple_of(jnp.where(there, at[dy, dz], at[-dy, -dz]), 8)
        return self.copy(self.sent.at[pl.ds(at[dy, dz], n), :], self.got.at[pl.ds(target, n), :], 1, peer)

    def copy(self, src, dst, k, peer):
        return pltpu.make_async_remote_copy(
            src_ref=src, dst_ref=dst, send_sem=self.ss.at[k], recv_sem=self.rs.at[k],
            device_id=peer, device_id_type=MESH,
        )

    def x_send(self):
        for c in self.x_copies:
            c.start()

    def settle(self, x=True):
        if x:
            self.x_sent()
        self.copy(self.sent, self.got, 1, self.partner).wait_send()

    def x_sent(self):
        self.copy(self.xr, self.xr, 0, self.partner).wait_send()

    def x_wait(self):
        self.copy(self.xr, self.xr, 0, self.partner).wait_recv()

    def x_fill(self):
        m0, m1 = self.place.x_masks
        o = 0
        for k, it in enumerate(self.plan.items):
            g, w, ref = it.g, it.w, self.refs[k]
            upper = ((lanes(g.R) + 8) & 127) >= 64
            for j in range(w):
                got = self.xr[pl.ds(o + j * g.R, g.R), :]
                top = ref[pl.ds(GUARD + (g.halo + g.nx - w + j) * g.R, g.R), :]
                low = ref[pl.ds(GUARD + (g.halo + j) * g.R, g.R), :]
                ref[pl.ds(GUARD + (g.halo - w + j) * g.R, g.R), :] = roll(jnp.where(upper, got * m1, top), 64)
                ref[pl.ds(GUARD + (g.halo + g.nx + j) * g.R, g.R), :] = roll(jnp.where(upper, low, got * m0), 64)
            o += w * g.R

    def pack_send(self):
        self.pack()
        self.send()

    def pack(self):
        for k in range(len(self.refs)):
            self.pack_item(k)

    def send(self):
        for c in self.d_copies + self.z_copies + self.y_copies:
            c.start()

    def pack_item(self, k):
        if k == 0:
            self.yo, self.co, self.corner = 0, 0, [None] * 4
        it = self.plan.items[k]
        g, w, ref = it.g, it.w, self.refs[k]
        n = self.plan.counts[k]
        lane = lanes(self.plan.drows) & 63
        for d in range(1, w + 1):
            at = self.co + (d - 1) * w
            for e, y in enumerate((g.ny - d, d - 1)):
                v = ref[pl.ds(self.source(k, 0, y), n, stride=g.R), :]
                self.sent[pl.ds(self.plan.y0[e] + self.yo, n), :] = v
                if d > it.deep:
                    continue
                if n < self.plan.drows:
                    v = jnp.concatenate([v, jnp.zeros((self.plan.drows - n, 128), F32)], axis=0)
                for q, z in enumerate((g.nz - w, 0)):
                    moved = roll(v, at - z)
                    old = self.corner[2 * e + q]
                    self.corner[2 * e + q] = moved if old is None else jnp.where(lane >= at, moved, old)
            self.yo += n
        self.co += w * w
        if k == len(self.refs) - 1:
            for q in range(4):
                self.sent[pl.ds(self.plan.d0[q], self.plan.drows), :] = self.corner[q]
        zo = 0
        for t, _, slots in self.plan.tiles:
            if slots[-1][0] == k:
                self.pack_tile(t, slots, zo)
            zo += t.ny

    def pack_tile(self, g, slots, zo):
        lane = lanes(g.ny)
        acc = [None, None]
        for k, x, at in slots:
            w = self.plan.items[k].w
            moved = roll(self.refs[k][pl.ds(self.source(k, x, 0), g.ny), :], at)
            for q, past in enumerate((g.nz - w, 0)):
                here = ((lane - past) & 63 >= at) & ((lane - past) & 63 < at + w)
                acc[q] = moved if acc[q] is None else jnp.where(here, moved, acc[q])
        for q in range(2):
            self.sent[pl.ds(self.plan.z0[q] + zo, g.ny), :] = acc[q]

    def unpack(self):
        my, mz = self.place.y_masks, self.place.z_masks
        self.copy(self.sent, self.got, 1, self.partner).wait_recv()
        yo, co = 0, 0
        for k, it in enumerate(self.plan.items):
            g, w = it.g, it.w
            n = self.plan.counts[k]
            lane = lanes(n) & 63
            into = (lane >= 64 - w, (lane >= g.nz) & (lane < g.nz + w))
            for d in range(1, w + 1):
                at = co + (d - 1) * w
                for e, y in enumerate((-d, g.ny + d - 1)):
                    v = self.got[pl.ds(self.plan.y0[e] + yo, n), :]
                    for q, z in enumerate((-w, g.nz) if d <= it.deep else ()):
                        got = self.got[pl.ds(self.plan.d0[2 * e + q], n), :] * mz[q]
                        v = jnp.where(into[q], roll(got, z - at), v)
                    ref, r = self.target(k, 0, y)
                    ref[pl.ds(r, n, stride=g.R), :] = v * my[e]
                yo += n
            co += w * w
        self.unpack_z(True)

    def unpack_rest(self):
        self.unpack_z(False)

    def unpack_z(self, edge):
        mz = self.place.z_masks
        zo = 0
        for g, _, slots in self.plan.tiles:
            lane = lanes(g.ny) & 63
            got = [self.got[pl.ds(self.plan.z0[q] + zo, g.ny), :] * mz[q] for q in range(2)]
            for k, x, at in slots:
                w = self.plan.items[k].w
                if (x < w or x >= g.nx - w) != edge:
                    continue
                ref, r = self.target(k, x, 0)
                rows = pl.ds(r, g.ny)
                v = ref[rows, :]
                v = jnp.where(lane >= 64 - w, roll(got[0], -g.nz - at), v)
                v = jnp.where((lane >= g.nz) & (lane < g.nz + w), roll(got[1], g.nz - at), v)
                ref[rows, :] = v
            zo += g.ny


class Cross(Exchange):
    def __init__(self, plan, main, scratch, place):
        self.plan, self.main, self.refs, self.place = plan, main, main.refs, place
        self.sent, self.got, self.ss, self.rs = scratch
        self.partner = main.partner
        self.segments(1)

    def source(self, k, x, y):
        it = self.plan.items[k]
        return GUARD + (it.g.halo + self.edge(it) + x) * it.g.R + it.g.y0 + y

    def target(self, k, x, y):
        o = sum(it.w * it.g.R for it in self.plan.items[:k])
        g = self.plan.items[k].g
        return self.main.xr, o + x * g.R + g.y0 + y


class Place:
    def __init__(self, sizes):
        self.sizes = sizes
        self.me = tuple(lax.axis_index(a) for a in ("gx", "gy", "gz"))
        gx, gy, gz = self.me
        one = lambda c: jnp.where(c, 1.0, 0.0).astype(F32)
        self.x_masks = (one(gx == 0), one(gx == 1))
        self.y_masks = (one(gy > 0), one(gy < sizes[1] - 1))
        self.z_masks = (one(gz > 0), one(gz < sizes[2] - 1))

    def exists(self, dy, dz):
        gx, gy, gz = self.me
        y, z = gy + dy, gz + dz
        return (y >= 0) & (y < self.sizes[1]) & (z >= 0) & (z < self.sizes[2])

    def beside(self, dx, dy, dz):
        return tuple(
            lax.rem(m + d % n, n) if d % n else m for m, d, n in zip(self.me, (dx, dy, dz), self.sizes)
        )


class Gather:
    rows = 24

    def __init__(self, place, scratch, whole):
        self.place, self.whole = place, whole
        self.mine, self.got, self.sum, self.parts, self.ss, self.rs = scratch
        n = place.sizes
        self.near = [(a, b) for a in range(n[0]) for b in range(n[1])][1:]
        self.near.sort(key=lambda p: -far((p[0], p[1], 0), n))
        self.line = sorted(range(1, n[2]), key=lambda c: -far((0, 0, c), n))
        self.at = pl.ds(pl.multiple_of(GUARD3 + self.rows * place.me[2], 8), self.rows)

    def copy(self, src, dst, k, peer):
        return pltpu.make_async_remote_copy(
            src_ref=src, dst_ref=dst, send_sem=self.ss.at[k], recv_sem=self.rs.at[k],
            device_id=peer, device_id_type=MESH,
        )

    def send(self):
        for k, (a, b) in enumerate(self.near):
            self.copy(self.mine, self.got.at[k], 0, self.place.beside(a, b, 0)).start()

    def relay(self):
        self.copy(self.got, self.got, 0, self.place.beside(1, 0, 0)).wait_recv()
        gx, gy, gz = self.place.me
        ny = self.place.sizes[1]
        lane = lanes(8)
        sums = [[], []], [[], []]
        for k, (a, b) in enumerate([(0, 0)] + self.near):
            tile = self.mine[...] if k == 0 else self.got[k - 1]
            start = 6 * lax.rem(gy + ny - b, ny)
            for h in range(2):
                y = (lane - 16 * h) & 31
                sums[a][h].append(jnp.where((y >= start) & (y < start + 6), tile, 0.0))
        for h in range(2):
            own, other = (roll(tree(sums[a][h]), -16 * h) for a in range(2))
            self.parts[pl.ds(16 * h, 8), :] = jnp.where(gx == 0, own, other)
            self.parts[pl.ds(16 * h + 8, 8), :] = jnp.where(gx == 0, other, own)
        for h in range(2):
            r = 16 * h
            self.sum[pl.ds(12 * h, 3, stride=4), :] = self.parts[pl.ds(r, 3), :]
            self.sum[pl.ds(12 * h + 1, 3, stride=4), :] = self.parts[pl.ds(r + 4, 3), :] + self.parts[pl.ds(r + 8, 3), :]
            self.sum[pl.ds(12 * h + 2, 3, stride=4), :] = self.parts[pl.ds(r + 12, 3), :]
        for c in self.line:
            self.copy(self.sum, self.whole.at[self.at, :], 1, self.place.beside(0, 0, c)).start()
        self.whole[self.at, :] = self.sum[...]

    def finish(self):
        self.most().wait_recv()

    def most(self):
        most = self.whole.at[pl.ds(GUARD3, self.rows * (self.place.sizes[2] - 1)), :]
        return self.copy(most, most, 1, self.place.beside(1, 0, 0))

    def settle(self):
        self.copy(self.got, self.got, 0, self.place.beside(1, 0, 0)).wait_send()
        self.most().wait_send()


def gather_scratch(sizes):
    return [
        pltpu.VMEM((8, 128), F32),
        pltpu.VMEM((sizes[0] * sizes[1] - 1, 8, 128), F32),
        pltpu.VMEM((24, 128), F32),
        pltpu.VMEM((32, 128), F32),
        pltpu.SemaphoreType.DMA((2,)),
        pltpu.SemaphoreType.DMA((2,)),
    ]


def spread_to_level3(place):
    gx, gy, gz = place.me
    r = iota2((128, 256), 0)
    l = iota2((128, 256), 1)
    x = 6 * gx + 3 * (r >> 6) + ((r & 63) >> 3)
    y = 6 * gy + (r & 7)
    hit = (x == (l >> 5) + 4 * gx) & (y == (l & 31)) & ((r & 7) < 6) & ((r & 63) < 24)
    return jnp.where(hit, 1.0, 0.0).astype(BF16)


def to_level3(src, mine, square, turned, chosen):
    g = L2
    for i in range(3):
        r = g.row(2 * i, 0)
        t = src[pl.ds(r, 6, stride=2), :] + src[pl.ds(r + 1, 6, stride=2), :]
        r = r + g.R
        t = t + (src[pl.ds(r, 6, stride=2), :] + src[pl.ds(r + 1, 6, stride=2), :])
        square[pl.ds(8 * i, 6), :] = t
    turned[...] = jnp.transpose(square[...])
    a = turned[pl.ds(0, 8, stride=2), :] + turned[pl.ds(1, 8, stride=2), :]
    b = turned[pl.ds(64, 8, stride=2), :] + turned[pl.ds(65, 8, stride=2), :]
    a = (a + roll(b, 64)) * 0.125
    out = mm(a, chosen[...])
    for k in range(2):
        turned[pl.ds(8 * k, 8), :] = out[:, 128 * k : 128 * k + 128]
    for k in range(2):
        mine[pl.ds(4 * k, 3), :] = turned[pl.ds(8 * k, 3), :] + roll(turned[pl.ds(8 * k + 3, 3), :], 16)


def image3(ref, s_ref, r, n):
    lane = lanes(n)
    c = ref[pl.ds(r, n), :]
    b = ref[pl.ds(r + 4, n), :] + ref[pl.ds(r - 4, n), :]
    b = b + (roll(c, 1) + roll(c, -1))
    b = b + roll(jnp.where(lane < 32, ref[pl.ds(r + 1, n), :], c), -32)
    b = b + roll(jnp.where(lane >= 96, ref[pl.ds(r - 1, n), :], c), 32)
    return c, FACTOR3 * (6.0 * c - b) + s_ref[pl.ds(r, n), :] * c


def chunks3(rows, ref, body):
    n = min(rows, 384)

    def step(i, carry):
        r = pl.multiple_of(GUARD3 + i * n, 8)
        ref[pl.ds(r, n), :] = body(r, n)
        return carry

    lax.fori_loop(0, rows // n, step, 0)


def match4(k, shape, coarse_dim, ny):
    c = iota2(shape, coarse_dim)
    l = iota2(shape, 1 - coarse_dim)
    return ((c >> 4) == 2 * k + (l >> 6)) & ((c & 15) == ((l & 31) >> 1)) & ((l & 31) < ny)


def restrict4(src, n, matrix):
    total = None
    for k in range(3):
        t = src[pl.ds(GUARD3 + k, n, stride=8), :] + src[pl.ds(GUARD3 + k + 4, n, stride=8), :]
        part = mm(t, matrix[k])
        total = part if total is None else total + part
    return total


def dot_all(a, b):
    return jnp.sum(jnp.sum(a * b, axis=0, keepdims=True), axis=1, keepdims=True)


def bottom(source, s4, p4, n, ny):
    estimate = jnp.zeros_like(source)
    left = source
    inside = (lanes(n) < 96) & ((lanes(n) & 15) < ny)
    shifted = 6.0 * FACTOR4 + s4[...]
    for it in range(BOTTOM_ITERS):
        p4[pl.ds(GUARD, n), :] = left
        b = p4[pl.ds(GUARD + 1, n), :] + p4[pl.ds(GUARD - 1, n), :]
        b = b + (roll(left, 1) + roll(left, -1))
        b = b + (roll(left, 16) + roll(left, -16))
        image = shifted * left - FACTOR4 * jnp.where(inside, b, 0.0)
        now = dot_all(left, left)
        bent = dot_all(left, image)
        if it == 0:
            denom = bent
            direction, turned = left, image
        else:
            ratio = now * inv_before
            denom = bent - ratio * ratio * denom
            direction = left + ratio * direction
            turned = image + ratio * turned
        step = now / denom
        inv_before = 1.0 / now
        estimate = estimate + step * direction
        if it < BOTTOM_ITERS - 1:
            left = left - step * turned
    return estimate


PLAN_A = Plan([Item(L0, 3), Item(L0, 2), Item(L0, 2)])
PLAN_S = Plan([Item(L1, 6), Item(L2, 5)])
PLAN_B = Plan([Item(L1, 6)])
PLAN_BX = Plan([Item(L1, 6)], True)
PLAN_C = Plan([Item(L0, 3)])
PLAN_D = Plan([Item(L2, 5)])
PLANS = (PLAN_A, PLAN_S, PLAN_B, PLAN_C, PLAN_D, PLAN_BX)


def far(p, sizes):
    ring = lambda d, n: min(d % n, -d % n)
    return p[0] + ring(p[1], sizes[1]) + ring(p[2], 4) + ring(p[2] // 4, 4)


def kernel(sizes, counts, right_in, guess_in, react_in, guess, r0, eb0, left0, step_out, *scratch):
    scratch = list(scratch)

    def take(n):
        out = scratch[:n]
        del scratch[:n]
        return out

    raw = take(3)
    (in_sems,) = take(1)
    right, react, inv0, ea0 = take(4)
    f1, s1, inv1, ea1, eb1, left1 = take(6)
    f2, s2, inv2, ea2, eb2, left2 = take(6)
    f3, s3, inv3, ea3, eb3, left3 = take(6)
    s4, p4, down_m, up_m, tmp, square, turned, spread, slab = take(9)
    chosen, picks, down4, up4 = take(4)
    scr = [take(n) for n in counts]
    place = Place(sizes)
    gx, gy, gz = place.me
    n3, n4, ny3 = 24 * sizes[2], 3 * sizes[2], 6 * sizes[1]

    inputs = (guess_in, right_in, react_in)
    for k in range(3):
        for q in range(4):
            at = pl.ds(12 * q, 12)
            pltpu.make_async_copy(inputs[k].at[at], raw[k].at[at], in_sems.at[k]).start()

    def clear(ref):
        n = ref.shape[0]
        size = next(k for k in (128, 122 * 8, 80, 8) if n % k == 0) if n > 128 else n
        size = {1808: 904, 976: 488, 416: 208}.get(n, size)

        def step(i, carry):
            ref[pl.ds(pl.multiple_of(i * size, 8), size), :] = jnp.zeros((size, 128), F32)
            return carry

        lax.fori_loop(0, n // size, step, 0)

    peers = [(a, b, c) for a in range(sizes[0]) for b in range(sizes[1]) for c in range(sizes[2])][1:]
    peers.sort(key=lambda p: -far(p, sizes))
    beside = {(a, b % sizes[1], c % sizes[2]) for a in range(2) for b in (1, -1) for c in (1, -1)}
    beside |= {(1, 0, c % sizes[2]) for c in (1, -1)}
    greeted = [p for p in peers if p[2] == 0 or p[:2] == (0, 0) or p in beside]
    barrier = pltpu.get_barrier_semaphore()
    for p in greeted:
        pl.semaphore_signal(barrier, inc=1, device_id=place.beside(*p), device_id_type=MESH)
    for ref in (guess, right, react):
        ref[...] = jnp.zeros_like(ref)

    ex_a = Exchange(PLAN_A, (guess, right, react), scr[0], place)
    ex_s = Exchange(PLAN_S, (s1, s2), scr[1], place)
    ex_b = Exchange(PLAN_B, (f1,), scr[2], place)
    ex_c = Exchange(PLAN_C, (eb0,), scr[3], place)
    ex_d = Exchange(PLAN_D, (f2,), scr[4], place)
    cx_b = Cross(PLAN_BX, ex_b, scr[5], place)
    ga_s = Gather(place, scr[6], s3)
    ga_f = Gather(place, scr[7], f3)
    for k, dst in enumerate((guess, right, react)):
        pltpu.make_async_copy(inputs[k], raw[k], in_sems.at[k]).wait()

        for i in range(24):
            dst[pl.ds(L0.row(i, 0), 48), 0:48] = raw[k][i]
            dst[pl.ds(L0.row(i, 0), 48), 64:112] = raw[k][i + 24]
        ex_a.pack_item(k)

    reduced, red_send, red_recv = scr[8]

    pl.semaphore_wait(barrier, len(greeted))
    ex_a.send()

    for ref in (f1, s1, ea1, eb1, f2, s2, ea2, eb2, ea3, eb3, p4, square):
        clear(ref)
    spread[...] = jnp.zeros_like(spread)
    for ref in (f3, s3, inv3):
        for r in (0, GUARD3 + n3):
            ref[pl.ds(r, GUARD3), :] = jnp.zeros((GUARD3, 128), F32)

    a = iota2((128, 128), 0)
    b = iota2((128, 128), 1)
    signed = lambda v: ((v + 8) & 63) - 8
    base = lambda v: ((v + 8) & 127) & 64
    zb = signed(b)
    hit = ((a == ((base(b) + 2 * zb) & 127)) | (a == ((base(b) + 2 * zb + 1) & 127))) & (zb >= -8) & (zb < 24)
    down_m[...] = jnp.where(hit, 0.125, 0.0).astype(BF16)
    hit = a == ((base(b) + (zb >> 1)) & 127)
    up_m[...] = jnp.where(hit, 1.0, 0.0).astype(BF16)


    restrict(react, L0, s1, L1, 0, 12, 0, 24, down_m, tmp)
    restrict(s1, L1, s2, L2, 0, 6, 0, 12, down_m, tmp)
    ex_s.pack()
    for e in (ga_s, ga_f):
        e.mine[...] = jnp.zeros((8, 128), F32)
        e.sum[...] = jnp.zeros((24, 128), F32)
    chosen[...] = spread_to_level3(place)
    to_level3(s2, ga_s.mine, square, turned, chosen)
    for h in range(2):
        r = iota2((112, 384), 0)
        l = iota2((112, 384), 1)
        hit = (6 * gx + 3 * h + (r >> 4) - 2 == (l >> 5)) & (6 * gy + (r & 15) - 2 == (l & 31)) & ((r & 15) < 10)
        picks[h] = jnp.where(hit, 1.0, 0.0).astype(BF16)
    for k in range(3):
        down4[k] = jnp.where(match4(k, (128, 128), 1, ny3), 0.125, 0.0).astype(BF16)
        up4[k] = jnp.where(match4(k, (128, 128), 0, ny3), 1.0, 0.0).astype(BF16)


    def start(r):
        at = pl.ds(r, L0.R)
        c, image = image_of(guess, react, L0, r)
        res = right[at, :] - image
        inv = inverse(react[at, :], 1.0)
        return [(r0, res), (inv0, inv), (ea0, inv * res)]

    ex_a.unpack()
    ex_a.x_send()
    ex_s.send()
    ga_s.send()
    ex_a.unpack_rest()
    planes(L0, 1, 23, start)
    ex_a.x_wait()
    ex_a.x_fill()
    planes(L0, -2, 1, start)
    planes(L0, 23, 26, start)
    relax(L0, ea0, eb0, r0, react, inv0, -1, 25)
    leftover(L0, eb0, left0, r0, react, 0, 24)
    restrict(left0, L0, f1, L1, 0, 12, 0, 24, down_m, tmp)
    ex_b.pack_send()
    cx_b.pack_send()
    ex_b.x_send()

    ex_c.pack()
    ex_s.unpack()
    ex_s.x_send()

    def inverse_of(g, sh, inv, first_plane, end):
        planes(g, first_plane, end, lambda r: [(inv, inverse(sh[pl.ds(r, g.R), :], g.factor))])

    inverse_of(L1, s1, inv1, 0, 12)

    ex_b.x_sent()
    ex_b.unpack()
    ex_c.send()
    first(L1, ea1, f1, inv1, 0, 12)
    relax(L1, ea1, eb1, f1, s1, inv1, 1, 11)
    ex_s.x_wait()
    ex_s.x_fill()
    inverse_of(L1, s1, inv1, -6, 0)
    inverse_of(L1, s1, inv1, 12, 18)
    inverse_of(L2, s2, inv2, -5, 11)
    ex_b.x_wait()
    cx_b.unpack()
    ex_b.x_fill()
    first(L1, ea1, f1, inv1, -6, 0)
    first(L1, ea1, f1, inv1, 12, 18)
    relax(L1, ea1, eb1, f1, s1, inv1, -5, 1)
    relax(L1, ea1, eb1, f1, s1, inv1, 11, 17)
    leftover(L1, eb1, left1, f1, s1, -4, 16)
    restrict(left1, L1, f2, L2, -2, 8, -2, 16, down_m, tmp)
    first(L2, ea2, f2, inv2, -2, 8)
    relax(L2, ea2, eb2, f2, s2, inv2, -1, 7)
    leftover(L2, eb2, left2, f2, s2, 0, 6)
    to_level3(left2, ga_f.mine, square, turned, chosen)
    ga_f.send()
    ex_d.pack_send()
    ga_s.relay()

    ga_f.relay()
    ex_c.unpack()
    ex_c.x_send()
    ex_c.unpack_rest()
    ex_d.unpack()
    ex_d.x_send()
    ex_c.x_wait()
    ex_c.x_fill()
    ex_d.x_wait()
    ex_d.x_fill()
    first(L2, ea2, f2, inv2, -5, 11)
    relax(L2, ea2, eb2, f2, s2, inv2, -4, 10)
    ga_s.finish()
    chunks3(n3, inv3, lambda r, n: inverse(s3[pl.ds(r, n), :], FACTOR3))
    s4[...] = restrict4(s3, n4, down4)
    for e in (ex_a, ex_s, ex_c, ex_d, ga_s):
        e.settle()
    for e in (ex_b, cx_b):
        e.settle(False)
    ga_f.finish()

    def relax3(src, dst):
        def body(r, n):
            c, image = image3(src, s3, r, n)
            at = pl.ds(r, n)
            return c + inv3[at, :] * (f3[at, :] - image)

        chunks3(n3, dst, body)

    chunks3(n3, ea3, lambda r, n: inv3[pl.ds(r, n), :] * f3[pl.ds(r, n), :])
    relax3(ea3, eb3)
    chunks3(n3, left3, lambda r, n: f3[pl.ds(r, n), :] - image3(eb3, s3, r, n)[1])
    e4 = bottom(restrict4(left3, n4, down4), s4, p4, n4, ny3 // 2)
    for k in range(3):
        u = mm(e4, up4[k])
        for q in (k, k + 4):
            at = pl.ds(GUARD3 + q, n4, stride=8)
            eb3[at, :] = eb3[at, :] + u
    for src, dst, n in ((eb3, ea3, 48), (ea3, slab, 40)):
        r = pl.multiple_of(GUARD3 + 24 * gz - (n - 24) // 2, 4)
        c, image = image3(src, s3, r, n)
        at = pl.ds(r, n)
        dst[at if n == 48 else pl.ds(0, n), :] = c + inv3[at, :] * (f3[at, :] - image)
    for k in range(3):
        v = slab[pl.ds(k, 10, stride=4), :]
        for h in range(2):
            for q in range(2):
                spread[k, pl.ds(64 * h + q, 10, stride=2), :] = v
    wide = [jnp.concatenate(p, axis=1) for p in zip(*[split(spread[k]) for k in range(3)])]
    coarse = []
    for h in range(2):
        pick = picks[h]
        parts = [
            lax.dot_general(pick, p, (((1,), (1,)), ((), ())), preferred_element_type=F32) for p in wide
        ]
        coarse.append(parts[0] + parts[1])
    fine = roll(jnp.where(lanes(112) < 64, coarse[0], coarse[1]), -4)
    for i in range(7):
        u = fine[16 * i : 16 * i + 10]
        tmp[pl.ds(24 * i, 10, stride=2), :] = u
        tmp[pl.ds(24 * i + 1, 10, stride=2), :] = u
    for i in range(7):
        v = tmp[pl.ds(24 * i, 20), :]
        for q in range(2):
            at = pl.ds(L2.row(2 * (i - 2) + q, -4), 20)
            eb2[at, :] = eb2[at, :] + v
    relax(L2, eb2, ea2, f2, s2, inv2, -3, 9)
    relax(L2, ea2, eb2, f2, s2, inv2, -2, 8)
    prolong(eb2, L2, eb1, L1, -2, 8, -2, 16, up_m, tmp)
    relax(L1, eb1, ea1, f1, s1, inv1, -3, 15)
    relax(L1, ea1, eb1, f1, s1, inv1, -2, 14)
    prolong(eb1, L1, eb0, L0, -2, 14, -2, 28, up_m, tmp)
    relax(L0, eb0, ea0, r0, react, inv0, -2, 26)
    relax(L0, ea0, eb0, r0, react, inv0, -1, 25)

    row = iota2((L0.R, 128), 0)
    inside = ((lanes(L0.R) & 63) < 48) & (row >= L0.y0) & (row < L0.y0 + 48)

    upper, lower = [], []
    for i in range(24):
        r = GUARD + (L0.halo + i) * L0.R
        c, image = image_of(eb0, react, L0, r)
        left0[pl.ds(r, L0.R), :] = image
        upper.append(c * r0[pl.ds(r, L0.R), :])
        lower.append(c * image)
    upper = jnp.where(inside, tree(upper), 0.0)
    lower = jnp.where(inside, tree(lower), 0.0)
    upper = jnp.sum(upper, axis=0, keepdims=True)
    lower = jnp.sum(lower, axis=0, keepdims=True)
    half = lanes(1) < 64
    number = (gx * sizes[1] + gy) * sizes[2] + gz
    reduced[number] = jnp.where(half, upper + roll(upper, 64), lower + roll(lower, 64))
    own = reduced.at[number]

    def summed(src, dst, p):
        return pltpu.make_async_remote_copy(
            src_ref=src, dst_ref=dst, send_sem=red_send.at[0], recv_sem=red_recv.at[0],
            device_id=place.beside(*p), device_id_type=MESH,
        )

    for p in peers:
        summed(own, own, p).start()
    ga_f.settle()
    most = reduced.at[pl.ds(0, len(peers))]
    summed(most, most, peers[0]).wait()
    sums = [reduced[k] for k in range(8)]
    for k in range(8, len(peers) + 1):
        sums[k % 8] = sums[k % 8] + reduced[k]
    total = tree(sums)
    upper = jnp.sum(jnp.where(half, total, 0.0), axis=1, keepdims=True)
    lower = jnp.sum(jnp.where(half, 0.0, total), axis=1, keepdims=True)
    step_out[...] = jnp.broadcast_to(upper / lower, (8, 128))


def finish(guess, r0, eb0, left0, step_ref, field_out, resid_out, field, resid, sems):
    step = step_ref[0:1, :]
    copies = []
    parts, size = 4, 6
    for p in range(parts):
        for x in range(p * size, p * size + size):
            at = pl.ds(L0.row(x, 0), 48)
            v = guess[at, :] + step * eb0[at, :]
            field[x] = v[:, 0:48]
            field[x + 24] = roll(v, 64)[:, 0:48]
            v = r0[at, :] - step * left0[at, :]
            resid[x] = v[:, 0:48]
            resid[x + 24] = roll(v, 64)[:, 0:48]
        for q, (src, dst) in enumerate(((field, field_out), (resid, resid_out))):
            for h in range(2):
                at = pl.ds(p * size + 24 * h, size)
                c = pltpu.make_async_copy(src.at[at], dst.at[at], sems.at[4 * p + 2 * q + h])
                c.start()
                copies.append(c)
    for c in copies:
        c.wait()


def solution(mesh):
    sizes = tuple(mesh.shape[a] for a in ("gx", "gy", "gz"))
    n3, n4 = 24 * sizes[2] + 2 * GUARD3, 3 * sizes[2]
    scratch = [pltpu.VMEM((48, 48, 48), F32)] * 3 + [pltpu.SemaphoreType.DMA((3,))]
    scratch += [pltpu.VMEM((L0.total, 128), F32)] * 4
    scratch += [pltpu.VMEM((L1.total, 128), F32)] * 6
    scratch += [pltpu.VMEM((L2.total, 128), F32)] * 6
    scratch += [pltpu.VMEM((n3, 128), F32)] * 6
    scratch += [pltpu.VMEM((n4, 128), F32), pltpu.VMEM((n4 + 2 * GUARD, 128), F32)]
    scratch += [pltpu.VMEM((128, 128), BF16)] * 2 + [pltpu.VMEM((16 * 56, 128), F32)]
    scratch += [pltpu.VMEM((128, 128), F32)] * 2
    scratch += [pltpu.VMEM((3, 128, 128), F32), pltpu.VMEM((40, 128), F32)]
    scratch += [pltpu.VMEM((128, 256), BF16), pltpu.VMEM((2, 112, 384), BF16)]
    scratch += [pltpu.VMEM((3, 128, 128), BF16)] * 2
    groups = [p.scratch() for p in PLANS] + [gather_scratch(sizes)] * 2
    devices = sizes[0] * sizes[1] * sizes[2]
    groups += [[pltpu.VMEM((devices, 1, 128), F32)] + [pltpu.SemaphoreType.DMA((1,))] * 2]
    for g in groups:
        scratch += g
    counts = tuple(len(g) for g in groups)
    vmem = pl.BlockSpec(memory_space=pltpu.VMEM)

    anywhere = pl.BlockSpec(memory_space=pl.ANY)

    def body(right_side, start_guess, reaction):
        whole = pltpu.VMEM((L0.total, 128), F32)
        parts = pl.pallas_call(
            functools.partial(kernel, sizes, counts),
            out_shape=[whole] * 4 + [pltpu.VMEM((8, 128), F32)],
            in_specs=[anywhere] * 3,
            out_specs=[vmem] * 5,
            scratch_shapes=scratch,
            compiler_params=pltpu.CompilerParams(
                collective_id=0, has_side_effects=True, vmem_limit_bytes=60 * 2**20
            ),
        )(right_side, start_guess, reaction)
        shape = jax.ShapeDtypeStruct(right_side.shape, F32)
        return tuple(
            pl.pallas_call(
                finish,
                out_shape=[shape, shape],
                in_specs=[vmem] * 5,
                out_specs=[anywhere] * 2,
                scratch_shapes=[pltpu.VMEM(right_side.shape, F32)] * 2 + [pltpu.SemaphoreType.DMA((16,))],
                compiler_params=pltpu.CompilerParams(vmem_limit_bytes=16 * 2**20),
            )(*parts)
        )

    placed = P("gx", "gy", "gz")
    return jax.shard_map(
        body, mesh=mesh, in_specs=(placed,) * 3, out_specs=(placed,) * 2, check_vma=False
    )
```

```python
import functools

import jax
import jax.numpy as jnp
from jax import lax
from jax.experimental import pallas as pl
from jax.experimental.pallas import tpu as pltpu
from jax.sharding import PartitionSpec as P

MESH = pl.DeviceIdType.MESH
F32 = jnp.float32
BF16 = jnp.bfloat16
DAMP = 6.0 / 7.0
GUARD = 8
GUARD3 = 16
BOTTOM_ITERS = 6


class Geo:
    def __init__(self, nx, ny, nz, halo, rows, y0, depth, unroll):
        self.nx, self.ny, self.nz, self.halo, self.R, self.y0 = nx, ny, nz, halo, rows, y0
        self.factor = 0.25**depth
        self.unroll = unroll
        self.total = 2 * GUARD + (nx + 2 * halo) * rows

    def row(self, x, y):
        return GUARD + (self.halo + x) * self.R + self.y0 + y


L0 = Geo(24, 48, 48, 4, 56, 4, 0, 28)
L1 = Geo(12, 24, 24, 6, 40, 8, 1, 24)
L2 = Geo(6, 12, 12, 5, 24, 6, 2, 16)
FACTOR3 = 0.25**3
FACTOR4 = 0.25**4


def lanes(rows):
    return lax.broadcasted_iota(jnp.int32, (rows, 128), 1)


def iota2(shape, dim):
    return lax.broadcasted_iota(jnp.int32, shape, dim)


def tree(terms):
    while len(terms) > 1:
        terms = [sum(terms[k + 1 : k + 2], terms[k]) for k in range(0, len(terms), 2)]
    return terms[0]


def roll(v, shift):
    shift = shift % 128
    return v if shift == 0 else pltpu.roll(v, shift, 1)


def split(a):
    hi = a.astype(BF16)
    return hi, (a - hi.astype(F32)).astype(BF16)


def mm(a, b):
    hi, low = split(a)
    return jnp.dot(hi, b, preferred_element_type=F32) + jnp.dot(low, b, preferred_element_type=F32)


def beside_of(ref, r, R):
    c = ref[pl.ds(r, R), :]
    b = ref[pl.ds(r + R, R), :] + ref[pl.ds(r - R, R), :]
    b = b + (ref[pl.ds(r + 1, R), :] + ref[pl.ds(r - 1, R), :])
    b = b + (roll(c, 1) + roll(c, -1))
    return c, b


def image_of(ref, s_ref, g, r):
    c, b = beside_of(ref, r, g.R)
    return c, g.factor * (6.0 * c - b) + s_ref[pl.ds(r, g.R), :] * c


def planes(g, a, b, body):
    unroll = g.unroll

    def group(start, count):
        todo = []
        for k in range(count):
            r = start + k * g.R
            r = r if isinstance(r, int) else pl.multiple_of(r, 8)
            todo.append((r, body(r)))
        for r, pairs in todo:
            for ref, value in pairs:
                ref[pl.ds(r, g.R), :] = value

    trips = (b - a) // unroll
    origin = GUARD + (g.halo + a) * g.R
    if trips == 1:
        group(origin, unroll)
    elif trips:

        def step(i, carry):
            group(pl.multiple_of(origin + i * (unroll * g.R), 8), unroll)
            return carry

        lax.fori_loop(0, trips, step, 0)
    if (b - a) % unroll:
        group(origin + trips * unroll * g.R, (b - a) % unroll)


def inverse(s, factor):
    return jnp.where(s > 0.0, DAMP / (6.0 * factor + s), 0.0)


def relax(g, src, dst, f, s, inv, a, b):
    def body(r):
        c, image = image_of(src, s, g, r)
        at = pl.ds(r, g.R)
        return [(dst, c + inv[at, :] * (f[at, :] - image))]

    planes(g, a, b, body)


def first(g, dst, f, inv, a, b):
    def body(r):
        at = pl.ds(r, g.R)
        return [(dst, inv[at, :] * f[at, :])]

    planes(g, a, b, body)


def leftover(g, src, dst, f, s, a, b):
    def body(r):
        c, image = image_of(src, s, g, r)
        return [(dst, f[pl.ds(r, g.R), :] - image)]

    planes(g, a, b, body)


def restrict(src, gs, dst, gd, x0, x1, y0, count, matrix, tmp):
    step = -(-count // 8) * 8
    for x in range(x0, x1):
        r = gs.row(2 * x, 2 * y0)
        t = src[pl.ds(r, count, stride=2), :] + src[pl.ds(r + 1, count, stride=2), :]
        r = r + gs.R
        t = t + (src[pl.ds(r, count, stride=2), :] + src[pl.ds(r + 1, count, stride=2), :])
        tmp[pl.ds((x - x0) * step, count), :] = t
    for x in range(x0, x1):
        out = mm(tmp[pl.ds((x - x0) * step, step), :], matrix[...])
        dst[pl.ds(gd.row(x, y0), count), :] = out[0:count]


def prolong(src, gc, dst, gf, x0, x1, y0, count, matrix, tmp):
    for x in range(x0, x1):
        o = (x - x0) * 56
        u = mm(src[pl.ds(gc.row(x, y0), count), :], matrix[...])
        tmp[pl.ds(o, count, stride=2), :] = u
        tmp[pl.ds(o + 1, count, stride=2), :] = u
    for x in range(x0, x1):
        o = (x - x0) * 56
        v = tmp[pl.ds(o, 2 * count), :]
        for k in range(2):
            at = pl.ds(gf.row(2 * x + k, 2 * y0), 2 * count)
            dst[at, :] = dst[at, :] + v


class Item:
    def __init__(self, geo, w):
        self.g, self.w = geo, w


class Plan:
    def __init__(self, items, cross=False):
        self.items, self.cross = items, cross
        self.counts = [it.w if cross else it.g.nx for it in items]
        self.yrows = sum(n * it.w for n, it in zip(self.counts, items))
        self.yrows = -(-self.yrows // 8) * 8
        self.tiles = []
        for k, it in enumerate(items):
            for x in range(self.counts[k]):
                for t in self.tiles:
                    if t[0] is it.g and t[1] + it.w <= 64:
                        break
                else:
                    t = [it.g, 0, []]
                    self.tiles.append(t)
                t[2].append((k, x, t[1]))
                t[1] += it.w
        self.zrows = sum(t[0].ny for t in self.tiles)
        self.zrows = -(-self.zrows // 8) * 8
        self.drows = max(self.counts)
        self.drows = -(-self.drows // 8) * 8
        assert sum(it.w * it.w for it in items) <= 64

        self.z0 = [0, self.zrows]
        self.d0 = [2 * self.zrows + q * self.drows for q in range(4)]
        self.y0 = [2 * self.zrows + 4 * self.drows + q * self.yrows for q in range(2)]
        self.total = 2 * (self.zrows + self.yrows) + 4 * self.drows
        self.xtotal = sum(it.w * it.g.R for it in items)

    def scratch(self):
        x = [] if self.cross else [pltpu.VMEM((self.xtotal, 128), F32)]
        return x + [
            pltpu.VMEM((self.total, 128), F32),
            pltpu.VMEM((self.total, 128), F32),
            pltpu.SemaphoreType.DMA((2,)),
            pltpu.SemaphoreType.DMA((2,)),
        ]


class Exchange:
    def __init__(self, plan, refs, scratch, place):
        self.plan, self.refs, self.place = plan, refs, place
        self.xr, self.sent, self.got, self.ss, self.rs = scratch
        gx, gy, gz = place.me
        self.partner = (1 - gx, gy, gz)
        self.x_copies = []
        o = 0
        for k, it in enumerate(plan.items):
            r = pl.multiple_of(GUARD + (it.g.halo + self.edge(it)) * it.g.R, 8)
            n = it.w * it.g.R
            self.x_copies.append(self.copy(refs[k].at[pl.ds(r, n), :], self.xr.at[pl.ds(o, n), :], 0, self.partner))
            o += n
        self.segments(0)

    def edge(self, it):
        return jnp.where(self.place.me[0] == 0, it.g.nx - it.w, 0)

    def source(self, k, x, y):
        return self.plan.items[k].g.row(x, y)

    def target(self, k, x, y):
        return self.refs[k], self.plan.items[k].g.row(x, y)

    def segments(self, dx):
        plan = self.plan
        at = {}
        for d in range(2):
            at[1 - 2 * d, 0] = plan.y0[d]
            at[0, 1 - 2 * d] = plan.z0[d]
            for e in range(2):
                at[1 - 2 * d, 1 - 2 * e] = plan.d0[2 * d + e]
        self.y_copies, self.z_copies, self.d_copies = [], [], []
        for d in (1, -1):
            self.y_copies.append(self.segment(at, dx, d, 0, plan.yrows))
            self.z_copies.append(self.segment(at, dx, 0, d, plan.zrows))
            for e in (1, -1):
                self.d_copies.append(self.segment(at, dx, d, e, plan.drows))

    def segment(self, at, dx, dy, dz, n):
        there = self.place.exists(dy, dz)
        peer = self.place.beside(dx, dy, dz)
        peer = tuple(jnp.where(there, p, q) for p, q in zip(peer, self.partner))
        target = pl.multiple_of(jnp.where(there, at[dy, dz], at[-dy, -dz]), 8)
        return self.copy(self.sent.at[pl.ds(at[dy, dz], n), :], self.got.at[pl.ds(target, n), :], 1, peer)

    def copy(self, src, dst, k, peer):
        return pltpu.make_async_remote_copy(
            src_ref=src, dst_ref=dst, send_sem=self.ss.at[k], recv_sem=self.rs.at[k],
            device_id=peer, device_id_type=MESH,
        )

    def x_send(self):
        for c in self.x_copies:
            c.start()

    def settle(self, x=True):
        if x:
            self.x_sent()
        self.copy(self.sent, self.got, 1, self.partner).wait_send()

    def x_sent(self):
        self.copy(self.xr, self.xr, 0, self.partner).wait_send()

    def x_wait(self):
        self.copy(self.xr, self.xr, 0, self.partner).wait_recv()

    def x_fill(self):
        m0, m1 = self.place.x_masks
        o = 0
        for k, it in enumerate(self.plan.items):
            g, w, ref = it.g, it.w, self.refs[k]
            upper = ((lanes(g.R) + 8) & 127) >= 64
            for j in range(w):
                got = self.xr[pl.ds(o + j * g.R, g.R), :]
                top = ref[pl.ds(GUARD + (g.halo + g.nx - w + j) * g.R, g.R), :]
                low = ref[pl.ds(GUARD + (g.halo + j) * g.R, g.R), :]
                ref[pl.ds(GUARD + (g.halo - w + j) * g.R, g.R), :] = roll(jnp.where(upper, got * m1, top), 64)
                ref[pl.ds(GUARD + (g.halo + g.nx + j) * g.R, g.R), :] = roll(jnp.where(upper, low, got * m0), 64)
            o += w * g.R

    def pack_send(self):
        self.pack()
        self.send()

    def pack(self):
        for k in range(len(self.refs)):
            self.pack_item(k)

    def send(self):
        for c in self.d_copies + self.z_copies + self.y_copies:
            c.start()

    def pack_item(self, k):
        if k == 0:
            self.yo, self.co, self.corner = 0, 0, [None] * 4
        it = self.plan.items[k]
        g, w, ref = it.g, it.w, self.refs[k]
        n = self.plan.counts[k]
        lane = lanes(self.plan.drows) & 63
        for d in range(1, w + 1):
            at = self.co + (d - 1) * w
            for e, y in enumerate((g.ny - d, d - 1)):
                v = ref[pl.ds(self.source(k, 0, y), n, stride=g.R), :]
                self.sent[pl.ds(self.plan.y0[e] + self.yo, n), :] = v
                if n < self.plan.drows:
                    v = jnp.concatenate([v, jnp.zeros((self.plan.drows - n, 128), F32)], axis=0)
                for q, z in enumerate((g.nz - w, 0)):
                    moved = roll(v, at - z)
                    old = self.corner[2 * e + q]
                    self.corner[2 * e + q] = moved if old is None else jnp.where(lane >= at, moved, old)
            self.yo += n
        self.co += w * w
        if k == len(self.refs) - 1:
            for q in range(4):
                self.sent[pl.ds(self.plan.d0[q], self.plan.drows), :] = self.corner[q]
        zo = 0
        for t, _, slots in self.plan.tiles:
            if slots[-1][0] == k:
                self.pack_tile(t, slots, zo)
            zo += t.ny

    def pack_tile(self, g, slots, zo):
        lane = lanes(g.ny)
        acc = [None, None]
        for k, x, at in slots:
            w = self.plan.items[k].w
            moved = roll(self.refs[k][pl.ds(self.source(k, x, 0), g.ny), :], at)
            for q, past in enumerate((g.nz - w, 0)):
                here = ((lane - past) & 63 >= at) & ((lane - past) & 63 < at + w)
                acc[q] = moved if acc[q] is None else jnp.where(here, moved, acc[q])
        for q in range(2):
            self.sent[pl.ds(self.plan.z0[q] + zo, g.ny), :] = acc[q]

    def unpack(self):
        my, mz = self.place.y_masks, self.place.z_masks
        self.copy(self.sent, self.got, 1, self.partner).wait_recv()
        yo, co = 0, 0
        for k, it in enumerate(self.plan.items):
            g, w = it.g, it.w
            n = self.plan.counts[k]
            lane = lanes(n) & 63
            into = (lane >= 64 - w, (lane >= g.nz) & (lane < g.nz + w))
            for d in range(1, w + 1):
                at = co + (d - 1) * w
                for e, y in enumerate((-d, g.ny + d - 1)):
                    v = self.got[pl.ds(self.plan.y0[e] + yo, n), :]
                    for q, z in enumerate((-w, g.nz)):
                        got = self.got[pl.ds(self.plan.d0[2 * e + q], n), :] * mz[q]
                        v = jnp.where(into[q], roll(got, z - at), v)
                    ref, r = self.target(k, 0, y)
                    ref[pl.ds(r, n, stride=g.R), :] = v * my[e]
                yo += n
            co += w * w
        self.unpack_z(True)

    def unpack_rest(self):
        self.unpack_z(False)

    def unpack_z(self, edge):
        mz = self.place.z_masks
        zo = 0
        for g, _, slots in self.plan.tiles:
            lane = lanes(g.ny) & 63
            got = [self.got[pl.ds(self.plan.z0[q] + zo, g.ny), :] * mz[q] for q in range(2)]
            for k, x, at in slots:
                w = self.plan.items[k].w
                if (x < w or x >= g.nx - w) != edge:
                    continue
                ref, r = self.target(k, x, 0)
                rows = pl.ds(r, g.ny)
                v = ref[rows, :]
                v = jnp.where(lane >= 64 - w, roll(got[0], -g.nz - at), v)
                v = jnp.where((lane >= g.nz) & (lane < g.nz + w), roll(got[1], g.nz - at), v)
                ref[rows, :] = v
            zo += g.ny


class Cross(Exchange):
    def __init__(self, plan, main, scratch, place):
        self.plan, self.main, self.refs, self.place = plan, main, main.refs, place
        self.sent, self.got, self.ss, self.rs = scratch
        self.partner = main.partner
        self.segments(1)

    def source(self, k, x, y):
        it = self.plan.items[k]
        return GUARD + (it.g.halo + self.edge(it) + x) * it.g.R + it.g.y0 + y

    def target(self, k, x, y):
        o = sum(it.w * it.g.R for it in self.plan.items[:k])
        g = self.plan.items[k].g
        return self.main.xr, o + x * g.R + g.y0 + y


class Place:
    def __init__(self, sizes):
        self.sizes = sizes
        self.me = tuple(lax.axis_index(a) for a in ("gx", "gy", "gz"))
        gx, gy, gz = self.me
        one = lambda c: jnp.where(c, 1.0, 0.0).astype(F32)
        self.x_masks = (one(gx == 0), one(gx == 1))
        self.y_masks = (one(gy > 0), one(gy < sizes[1] - 1))
        self.z_masks = (one(gz > 0), one(gz < sizes[2] - 1))

    def exists(self, dy, dz):
        gx, gy, gz = self.me
        y, z = gy + dy, gz + dz
        return (y >= 0) & (y < self.sizes[1]) & (z >= 0) & (z < self.sizes[2])

    def beside(self, dx, dy, dz):
        return tuple(
            lax.rem(m + d % n, n) if d % n else m for m, d, n in zip(self.me, (dx, dy, dz), self.sizes)
        )


class Gather:
    rows = 24

    def __init__(self, place, scratch, whole):
        self.place, self.whole = place, whole
        self.mine, self.got, self.sum, self.parts, self.ss, self.rs = scratch
        n = place.sizes
        self.near = [(a, b) for a in range(n[0]) for b in range(n[1])][1:]
        self.near.sort(key=lambda p: -far((p[0], p[1], 0), n))
        self.line = sorted(range(1, n[2]), key=lambda c: -far((0, 0, c), n))
        self.at = pl.ds(pl.multiple_of(GUARD3 + self.rows * place.me[2], 8), self.rows)

    def copy(self, src, dst, k, peer):
        return pltpu.make_async_remote_copy(
            src_ref=src, dst_ref=dst, send_sem=self.ss.at[k], recv_sem=self.rs.at[k],
            device_id=peer, device_id_type=MESH,
        )

    def send(self):
        for k, (a, b) in enumerate(self.near):
            self.copy(self.mine, self.got.at[k], 0, self.place.beside(a, b, 0)).start()

    def relay(self):
        self.copy(self.got, self.got, 0, self.place.beside(1, 0, 0)).wait_recv()
        gx, gy, gz = self.place.me
        ny = self.place.sizes[1]
        lane = lanes(8)
        sums = [[], []], [[], []]
        for k, (a, b) in enumerate([(0, 0)] + self.near):
            tile = self.mine[...] if k == 0 else self.got[k - 1]
            start = 6 * lax.rem(gy + ny - b, ny)
            for h in range(2):
                y = (lane - 16 * h) & 31
                sums[a][h].append(jnp.where((y >= start) & (y < start + 6), tile, 0.0))
        for h in range(2):
            own, other = (roll(tree(sums[a][h]), -16 * h) for a in range(2))
            self.parts[pl.ds(16 * h, 8), :] = jnp.where(gx == 0, own, other)
            self.parts[pl.ds(16 * h + 8, 8), :] = jnp.where(gx == 0, other, own)
        for h in range(2):
            r = 16 * h
            self.sum[pl.ds(12 * h, 3, stride=4), :] = self.parts[pl.ds(r, 3), :]
            self.sum[pl.ds(12 * h + 1, 3, stride=4), :] = self.parts[pl.ds(r + 4, 3), :] + self.parts[pl.ds(r + 8, 3), :]
            self.sum[pl.ds(12 * h + 2, 3, stride=4), :] = self.parts[pl.ds(r + 12, 3), :]
        for c in self.line:
            self.copy(self.sum, self.whole.at[self.at, :], 1, self.place.beside(0, 0, c)).start()
        self.whole[self.at, :] = self.sum[...]

    def finish(self):
        self.most().wait_recv()

    def most(self):
        most = self.whole.at[pl.ds(GUARD3, self.rows * (self.place.sizes[2] - 1)), :]
        return self.copy(most, most, 1, self.place.beside(1, 0, 0))

    def settle(self):
        self.copy(self.got, self.got, 0, self.place.beside(1, 0, 0)).wait_send()
        self.most().wait_send()


def gather_scratch(sizes):
    return [
        pltpu.VMEM((8, 128), F32),
        pltpu.VMEM((sizes[0] * sizes[1] - 1, 8, 128), F32),
        pltpu.VMEM((24, 128), F32),
        pltpu.VMEM((32, 128), F32),
        pltpu.SemaphoreType.DMA((2,)),
        pltpu.SemaphoreType.DMA((2,)),
    ]


def spread_to_level3(place):
    gx, gy, gz = place.me
    r = iota2((128, 256), 0)
    l = iota2((128, 256), 1)
    x = 6 * gx + 3 * (r >> 6) + ((r & 63) >> 3)
    y = 6 * gy + (r & 7)
    hit = (x == (l >> 5) + 4 * gx) & (y == (l & 31)) & ((r & 7) < 6) & ((r & 63) < 24)
    return jnp.where(hit, 1.0, 0.0).astype(BF16)


def to_level3(src, mine, square, turned, chosen):
    g = L2
    for i in range(3):
        r = g.row(2 * i, 0)
        t = src[pl.ds(r, 6, stride=2), :] + src[pl.ds(r + 1, 6, stride=2), :]
        r = r + g.R
        t = t + (src[pl.ds(r, 6, stride=2), :] + src[pl.ds(r + 1, 6, stride=2), :])
        square[pl.ds(8 * i, 6), :] = t
    turned[...] = jnp.transpose(square[...])
    a = turned[pl.ds(0, 8, stride=2), :] + turned[pl.ds(1, 8, stride=2), :]
    b = turned[pl.ds(64, 8, stride=2), :] + turned[pl.ds(65, 8, stride=2), :]
    a = (a + roll(b, 64)) * 0.125
    out = mm(a, chosen[...])
    for k in range(2):
        turned[pl.ds(8 * k, 8), :] = out[:, 128 * k : 128 * k + 128]
    for k in range(2):
        mine[pl.ds(4 * k, 3), :] = turned[pl.ds(8 * k, 3), :] + roll(turned[pl.ds(8 * k + 3, 3), :], 16)


def image3(ref, s_ref, r, n):
    lane = lanes(n)
    c = ref[pl.ds(r, n), :]
    b = ref[pl.ds(r + 4, n), :] + ref[pl.ds(r - 4, n), :]
    b = b + (roll(c, 1) + roll(c, -1))
    b = b + roll(jnp.where(lane < 32, ref[pl.ds(r + 1, n), :], c), -32)
    b = b + roll(jnp.where(lane >= 96, ref[pl.ds(r - 1, n), :], c), 32)
    return c, FACTOR3 * (6.0 * c - b) + s_ref[pl.ds(r, n), :] * c


def chunks3(rows, ref, body):
    n = min(rows, 384)

    def step(i, carry):
        r = pl.multiple_of(GUARD3 + i * n, 8)
        ref[pl.ds(r, n), :] = body(r, n)
        return carry

    lax.fori_loop(0, rows // n, step, 0)


def match4(k, shape, coarse_dim, ny):
    c = iota2(shape, coarse_dim)
    l = iota2(shape, 1 - coarse_dim)
    return ((c >> 4) == 2 * k + (l >> 6)) & ((c & 15) == ((l & 31) >> 1)) & ((l & 31) < ny)


def restrict4(src, n, matrix):
    total = None
    for k in range(3):
        t = src[pl.ds(GUARD3 + k, n, stride=8), :] + src[pl.ds(GUARD3 + k + 4, n, stride=8), :]
        part = mm(t, matrix[k])
        total = part if total is None else total + part
    return total


def both_sums(a, b):
    fold = lambda v: tree([v[k : k + 8] for k in range(0, v.shape[0], 8)])
    rest = jnp.concatenate([fold(a), fold(b)], axis=0)
    ones = jnp.ones((128, 128), BF16)
    parts = []
    for _ in range(3):
        part = rest.astype(BF16)
        rest = rest - part.astype(F32)
        parts.append(jnp.dot(part, ones, preferred_element_type=F32))
    total = parts[0] + (parts[1] + parts[2])
    return jnp.sum(total[0:8], axis=0, keepdims=True), jnp.sum(total[8:16], axis=0, keepdims=True)


def bottom(source, s4, p4, n, ny):
    estimate = jnp.zeros_like(source)
    left = source
    inside = (lanes(n) < 96) & ((lanes(n) & 15) < ny)
    shifted = 6.0 * FACTOR4 + s4[...]
    for it in range(BOTTOM_ITERS):
        p4[pl.ds(GUARD, n), :] = left
        b = p4[pl.ds(GUARD + 1, n), :] + p4[pl.ds(GUARD - 1, n), :]
        b = b + (roll(left, 1) + roll(left, -1))
        b = b + (roll(left, 16) + roll(left, -16))
        image = shifted * left - FACTOR4 * jnp.where(inside, b, 0.0)
        now, bent = both_sums(left * left, left * image)
        if it == 0:
            denom = bent
            direction, turned = left, image
        else:
            ratio = now * inv_before
            denom = bent - ratio * ratio * denom
            direction = left + ratio * direction
            turned = image + ratio * turned
        step = now / denom
        inv_before = 1.0 / now
        estimate = estimate + step * direction
        if it < BOTTOM_ITERS - 1:
            left = left - step * turned
    return estimate


PLAN_A = Plan([Item(L0, 3), Item(L0, 2), Item(L0, 2)])
PLAN_S = Plan([Item(L1, 6), Item(L2, 5)])
PLAN_B = Plan([Item(L1, 6)])
PLAN_BX = Plan([Item(L1, 6)], True)
PLAN_C = Plan([Item(L0, 3)])
PLAN_D = Plan([Item(L2, 5)])
PLANS = (PLAN_A, PLAN_S, PLAN_B, PLAN_C, PLAN_D, PLAN_BX)


def far(p, sizes):
    ring = lambda d, n: min(d % n, -d % n)
    return p[0] + ring(p[1], sizes[1]) + ring(p[2], 4) + ring(p[2] // 4, 4)


def kernel(sizes, counts, right_in, guess_in, react_in, guess, r0, eb0, left0, step_out, *scratch):
    scratch = list(scratch)

    def take(n):
        out = scratch[:n]
        del scratch[:n]
        return out

    raw = take(3)
    (in_sems,) = take(1)
    right, react, inv0, ea0 = take(4)
    f1, s1, inv1, ea1, eb1, left1 = take(6)
    f2, s2, inv2, ea2, eb2, left2 = take(6)
    f3, s3, inv3, ea3, eb3, left3 = take(6)
    s4, p4, down_m, up_m, tmp, square, turned, spread, slab = take(9)
    chosen, picks, down4, up4 = take(4)
    scr = [take(n) for n in counts]
    place = Place(sizes)
    gx, gy, gz = place.me
    n3, n4, ny3 = 24 * sizes[2], 3 * sizes[2], 6 * sizes[1]

    inputs = (guess_in, right_in, react_in)
    for k in range(3):
        for q in range(4):
            at = pl.ds(12 * q, 12)
            pltpu.make_async_copy(inputs[k].at[at], raw[k].at[at], in_sems.at[k]).start()

    def clear(ref):
        n = ref.shape[0]
        size = next(k for k in (128, 122 * 8, 80, 8) if n % k == 0) if n > 128 else n
        size = {1808: 904, 976: 488, 416: 208}.get(n, size)

        def step(i, carry):
            ref[pl.ds(pl.multiple_of(i * size, 8), size), :] = jnp.zeros((size, 128), F32)
            return carry

        lax.fori_loop(0, n // size, step, 0)

    peers = [(a, b, c) for a in range(sizes[0]) for b in range(sizes[1]) for c in range(sizes[2])][1:]
    peers.sort(key=lambda p: -far(p, sizes))
    beside = {(a, b % sizes[1], c % sizes[2]) for a in range(2) for b in (1, -1) for c in (1, -1)}
    beside |= {(1, 0, c % sizes[2]) for c in (1, -1)}
    greeted = [p for p in peers if p[2] == 0 or p[:2] == (0, 0) or p in beside]
    barrier = pltpu.get_barrier_semaphore()
    for p in greeted:
        pl.semaphore_signal(barrier, inc=1, device_id=place.beside(*p), device_id_type=MESH)
    for ref in (guess, right, react):
        ref[...] = jnp.zeros_like(ref)

    ex_a = Exchange(PLAN_A, (guess, right, react), scr[0], place)
    ex_s = Exchange(PLAN_S, (s1, s2), scr[1], place)
    ex_b = Exchange(PLAN_B, (f1,), scr[2], place)
    ex_c = Exchange(PLAN_C, (eb0,), scr[3], place)
    ex_d = Exchange(PLAN_D, (f2,), scr[4], place)
    cx_b = Cross(PLAN_BX, ex_b, scr[5], place)
    ga_s = Gather(place, scr[6], s3)
    ga_f = Gather(place, scr[7], f3)
    for k, dst in enumerate((guess, right, react)):
        pltpu.make_async_copy(inputs[k], raw[k], in_sems.at[k]).wait()

        for i in range(24):
            dst[pl.ds(L0.row(i, 0), 48), 0:48] = raw[k][i]
            dst[pl.ds(L0.row(i, 0), 48), 64:112] = raw[k][i + 24]
        ex_a.pack_item(k)

    reduced, red_send, red_recv = scr[8]

    pl.semaphore_wait(barrier, len(greeted))
    ex_a.send()

    for ref in (f1, s1, ea1, eb1, f2, s2, ea2, eb2, ea3, eb3, p4, square):
        clear(ref)
    spread[...] = jnp.zeros_like(spread)
    for ref in (f3, s3, inv3):
        for r in (0, GUARD3 + n3):
            ref[pl.ds(r, GUARD3), :] = jnp.zeros((GUARD3, 128), F32)

    a = iota2((128, 128), 0)
    b = iota2((128, 128), 1)
    signed = lambda v: ((v + 8) & 63) - 8
    base = lambda v: ((v + 8) & 127) & 64
    zb = signed(b)
    hit = ((a == ((base(b) + 2 * zb) & 127)) | (a == ((base(b) + 2 * zb + 1) & 127))) & (zb >= -8) & (zb < 24)
    down_m[...] = jnp.where(hit, 0.125, 0.0).astype(BF16)
    hit = a == ((base(b) + (zb >> 1)) & 127)
    up_m[...] = jnp.where(hit, 1.0, 0.0).astype(BF16)


    restrict(react, L0, s1, L1, 0, 12, 0, 24, down_m, tmp)
    restrict(s1, L1, s2, L2, 0, 6, 0, 12, down_m, tmp)
    ex_s.pack()
    for e in (ga_s, ga_f):
        e.mine[...] = jnp.zeros((8, 128), F32)
        e.sum[...] = jnp.zeros((24, 128), F32)
    chosen[...] = spread_to_level3(place)
    to_level3(s2, ga_s.mine, square, turned, chosen)
    for h in range(2):
        r = iota2((112, 384), 0)
        l = iota2((112, 384), 1)
        hit = (6 * gx + 3 * h + (r >> 4) - 2 == (l >> 5)) & (6 * gy + (r & 15) - 2 == (l & 31)) & ((r & 15) < 10)
        picks[h] = jnp.where(hit, 1.0, 0.0).astype(BF16)
    for k in range(3):
        down4[k] = jnp.where(match4(k, (128, 128), 1, ny3), 0.125, 0.0).astype(BF16)
        up4[k] = jnp.where(match4(k, (128, 128), 0, ny3), 1.0, 0.0).astype(BF16)


    def start(r):
        at = pl.ds(r, L0.R)
        c, image = image_of(guess, react, L0, r)
        res = right[at, :] - image
        inv = inverse(react[at, :], 1.0)
        return [(r0, res), (inv0, inv), (ea0, inv * res)]

    ex_a.unpack()
    ex_a.x_send()
    ex_s.send()
    ga_s.send()
    ex_a.unpack_rest()
    planes(L0, 1, 23, start)
    ex_a.x_wait()
    ex_a.x_fill()
    planes(L0, -2, 1, start)
    planes(L0, 23, 26, start)
    relax(L0, ea0, eb0, r0, react, inv0, -1, 25)
    leftover(L0, eb0, left0, r0, react, 0, 24)
    restrict(left0, L0, f1, L1, 0, 12, 0, 24, down_m, tmp)
    ex_b.pack_send()
    cx_b.pack_send()
    ex_b.x_send()

    ex_c.pack()
    ex_s.unpack()
    ex_s.x_send()

    def inverse_of(g, sh, inv, first_plane, end):
        planes(g, first_plane, end, lambda r: [(inv, inverse(sh[pl.ds(r, g.R), :], g.factor))])

    inverse_of(L1, s1, inv1, 0, 12)

    ex_b.x_sent()
    ex_b.unpack()
    ex_c.send()
    first(L1, ea1, f1, inv1, 0, 12)
    relax(L1, ea1, eb1, f1, s1, inv1, 1, 11)
    ex_s.x_wait()
    ex_s.x_fill()
    inverse_of(L1, s1, inv1, -6, 0)
    inverse_of(L1, s1, inv1, 12, 18)
    inverse_of(L2, s2, inv2, -5, 11)
    ex_b.x_wait()
    cx_b.unpack()
    ex_b.x_fill()
    first(L1, ea1, f1, inv1, -6, 0)
    first(L1, ea1, f1, inv1, 12, 18)
    relax(L1, ea1, eb1, f1, s1, inv1, -5, 1)
    relax(L1, ea1, eb1, f1, s1, inv1, 11, 17)
    leftover(L1, eb1, left1, f1, s1, -4, 16)
    restrict(left1, L1, f2, L2, -2, 8, -2, 16, down_m, tmp)
    first(L2, ea2, f2, inv2, -2, 8)
    relax(L2, ea2, eb2, f2, s2, inv2, -1, 7)
    leftover(L2, eb2, left2, f2, s2, 0, 6)
    to_level3(left2, ga_f.mine, square, turned, chosen)
    ga_f.send()
    ex_d.pack_send()
    ga_s.relay()

    ga_f.relay()
    ex_c.unpack()
    ex_c.x_send()
    ex_c.unpack_rest()
    ex_d.unpack()
    ex_d.x_send()
    ex_c.x_wait()
    ex_c.x_fill()
    ex_d.x_wait()
    ex_d.x_fill()
    first(L2, ea2, f2, inv2, -5, 11)
    relax(L2, ea2, eb2, f2, s2, inv2, -4, 10)
    ga_s.finish()
    chunks3(n3, inv3, lambda r, n: inverse(s3[pl.ds(r, n), :], FACTOR3))
    s4[...] = restrict4(s3, n4, down4)
    for e in (ex_a, ex_s, ex_c, ex_d, ga_s):
        e.settle()
    for e in (ex_b, cx_b):
        e.settle(False)
    ga_f.finish()

    def relax3(src, dst):
        def body(r, n):
            c, image = image3(src, s3, r, n)
            at = pl.ds(r, n)
            return c + inv3[at, :] * (f3[at, :] - image)

        chunks3(n3, dst, body)

    chunks3(n3, ea3, lambda r, n: inv3[pl.ds(r, n), :] * f3[pl.ds(r, n), :])
    relax3(ea3, eb3)
    chunks3(n3, left3, lambda r, n: f3[pl.ds(r, n), :] - image3(eb3, s3, r, n)[1])
    e4 = bottom(restrict4(left3, n4, down4), s4, p4, n4, ny3 // 2)
    for k in range(3):
        u = mm(e4, up4[k])
        for q in (k, k + 4):
            at = pl.ds(GUARD3 + q, n4, stride=8)
            eb3[at, :] = eb3[at, :] + u
    for src, dst, n in ((eb3, ea3, 48), (ea3, slab, 40)):
        r = pl.multiple_of(GUARD3 + 24 * gz - (n - 24) // 2, 4)
        c, image = image3(src, s3, r, n)
        at = pl.ds(r, n)
        dst[at if n == 48 else pl.ds(0, n), :] = c + inv3[at, :] * (f3[at, :] - image)
    for k in range(3):
        v = slab[pl.ds(k, 10, stride=4), :]
        for h in range(2):
            for q in range(2):
                spread[k, pl.ds(64 * h + q, 10, stride=2), :] = v
    wide = [jnp.concatenate(p, axis=1) for p in zip(*[split(spread[k]) for k in range(3)])]
    coarse = []
    for h in range(2):
        pick = picks[h]
        parts = [
            lax.dot_general(pick, p, (((1,), (1,)), ((), ())), preferred_element_type=F32) for p in wide
        ]
        coarse.append(parts[0] + parts[1])
    fine = roll(jnp.where(lanes(112) < 64, coarse[0], coarse[1]), -4)
    for i in range(7):
        u = fine[16 * i : 16 * i + 10]
        tmp[pl.ds(24 * i, 10, stride=2), :] = u
        tmp[pl.ds(24 * i + 1, 10, stride=2), :] = u
    for i in range(7):
        v = tmp[pl.ds(24 * i, 20), :]
        for q in range(2):
            at = pl.ds(L2.row(2 * (i - 2) + q, -4), 20)
            eb2[at, :] = eb2[at, :] + v
    relax(L2, eb2, ea2, f2, s2, inv2, -3, 9)
    relax(L2, ea2, eb2, f2, s2, inv2, -2, 8)
    prolong(eb2, L2, eb1, L1, -2, 8, -2, 16, up_m, tmp)
    relax(L1, eb1, ea1, f1, s1, inv1, -3, 15)
    relax(L1, ea1, eb1, f1, s1, inv1, -2, 14)
    prolong(eb1, L1, eb0, L0, -2, 14, -2, 28, up_m, tmp)
    relax(L0, eb0, ea0, r0, react, inv0, -2, 26)
    relax(L0, ea0, eb0, r0, react, inv0, -1, 25)

    row = iota2((L0.R, 128), 0)
    inside = ((lanes(L0.R) & 63) < 48) & (row >= L0.y0) & (row < L0.y0 + 48)

    upper, lower = [], []
    for i in range(24):
        r = GUARD + (L0.halo + i) * L0.R
        c, image = image_of(eb0, react, L0, r)
        left0[pl.ds(r, L0.R), :] = image
        upper.append(c * r0[pl.ds(r, L0.R), :])
        lower.append(c * image)
    upper = jnp.where(inside, tree(upper), 0.0)
    lower = jnp.where(inside, tree(lower), 0.0)
    upper = jnp.sum(upper, axis=0, keepdims=True)
    lower = jnp.sum(lower, axis=0, keepdims=True)
    half = lanes(1) < 64
    number = (gx * sizes[1] + gy) * sizes[2] + gz
    reduced[number] = jnp.where(half, upper + roll(upper, 64), lower + roll(lower, 64))
    own = reduced.at[number]

    def summed(src, dst, p):
        return pltpu.make_async_remote_copy(
            src_ref=src, dst_ref=dst, send_sem=red_send.at[0], recv_sem=red_recv.at[0],
            device_id=place.beside(*p), device_id_type=MESH,
        )

    for p in peers:
        summed(own, own, p).start()
    ga_f.settle()
    most = reduced.at[pl.ds(0, len(peers))]
    summed(most, most, peers[0]).wait()
    sums = [reduced[k] for k in range(8)]
    for k in range(8, len(peers) + 1):
        sums[k % 8] = sums[k % 8] + reduced[k]
    total = tree(sums)
    upper = jnp.sum(jnp.where(half, total, 0.0), axis=1, keepdims=True)
    lower = jnp.sum(jnp.where(half, 0.0, total), axis=1, keepdims=True)
    step_out[...] = jnp.broadcast_to(upper / lower, (8, 128))


def finish(guess, r0, eb0, left0, step_ref, field_out, resid_out, field, resid, sems):
    step = step_ref[0:1, :]
    copies = []
    parts, size = 4, 6
    for p in range(parts):
        for x in range(p * size, p * size + size):
            at = pl.ds(L0.row(x, 0), 48)
            v = guess[at, :] + step * eb0[at, :]
            field[x] = v[:, 0:48]
            field[x + 24] = roll(v, 64)[:, 0:48]
            v = r0[at, :] - step * left0[at, :]
            resid[x] = v[:, 0:48]
            resid[x + 24] = roll(v, 64)[:, 0:48]
        for q, (src, dst) in enumerate(((field, field_out), (resid, resid_out))):
            for h in range(2):
                at = pl.ds(p * size + 24 * h, size)
                c = pltpu.make_async_copy(src.at[at], dst.at[at], sems.at[4 * p + 2 * q + h])
                c.start()
                copies.append(c)
    for c in copies:
        c.wait()


def solution(mesh):
    sizes = tuple(mesh.shape[a] for a in ("gx", "gy", "gz"))
    n3, n4 = 24 * sizes[2] + 2 * GUARD3, 3 * sizes[2]
    scratch = [pltpu.VMEM((48, 48, 48), F32)] * 3 + [pltpu.SemaphoreType.DMA((3,))]
    scratch += [pltpu.VMEM((L0.total, 128), F32)] * 4
    scratch += [pltpu.VMEM((L1.total, 128), F32)] * 6
    scratch += [pltpu.VMEM((L2.total, 128), F32)] * 6
    scratch += [pltpu.VMEM((n3, 128), F32)] * 6
    scratch += [pltpu.VMEM((n4, 128), F32), pltpu.VMEM((n4 + 2 * GUARD, 128), F32)]
    scratch += [pltpu.VMEM((128, 128), BF16)] * 2 + [pltpu.VMEM((16 * 56, 128), F32)]
    scratch += [pltpu.VMEM((128, 128), F32)] * 2
    scratch += [pltpu.VMEM((3, 128, 128), F32), pltpu.VMEM((40, 128), F32)]
    scratch += [pltpu.VMEM((128, 256), BF16), pltpu.VMEM((2, 112, 384), BF16)]
    scratch += [pltpu.VMEM((3, 128, 128), BF16)] * 2
    groups = [p.scratch() for p in PLANS] + [gather_scratch(sizes)] * 2
    devices = sizes[0] * sizes[1] * sizes[2]
    groups += [[pltpu.VMEM((devices, 1, 128), F32)] + [pltpu.SemaphoreType.DMA((1,))] * 2]
    for g in groups:
        scratch += g
    counts = tuple(len(g) for g in groups)
    vmem = pl.BlockSpec(memory_space=pltpu.VMEM)

    anywhere = pl.BlockSpec(memory_space=pl.ANY)

    def body(right_side, start_guess, reaction):
        whole = pltpu.VMEM((L0.total, 128), F32)
        parts = pl.pallas_call(
            functools.partial(kernel, sizes, counts),
            out_shape=[whole] * 4 + [pltpu.VMEM((8, 128), F32)],
            in_specs=[anywhere] * 3,
            out_specs=[vmem] * 5,
            scratch_shapes=scratch,
            compiler_params=pltpu.CompilerParams(
                collective_id=0, has_side_effects=True, vmem_limit_bytes=60 * 2**20
            ),
        )(right_side, start_guess, reaction)
        shape = jax.ShapeDtypeStruct(right_side.shape, F32)
        return tuple(
            pl.pallas_call(
                finish,
                out_shape=[shape, shape],
                in_specs=[vmem] * 5,
                out_specs=[anywhere] * 2,
                scratch_shapes=[pltpu.VMEM(right_side.shape, F32)] * 2 + [pltpu.SemaphoreType.DMA((16,))],
                compiler_params=pltpu.CompilerParams(vmem_limit_bytes=16 * 2**20),
            )(*parts)
        )

    placed = P("gx", "gy", "gz")
    return jax.shard_map(
        body, mesh=mesh, in_specs=(placed,) * 3, out_specs=(placed,) * 2, check_vma=False
    )
```

```python
import functools

import jax
import jax.numpy as jnp
from jax import lax
from jax.experimental import pallas as pl
from jax.experimental.pallas import tpu as pltpu
from jax.sharding import PartitionSpec as P

MESH = pl.DeviceIdType.MESH
F32 = jnp.float32
BF16 = jnp.bfloat16
DAMP = 6.0 / 7.0
GUARD = 8
GUARD3 = 16
BOTTOM_ITERS = 6


class Geo:
    def __init__(self, nx, ny, nz, halo, rows, y0, depth, unroll):
        self.nx, self.ny, self.nz, self.halo, self.R, self.y0 = nx, ny, nz, halo, rows, y0
        self.factor = 0.25**depth
        self.unroll = unroll
        self.total = 2 * GUARD + (nx + 2 * halo) * rows

    def row(self, x, y):
        return GUARD + (self.halo + x) * self.R + self.y0 + y


L0 = Geo(24, 48, 48, 4, 56, 4, 0, 28)
L1 = Geo(12, 24, 24, 6, 40, 8, 1, 24)
L2 = Geo(6, 12, 12, 5, 24, 6, 2, 16)
FACTOR3 = 0.25**3
FACTOR4 = 0.25**4


def lanes(rows):
    return lax.broadcasted_iota(jnp.int32, (rows, 128), 1)


def iota2(shape, dim):
    return lax.broadcasted_iota(jnp.int32, shape, dim)


def tree(terms):
    while len(terms) > 1:
        terms = [sum(terms[k + 1 : k + 2], terms[k]) for k in range(0, len(terms), 2)]
    return terms[0]


def roll(v, shift):
    shift = shift % 128
    return v if shift == 0 else pltpu.roll(v, shift, 1)


def split(a):
    hi = a.astype(BF16)
    return hi, (a - hi.astype(F32)).astype(BF16)


def mm(a, b):
    hi, low = split(a)
    return jnp.dot(hi, b, preferred_element_type=F32) + jnp.dot(low, b, preferred_element_type=F32)


def beside_of(ref, r, R):
    c = ref[pl.ds(r, R), :]
    b = ref[pl.ds(r + R, R), :] + ref[pl.ds(r - R, R), :]
    b = b + (ref[pl.ds(r + 1, R), :] + ref[pl.ds(r - 1, R), :])
    b = b + (roll(c, 1) + roll(c, -1))
    return c, b


def image_of(ref, s_ref, g, r):
    c, b = beside_of(ref, r, g.R)
    return c, g.factor * (6.0 * c - b) + s_ref[pl.ds(r, g.R), :] * c


def planes(g, a, b, body):
    unroll = g.unroll

    def group(start, count):
        todo = []
        for k in range(count):
            r = start + k * g.R
            r = r if isinstance(r, int) else pl.multiple_of(r, 8)
            todo.append((r, body(r)))
        for r, pairs in todo:
            for ref, value in pairs:
                ref[pl.ds(r, g.R), :] = value

    trips = (b - a) // unroll
    origin = GUARD + (g.halo + a) * g.R
    if trips == 1:
        group(origin, unroll)
    elif trips:

        def step(i, carry):
            group(pl.multiple_of(origin + i * (unroll * g.R), 8), unroll)
            return carry

        lax.fori_loop(0, trips, step, 0)
    if (b - a) % unroll:
        group(origin + trips * unroll * g.R, (b - a) % unroll)


def inverse(s, factor):
    return jnp.where(s > 0.0, DAMP / (6.0 * factor + s), 0.0)


def relax(g, src, dst, f, s, inv, a, b):
    def body(r):
        c, image = image_of(src, s, g, r)
        at = pl.ds(r, g.R)
        return [(dst, c + inv[at, :] * (f[at, :] - image))]

    planes(g, a, b, body)


def first(g, dst, f, inv, a, b):
    def body(r):
        at = pl.ds(r, g.R)
        return [(dst, inv[at, :] * f[at, :])]

    planes(g, a, b, body)


def leftover(g, src, dst, f, s, a, b):
    def body(r):
        c, image = image_of(src, s, g, r)
        return [(dst, f[pl.ds(r, g.R), :] - image)]

    planes(g, a, b, body)


def restrict(src, gs, dst, gd, x0, x1, y0, count, matrix, tmp):
    step = -(-count // 8) * 8
    for x in range(x0, x1):
        r = gs.row(2 * x, 2 * y0)
        t = src[pl.ds(r, count, stride=2), :] + src[pl.ds(r + 1, count, stride=2), :]
        r = r + gs.R
        t = t + (src[pl.ds(r, count, stride=2), :] + src[pl.ds(r + 1, count, stride=2), :])
        tmp[pl.ds((x - x0) * step, count), :] = t
    for x in range(x0, x1):
        out = mm(tmp[pl.ds((x - x0) * step, step), :], matrix[...])
        dst[pl.ds(gd.row(x, y0), count), :] = out[0:count]


def prolong(src, gc, dst, gf, x0, x1, y0, count, matrix, tmp):
    for x in range(x0, x1):
        o = (x - x0) * 56
        u = mm(src[pl.ds(gc.row(x, y0), count), :], matrix[...])
        tmp[pl.ds(o, count, stride=2), :] = u
        tmp[pl.ds(o + 1, count, stride=2), :] = u
    for x in range(x0, x1):
        o = (x - x0) * 56
        v = tmp[pl.ds(o, 2 * count), :]
        for k in range(2):
            at = pl.ds(gf.row(2 * x + k, 2 * y0), 2 * count)
            dst[at, :] = dst[at, :] + v


class Item:
    def __init__(self, geo, w):
        self.g, self.w = geo, w


class Plan:
    def __init__(self, items, cross=False):
        self.items, self.cross = items, cross
        self.counts = [it.w if cross else it.g.nx for it in items]
        self.yrows = sum(n * it.w for n, it in zip(self.counts, items))
        self.yrows = -(-self.yrows // 8) * 8
        self.tiles = []
        for k, it in enumerate(items):
            for x in range(self.counts[k]):
                for t in self.tiles:
                    if t[0] is it.g and t[1] + it.w <= 64:
                        break
                else:
                    t = [it.g, 0, []]
                    self.tiles.append(t)
                t[2].append((k, x, t[1]))
                t[1] += it.w
        self.zrows = sum(t[0].ny for t in self.tiles)
        self.zrows = -(-self.zrows // 8) * 8
        self.drows = max(self.counts)
        self.drows = -(-self.drows // 8) * 8
        assert sum(it.w * it.w for it in items) <= 64

        self.z0 = [0, self.zrows]
        self.d0 = [2 * self.zrows + q * self.drows for q in range(4)]
        self.y0 = [2 * self.zrows + 4 * self.drows + q * self.yrows for q in range(2)]
        self.total = 2 * (self.zrows + self.yrows) + 4 * self.drows
        self.xtotal = sum(it.w * it.g.R for it in items)

    def scratch(self):
        x = [] if self.cross else [pltpu.VMEM((self.xtotal, 128), F32)]
        return x + [
            pltpu.VMEM((self.total, 128), F32),
            pltpu.VMEM((self.total, 128), F32),
            pltpu.SemaphoreType.DMA((2,)),
            pltpu.SemaphoreType.DMA((2,)),
        ]


class Exchange:
    def __init__(self, plan, refs, scratch, place):
        self.plan, self.refs, self.place = plan, refs, place
        self.xr, self.sent, self.got, self.ss, self.rs = scratch
        gx, gy, gz = place.me
        self.partner = (1 - gx, gy, gz)
        self.x_copies = []
        o = 0
        for k, it in enumerate(plan.items):
            r = pl.multiple_of(GUARD + (it.g.halo + self.edge(it)) * it.g.R, 8)
            n = it.w * it.g.R
            self.x_copies.append(self.copy(refs[k].at[pl.ds(r, n), :], self.xr.at[pl.ds(o, n), :], 0, self.partner))
            o += n
        self.segments(0)

    def edge(self, it):
        return jnp.where(self.place.me[0] == 0, it.g.nx - it.w, 0)

    def source(self, k, x, y):
        return self.plan.items[k].g.row(x, y)

    def target(self, k, x, y):
        return self.refs[k], self.plan.items[k].g.row(x, y)

    def segments(self, dx):
        plan = self.plan
        at = {}
        for d in range(2):
            at[1 - 2 * d, 0] = plan.y0[d]
            at[0, 1 - 2 * d] = plan.z0[d]
            for e in range(2):
                at[1 - 2 * d, 1 - 2 * e] = plan.d0[2 * d + e]
        self.y_copies, self.z_copies, self.d_copies = [], [], []
        for d in (1, -1):
            self.y_copies.append(self.segment(at, dx, d, 0, plan.yrows))
            self.z_copies.append(self.segment(at, dx, 0, d, plan.zrows))
            for e in (1, -1):
                self.d_copies.append(self.segment(at, dx, d, e, plan.drows))

    def segment(self, at, dx, dy, dz, n):
        there = self.place.exists(dy, dz)
        peer = self.place.beside(dx, dy, dz)
        peer = tuple(jnp.where(there, p, q) for p, q in zip(peer, self.partner))
        target = pl.multiple_of(jnp.where(there, at[dy, dz], at[-dy, -dz]), 8)
        return self.copy(self.sent.at[pl.ds(at[dy, dz], n), :], self.got.at[pl.ds(target, n), :], 1, peer)

    def copy(self, src, dst, k, peer):
        return pltpu.make_async_remote_copy(
            src_ref=src, dst_ref=dst, send_sem=self.ss.at[k], recv_sem=self.rs.at[k],
            device_id=peer, device_id_type=MESH,
        )

    def x_send(self):
        for c in self.x_copies:
            c.start()

    def settle(self, x=True):
        if x:
            self.x_sent()
        self.copy(self.sent, self.got, 1, self.partner).wait_send()

    def x_sent(self):
        self.copy(self.xr, self.xr, 0, self.partner).wait_send()

    def x_wait(self):
        self.copy(self.xr, self.xr, 0, self.partner).wait_recv()

    def x_fill(self):
        m0, m1 = self.place.x_masks
        o = 0
        for k, it in enumerate(self.plan.items):
            g, w, ref = it.g, it.w, self.refs[k]
            upper = ((lanes(g.R) + 8) & 127) >= 64
            for j in range(w):
                got = self.xr[pl.ds(o + j * g.R, g.R), :]
                top = ref[pl.ds(GUARD + (g.halo + g.nx - w + j) * g.R, g.R), :]
                low = ref[pl.ds(GUARD + (g.halo + j) * g.R, g.R), :]
                ref[pl.ds(GUARD + (g.halo - w + j) * g.R, g.R), :] = roll(jnp.where(upper, got * m1, top), 64)
                ref[pl.ds(GUARD + (g.halo + g.nx + j) * g.R, g.R), :] = roll(jnp.where(upper, low, got * m0), 64)
            o += w * g.R

    def pack_send(self):
        self.pack()
        self.send()

    def pack(self):
        for k in range(len(self.refs)):
            self.pack_item(k)

    def send(self):
        for c in self.d_copies + self.z_copies + self.y_copies:
            c.start()

    def pack_item(self, k):
        if k == 0:
            self.yo, self.co, self.corner = 0, 0, [None] * 4
        it = self.plan.items[k]
        g, w, ref = it.g, it.w, self.refs[k]
        n = self.plan.counts[k]
        lane = lanes(self.plan.drows) & 63
        for d in range(1, w + 1):
            at = self.co + (d - 1) * w
            for e, y in enumerate((g.ny - d, d - 1)):
                v = ref[pl.ds(self.source(k, 0, y), n, stride=g.R), :]
                self.sent[pl.ds(self.plan.y0[e] + self.yo, n), :] = v
                if n < self.plan.drows:
                    v = jnp.concatenate([v, jnp.zeros((self.plan.drows - n, 128), F32)], axis=0)
                for q, z in enumerate((g.nz - w, 0)):
                    moved = roll(v, at - z)
                    old = self.corner[2 * e + q]
                    self.corner[2 * e + q] = moved if old is None else jnp.where(lane >= at, moved, old)
            self.yo += n
        self.co += w * w
        if k == len(self.refs) - 1:
            for q in range(4):
                self.sent[pl.ds(self.plan.d0[q], self.plan.drows), :] = self.corner[q]
        zo = 0
        for t, _, slots in self.plan.tiles:
            if slots[-1][0] == k:
                self.pack_tile(t, slots, zo)
            zo += t.ny

    def pack_tile(self, g, slots, zo):
        lane = lanes(g.ny)
        acc = [None, None]
        for k, x, at in slots:
            w = self.plan.items[k].w
            moved = roll(self.refs[k][pl.ds(self.source(k, x, 0), g.ny), :], at)
            for q, past in enumerate((g.nz - w, 0)):
                here = ((lane - past) & 63 >= at) & ((lane - past) & 63 < at + w)
                acc[q] = moved if acc[q] is None else jnp.where(here, moved, acc[q])
        for q in range(2):
            self.sent[pl.ds(self.plan.z0[q] + zo, g.ny), :] = acc[q]

    def unpack(self):
        my, mz = self.place.y_masks, self.place.z_masks
        self.copy(self.sent, self.got, 1, self.partner).wait_recv()
        yo, co = 0, 0
        for k, it in enumerate(self.plan.items):
            g, w = it.g, it.w
            n = self.plan.counts[k]
            lane = lanes(n) & 63
            into = (lane >= 64 - w, (lane >= g.nz) & (lane < g.nz + w))
            for d in range(1, w + 1):
                at = co + (d - 1) * w
                for e, y in enumerate((-d, g.ny + d - 1)):
                    v = self.got[pl.ds(self.plan.y0[e] + yo, n), :]
                    for q, z in enumerate((-w, g.nz)):
                        got = self.got[pl.ds(self.plan.d0[2 * e + q], n), :] * mz[q]
                        v = jnp.where(into[q], roll(got, z - at), v)
                    ref, r = self.target(k, 0, y)
                    ref[pl.ds(r, n, stride=g.R), :] = v * my[e]
                yo += n
            co += w * w
        self.unpack_z(True)

    def unpack_rest(self):
        self.unpack_z(False)

    def unpack_z(self, edge):
        mz = self.place.z_masks
        zo = 0
        for g, _, slots in self.plan.tiles:
            lane = lanes(g.ny) & 63
            got = [self.got[pl.ds(self.plan.z0[q] + zo, g.ny), :] * mz[q] for q in range(2)]
            for k, x, at in slots:
                w = self.plan.items[k].w
                if (x < w or x >= g.nx - w) != edge:
                    continue
                ref, r = self.target(k, x, 0)
                rows = pl.ds(r, g.ny)
                v = ref[rows, :]
                v = jnp.where(lane >= 64 - w, roll(got[0], -g.nz - at), v)
                v = jnp.where((lane >= g.nz) & (lane < g.nz + w), roll(got[1], g.nz - at), v)
                ref[rows, :] = v
            zo += g.ny


class Cross(Exchange):
    def __init__(self, plan, main, scratch, place):
        self.plan, self.main, self.refs, self.place = plan, main, main.refs, place
        self.sent, self.got, self.ss, self.rs = scratch
        self.partner = main.partner
        self.segments(1)

    def source(self, k, x, y):
        it = self.plan.items[k]
        return GUARD + (it.g.halo + self.edge(it) + x) * it.g.R + it.g.y0 + y

    def target(self, k, x, y):
        o = sum(it.w * it.g.R for it in self.plan.items[:k])
        g = self.plan.items[k].g
        return self.main.xr, o + x * g.R + g.y0 + y


class Place:
    def __init__(self, sizes):
        self.sizes = sizes
        self.me = tuple(lax.axis_index(a) for a in ("gx", "gy", "gz"))
        gx, gy, gz = self.me
        one = lambda c: jnp.where(c, 1.0, 0.0).astype(F32)
        self.x_masks = (one(gx == 0), one(gx == 1))
        self.y_masks = (one(gy > 0), one(gy < sizes[1] - 1))
        self.z_masks = (one(gz > 0), one(gz < sizes[2] - 1))

    def exists(self, dy, dz):
        gx, gy, gz = self.me
        y, z = gy + dy, gz + dz
        return (y >= 0) & (y < self.sizes[1]) & (z >= 0) & (z < self.sizes[2])

    def beside(self, dx, dy, dz):
        return tuple(
            lax.rem(m + d % n, n) if d % n else m for m, d, n in zip(self.me, (dx, dy, dz), self.sizes)
        )


class Gather:
    rows = 24

    def __init__(self, place, scratch, whole):
        self.place, self.whole = place, whole
        self.mine, self.got, self.sum, self.parts, self.ss, self.rs = scratch
        n = place.sizes
        self.near = [(a, b) for a in range(n[0]) for b in range(n[1])][1:]
        self.near.sort(key=lambda p: -far((p[0], p[1], 0), n))
        self.line = sorted(range(1, n[2]), key=lambda c: -far((0, 0, c), n))
        self.at = pl.ds(pl.multiple_of(GUARD3 + self.rows * place.me[2], 8), self.rows)

    def copy(self, src, dst, k, peer):
        return pltpu.make_async_remote_copy(
            src_ref=src, dst_ref=dst, send_sem=self.ss.at[k], recv_sem=self.rs.at[k],
            device_id=peer, device_id_type=MESH,
        )

    def send(self):
        for k, (a, b) in enumerate(self.near):
            self.copy(self.mine, self.got.at[k], 0, self.place.beside(a, b, 0)).start()

    def relay(self):
        self.copy(self.got, self.got, 0, self.place.beside(1, 0, 0)).wait_recv()
        gx, gy, gz = self.place.me
        ny = self.place.sizes[1]
        lane = lanes(8)
        sums = [[], []], [[], []]
        for k, (a, b) in enumerate([(0, 0)] + self.near):
            tile = self.mine[...] if k == 0 else self.got[k - 1]
            start = 6 * lax.rem(gy + ny - b, ny)
            for h in range(2):
                y = (lane - 16 * h) & 31
                sums[a][h].append(jnp.where((y >= start) & (y < start + 6), tile, 0.0))
        for h in range(2):
            own, other = (roll(tree(sums[a][h]), -16 * h) for a in range(2))
            self.parts[pl.ds(16 * h, 8), :] = jnp.where(gx == 0, own, other)
            self.parts[pl.ds(16 * h + 8, 8), :] = jnp.where(gx == 0, other, own)
        for h in range(2):
            r = 16 * h
            self.sum[pl.ds(12 * h, 3, stride=4), :] = self.parts[pl.ds(r, 3), :]
            self.sum[pl.ds(12 * h + 1, 3, stride=4), :] = self.parts[pl.ds(r + 4, 3), :] + self.parts[pl.ds(r + 8, 3), :]
            self.sum[pl.ds(12 * h + 2, 3, stride=4), :] = self.parts[pl.ds(r + 12, 3), :]
        for c in self.line:
            self.copy(self.sum, self.whole.at[self.at, :], 1, self.place.beside(0, 0, c)).start()
        self.whole[self.at, :] = self.sum[...]

    def finish(self):
        self.most().wait_recv()

    def most(self):
        most = self.whole.at[pl.ds(GUARD3, self.rows * (self.place.sizes[2] - 1)), :]
        return self.copy(most, most, 1, self.place.beside(1, 0, 0))

    def settle(self):
        self.copy(self.got, self.got, 0, self.place.beside(1, 0, 0)).wait_send()
        self.most().wait_send()


def gather_scratch(sizes):
    return [
        pltpu.VMEM((8, 128), F32),
        pltpu.VMEM((sizes[0] * sizes[1] - 1, 8, 128), F32),
        pltpu.VMEM((24, 128), F32),
        pltpu.VMEM((32, 128), F32),
        pltpu.SemaphoreType.DMA((2,)),
        pltpu.SemaphoreType.DMA((2,)),
    ]


def spread_to_level3(place):
    gx, gy, gz = place.me
    r = iota2((128, 256), 0)
    l = iota2((128, 256), 1)
    x = 6 * gx + 3 * (r >> 6) + ((r & 63) >> 3)
    y = 6 * gy + (r & 7)
    hit = (x == (l >> 5) + 4 * gx) & (y == (l & 31)) & ((r & 7) < 6) & ((r & 63) < 24)
    return jnp.where(hit, 1.0, 0.0).astype(BF16)


def to_level3(src, mine, square, turned, chosen):
    g = L2
    for i in range(3):
        r = g.row(2 * i, 0)
        t = src[pl.ds(r, 6, stride=2), :] + src[pl.ds(r + 1, 6, stride=2), :]
        r = r + g.R
        t = t + (src[pl.ds(r, 6, stride=2), :] + src[pl.ds(r + 1, 6, stride=2), :])
        square[pl.ds(8 * i, 6), :] = t
    turned[...] = jnp.transpose(square[...])
    a = turned[pl.ds(0, 8, stride=2), :] + turned[pl.ds(1, 8, stride=2), :]
    b = turned[pl.ds(64, 8, stride=2), :] + turned[pl.ds(65, 8, stride=2), :]
    a = (a + roll(b, 64)) * 0.125
    out = mm(a, chosen[...])
    for k in range(2):
        turned[pl.ds(8 * k, 8), :] = out[:, 128 * k : 128 * k + 128]
    for k in range(2):
        mine[pl.ds(4 * k, 3), :] = turned[pl.ds(8 * k, 3), :] + roll(turned[pl.ds(8 * k + 3, 3), :], 16)


def image3(ref, s_ref, r, n):
    lane = lanes(n)
    c = ref[pl.ds(r, n), :]
    b = ref[pl.ds(r + 4, n), :] + ref[pl.ds(r - 4, n), :]
    b = b + (roll(c, 1) + roll(c, -1))
    b = b + roll(jnp.where(lane < 32, ref[pl.ds(r + 1, n), :], c), -32)
    b = b + roll(jnp.where(lane >= 96, ref[pl.ds(r - 1, n), :], c), 32)
    return c, FACTOR3 * (6.0 * c - b) + s_ref[pl.ds(r, n), :] * c


def chunks3(rows, ref, body):
    n = min(rows, 384)

    def step(i, carry):
        r = pl.multiple_of(GUARD3 + i * n, 8)
        ref[pl.ds(r, n), :] = body(r, n)
        return carry

    lax.fori_loop(0, rows // n, step, 0)


def match4(k, shape, coarse_dim, ny):
    c = iota2(shape, coarse_dim)
    l = iota2(shape, 1 - coarse_dim)
    return ((c >> 4) == 2 * k + (l >> 6)) & ((c & 15) == ((l & 31) >> 1)) & ((l & 31) < ny)


def restrict4(src, n, matrix):
    total = None
    for k in range(3):
        t = src[pl.ds(GUARD3 + k, n, stride=8), :] + src[pl.ds(GUARD3 + k + 4, n, stride=8), :]
        part = mm(t, matrix[k])
        total = part if total is None else total + part
    return total


def dot_all(a, b):
    return jnp.sum(jnp.sum(a * b, axis=0, keepdims=True), axis=1, keepdims=True)


def bottom(source, s4, p4, n, ny):
    estimate = jnp.zeros_like(source)
    left = source
    inside = (lanes(n) < 96) & ((lanes(n) & 15) < ny)
    shifted = 6.0 * FACTOR4 + s4[...]
    for it in range(BOTTOM_ITERS):
        p4[pl.ds(GUARD, n), :] = left
        b = p4[pl.ds(GUARD + 1, n), :] + p4[pl.ds(GUARD - 1, n), :]
        b = b + (roll(left, 1) + roll(left, -1))
        b = b + (roll(left, 16) + roll(left, -16))
        image = shifted * left - FACTOR4 * jnp.where(inside, b, 0.0)
        now = dot_all(left, left)
        bent = dot_all(left, image)
        if it == 0:
            denom = bent
            direction, turned = left, image
        else:
            ratio = now * inv_before
            denom = bent - ratio * ratio * denom
            direction = left + ratio * direction
            turned = image + ratio * turned
        step = now / denom
        inv_before = 1.0 / now
        estimate = estimate + step * direction
        if it < BOTTOM_ITERS - 1:
            left = left - step * turned
    return estimate


PLAN_A = Plan([Item(L0, 3), Item(L0, 2), Item(L0, 2)])
PLAN_S = Plan([Item(L1, 6), Item(L2, 5)])
PLAN_B = Plan([Item(L1, 6)])
PLAN_BX = Plan([Item(L1, 6)], True)
PLAN_C = Plan([Item(L0, 3)])
PLAN_D = Plan([Item(L2, 5)])
PLANS = (PLAN_A, PLAN_S, PLAN_B, PLAN_C, PLAN_D, PLAN_BX)


def far(p, sizes):
    ring = lambda d, n: min(d % n, -d % n)
    return p[0] + ring(p[1], sizes[1]) + ring(p[2], 4) + ring(p[2] // 4, 4)


def kernel(sizes, counts, right_in, guess_in, react_in, guess, r0, eb0, left0, step_out, *scratch):
    scratch = list(scratch)

    def take(n):
        out = scratch[:n]
        del scratch[:n]
        return out

    raw = take(3)
    (in_sems,) = take(1)
    right, react, inv0, ea0 = take(4)
    f1, s1, inv1, ea1, eb1, left1 = take(6)
    f2, s2, inv2, ea2, eb2, left2 = take(6)
    f3, s3, inv3, ea3, eb3, left3 = take(6)
    s4, p4, down_m, up_m, tmp, square, turned, spread, slab = take(9)
    chosen, picks, down4, up4 = take(4)
    scr = [take(n) for n in counts]
    place = Place(sizes)
    gx, gy, gz = place.me
    n3, n4, ny3 = 24 * sizes[2], 3 * sizes[2], 6 * sizes[1]

    inputs = (guess_in, right_in, react_in)
    for k in range(3):
        for q in range(4):
            at = pl.ds(12 * q, 12)
            pltpu.make_async_copy(inputs[k].at[at], raw[k].at[at], in_sems.at[k]).start()

    def clear(ref):
        n = ref.shape[0]
        size = next(k for k in (128, 122 * 8, 80, 8) if n % k == 0) if n > 128 else n
        size = {1808: 904, 976: 488, 416: 208}.get(n, size)

        def step(i, carry):
            ref[pl.ds(pl.multiple_of(i * size, 8), size), :] = jnp.zeros((size, 128), F32)
            return carry

        lax.fori_loop(0, n // size, step, 0)

    peers = [(a, b, c) for a in range(sizes[0]) for b in range(sizes[1]) for c in range(sizes[2])][1:]
    peers.sort(key=lambda p: -far(p, sizes))
    beside = {(a, b % sizes[1], c % sizes[2]) for a in range(2) for b in (1, -1) for c in (1, -1)}
    beside |= {(1, 0, c % sizes[2]) for c in (1, -1)}
    greeted = [p for p in peers if p[2] == 0 or p[:2] == (0, 0) or p in beside]
    barrier = pltpu.get_barrier_semaphore()
    for p in greeted:
        pl.semaphore_signal(barrier, inc=1, device_id=place.beside(*p), device_id_type=MESH)
    for ref in (guess, right, react):
        ref[...] = jnp.zeros_like(ref)

    ex_a = Exchange(PLAN_A, (guess, right, react), scr[0], place)
    ex_s = Exchange(PLAN_S, (s1, s2), scr[1], place)
    ex_b = Exchange(PLAN_B, (f1,), scr[2], place)
    ex_c = Exchange(PLAN_C, (eb0,), scr[3], place)
    ex_d = Exchange(PLAN_D, (f2,), scr[4], place)
    cx_b = Cross(PLAN_BX, ex_b, scr[5], place)
    ga_s = Gather(place, scr[6], s3)
    ga_f = Gather(place, scr[7], f3)
    for k, dst in enumerate((guess, right, react)):
        pltpu.make_async_copy(inputs[k], raw[k], in_sems.at[k]).wait()

        for i in range(24):
            dst[pl.ds(L0.row(i, 0), 48), 0:48] = raw[k][i]
            dst[pl.ds(L0.row(i, 0), 48), 64:112] = raw[k][i + 24]
        ex_a.pack_item(k)

    reduced, red_send, red_recv = scr[8]

    pl.semaphore_wait(barrier, len(greeted))
    ex_a.send()

    for ref in (f1, s1, ea1, eb1, f2, s2, ea2, eb2, ea3, eb3, p4, square):
        clear(ref)
    spread[...] = jnp.zeros_like(spread)
    for ref in (f3, s3, inv3):
        for r in (0, GUARD3 + n3):
            ref[pl.ds(r, GUARD3), :] = jnp.zeros((GUARD3, 128), F32)

    a = iota2((128, 128), 0)
    b = iota2((128, 128), 1)
    signed = lambda v: ((v + 8) & 63) - 8
    base = lambda v: ((v + 8) & 127) & 64
    zb = signed(b)
    hit = ((a == ((base(b) + 2 * zb) & 127)) | (a == ((base(b) + 2 * zb + 1) & 127))) & (zb >= -8) & (zb < 24)
    down_m[...] = jnp.where(hit, 0.125, 0.0).astype(BF16)
    hit = a == ((base(b) + (zb >> 1)) & 127)
    up_m[...] = jnp.where(hit, 1.0, 0.0).astype(BF16)


    restrict(react, L0, s1, L1, 0, 12, 0, 24, down_m, tmp)
    restrict(s1, L1, s2, L2, 0, 6, 0, 12, down_m, tmp)
    ex_s.pack()
    for e in (ga_s, ga_f):
        e.mine[...] = jnp.zeros((8, 128), F32)
        e.sum[...] = jnp.zeros((24, 128), F32)
    chosen[...] = spread_to_level3(place)
    to_level3(s2, ga_s.mine, square, turned, chosen)
    for h in range(2):
        r = iota2((112, 384), 0)
        l = iota2((112, 384), 1)
        hit = (6 * gx + 3 * h + (r >> 4) - 2 == (l >> 5)) & (6 * gy + (r & 15) - 2 == (l & 31)) & ((r & 15) < 10)
        picks[h] = jnp.where(hit, 1.0, 0.0).astype(BF16)
    for k in range(3):
        down4[k] = jnp.where(match4(k, (128, 128), 1, ny3), 0.125, 0.0).astype(BF16)
        up4[k] = jnp.where(match4(k, (128, 128), 0, ny3), 1.0, 0.0).astype(BF16)


    def start(r):
        at = pl.ds(r, L0.R)
        c, image = image_of(guess, react, L0, r)
        res = right[at, :] - image
        inv = inverse(react[at, :], 1.0)
        return [(r0, res), (inv0, inv), (ea0, inv * res)]

    ex_a.unpack()
    ex_a.x_send()
    ex_s.send()
    ga_s.send()
    ex_a.unpack_rest()
    planes(L0, 1, 23, start)
    ex_a.x_wait()
    ex_a.x_fill()
    planes(L0, -2, 1, start)
    planes(L0, 23, 26, start)
    relax(L0, ea0, eb0, r0, react, inv0, -1, 25)
    leftover(L0, eb0, left0, r0, react, 0, 24)
    restrict(left0, L0, f1, L1, 0, 12, 0, 24, down_m, tmp)
    ex_b.pack_send()
    cx_b.pack_send()
    ex_b.x_send()

    ex_c.pack()
    ex_s.unpack()
    ex_s.x_send()

    def inverse_of(g, sh, inv, first_plane, end):
        planes(g, first_plane, end, lambda r: [(inv, inverse(sh[pl.ds(r, g.R), :], g.factor))])

    inverse_of(L1, s1, inv1, 0, 12)

    ex_b.x_sent()
    ex_b.unpack()
    ex_c.send()
    first(L1, ea1, f1, inv1, 0, 12)
    relax(L1, ea1, eb1, f1, s1, inv1, 1, 11)
    ex_s.x_wait()
    ex_s.x_fill()
    inverse_of(L1, s1, inv1, -6, 0)
    inverse_of(L1, s1, inv1, 12, 18)
    inverse_of(L2, s2, inv2, -5, 11)
    ex_b.x_wait()
    cx_b.unpack()
    ex_b.x_fill()
    first(L1, ea1, f1, inv1, -6, 0)
    first(L1, ea1, f1, inv1, 12, 18)
    relax(L1, ea1, eb1, f1, s1, inv1, -5, 1)
    relax(L1, ea1, eb1, f1, s1, inv1, 11, 17)
    leftover(L1, eb1, left1, f1, s1, -4, 16)
    restrict(left1, L1, f2, L2, -2, 8, -2, 16, down_m, tmp)
    first(L2, ea2, f2, inv2, -2, 8)
    relax(L2, ea2, eb2, f2, s2, inv2, -1, 7)
    leftover(L2, eb2, left2, f2, s2, 0, 6)
    to_level3(left2, ga_f.mine, square, turned, chosen)
    ga_f.send()
    ex_d.pack_send()
    ga_s.relay()

    ga_f.relay()
    ex_c.unpack()
    ex_c.x_send()
    ex_c.unpack_rest()
    ex_d.unpack()
    ex_d.x_send()
    ex_c.x_wait()
    ex_c.x_fill()
    ex_d.x_wait()
    ex_d.x_fill()
    first(L2, ea2, f2, inv2, -5, 11)
    relax(L2, ea2, eb2, f2, s2, inv2, -4, 10)
    ga_s.finish()
    chunks3(n3, inv3, lambda r, n: inverse(s3[pl.ds(r, n), :], FACTOR3))
    s4[...] = restrict4(s3, n4, down4)
    for e in (ex_a, ex_s, ex_c, ex_d, ga_s):
        e.settle()
    for e in (ex_b, cx_b):
        e.settle(False)
    ga_f.finish()

    def relax3(src, dst):
        def body(r, n):
            c, image = image3(src, s3, r, n)
            at = pl.ds(r, n)
            return c + inv3[at, :] * (f3[at, :] - image)

        chunks3(n3, dst, body)

    chunks3(n3, ea3, lambda r, n: inv3[pl.ds(r, n), :] * f3[pl.ds(r, n), :])
    relax3(ea3, eb3)
    chunks3(n3, left3, lambda r, n: f3[pl.ds(r, n), :] - image3(eb3, s3, r, n)[1])
    e4 = bottom(restrict4(left3, n4, down4), s4, p4, n4, ny3 // 2)
    for k in range(3):
        u = mm(e4, up4[k])
        for q in (k, k + 4):
            at = pl.ds(GUARD3 + q, n4, stride=8)
            eb3[at, :] = eb3[at, :] + u
    for src, dst, n in ((eb3, ea3, 48), (ea3, slab, 40)):
        r = pl.multiple_of(GUARD3 + 24 * gz - (n - 24) // 2, 4)
        c, image = image3(src, s3, r, n)
        at = pl.ds(r, n)
        dst[at if n == 48 else pl.ds(0, n), :] = c + inv3[at, :] * (f3[at, :] - image)
    for k in range(3):
        v = slab[pl.ds(k, 10, stride=4), :]
        for h in range(2):
            for q in range(2):
                spread[k, pl.ds(64 * h + q, 10, stride=2), :] = v
    wide = [jnp.concatenate(p, axis=1) for p in zip(*[split(spread[k]) for k in range(3)])]
    coarse = []
    for h in range(2):
        pick = picks[h]
        parts = [
            lax.dot_general(pick, p, (((1,), (1,)), ((), ())), preferred_element_type=F32) for p in wide
        ]
        coarse.append(parts[0] + parts[1])
    fine = roll(jnp.where(lanes(112) < 64, coarse[0], coarse[1]), -4)
    for i in range(7):
        u = fine[16 * i : 16 * i + 10]
        tmp[pl.ds(24 * i, 10, stride=2), :] = u
        tmp[pl.ds(24 * i + 1, 10, stride=2), :] = u
    for i in range(7):
        v = tmp[pl.ds(24 * i, 20), :]
        for q in range(2):
            at = pl.ds(L2.row(2 * (i - 2) + q, -4), 20)
            eb2[at, :] = eb2[at, :] + v
    relax(L2, eb2, ea2, f2, s2, inv2, -3, 9)
    relax(L2, ea2, eb2, f2, s2, inv2, -2, 8)
    prolong(eb2, L2, eb1, L1, -2, 8, -2, 16, up_m, tmp)
    relax(L1, eb1, ea1, f1, s1, inv1, -3, 15)
    relax(L1, ea1, eb1, f1, s1, inv1, -2, 14)
    prolong(eb1, L1, eb0, L0, -2, 14, -2, 28, up_m, tmp)
    relax(L0, eb0, ea0, r0, react, inv0, -2, 26)
    relax(L0, ea0, eb0, r0, react, inv0, -1, 25)

    row = iota2((L0.R, 128), 0)
    inside = ((lanes(L0.R) & 63) < 48) & (row >= L0.y0) & (row < L0.y0 + 48)

    upper, lower = [], []
    for i in range(24):
        r = GUARD + (L0.halo + i) * L0.R
        c, image = image_of(eb0, react, L0, r)
        left0[pl.ds(r, L0.R), :] = image
        upper.append(c * r0[pl.ds(r, L0.R), :])
        lower.append(c * image)
    upper = jnp.where(inside, tree(upper), 0.0)
    lower = jnp.where(inside, tree(lower), 0.0)
    upper = jnp.sum(upper, axis=0, keepdims=True)
    lower = jnp.sum(lower, axis=0, keepdims=True)
    half = lanes(1) < 64
    number = (gx * sizes[1] + gy) * sizes[2] + gz
    reduced[number] = jnp.where(half, upper + roll(upper, 64), lower + roll(lower, 64))
    own = reduced.at[number]

    def summed(src, dst, p):
        return pltpu.make_async_remote_copy(
            src_ref=src, dst_ref=dst, send_sem=red_send.at[0], recv_sem=red_recv.at[0],
            device_id=place.beside(*p), device_id_type=MESH,
        )

    for p in peers:
        summed(own, own, p).start()
    ga_f.settle()
    most = reduced.at[pl.ds(0, len(peers))]
    summed(most, most, peers[0]).wait()
    sums = [reduced[k] for k in range(8)]
    for k in range(8, len(peers) + 1):
        sums[k % 8] = sums[k % 8] + reduced[k]
    total = tree(sums)
    upper = jnp.sum(jnp.where(half, total, 0.0), axis=1, keepdims=True)
    lower = jnp.sum(jnp.where(half, 0.0, total), axis=1, keepdims=True)
    step_out[...] = jnp.broadcast_to(upper / lower, (8, 128))


def finish(guess, r0, eb0, left0, step_ref, field_out, resid_out, field, resid, sems):
    step = step_ref[0:1, :]
    parts, size = 6, 4
    for p in range(parts):
        for x in range(p * size, p * size + size):
            at = pl.ds(L0.row(x, 0), 48)
            v = guess[at, :] + step * eb0[at, :]
            field[x] = v[:, 0:48]
            field[x + 24] = roll(v, 64)[:, 0:48]
            v = r0[at, :] - step * left0[at, :]
            resid[x] = v[:, 0:48]
            resid[x + 24] = roll(v, 64)[:, 0:48]
        for q, (src, dst) in enumerate(((field, field_out), (resid, resid_out))):
            for h in range(2):
                at = pl.ds(p * size + 24 * h, size)
                pltpu.make_async_copy(src.at[at], dst.at[at], sems.at[q]).start()
    for q, (src, dst) in enumerate(((field, field_out), (resid, resid_out))):
        pltpu.make_async_copy(src, dst, sems.at[q]).wait()


def solution(mesh):
    sizes = tuple(mesh.shape[a] for a in ("gx", "gy", "gz"))
    n3, n4 = 24 * sizes[2] + 2 * GUARD3, 3 * sizes[2]
    scratch = [pltpu.VMEM((48, 48, 48), F32)] * 3 + [pltpu.SemaphoreType.DMA((3,))]
    scratch += [pltpu.VMEM((L0.total, 128), F32)] * 4
    scratch += [pltpu.VMEM((L1.total, 128), F32)] * 6
    scratch += [pltpu.VMEM((L2.total, 128), F32)] * 6
    scratch += [pltpu.VMEM((n3, 128), F32)] * 6
    scratch += [pltpu.VMEM((n4, 128), F32), pltpu.VMEM((n4 + 2 * GUARD, 128), F32)]
    scratch += [pltpu.VMEM((128, 128), BF16)] * 2 + [pltpu.VMEM((16 * 56, 128), F32)]
    scratch += [pltpu.VMEM((128, 128), F32)] * 2
    scratch += [pltpu.VMEM((3, 128, 128), F32), pltpu.VMEM((40, 128), F32)]
    scratch += [pltpu.VMEM((128, 256), BF16), pltpu.VMEM((2, 112, 384), BF16)]
    scratch += [pltpu.VMEM((3, 128, 128), BF16)] * 2
    groups = [p.scratch() for p in PLANS] + [gather_scratch(sizes)] * 2
    devices = sizes[0] * sizes[1] * sizes[2]
    groups += [[pltpu.VMEM((devices, 1, 128), F32)] + [pltpu.SemaphoreType.DMA((1,))] * 2]
    for g in groups:
        scratch += g
    counts = tuple(len(g) for g in groups)
    vmem = pl.BlockSpec(memory_space=pltpu.VMEM)

    anywhere = pl.BlockSpec(memory_space=pl.ANY)

    def body(right_side, start_guess, reaction):
        whole = pltpu.VMEM((L0.total, 128), F32)
        parts = pl.pallas_call(
            functools.partial(kernel, sizes, counts),
            out_shape=[whole] * 4 + [pltpu.VMEM((8, 128), F32)],
            in_specs=[anywhere] * 3,
            out_specs=[vmem] * 5,
            scratch_shapes=scratch,
            compiler_params=pltpu.CompilerParams(
                collective_id=0, has_side_effects=True, vmem_limit_bytes=60 * 2**20
            ),
        )(right_side, start_guess, reaction)
        shape = jax.ShapeDtypeStruct(right_side.shape, F32)
        return tuple(
            pl.pallas_call(
                finish,
                out_shape=[shape, shape],
                in_specs=[vmem] * 5,
                out_specs=[anywhere] * 2,
                scratch_shapes=[pltpu.VMEM(right_side.shape, F32)] * 2 + [pltpu.SemaphoreType.DMA((2,))],
                compiler_params=pltpu.CompilerParams(vmem_limit_bytes=16 * 2**20),
            )(*parts)
        )

    placed = P("gx", "gy", "gz")
    return jax.shard_map(
        body, mesh=mesh, in_specs=(placed,) * 3, out_specs=(placed,) * 2, check_vma=False
    )
```

```python
import functools

import jax
import jax.numpy as jnp
from jax import lax
from jax.experimental import pallas as pl
from jax.experimental.pallas import tpu as pltpu
from jax.sharding import PartitionSpec as P

MESH = pl.DeviceIdType.MESH
F32 = jnp.float32
BF16 = jnp.bfloat16
DAMP = 6.0 / 7.0
GUARD = 8
GUARD3 = 16
BOTTOM_ITERS = 6


class Geo:
    def __init__(self, nx, ny, nz, halo, rows, y0, depth, unroll):
        self.nx, self.ny, self.nz, self.halo, self.R, self.y0 = nx, ny, nz, halo, rows, y0
        self.factor = 0.25**depth
        self.unroll = unroll
        self.total = 2 * GUARD + (nx + 2 * halo) * rows

    def row(self, x, y):
        return GUARD + (self.halo + x) * self.R + self.y0 + y


L0 = Geo(24, 48, 48, 4, 56, 4, 0, 28)
L1 = Geo(12, 24, 24, 6, 40, 8, 1, 24)
L2 = Geo(6, 12, 12, 5, 24, 6, 2, 16)
FACTOR3 = 0.25**3
FACTOR4 = 0.25**4


def lanes(rows):
    return lax.broadcasted_iota(jnp.int32, (rows, 128), 1)


def iota2(shape, dim):
    return lax.broadcasted_iota(jnp.int32, shape, dim)


def tree(terms):
    while len(terms) > 1:
        terms = [sum(terms[k + 1 : k + 2], terms[k]) for k in range(0, len(terms), 2)]
    return terms[0]


def roll(v, shift):
    shift = shift % 128
    return v if shift == 0 else pltpu.roll(v, shift, 1)


def split(a):
    hi = a.astype(BF16)
    return hi, (a - hi.astype(F32)).astype(BF16)


def mm(a, b):
    hi, low = split(a)
    return jnp.dot(hi, b, preferred_element_type=F32) + jnp.dot(low, b, preferred_element_type=F32)


def beside_of(ref, r, R):
    c = ref[pl.ds(r, R), :]
    b = ref[pl.ds(r + R, R), :] + ref[pl.ds(r - R, R), :]
    b = b + (ref[pl.ds(r + 1, R), :] + ref[pl.ds(r - 1, R), :])
    b = b + (roll(c, 1) + roll(c, -1))
    return c, b


def image_of(ref, s_ref, g, r):
    c, b = beside_of(ref, r, g.R)
    return c, g.factor * (6.0 * c - b) + s_ref[pl.ds(r, g.R), :] * c


def planes(g, a, b, body):
    unroll = g.unroll

    def group(start, count):
        todo = []
        for k in range(count):
            r = start + k * g.R
            r = r if isinstance(r, int) else pl.multiple_of(r, 8)
            todo.append((r, body(r)))
        for r, pairs in todo:
            for ref, value in pairs:
                ref[pl.ds(r, g.R), :] = value

    trips = (b - a) // unroll
    origin = GUARD + (g.halo + a) * g.R
    if trips == 1:
        group(origin, unroll)
    elif trips:

        def step(i, carry):
            group(pl.multiple_of(origin + i * (unroll * g.R), 8), unroll)
            return carry

        lax.fori_loop(0, trips, step, 0)
    if (b - a) % unroll:
        group(origin + trips * unroll * g.R, (b - a) % unroll)


def inverse(s, factor):
    return jnp.where(s > 0.0, DAMP / (6.0 * factor + s), 0.0)


def relax(g, src, dst, f, s, inv, a, b):
    def body(r):
        c, image = image_of(src, s, g, r)
        at = pl.ds(r, g.R)
        return [(dst, c + inv[at, :] * (f[at, :] - image))]

    planes(g, a, b, body)


def first(g, dst, f, inv, a, b):
    def body(r):
        at = pl.ds(r, g.R)
        return [(dst, inv[at, :] * f[at, :])]

    planes(g, a, b, body)


def leftover(g, src, dst, f, s, a, b):
    def body(r):
        c, image = image_of(src, s, g, r)
        return [(dst, f[pl.ds(r, g.R), :] - image)]

    planes(g, a, b, body)


def restrict(src, gs, dst, gd, x0, x1, y0, count, matrix, tmp):
    step = -(-count // 8) * 8
    for x in range(x0, x1):
        r = gs.row(2 * x, 2 * y0)
        t = src[pl.ds(r, count, stride=2), :] + src[pl.ds(r + 1, count, stride=2), :]
        r = r + gs.R
        t = t + (src[pl.ds(r, count, stride=2), :] + src[pl.ds(r + 1, count, stride=2), :])
        tmp[pl.ds((x - x0) * step, count), :] = t
    for x in range(x0, x1):
        out = mm(tmp[pl.ds((x - x0) * step, step), :], matrix[...])
        dst[pl.ds(gd.row(x, y0), count), :] = out[0:count]


def prolong(src, gc, dst, gf, x0, x1, y0, count, matrix, tmp):
    for x in range(x0, x1):
        o = (x - x0) * 56
        u = mm(src[pl.ds(gc.row(x, y0), count), :], matrix[...])
        tmp[pl.ds(o, count, stride=2), :] = u
        tmp[pl.ds(o + 1, count, stride=2), :] = u
    for x in range(x0, x1):
        o = (x - x0) * 56
        v = tmp[pl.ds(o, 2 * count), :]
        for k in range(2):
            at = pl.ds(gf.row(2 * x + k, 2 * y0), 2 * count)
            dst[at, :] = dst[at, :] + v


class Item:
    def __init__(self, geo, w):
        self.g, self.w = geo, w
        self.deep = w - 1 if geo is L0 else w


class Plan:
    def __init__(self, items, cross=False):
        self.items, self.cross = items, cross
        self.counts = [it.w if cross else it.g.nx for it in items]
        self.yrows = sum(n * it.w for n, it in zip(self.counts, items))
        self.yrows = -(-self.yrows // 8) * 8
        self.tiles = []
        for k, it in enumerate(items):
            for x in range(self.counts[k]):
                for t in self.tiles:
                    if t[0] is it.g and t[1] + it.w <= 64:
                        break
                else:
                    t = [it.g, 0, []]
                    self.tiles.append(t)
                t[2].append((k, x, t[1]))
                t[1] += it.w
        self.zrows = sum(t[0].ny for t in self.tiles)
        self.zrows = -(-self.zrows // 8) * 8
        self.drows = max(self.counts)
        self.drows = -(-self.drows // 8) * 8
        assert sum(it.w * it.w for it in items) <= 64

        self.z0 = [0, self.zrows]
        self.d0 = [2 * self.zrows + q * self.drows for q in range(4)]
        self.y0 = [2 * self.zrows + 4 * self.drows + q * self.yrows for q in range(2)]
        self.total = 2 * (self.zrows + self.yrows) + 4 * self.drows
        self.xtotal = sum(it.w * it.g.R for it in items)

    def scratch(self):
        x = [] if self.cross else [pltpu.VMEM((self.xtotal, 128), F32)]
        return x + [
            pltpu.VMEM((self.total, 128), F32),
            pltpu.VMEM((self.total, 128), F32),
            pltpu.SemaphoreType.DMA((2,)),
            pltpu.SemaphoreType.DMA((2,)),
        ]


class Exchange:
    def __init__(self, plan, refs, scratch, place):
        self.plan, self.refs, self.place = plan, refs, place
        self.xr, self.sent, self.got, self.ss, self.rs = scratch
        gx, gy, gz = place.me
        self.partner = (1 - gx, gy, gz)
        self.x_copies = []
        o = 0
        for k, it in enumerate(plan.items):
            r = pl.multiple_of(GUARD + (it.g.halo + self.edge(it)) * it.g.R, 8)
            n = it.w * it.g.R
            self.x_copies.append(self.copy(refs[k].at[pl.ds(r, n), :], self.xr.at[pl.ds(o, n), :], 0, self.partner))
            o += n
        self.segments(0)

    def edge(self, it):
        return jnp.where(self.place.me[0] == 0, it.g.nx - it.w, 0)

    def source(self, k, x, y):
        return self.plan.items[k].g.row(x, y)

    def target(self, k, x, y):
        return self.refs[k], self.plan.items[k].g.row(x, y)

    def segments(self, dx):
        plan = self.plan
        at = {}
        for d in range(2):
            at[1 - 2 * d, 0] = plan.y0[d]
            at[0, 1 - 2 * d] = plan.z0[d]
            for e in range(2):
                at[1 - 2 * d, 1 - 2 * e] = plan.d0[2 * d + e]
        self.y_copies, self.z_copies, self.d_copies = [], [], []
        for d in (1, -1):
            self.y_copies.append(self.segment(at, dx, d, 0, plan.yrows))
            self.z_copies.append(self.segment(at, dx, 0, d, plan.zrows))
            for e in (1, -1):
                self.d_copies.append(self.segment(at, dx, d, e, plan.drows))

    def segment(self, at, dx, dy, dz, n):
        there = self.place.exists(dy, dz)
        peer = self.place.beside(dx, dy, dz)
        peer = tuple(jnp.where(there, p, q) for p, q in zip(peer, self.partner))
        target = pl.multiple_of(jnp.where(there, at[dy, dz], at[-dy, -dz]), 8)
        return self.copy(self.sent.at[pl.ds(at[dy, dz], n), :], self.got.at[pl.ds(target, n), :], 1, peer)

    def copy(self, src, dst, k, peer):
        return pltpu.make_async_remote_copy(
            src_ref=src, dst_ref=dst, send_sem=self.ss.at[k], recv_sem=self.rs.at[k],
            device_id=peer, device_id_type=MESH,
        )

    def x_send(self):
        for c in self.x_copies:
            c.start()

    def settle(self, x=True):
        if x:
            self.x_sent()
        self.copy(self.sent, self.got, 1, self.partner).wait_send()

    def x_sent(self):
        self.copy(self.xr, self.xr, 0, self.partner).wait_send()

    def x_wait(self):
        self.copy(self.xr, self.xr, 0, self.partner).wait_recv()

    def x_fill(self):
        m0, m1 = self.place.x_masks
        o = 0
        for k, it in enumerate(self.plan.items):
            g, w, ref = it.g, it.w, self.refs[k]
            upper = ((lanes(g.R) + 8) & 127) >= 64
            for j in range(w):
                got = self.xr[pl.ds(o + j * g.R, g.R), :]
                top = ref[pl.ds(GUARD + (g.halo + g.nx - w + j) * g.R, g.R), :]
                low = ref[pl.ds(GUARD + (g.halo + j) * g.R, g.R), :]
                ref[pl.ds(GUARD + (g.halo - w + j) * g.R, g.R), :] = roll(jnp.where(upper, got * m1, top), 64)
                ref[pl.ds(GUARD + (g.halo + g.nx + j) * g.R, g.R), :] = roll(jnp.where(upper, low, got * m0), 64)
            o += w * g.R

    def pack_send(self):
        self.pack()
        self.send()

    def pack(self):
        for k in range(len(self.refs)):
            self.pack_item(k)

    def send(self):
        for c in self.d_copies + self.z_copies + self.y_copies:
            c.start()

    def pack_item(self, k):
        if k == 0:
            self.yo, self.co, self.corner = 0, 0, [None] * 4
        it = self.plan.items[k]
        g, w, ref = it.g, it.w, self.refs[k]
        n = self.plan.counts[k]
        lane = lanes(self.plan.drows) & 63
        for d in range(1, w + 1):
            at = self.co + (d - 1) * w
            for e, y in enumerate((g.ny - d, d - 1)):
                v = ref[pl.ds(self.source(k, 0, y), n, stride=g.R), :]
                self.sent[pl.ds(self.plan.y0[e] + self.yo, n), :] = v
                if d > it.deep:
                    continue
                if n < self.plan.drows:
                    v = jnp.concatenate([v, jnp.zeros((self.plan.drows - n, 128), F32)], axis=0)
                for q, z in enumerate((g.nz - w, 0)):
                    moved = roll(v, at - z)
                    old = self.corner[2 * e + q]
                    self.corner[2 * e + q] = moved if old is None else jnp.where(lane >= at, moved, old)
            self.yo += n
        self.co += w * w
        if k == len(self.refs) - 1:
            for q in range(4):
                self.sent[pl.ds(self.plan.d0[q], self.plan.drows), :] = self.corner[q]
        zo = 0
        for t, _, slots in self.plan.tiles:
            if slots[-1][0] == k:
                self.pack_tile(t, slots, zo)
            zo += t.ny

    def pack_tile(self, g, slots, zo):
        lane = lanes(g.ny)
        acc = [None, None]
        for k, x, at in slots:
            w = self.plan.items[k].w
            moved = roll(self.refs[k][pl.ds(self.source(k, x, 0), g.ny), :], at)
            for q, past in enumerate((g.nz - w, 0)):
                here = ((lane - past) & 63 >= at) & ((lane - past) & 63 < at + w)
                acc[q] = moved if acc[q] is None else jnp.where(here, moved, acc[q])
        for q in range(2):
            self.sent[pl.ds(self.plan.z0[q] + zo, g.ny), :] = acc[q]

    def unpack(self):
        my, mz = self.place.y_masks, self.place.z_masks
        self.copy(self.sent, self.got, 1, self.partner).wait_recv()
        yo, co = 0, 0
        for k, it in enumerate(self.plan.items):
            g, w = it.g, it.w
            n = self.plan.counts[k]
            lane = lanes(n) & 63
            into = (lane >= 64 - w, (lane >= g.nz) & (lane < g.nz + w))
            for d in range(1, w + 1):
                at = co + (d - 1) * w
                for e, y in enumerate((-d, g.ny + d - 1)):
                    v = self.got[pl.ds(self.plan.y0[e] + yo, n), :]
                    for q, z in enumerate((-w, g.nz) if d <= it.deep else ()):
                        got = self.got[pl.ds(self.plan.d0[2 * e + q], n), :] * mz[q]
                        v = jnp.where(into[q], roll(got, z - at), v)
                    ref, r = self.target(k, 0, y)
                    ref[pl.ds(r, n, stride=g.R), :] = v * my[e]
                yo += n
            co += w * w
        self.unpack_z(True)

    def unpack_rest(self):
        self.unpack_z(False)

    def unpack_z(self, edge):
        mz = self.place.z_masks
        zo = 0
        for g, _, slots in self.plan.tiles:
            lane = lanes(g.ny) & 63
            got = [self.got[pl.ds(self.plan.z0[q] + zo, g.ny), :] * mz[q] for q in range(2)]
            for k, x, at in slots:
                w = self.plan.items[k].w
                if (x < w or x >= g.nx - w) != edge:
                    continue
                ref, r = self.target(k, x, 0)
                rows = pl.ds(r, g.ny)
                v = ref[rows, :]
                v = jnp.where(lane >= 64 - w, roll(got[0], -g.nz - at), v)
                v = jnp.where((lane >= g.nz) & (lane < g.nz + w), roll(got[1], g.nz - at), v)
                ref[rows, :] = v
            zo += g.ny


class Cross(Exchange):
    def __init__(self, plan, main, scratch, place):
        self.plan, self.main, self.refs, self.place = plan, main, main.refs, place
        self.sent, self.got, self.ss, self.rs = scratch
        self.partner = main.partner
        self.segments(1)

    def source(self, k, x, y):
        it = self.plan.items[k]
        return GUARD + (it.g.halo + self.edge(it) + x) * it.g.R + it.g.y0 + y

    def target(self, k, x, y):
        o = sum(it.w * it.g.R for it in self.plan.items[:k])
        g = self.plan.items[k].g
        return self.main.xr, o + x * g.R + g.y0 + y


class Place:
    def __init__(self, sizes):
        self.sizes = sizes
        self.me = tuple(lax.axis_index(a) for a in ("gx", "gy", "gz"))
        gx, gy, gz = self.me
        one = lambda c: jnp.where(c, 1.0, 0.0).astype(F32)
        self.x_masks = (one(gx == 0), one(gx == 1))
        self.y_masks = (one(gy > 0), one(gy < sizes[1] - 1))
        self.z_masks = (one(gz > 0), one(gz < sizes[2] - 1))

    def exists(self, dy, dz):
        gx, gy, gz = self.me
        y, z = gy + dy, gz + dz
        return (y >= 0) & (y < self.sizes[1]) & (z >= 0) & (z < self.sizes[2])

    def beside(self, dx, dy, dz):
        return tuple(
            lax.rem(m + d % n, n) if d % n else m for m, d, n in zip(self.me, (dx, dy, dz), self.sizes)
        )


class Gather:
    rows = 24

    def __init__(self, place, scratch, whole):
        self.place, self.whole = place, whole
        self.mine, self.got, self.sum, self.parts, self.ss, self.rs = scratch
        n = place.sizes
        self.near = [(a, b) for a in range(n[0]) for b in range(n[1])][1:]
        self.near.sort(key=lambda p: -far((p[0], p[1], 0), n))
        self.line = sorted(range(1, n[2]), key=lambda c: -far((0, 0, c), n))
        self.at = pl.ds(pl.multiple_of(GUARD3 + self.rows * place.me[2], 8), self.rows)

    def copy(self, src, dst, k, peer):
        return pltpu.make_async_remote_copy(
            src_ref=src, dst_ref=dst, send_sem=self.ss.at[k], recv_sem=self.rs.at[k],
            device_id=peer, device_id_type=MESH,
        )

    def send(self):
        for k, (a, b) in enumerate(self.near):
            self.copy(self.mine, self.got.at[k], 0, self.place.beside(a, b, 0)).start()

    def relay(self):
        self.copy(self.got, self.got, 0, self.place.beside(1, 0, 0)).wait_recv()
        gx, gy, gz = self.place.me
        ny = self.place.sizes[1]
        lane = lanes(8)
        sums = [[], []], [[], []]
        for k, (a, b) in enumerate([(0, 0)] + self.near):
            tile = self.mine[...] if k == 0 else self.got[k - 1]
            start = 6 * lax.rem(gy + ny - b, ny)
            for h in range(2):
                y = (lane - 16 * h) & 31
                sums[a][h].append(jnp.where((y >= start) & (y < start + 6), tile, 0.0))
        for h in range(2):
            own, other = (roll(tree(sums[a][h]), -16 * h) for a in range(2))
            self.parts[pl.ds(16 * h, 8), :] = jnp.where(gx == 0, own, other)
            self.parts[pl.ds(16 * h + 8, 8), :] = jnp.where(gx == 0, other, own)
        for h in range(2):
            r = 16 * h
            self.sum[pl.ds(12 * h, 3, stride=4), :] = self.parts[pl.ds(r, 3), :]
            self.sum[pl.ds(12 * h + 1, 3, stride=4), :] = self.parts[pl.ds(r + 4, 3), :] + self.parts[pl.ds(r + 8, 3), :]
            self.sum[pl.ds(12 * h + 2, 3, stride=4), :] = self.parts[pl.ds(r + 12, 3), :]
        for c in self.line:
            self.copy(self.sum, self.whole.at[self.at, :], 1, self.place.beside(0, 0, c)).start()
        self.whole[self.at, :] = self.sum[...]

    def finish(self):
        self.most().wait_recv()

    def most(self):
        most = self.whole.at[pl.ds(GUARD3, self.rows * (self.place.sizes[2] - 1)), :]
        return self.copy(most, most, 1, self.place.beside(1, 0, 0))

    def settle(self):
        self.copy(self.got, self.got, 0, self.place.beside(1, 0, 0)).wait_send()
        self.most().wait_send()


def gather_scratch(sizes):
    return [
        pltpu.VMEM((8, 128), F32),
        pltpu.VMEM((sizes[0] * sizes[1] - 1, 8, 128), F32),
        pltpu.VMEM((24, 128), F32),
        pltpu.VMEM((32, 128), F32),
        pltpu.SemaphoreType.DMA((2,)),
        pltpu.SemaphoreType.DMA((2,)),
    ]


def spread_to_level3(place):
    gx, gy, gz = place.me
    r = iota2((128, 256), 0)
    l = iota2((128, 256), 1)
    x = 6 * gx + 3 * (r >> 6) + ((r & 63) >> 3)
    y = 6 * gy + (r & 7)
    hit = (x == (l >> 5) + 4 * gx) & (y == (l & 31)) & ((r & 7) < 6) & ((r & 63) < 24)
    return jnp.where(hit, 1.0, 0.0).astype(BF16)


def to_level3(src, mine, square, turned, chosen):
    g = L2
    for i in range(3):
        r = g.row(2 * i, 0)
        t = src[pl.ds(r, 6, stride=2), :] + src[pl.ds(r + 1, 6, stride=2), :]
        r = r + g.R
        t = t + (src[pl.ds(r, 6, stride=2), :] + src[pl.ds(r + 1, 6, stride=2), :])
        square[pl.ds(8 * i, 6), :] = t
    turned[...] = jnp.transpose(square[...])
    a = turned[pl.ds(0, 8, stride=2), :] + turned[pl.ds(1, 8, stride=2), :]
    b = turned[pl.ds(64, 8, stride=2), :] + turned[pl.ds(65, 8, stride=2), :]
    a = (a + roll(b, 64)) * 0.125
    out = mm(a, chosen[...])
    for k in range(2):
        turned[pl.ds(8 * k, 8), :] = out[:, 128 * k : 128 * k + 128]
    for k in range(2):
        mine[pl.ds(4 * k, 3), :] = turned[pl.ds(8 * k, 3), :] + roll(turned[pl.ds(8 * k + 3, 3), :], 16)


def image3(ref, s_ref, r, n):
    lane = lanes(n)
    c = ref[pl.ds(r, n), :]
    b = ref[pl.ds(r + 4, n), :] + ref[pl.ds(r - 4, n), :]
    b = b + (roll(c, 1) + roll(c, -1))
    b = b + roll(jnp.where(lane < 32, ref[pl.ds(r + 1, n), :], c), -32)
    b = b + roll(jnp.where(lane >= 96, ref[pl.ds(r - 1, n), :], c), 32)
    return c, FACTOR3 * (6.0 * c - b) + s_ref[pl.ds(r, n), :] * c


def chunks3(rows, ref, body):
    n = min(rows, 384)

    def step(i, carry):
        r = pl.multiple_of(GUARD3 + i * n, 8)
        ref[pl.ds(r, n), :] = body(r, n)
        return carry

    lax.fori_loop(0, rows // n, step, 0)


def match4(k, shape, coarse_dim, ny):
    c = iota2(shape, coarse_dim)
    l = iota2(shape, 1 - coarse_dim)
    return ((c >> 4) == 2 * k + (l >> 6)) & ((c & 15) == ((l & 31) >> 1)) & ((l & 31) < ny)


def restrict4(src, n, matrix):
    total = None
    for k in range(3):
        t = src[pl.ds(GUARD3 + k, n, stride=8), :] + src[pl.ds(GUARD3 + k + 4, n, stride=8), :]
        part = mm(t, matrix[k])
        total = part if total is None else total + part
    return total


def dot_all(a, b):
    return jnp.sum(jnp.sum(a * b, axis=0, keepdims=True), axis=1, keepdims=True)


def bottom(source, s4, p4, n, ny):
    estimate = jnp.zeros_like(source)
    left = source
    inside = (lanes(n) < 96) & ((lanes(n) & 15) < ny)
    shifted = 6.0 * FACTOR4 + s4[...]
    for it in range(BOTTOM_ITERS):
        p4[pl.ds(GUARD, n), :] = left
        b = p4[pl.ds(GUARD + 1, n), :] + p4[pl.ds(GUARD - 1, n), :]
        b = b + (roll(left, 1) + roll(left, -1))
        b = b + (roll(left, 16) + roll(left, -16))
        image = shifted * left - FACTOR4 * jnp.where(inside, b, 0.0)
        now = dot_all(left, left)
        bent = dot_all(left, image)
        if it == 0:
            denom = bent
            direction, turned = left, image
        else:
            ratio = now * inv_before
            denom = bent - ratio * ratio * denom
            direction = left + ratio * direction
            turned = image + ratio * turned
        step = now / denom
        inv_before = 1.0 / now
        estimate = estimate + step * direction
        if it < BOTTOM_ITERS - 1:
            left = left - step * turned
    return estimate


PLAN_A = Plan([Item(L0, 3), Item(L0, 2), Item(L0, 2)])
PLAN_S = Plan([Item(L1, 6), Item(L2, 5)])
PLAN_B = Plan([Item(L1, 6)])
PLAN_BX = Plan([Item(L1, 6)], True)
PLAN_C = Plan([Item(L0, 3)])
PLAN_D = Plan([Item(L2, 5)])
PLANS = (PLAN_A, PLAN_S, PLAN_B, PLAN_C, PLAN_D, PLAN_BX)


def far(p, sizes):
    ring = lambda d, n: min(d % n, -d % n)
    return p[0] + ring(p[1], sizes[1]) + ring(p[2], 4) + ring(p[2] // 4, 4)


def kernel(sizes, counts, right_in, guess_in, react_in, guess, r0, eb0, left0, step_out, *scratch):
    scratch = list(scratch)

    def take(n):
        out = scratch[:n]
        del scratch[:n]
        return out

    raw = take(3)
    (in_sems,) = take(1)
    right, react, inv0, ea0 = take(4)
    f1, s1, inv1, ea1, eb1, left1 = take(6)
    f2, s2, inv2, ea2, eb2, left2 = take(6)
    f3, s3, inv3, ea3, eb3, left3 = take(6)
    s4, p4, down_m, up_m, tmp, square, turned, spread, slab = take(9)
    chosen, picks, down4, up4 = take(4)
    scr = [take(n) for n in counts]
    place = Place(sizes)
    gx, gy, gz = place.me
    n3, n4, ny3 = 24 * sizes[2], 3 * sizes[2], 6 * sizes[1]

    inputs = (guess_in, right_in, react_in)
    for k in range(3):
        for q in range(4):
            at = pl.ds(12 * q, 12)
            pltpu.make_async_copy(inputs[k].at[at], raw[k].at[at], in_sems.at[k]).start()

    def clear(ref):
        n = ref.shape[0]
        size = next(k for k in (128, 122 * 8, 80, 8) if n % k == 0) if n > 128 else n
        size = {1808: 904, 976: 488, 416: 208}.get(n, size)

        def step(i, carry):
            ref[pl.ds(pl.multiple_of(i * size, 8), size), :] = jnp.zeros((size, 128), F32)
            return carry

        lax.fori_loop(0, n // size, step, 0)

    peers = [(a, b, c) for a in range(sizes[0]) for b in range(sizes[1]) for c in range(sizes[2])][1:]
    peers.sort(key=lambda p: -far(p, sizes))
    beside = {(a, b % sizes[1], c % sizes[2]) for a in range(2) for b in (1, -1) for c in (1, -1)}
    beside |= {(1, 0, c % sizes[2]) for c in (1, -1)}
    greeted = [p for p in peers if p[2] == 0 or p[:2] == (0, 0) or p in beside]
    barrier = pltpu.get_barrier_semaphore()
    for p in greeted:
        pl.semaphore_signal(barrier, inc=1, device_id=place.beside(*p), device_id_type=MESH)
    for ref in (guess, right, react):
        ref[...] = jnp.zeros_like(ref)

    ex_a = Exchange(PLAN_A, (guess, right, react), scr[0], place)
    ex_s = Exchange(PLAN_S, (s1, s2), scr[1], place)
    ex_b = Exchange(PLAN_B, (f1,), scr[2], place)
    ex_c = Exchange(PLAN_C, (eb0,), scr[3], place)
    ex_d = Exchange(PLAN_D, (f2,), scr[4], place)
    cx_b = Cross(PLAN_BX, ex_b, scr[5], place)
    ga_s = Gather(place, scr[6], s3)
    ga_f = Gather(place, scr[7], f3)
    for k, dst in enumerate((guess, right, react)):
        pltpu.make_async_copy(inputs[k], raw[k], in_sems.at[k]).wait()

        for i in range(24):
            dst[pl.ds(L0.row(i, 0), 48), 0:48] = raw[k][i]
            dst[pl.ds(L0.row(i, 0), 48), 64:112] = raw[k][i + 24]
        ex_a.pack_item(k)

    reduced, red_send, red_recv = scr[8]

    pl.semaphore_wait(barrier, len(greeted))
    ex_a.send()

    for ref in (f1, s1, ea1, eb1, f2, s2, ea2, eb2, ea3, eb3, p4, square):
        clear(ref)
    spread[...] = jnp.zeros_like(spread)
    for ref in (f3, s3, inv3):
        for r in (0, GUARD3 + n3):
            ref[pl.ds(r, GUARD3), :] = jnp.zeros((GUARD3, 128), F32)

    a = iota2((128, 128), 0)
    b = iota2((128, 128), 1)
    signed = lambda v: ((v + 8) & 63) - 8
    base = lambda v: ((v + 8) & 127) & 64
    zb = signed(b)
    hit = ((a == ((base(b) + 2 * zb) & 127)) | (a == ((base(b) + 2 * zb + 1) & 127))) & (zb >= -8) & (zb < 24)
    down_m[...] = jnp.where(hit, 0.125, 0.0).astype(BF16)
    hit = a == ((base(b) + (zb >> 1)) & 127)
    up_m[...] = jnp.where(hit, 1.0, 0.0).astype(BF16)


    restrict(react, L0, s1, L1, 0, 12, 0, 24, down_m, tmp)
    restrict(s1, L1, s2, L2, 0, 6, 0, 12, down_m, tmp)
    ex_s.pack()
    for e in (ga_s, ga_f):
        e.mine[...] = jnp.zeros((8, 128), F32)
        e.sum[...] = jnp.zeros((24, 128), F32)
    chosen[...] = spread_to_level3(place)
    to_level3(s2, ga_s.mine, square, turned, chosen)
    for h in range(2):
        r = iota2((112, 384), 0)
        l = iota2((112, 384), 1)
        hit = (6 * gx + 3 * h + (r >> 4) - 2 == (l >> 5)) & (6 * gy + (r & 15) - 2 == (l & 31)) & ((r & 15) < 10)
        picks[h] = jnp.where(hit, 1.0, 0.0).astype(BF16)
    for k in range(3):
        down4[k] = jnp.where(match4(k, (128, 128), 1, ny3), 0.125, 0.0).astype(BF16)
        up4[k] = jnp.where(match4(k, (128, 128), 0, ny3), 1.0, 0.0).astype(BF16)


    def start(r):
        at = pl.ds(r, L0.R)
        c, image = image_of(guess, react, L0, r)
        res = right[at, :] - image
        inv = inverse(react[at, :], 1.0)
        return [(r0, res), (inv0, inv), (ea0, inv * res)]

    ex_a.unpack()
    ex_a.x_send()
    ex_s.send()
    ga_s.send()
    ex_a.unpack_rest()
    planes(L0, 1, 23, start)
    ex_a.x_wait()
    ex_a.x_fill()
    planes(L0, -2, 1, start)
    planes(L0, 23, 26, start)
    relax(L0, ea0, eb0, r0, react, inv0, -1, 25)
    leftover(L0, eb0, left0, r0, react, 0, 24)
    restrict(left0, L0, f1, L1, 0, 12, 0, 24, down_m, tmp)
    ex_b.pack_send()
    cx_b.pack_send()
    ex_b.x_send()

    ex_c.pack()
    ex_s.unpack()
    ex_s.x_send()

    def inverse_of(g, sh, inv, first_plane, end):
        planes(g, first_plane, end, lambda r: [(inv, inverse(sh[pl.ds(r, g.R), :], g.factor))])

    inverse_of(L1, s1, inv1, 0, 12)

    ex_b.x_sent()
    ex_b.unpack()
    ex_c.send()
    first(L1, ea1, f1, inv1, 0, 12)
    relax(L1, ea1, eb1, f1, s1, inv1, 1, 11)
    ex_s.x_wait()
    ex_s.x_fill()
    inverse_of(L1, s1, inv1, -6, 0)
    inverse_of(L1, s1, inv1, 12, 18)
    inverse_of(L2, s2, inv2, -5, 11)
    ex_b.x_wait()
    cx_b.unpack()
    ex_b.x_fill()
    first(L1, ea1, f1, inv1, -6, 0)
    first(L1, ea1, f1, inv1, 12, 18)
    relax(L1, ea1, eb1, f1, s1, inv1, -5, 1)
    relax(L1, ea1, eb1, f1, s1, inv1, 11, 17)
    leftover(L1, eb1, left1, f1, s1, -4, 16)
    restrict(left1, L1, f2, L2, -2, 8, -2, 16, down_m, tmp)
    first(L2, ea2, f2, inv2, -2, 8)
    relax(L2, ea2, eb2, f2, s2, inv2, -1, 7)
    leftover(L2, eb2, left2, f2, s2, 0, 6)
    to_level3(left2, ga_f.mine, square, turned, chosen)
    ga_f.send()
    ex_d.pack_send()
    ga_s.relay()

    ga_f.relay()
    ex_c.unpack()
    ex_c.x_send()
    ex_c.unpack_rest()
    ex_d.unpack()
    ex_d.x_send()
    ex_c.x_wait()
    ex_c.x_fill()
    ex_d.x_wait()
    ex_d.x_fill()
    first(L2, ea2, f2, inv2, -5, 11)
    relax(L2, ea2, eb2, f2, s2, inv2, -4, 10)
    ga_s.finish()
    chunks3(n3, inv3, lambda r, n: inverse(s3[pl.ds(r, n), :], FACTOR3))
    s4[...] = restrict4(s3, n4, down4)
    for e in (ex_a, ex_s, ex_c, ex_d, ga_s):
        e.settle()
    for e in (ex_b, cx_b):
        e.settle(False)
    ga_f.finish()

    def relax3(src, dst):
        def body(r, n):
            c, image = image3(src, s3, r, n)
            at = pl.ds(r, n)
            return c + inv3[at, :] * (f3[at, :] - image)

        chunks3(n3, dst, body)

    chunks3(n3, ea3, lambda r, n: inv3[pl.ds(r, n), :] * f3[pl.ds(r, n), :])
    relax3(ea3, eb3)
    chunks3(n3, left3, lambda r, n: f3[pl.ds(r, n), :] - image3(eb3, s3, r, n)[1])
    e4 = bottom(restrict4(left3, n4, down4), s4, p4, n4, ny3 // 2)
    for k in range(3):
        u = mm(e4, up4[k])
        for q in (k, k + 4):
            at = pl.ds(GUARD3 + q, n4, stride=8)
            eb3[at, :] = eb3[at, :] + u
    for src, dst, n in ((eb3, ea3, 48), (ea3, slab, 40)):
        r = pl.multiple_of(GUARD3 + 24 * gz - (n - 24) // 2, 4)
        c, image = image3(src, s3, r, n)
        at = pl.ds(r, n)
        dst[at if n == 48 else pl.ds(0, n), :] = c + inv3[at, :] * (f3[at, :] - image)
    for k in range(3):
        v = slab[pl.ds(k, 10, stride=4), :]
        for h in range(2):
            for q in range(2):
                spread[k, pl.ds(64 * h + q, 10, stride=2), :] = v
    wide = [jnp.concatenate(p, axis=1) for p in zip(*[split(spread[k]) for k in range(3)])]
    coarse = []
    for h in range(2):
        pick = picks[h]
        parts = [
            lax.dot_general(pick, p, (((1,), (1,)), ((), ())), preferred_element_type=F32) for p in wide
        ]
        coarse.append(parts[0] + parts[1])
    fine = roll(jnp.where(lanes(112) < 64, coarse[0], coarse[1]), -4)
    for i in range(7):
        u = fine[16 * i : 16 * i + 10]
        tmp[pl.ds(24 * i, 10, stride=2), :] = u
        tmp[pl.ds(24 * i + 1, 10, stride=2), :] = u
    for i in range(7):
        v = tmp[pl.ds(24 * i, 20), :]
        for q in range(2):
            at = pl.ds(L2.row(2 * (i - 2) + q, -4), 20)
            eb2[at, :] = eb2[at, :] + v
    relax(L2, eb2, ea2, f2, s2, inv2, -3, 9)
    relax(L2, ea2, eb2, f2, s2, inv2, -2, 8)
    prolong(eb2, L2, eb1, L1, -2, 8, -2, 16, up_m, tmp)
    relax(L1, eb1, ea1, f1, s1, inv1, -3, 15)
    relax(L1, ea1, eb1, f1, s1, inv1, -2, 14)
    prolong(eb1, L1, eb0, L0, -2, 14, -2, 28, up_m, tmp)
    relax(L0, eb0, ea0, r0, react, inv0, -2, 26)
    relax(L0, ea0, eb0, r0, react, inv0, -1, 25)

    row = iota2((L0.R, 128), 0)
    inside = ((lanes(L0.R) & 63) < 48) & (row >= L0.y0) & (row < L0.y0 + 48)

    upper, lower = [], []
    for i in range(24):
        r = GUARD + (L0.halo + i) * L0.R
        c, image = image_of(eb0, react, L0, r)
        left0[pl.ds(r, L0.R), :] = image
        upper.append(c * r0[pl.ds(r, L0.R), :])
        lower.append(c * image)
    upper = jnp.where(inside, tree(upper), 0.0)
    lower = jnp.where(inside, tree(lower), 0.0)
    upper = jnp.sum(upper, axis=0, keepdims=True)
    lower = jnp.sum(lower, axis=0, keepdims=True)
    half = lanes(1) < 64
    number = (gx * sizes[1] + gy) * sizes[2] + gz
    reduced[number] = jnp.where(half, upper + roll(upper, 64), lower + roll(lower, 64))
    own = reduced.at[number]

    def summed(src, dst, p):
        return pltpu.make_async_remote_copy(
            src_ref=src, dst_ref=dst, send_sem=red_send.at[0], recv_sem=red_recv.at[0],
            device_id=place.beside(*p), device_id_type=MESH,
        )

    for p in peers:
        summed(own, own, p).start()
    ga_f.settle()
    most = reduced.at[pl.ds(0, len(peers))]
    summed(most, most, peers[0]).wait()
    sums = [reduced[k] for k in range(8)]
    for k in range(8, len(peers) + 1):
        sums[k % 8] = sums[k % 8] + reduced[k]
    total = tree(sums)
    upper = jnp.sum(jnp.where(half, total, 0.0), axis=1, keepdims=True)
    lower = jnp.sum(jnp.where(half, 0.0, total), axis=1, keepdims=True)
    step_out[...] = jnp.broadcast_to(upper / lower, (8, 128))


def finish(guess, r0, eb0, left0, step_ref, field_out, resid_out, field, resid, sems):
    step = step_ref[0:1, :]
    parts, size = 6, 4
    for p in range(parts):
        for x in range(p * size, p * size + size):
            at = pl.ds(L0.row(x, 0), 48)
            v = guess[at, :] + step * eb0[at, :]
            field[x] = v[:, 0:48]
            field[x + 24] = roll(v, 64)[:, 0:48]
            v = r0[at, :] - step * left0[at, :]
            resid[x] = v[:, 0:48]
            resid[x + 24] = roll(v, 64)[:, 0:48]
        for q, (src, dst) in enumerate(((field, field_out), (resid, resid_out))):
            for h in range(2):
                at = pl.ds(p * size + 24 * h, size)
                pltpu.make_async_copy(src.at[at], dst.at[at], sems.at[q]).start()
    for q, (src, dst) in enumerate(((field, field_out), (resid, resid_out))):
        pltpu.make_async_copy(src, dst, sems.at[q]).wait()


def solution(mesh):
    sizes = tuple(mesh.shape[a] for a in ("gx", "gy", "gz"))
    n3, n4 = 24 * sizes[2] + 2 * GUARD3, 3 * sizes[2]
    scratch = [pltpu.VMEM((48, 48, 48), F32)] * 3 + [pltpu.SemaphoreType.DMA((3,))]
    scratch += [pltpu.VMEM((L0.total, 128), F32)] * 4
    scratch += [pltpu.VMEM((L1.total, 128), F32)] * 6
    scratch += [pltpu.VMEM((L2.total, 128), F32)] * 6
    scratch += [pltpu.VMEM((n3, 128), F32)] * 6
    scratch += [pltpu.VMEM((n4, 128), F32), pltpu.VMEM((n4 + 2 * GUARD, 128), F32)]
    scratch += [pltpu.VMEM((128, 128), BF16)] * 2 + [pltpu.VMEM((16 * 56, 128), F32)]
    scratch += [pltpu.VMEM((128, 128), F32)] * 2
    scratch += [pltpu.VMEM((3, 128, 128), F32), pltpu.VMEM((40, 128), F32)]
    scratch += [pltpu.VMEM((128, 256), BF16), pltpu.VMEM((2, 112, 384), BF16)]
    scratch += [pltpu.VMEM((3, 128, 128), BF16)] * 2
    groups = [p.scratch() for p in PLANS] + [gather_scratch(sizes)] * 2
    devices = sizes[0] * sizes[1] * sizes[2]
    groups += [[pltpu.VMEM((devices, 1, 128), F32)] + [pltpu.SemaphoreType.DMA((1,))] * 2]
    for g in groups:
        scratch += g
    counts = tuple(len(g) for g in groups)
    vmem = pl.BlockSpec(memory_space=pltpu.VMEM)

    anywhere = pl.BlockSpec(memory_space=pl.ANY)

    def body(right_side, start_guess, reaction):
        whole = pltpu.VMEM((L0.total, 128), F32)
        parts = pl.pallas_call(
            functools.partial(kernel, sizes, counts),
            out_shape=[whole] * 4 + [pltpu.VMEM((8, 128), F32)],
            in_specs=[anywhere] * 3,
            out_specs=[vmem] * 5,
            scratch_shapes=scratch,
            compiler_params=pltpu.CompilerParams(
                collective_id=0, has_side_effects=True, vmem_limit_bytes=60 * 2**20
            ),
        )(right_side, start_guess, reaction)
        shape = jax.ShapeDtypeStruct(right_side.shape, F32)
        return tuple(
            pl.pallas_call(
                finish,
                out_shape=[shape, shape],
                in_specs=[vmem] * 5,
                out_specs=[anywhere] * 2,
                scratch_shapes=[pltpu.VMEM(right_side.shape, F32)] * 2 + [pltpu.SemaphoreType.DMA((2,))],
                compiler_params=pltpu.CompilerParams(vmem_limit_bytes=16 * 2**20),
            )(*parts)
        )

    placed = P("gx", "gy", "gz")
    return jax.shard_map(
        body, mesh=mesh, in_specs=(placed,) * 3, out_specs=(placed,) * 2, check_vma=False
    )
```
